8 devices in a mesh: dp: 1 (over z), gp: 8 (over y, x, core).
Axes of the slice: x: 2, y: 2, z: 1, core: 2. Of those that a mesh axis runs over, the one named last changes fastest.
Arguments:
- x_prev: float32 [8192, 84], P(('dp', 'gp'))
- x_cur: float32 [8192, 84], P(('dp', 'gp'))
- forcing: float32 [8192, 2, 5], P(('dp', 'gp'))
- grid_static: float32 [8192, 5], P(('dp', 'gp'))
- g2m_feat: float32 [8192, 4], P(('dp', 'gp'))
- m2g_feat: float32 [8192, 4], P(('dp', 'gp'))
- mesh_feat: float32 [4096, 3], P(('dp', 'gp'))
- mesh_edge_feat: float32 [4096, 6, 4], P(('dp', 'gp'))
- norm_stats: float32 [4, 84], replicated
- w_grid_in: bfloat16 [178, 512], replicated
- w_mesh_in: bfloat16 [3, 512], replicated
- w_eemb_in: bfloat16 [3, 4, 512], replicated
- w_embed_out: bfloat16 [5, 512, 512], replicated
- w_edge_in: bfloat16 [18, 1536, 512], replicated
- w_edge_out: bfloat16 [18, 512, 512], replicated
- w_node_in: bfloat16 [18, 1024, 512], replicated
- w_node_out: bfloat16 [18, 512, 512], replicated
- w_grid_self: bfloat16 [2, 512, 512], replicated
- w_out_hidden: bfloat16 [512, 512], replicated
- w_out_final: bfloat16 [512, 84], replicated
Outputs:
- output 1: float32 [8192, 84], P(('dp', 'gp'))
- output 2: float32 [8192, 84], P(('dp', 'gp'))
All inputs are finite; a program needn't handle non-finite values.
Results may differ from the reference program's by a relative error of at most 0.00822618.
Values are sent between devices in bfloat16 or wider.
A program may use at most 1 GiB of HBM per device.

```python
import jax
import jax.numpy as jnp
from jax import lax

GRID_NODES = 8192
MESH_NODES = 4096
SHIFT = 256
LATENT = 512
VARS = 84
FORCE = 5
STATIC = 5
LAYERS = 16
EDGE_FEAT = 4
MESH_FEAT = 3
OFFSET_COUNT = 6

GRID_RATIO = GRID_NODES // MESH_NODES
QUARTER = MESH_NODES // 4
BLOCKS = LAYERS + 2
IN_FEAT = 2 * VARS + FORCE + STATIC
OFFSETS = (1, -1, SHIFT, -SHIFT, QUARTER, -QUARTER)


def normal_weight(key_in, out_shape, fan_in):
    return (jax.random.normal(key_in, out_shape, jnp.float32) * fan_in ** -0.5).astype(jnp.bfloat16)


def setup_inputs(seed: int = 0, part: int = 0) -> dict:
    root_key = jax.random.key(seed)
    part_keys = jax.random.split(jax.random.fold_in(root_key, part), 8)
    weight_keys = jax.random.split(jax.random.key(seed + 1), 15)
    norm_stats = jnp.stack([
        0.5 * jax.random.normal(weight_keys[0], (VARS,), jnp.float32),
        jax.random.uniform(weight_keys[1], (VARS,), jnp.float32, 0.5, 1.5),
        0.2 * jax.random.normal(weight_keys[2], (VARS,), jnp.float32),
        jax.random.uniform(weight_keys[3], (VARS,), jnp.float32, 0.2, 0.6)])
    return {
        "x_prev": jax.random.normal(part_keys[0], (GRID_NODES, VARS), jnp.float32),
        "x_cur": jax.random.normal(part_keys[1], (GRID_NODES, VARS), jnp.float32),
        "forcing": jax.random.normal(part_keys[2], (GRID_NODES, 2, FORCE), jnp.float32),
        "grid_static": jax.random.normal(part_keys[3], (GRID_NODES, STATIC), jnp.float32),
        "g2m_feat": jax.random.normal(part_keys[4], (GRID_NODES, EDGE_FEAT), jnp.float32),
        "m2g_feat": jax.random.normal(part_keys[5], (GRID_NODES, EDGE_FEAT), jnp.float32),
        "mesh_feat": jax.random.normal(part_keys[6], (MESH_NODES, MESH_FEAT), jnp.float32),
        "mesh_edge_feat": jax.random.normal(part_keys[7], (MESH_NODES, OFFSET_COUNT, EDGE_FEAT), jnp.float32),
        "norm_stats": norm_stats,
        "w_grid_in": normal_weight(weight_keys[4], (IN_FEAT, LATENT), IN_FEAT),
        "w_mesh_in": normal_weight(weight_keys[5], (MESH_FEAT, LATENT), MESH_FEAT),
        "w_eemb_in": normal_weight(weight_keys[6], (3, EDGE_FEAT, LATENT), EDGE_FEAT),
        "w_embed_out": normal_weight(weight_keys[7], (5, LATENT, LATENT), LATENT),
        "w_edge_in": normal_weight(weight_keys[8], (BLOCKS, 3 * LATENT, LATENT), 3 * LATENT),
        "w_edge_out": normal_weight(weight_keys[9], (BLOCKS, LATENT, LATENT), LATENT),
        "w_node_in": normal_weight(weight_keys[10], (BLOCKS, 2 * LATENT, LATENT), 2 * LATENT),
        "w_node_out": normal_weight(weight_keys[11], (BLOCKS, LATENT, LATENT), LATENT),
        "w_grid_self": normal_weight(weight_keys[12], (2, LATENT, LATENT), LATENT),
        "w_out_hidden": normal_weight(weight_keys[13], (LATENT, LATENT), LATENT),
        "w_out_final": normal_weight(weight_keys[14], (LATENT, VARS), LATENT),
    }


def layer_norm(values):
    centre = jnp.mean(values, axis=-1, keepdims=True)
    centred = values - centre
    spread = jnp.mean(centred * centred, axis=-1, keepdims=True)
    return centred * lax.rsqrt(spread + 1e-5)


def matmul_f32(values, weight):
    return jnp.dot(values, weight, preferred_element_type=jnp.float32)


def mlp_tail(pre_act, w_second):
    hidden = jax.nn.silu(pre_act).astype(jnp.bfloat16)
    return layer_norm(matmul_f32(hidden, w_second))


def residual(base, update):
    return (base.astype(jnp.float32) + update).astype(jnp.bfloat16)


def embed_static(features, w_first, w_second):
    return mlp_tail(matmul_f32(features.astype(jnp.bfloat16), w_first), w_second).astype(jnp.bfloat16)


def reference(x_prev, x_cur, forcing, grid_static, g2m_feat, m2g_feat, mesh_feat, mesh_edge_feat, norm_stats, w_grid_in, w_mesh_in, w_eemb_in, w_embed_out, w_edge_in, w_edge_out, w_node_in, w_node_out, w_grid_self, w_out_hidden, w_out_final):
    mesh_lat = embed_static(mesh_feat, w_mesh_in, w_embed_out[1])
    g2m_lat = embed_static(g2m_feat, w_eemb_in[0], w_embed_out[2])
    m2g_lat = embed_static(m2g_feat, w_eemb_in[1], w_embed_out[3])
    edge_base = embed_static(mesh_edge_feat.reshape(MESH_NODES * OFFSET_COUNT, EDGE_FEAT), w_eemb_in[2], w_embed_out[4])
    in_mean = norm_stats[0]
    in_std = norm_stats[1]
    diff_mean = norm_stats[2]
    diff_std = norm_stats[3]

    def proc_layer(layer_state, layer_weights):
        mesh_cur, edge_lat = layer_state
        w_edge, w_edge_two, w_node, w_node_two = layer_weights
        send_proj = matmul_f32(mesh_cur, w_edge[LATENT:2 * LATENT])
        send_term = jnp.stack([jnp.roll(send_proj, -offset, axis=0) for offset in OFFSETS], axis=1).reshape(MESH_NODES * OFFSET_COUNT, LATENT)
        recv_term = matmul_f32(mesh_cur, w_edge[2 * LATENT:])
        pre_act = matmul_f32(edge_lat, w_edge[:LATENT]) + send_term
        pre_act = (pre_act.reshape(MESH_NODES, OFFSET_COUNT, LATENT) + recv_term[:, None, :]).reshape(MESH_NODES * OFFSET_COUNT, LATENT)
        edge_lat = residual(edge_lat, mlp_tail(pre_act, w_edge_two))
        edge_sum = jnp.sum(edge_lat.reshape(MESH_NODES, OFFSET_COUNT, LATENT).astype(jnp.float32), axis=1).astype(jnp.bfloat16)
        mesh_cur = residual(mesh_cur, mlp_tail(matmul_f32(mesh_cur, w_node[:LATENT]) + matmul_f32(edge_sum, w_node[LATENT:]), w_node_two))
        return (mesh_cur, edge_lat), None

    def forecast_step(state_pair, force_now):
        state_prev, state_cur = state_pair
        features = jnp.concatenate([(state_prev - in_mean) / in_std, (state_cur - in_mean) / in_std, force_now, grid_static], axis=1)
        grid_lat = embed_static(features, w_grid_in, w_embed_out[0])
        w_first = w_edge_in[0]
        senders = jnp.roll(grid_lat, SHIFT * GRID_RATIO, axis=0)
        recv_term = matmul_f32(mesh_lat, w_first[2 * LATENT:])
        pre_act = matmul_f32(g2m_lat, w_first[:LATENT]) + matmul_f32(senders, w_first[LATENT:2 * LATENT])
        pre_act = (pre_act.reshape(MESH_NODES, GRID_RATIO, LATENT) + recv_term[:, None, :]).reshape(GRID_NODES, LATENT)
        enc_edge = residual(g2m_lat, mlp_tail(pre_act, w_edge_out[0]))
        enc_sum = jnp.sum(enc_edge.reshape(MESH_NODES, GRID_RATIO, LATENT).astype(jnp.float32), axis=1).astype(jnp.bfloat16)
        node_first = w_node_in[0]
        mesh_cur = residual(mesh_lat, mlp_tail(matmul_f32(mesh_lat, node_first[:LATENT]) + matmul_f32(enc_sum, node_first[LATENT:]), w_node_out[0]))
        grid_cur = residual(grid_lat, mlp_tail(matmul_f32(grid_lat, w_grid_self[0]), w_grid_self[1]))
        layer_weights = (w_edge_in[1:BLOCKS - 1], w_edge_out[1:BLOCKS - 1], w_node_in[1:BLOCKS - 1], w_node_out[1:BLOCKS - 1])
        layer_out, no_stack = lax.scan(proc_layer, (mesh_cur, edge_base), layer_weights)
        mesh_cur = layer_out[0]
        w_last = w_edge_in[BLOCKS - 1]
        send_term = matmul_f32(jnp.roll(mesh_cur, -SHIFT, axis=0), w_last[LATENT:2 * LATENT])
        pre_act = matmul_f32(m2g_lat, w_last[:LATENT]) + matmul_f32(grid_cur, w_last[2 * LATENT:])
        pre_act = (pre_act.reshape(MESH_NODES, GRID_RATIO, LATENT) + send_term[:, None, :]).reshape(GRID_NODES, LATENT)
        dec_edge = residual(m2g_lat, mlp_tail(pre_act, w_edge_out[BLOCKS - 1]))
        node_last = w_node_in[BLOCKS - 1]
        grid_out = residual(grid_cur, mlp_tail(matmul_f32(grid_cur, node_last[:LATENT]) + matmul_f32(dec_edge, node_last[LATENT:]), w_node_out[BLOCKS - 1]))
        hidden = jax.nn.silu(matmul_f32(grid_out, w_out_hidden)).astype(jnp.bfloat16)
        prediction = matmul_f32(hidden, w_out_final)
        state_next = state_cur + diff_std * prediction + diff_mean
        return (state_cur, state_next), state_next

    final_pair, stacked = lax.scan(forecast_step, (x_prev, x_cur), jnp.swapaxes(forcing, 0, 1))
    return stacked[0], stacked[1]
```

```python
import functools

import jax
import jax.numpy as jnp
from jax import lax
from jax.experimental import pallas as pl
from jax.experimental.pallas import tpu as pltpu
from jax.sharding import PartitionSpec as P

F32 = jnp.float32
BF16 = jnp.bfloat16

RUNS = 16
RUN = 32
ROWS = RUNS * RUN
LAT = 512
VARS = 84
PAD = 48
TILE = 256
TILES = ROWS // TILE
CH = 32
RING = 8
LAYERS = 16
BLOCKS = LAYERS + 2
FAR = ((2, 1), (3, -1), (4, 4), (5, -4))
NEAR = ((0, 1), (1, -1))


def dot(a, b):
    return jnp.dot(a, b, preferred_element_type=F32)


def silu(pre):
    return pre * jax.nn.sigmoid(pre)


def norm(y):
    centred = y - jnp.mean(y, axis=-1, keepdims=True)
    return centred * lax.rsqrt(jnp.mean(centred * centred, axis=-1, keepdims=True) + 1e-5)


def ring_place(dev):
    high = lax.div(dev, 4)
    return high * (4 + lax.rem(dev + 2, 4)) + (1 - high) * dev


def chunks():
    return range(0, TILE, CH)


def get_tiles(ref, rows):
    return jnp.concatenate([ref[j, rows, :] for j in range(ref.shape[0])], axis=1)


def set_tiles(ref, rows, value):
    for j in range(ref.shape[0]):
        ref[j, rows, :] = value[:, 128 * j:128 * j + 128]


def kernel(g_in, mf_in, xc_in, stats, wemb, w_embed_out, w_edge_in, w_edge_out, w_node_in, w_node_out, w_grid_self,
           w_out_hidden, w_out_final, out0, out1,
           g_buf, mf_buf, xc_buf, x_buf, gf, feat, we, weo, wei, wedo, wni, wno, wself, woh, wof,
           edge_base, edge, h_mesh, h, hf, g2m, m2g, v, vc, proj, recv, acc, hid, hid2, esum, dec,
           send_buf, halo_buf,
           in_send, in_recv, w_sem, big_sem, halo_send, halo_recv, out_send, out_recv):
    me = lax.axis_index("gp")
    place = ring_place(me)

    def at(dev):
        return {"gp": dev}

    mesh_id = pl.DeviceIdType.MESH

    def block_copies(block, slot):
        return [
            pltpu.make_async_copy(w_edge_in.at[block], wei.at[slot], big_sem.at[slot, 0]),
            pltpu.make_async_copy(w_edge_out.at[block], wedo.at[slot], big_sem.at[slot, 1]),
            pltpu.make_async_copy(w_node_in.at[block], wni.at[slot], big_sem.at[slot, 2]),
            pltpu.make_async_copy(w_node_out.at[block], wno.at[slot], big_sem.at[slot, 3]),
        ]

    small = [
        pltpu.make_async_copy(wemb, we, w_sem.at[0]),
        pltpu.make_async_copy(w_embed_out, weo, w_sem.at[1]),
        pltpu.make_async_copy(w_grid_self, wself, w_sem.at[2]),
        pltpu.make_async_copy(w_out_hidden, woh, w_sem.at[3]),
        pltpu.make_async_copy(w_out_final, wof, w_sem.at[4]),
    ]
    for copy in small:
        copy.start()
    for copy in block_copies(0, 0):
        copy.start()

    barrier = pltpu.get_barrier_semaphore()
    for hop in range(1, RING):
        pl.semaphore_signal(barrier, inc=1, device_id=at(lax.rem(me + hop, RING)), device_id_type=mesh_id)
    pl.semaphore_wait(barrier, RING - 1)

    parts = ((mf_in, mf_buf), (g_in, g_buf), (xc_in, xc_buf))

    def in_copy(part, hop):
        src, dst = parts[part]
        target = lax.rem(me + hop, RING)
        src = src.at[:, ring_place(target)]
        dst = dst.at[pl.ds(2 * me, 2)]
        if hop == 0:
            return pltpu.make_async_copy(src, dst, in_recv.at[part, 0])
        return pltpu.make_async_remote_copy(src_ref=src, dst_ref=dst, send_sem=in_send.at[part, hop],
                                            recv_sem=in_recv.at[part, hop], device_id=at(target),
                                            device_id_type=mesh_id)

    in_copies = [[in_copy(part, hop) for hop in range(RING)] for part in range(3)]
    for part in range(3):
        for copy in in_copies[part]:
            copy.start()

    def wait_in(part):
        in_copies[part][0].wait()
        for hop in range(1, RING):
            in_copies[part][hop].wait_recv()

    def pipeline(items):
        depth = max(len(item) for item in items)
        for beat in range(len(items) + depth - 1):
            for stage in range(depth):
                index = beat - stage
                if 0 <= index < len(items) and stage < len(items[index]):
                    items[index][stage](index)

    def embed_item(load, w_first, second, store):
        def first(i):
            pre = dot(load(), we[w_first])
            for c in chunks():
                hid[i % 2, pl.ds(c, CH), :] = silu(pre[c:c + CH]).astype(BF16)

        def last(i):
            y = dot(hid[i % 2], weo[second])
            for c in chunks():
                store(c, norm(y[c:c + CH]).astype(BF16))

        return [first, last]

    def mesh_features(t):
        runs = range(t * TILE // RUN, (t + 1) * TILE // RUN)
        return jnp.concatenate([mf_buf[(q + 1) % RUNS] for q in runs], axis=0)

    wait_in(0)
    for copy in small[:2]:
        copy.wait()
    items = []
    for t in range(TILES):
        def store_mesh(c, value, t=t):
            h_mesh[pl.ds(t * TILE + c, CH), :] = value
        items.append(embed_item(lambda t=t: mesh_features(t), 0, 1, store_mesh))
        for p in range(2):
            def store_g2m(c, value, t=t, p=p):
                g2m[p, pl.ds(t * TILE + c, CH), :] = value
            items.append(embed_item(lambda t=t: mesh_features(t), 1 + p, 2, store_g2m))
        for k in range(6):
            def store_edge(c, value, t=t, k=k):
                edge_base[k, pl.ds(t * TILE + c, CH), :] = value
            items.append(embed_item(lambda t=t: mesh_features(t), 3 + k, 4, store_edge))
    pipeline(items)

    wait_in(1)
    for q in range(RUNS):
        set_tiles(gf, pl.ds(q * 2 * RUN, 2 * RUN), g_buf[q].astype(F32))
    for q in range(RUNS):
        for p in range(2):
            feat[p, pl.ds(q * RUN, RUN), :] = get_tiles(gf, pl.ds(q * 2 * RUN + p, RUN, stride=2)).astype(BF16)
    items = []
    for t in range(TILES):
        for p in range(2):
            def store_m2g(c, value, t=t, p=p):
                m2g[p, pl.ds(t * TILE + c, CH), :] = value
            items.append(embed_item(lambda t=t, p=p: feat[p, pl.ds(t * TILE, TILE), pl.ds(0, 128)], 9, 3, store_m2g))
    pipeline(items)
    for copy in small[2:]:
        copy.wait()

    left = ring_place(lax.rem(place + RING - 1, RING))
    right = ring_place(lax.rem(place + 1, RING))

    def halo_copies(slot):
        return [
            pltpu.make_async_remote_copy(src_ref=send_buf.at[side], dst_ref=halo_buf.at[slot, side],
                                         send_sem=halo_send.at[side], recv_sem=halo_recv.at[slot, side],
                                         device_id=at(target), device_id_type=mesh_id)
            for side, target in ((0, left), (1, right))
        ]

    def send_halo(slot):
        first = get_tiles(hf, pl.ds(0, RUNS, stride=RUN))
        final = get_tiles(hf, pl.ds(RUN - 1, RUNS, stride=RUN))
        first_on = jnp.concatenate([first[1:], first[:1]], axis=0)
        final_back = jnp.concatenate([final[-1:], final[:-1]], axis=0)
        send_buf[0] = jnp.where(place == 0, first_on, first).astype(BF16)
        send_buf[1] = jnp.where(place == RING - 1, final_back, final).astype(BF16)
        for copy in halo_copies(slot):
            copy.start()

    def node_item(t, base, slot, sums):
        rows = pl.ds(t * TILE, TILE)

        def first(i):
            pre = dot(base[rows, :], wni[slot, pl.ds(0, LAT), :]) + dot(sums[rows, :], wni[slot, pl.ds(LAT, LAT), :])
            for c in chunks():
                hid2[t, pl.ds(c, CH), :] = silu(pre[c:c + CH]).astype(BF16)

        def last(i):
            y = dot(hid2[t], wno[slot])
            for c in chunks():
                part = pl.ds(t * TILE + c, CH)
                value = (base[part, :].astype(F32) + norm(y[c:c + CH])).astype(BF16)
                h[part, :] = value
                set_tiles(hf, part, value.astype(F32))

        return [first, last]

    def proj_rows(q, offset):
        return get_tiles(proj, pl.ds(q * PAD + 8 + offset, RUN))

    def layer(block, slot, halo_slot, more):
        w_edge = wei.at[slot]
        for t in range(TILES):
            out = dot(h[pl.ds(t * TILE, TILE), :], w_edge[pl.ds(LAT, LAT), :])
            for c in range(0, TILE, RUN):
                set_tiles(proj, pl.ds((t * TILE + c) // RUN * PAD + 8, RUN), out[c:c + RUN])
            recv[pl.ds(t * TILE, TILE), :] = dot(h[pl.ds(t * TILE, TILE), :], w_edge[pl.ds(2 * LAT, LAT), :])

        def edge_item(t, k, run_shift, offset, first_one, final_one):
            def first(i):
                pre = dot(edge[k, pl.ds(t * TILE, TILE), :], w_edge[pl.ds(0, LAT), :])
                for c in chunks():
                    q = (t * TILE + c) // RUN
                    sender = proj_rows((q + run_shift) % RUNS, offset)
                    value = pre[c:c + CH] + (sender + recv[pl.ds(t * TILE + c, CH), :])
                    hid[i % 2, pl.ds(c, CH), :] = silu(value).astype(BF16)

            def last(i):
                y = dot(hid[i % 2], wedo[slot])
                for c in chunks():
                    part = pl.ds(t * TILE + c, CH)
                    value = (edge[k, part, :].astype(F32) + norm(y[c:c + CH])).astype(BF16)
                    edge[k, part, :] = value
                    total = value.astype(F32)
                    if not first_one:
                        total = total + acc[part, :]
                    if final_one:
                        esum[part, :] = total.astype(BF16)
                    else:
                        acc[part, :] = total

            return [first, last]

        def halo(i):
            for side, copy in enumerate(halo_copies(halo_slot)):
                copy.wait()
            rows = jnp.concatenate([halo_buf[halo_slot, 0], halo_buf[halo_slot, 1]], axis=0)
            out = dot(rows, w_edge[pl.ds(LAT, LAT), :])
            set_tiles(proj, pl.ds(8 + RUN, RUNS, stride=PAD), out[:RUNS])
            set_tiles(proj, pl.ds(7, RUNS, stride=PAD), out[RUNS:])

        far = [edge_item(t, k, s, 0, n == 0, False) for t in range(TILES) for n, (k, s) in enumerate(FAR)]
        near = [edge_item(t, k, 0, s, False, n == 1) for t in range(TILES) for n, (k, s) in enumerate(NEAR)]
        node = [node_item(t, h, slot, esum) for t in range(TILES)]
        edges = far + near
        for n, item in enumerate(edges):
            if n == len(far):
                halo(n)
            item[0](n)
            if n:
                edges[n - 1][1](n - 1)
            if n > len(far) and (n - len(far)) % 2 == 0:
                node[(n - len(far)) // 2 - 1][0](n)
            if n > len(far) + 1 and (n - len(far)) % 2 == 1:
                node[(n - len(far) - 1) // 2 - 1][1](n)
        edges[-1][1](len(edges) - 1)
        node[-1][0](0)
        node[-1][1](0)

        @pl.when(more)
        def _():
            send_halo(1 - halo_slot)

    def encoder(step, slot):
        w_edge = wei.at[slot]
        for k in range(6):
            for c in range(0, ROWS, 128):
                edge[k, pl.ds(c, 128), :] = edge_base[k, pl.ds(c, 128), :]
        for t in range(TILES):
            recv[pl.ds(t * TILE, TILE), :] = dot(h_mesh[pl.ds(t * TILE, TILE), :], w_edge[pl.ds(2 * LAT, LAT), :])
        items = []
        for t in range(TILES):
            for p in range(2):
                rows = pl.ds(t * TILE, TILE)

                def in_first(i, rows=rows, p=p):
                    pre = dot(feat[p, rows, :], we[pl.ds(10 + 2 * step, 2)].reshape(256, LAT))
                    for c in chunks():
                        hid[i % 2, pl.ds(c, CH), :] = silu(pre[c:c + CH]).astype(BF16)

                def in_last(i, t=t, p=p):
                    y = dot(hid[i % 2], weo[0])
                    for c in chunks():
                        v[p, pl.ds(t * TILE + c, CH), :] = norm(y[c:c + CH]).astype(BF16)

                def edge_first(i, rows=rows, t=t, p=p):
                    pre = dot(g2m[p, rows, :], w_edge[pl.ds(0, LAT), :]) + dot(v[p, rows, :], w_edge[pl.ds(LAT, LAT), :])
                    for c in chunks():
                        value = pre[c:c + CH] + recv[pl.ds(t * TILE + c, CH), :]
                        hid2[i % 2, pl.ds(c, CH), :] = silu(value).astype(BF16)

                def edge_last(i, t=t, p=p):
                    y = dot(hid2[i % 2], wedo[slot])
                    for c in chunks():
                        part = pl.ds(t * TILE + c, CH)
                        total = (g2m[p, part, :].astype(F32) + norm(y[c:c + CH])).astype(BF16).astype(F32)
                        if p == 0:
                            acc[part, :] = total
                        else:
                            esum[part, :] = (acc[part, :] + total).astype(BF16)

                items.append([in_first, in_last, edge_first, edge_last])
        pipeline(items)
        pipeline([node_item(t, h_mesh, slot, esum) for t in range(TILES)])
        send_halo(0)
        items = []
        for t in range(TILES):
            for p in range(2):
                rows = pl.ds(t * TILE, TILE)

                def self_first(i, rows=rows, p=p):
                    pre = dot(v[p, rows, :], wself[0])
                    for c in chunks():
                        hid[i % 2, pl.ds(c, CH), :] = silu(pre[c:c + CH]).astype(BF16)

                def self_last(i, t=t, p=p):
                    y = dot(hid[i % 2], wself[1])
                    for c in chunks():
                        part = pl.ds(t * TILE + c, CH)
                        vc[p, part, :] = (v[p, part, :].astype(F32) + norm(y[c:c + CH])).astype(BF16)

                items.append([self_first, self_last])
        pipeline(items)

    def out_copies(step, out):
        copies = []
        for hop in range(RING):
            target = lax.rem(me + hop, RING)
            src, dst = x_buf.at[step + 1, pl.ds(2 * target, 2)], out.at[:, place]
            if hop == 0:
                copies.append(pltpu.make_async_copy(src, dst, out_recv.at[step, hop]))
            else:
                copies.append(pltpu.make_async_remote_copy(
                    src_ref=src, dst_ref=dst, send_sem=out_send.at[step, hop], recv_sem=out_recv.at[step, hop],
                    device_id=at(target), device_id_type=mesh_id))
        return copies

    def decoder(step, slot):
        w_edge = wei.at[slot]
        for t in range(TILES):
            recv[pl.ds(t * TILE, TILE), :] = dot(h[pl.ds(t * TILE, TILE), :], w_edge[pl.ds(LAT, LAT), :])
        in_mean = stats[0:1, :]
        in_std = stats[1:2, :]
        diff_mean = stats[2:3, :]
        diff_std = stats[3:4, :]
        items = []
        for t in range(TILES):
            for p in range(2):
                rows = pl.ds(t * TILE, TILE)

                def edge_first(i, rows=rows, t=t, p=p):
                    pre = dot(m2g[p, rows, :], w_edge[pl.ds(0, LAT), :]) + dot(vc[p, rows, :], w_edge[pl.ds(2 * LAT, LAT), :])
                    for c in chunks():
                        value = pre[c:c + CH] + recv[pl.ds(t * TILE + c, CH), :]
                        hid[i % 2, pl.ds(c, CH), :] = silu(value).astype(BF16)

                def edge_last(i, t=t, p=p):
                    y = dot(hid[i % 2], wedo[slot])
                    for c in chunks():
                        part = pl.ds(t * TILE + c, CH)
                        dec[i % 2, pl.ds(c, CH), :] = (m2g[p, part, :].astype(F32) + norm(y[c:c + CH])).astype(BF16)

                def node_first(i, rows=rows, p=p):
                    pre = dot(vc[p, rows, :], wni[slot, pl.ds(0, LAT), :]) + dot(dec[i % 2], wni[slot, pl.ds(LAT, LAT), :])
                    for c in chunks():
                        hid2[i % 2, pl.ds(c, CH), :] = silu(pre[c:c + CH]).astype(BF16)

                def node_last(i, t=t, p=p):
                    y = dot(hid2[i % 2], wno[slot])
                    for c in chunks():
                        part = pl.ds(t * TILE + c, CH)
                        v[p, part, :] = (vc[p, part, :].astype(F32) + norm(y[c:c + CH])).astype(BF16)

                def out_first(i, rows=rows, t=t, p=p):
                    pre = dot(v[p, rows, :], woh[...])
                    for c in chunks():
                        vc[p, pl.ds(t * TILE + c, CH), :] = silu(pre[c:c + CH]).astype(BF16)

                def out_last(i, rows=rows, t=t, p=p):
                    pred = dot(vc[p, rows, :], wof[...])
                    for c in chunks():
                        q = (t * TILE + c) // RUN
                        now = x_buf[step, q, pl.ds(p, RUN, stride=2), :][:, :VARS]
                        new = now + diff_std * pred[c:c + CH] + diff_mean
                        wide = jnp.concatenate([new, jnp.zeros((CH, 128 - VARS), F32)], axis=1)
                        x_buf[step + 1, q, pl.ds(p, RUN, stride=2), :] = wide
                        feat[p, pl.ds(t * TILE + c, CH), pl.ds(0, VARS)] = ((new - in_mean) / in_std).astype(BF16)

                items.append([edge_first, edge_last, node_first, node_last, out_first, out_last])
        pipeline(items)

    def one_step(step, carry):
        def fetch(block, slot):
            for copy in block_copies(block, slot):
                copy.wait()

        def prefetch(block, slot):
            for copy in block_copies(block, slot):
                copy.start()

        fetch(0, 0)
        prefetch(1, 1)
        encoder(step, 0)

        def one_layer(index, carry):
            block = index + 1
            slot = lax.rem(block, 2)
            fetch(block, slot)
            prefetch(block + 1, 1 - slot)
            layer(block, slot, lax.rem(index, 2), index < LAYERS - 1)
            return carry

        lax.fori_loop(0, LAYERS, one_layer, 0)
        fetch(BLOCKS - 1, 1)

        @pl.when(step == 0)
        def _():
            prefetch(0, 0)
            wait_in(2)
            for q in range(RUNS):
                x_buf[0, q, :, pl.ds(0, VARS)] = xc_buf[q]
                x_buf[0, q, :, pl.ds(VARS, 128 - VARS)] = jnp.zeros((2 * RUN, 128 - VARS), F32)

        decoder(step, 1)

        @pl.when(step == 0)
        def _():
            for copy in out_copies(0, out0):
                copy.start()

        @pl.when(step == 1)
        def _():
            for copy in out_copies(1, out1):
                copy.start()
        return carry

    lax.fori_loop(0, 2, one_step, 0)
    for part in range(3):
        for hop in range(1, RING):
            in_copies[part][hop].wait_send()
    for step, out in ((0, out0), (1, out1)):
        for copy in out_copies(step, out):
            copy.wait()


def solution(mesh):
    row_spec = P(("dp", "gp"))
    edge_spec = P(("dp", "gp"), None, None)
    whole = P()

    def local_run(x_prev, x_cur, forcing, grid_static, g2m_feat, m2g_feat, mesh_feat, mesh_edge_feat, norm_stats,
                  w_grid_in, w_mesh_in, w_eemb_in, w_embed_out, w_edge_in, w_edge_out, w_node_in, w_node_out,
                  w_grid_self, w_out_hidden, w_out_final):
        grid_dev = x_prev.shape[0]
        mesh_dev = mesh_feat.shape[0]
        mean, std = norm_stats[0], norm_stats[1]

        def lanes(pieces, width):
            have = sum(piece.shape[1] for piece in pieces)
            rows = pieces[0].shape[0]
            return jnp.concatenate([piece.astype(BF16) for piece in pieces] + [jnp.zeros((rows, width - have), BF16)], axis=1)

        grid_lanes = jnp.concatenate([
            lanes([(x_prev - mean) / std, forcing[:, 0], grid_static, forcing[:, 1], m2g_feat], 128),
            lanes([(x_cur - mean) / std], 128)], axis=1)
        mesh_lanes = lanes([mesh_feat, mesh_edge_feat.reshape(mesh_dev, 24), g2m_feat.reshape(mesh_dev, 8)], 128)

        def placed(rows, start, height=128):
            return jnp.pad(rows, ((start, height - start - rows.shape[0]), (0, 0)))

        prev_rows, cur_rows = w_grid_in[:VARS], w_grid_in[VARS:2 * VARS]
        force_rows, static_rows = w_grid_in[2 * VARS:2 * VARS + 5], w_grid_in[2 * VARS + 5:]
        first_step = [placed(jnp.concatenate([prev_rows, force_rows, static_rows], axis=0), 0), placed(cur_rows, 0)]
        second_step = [placed(cur_rows, 0) + placed(static_rows, 89) + placed(force_rows, 94), placed(prev_rows, 0)]
        wemb = jnp.stack(
            [placed(w_mesh_in, 0)] + [placed(w_eemb_in[0], 27 + 4 * p) for p in range(2)]
            + [placed(w_eemb_in[2], 3 + 4 * k) for k in range(6)] + [placed(w_eemb_in[1], 99)]
            + first_step + second_step)

        any_spec = pl.BlockSpec(memory_space=pl.ANY)
        vmem_spec = pl.BlockSpec(memory_space=pltpu.VMEM)
        dma = pltpu.SemaphoreType.DMA
        out = jax.ShapeDtypeStruct((2, RING, 2 * RUN, 128), F32)
        scratch = [
            pltpu.VMEM((RUNS, 2 * RUN, 256), BF16),
            pltpu.VMEM((RUNS, RUN, 128), BF16),
            pltpu.VMEM((RUNS, 2 * RUN, VARS), F32),
            pltpu.VMEM((3, RUNS, 2 * RUN, 128), F32),
            pltpu.VMEM((2, RUNS * 2 * RUN, 128), F32),
            pltpu.VMEM((2, ROWS, 256), BF16),
            pltpu.VMEM((14, 128, LAT), BF16),
            pltpu.VMEM((5, LAT, LAT), BF16),
            pltpu.VMEM((2, 3 * LAT, LAT), BF16),
            pltpu.VMEM((2, LAT, LAT), BF16),
            pltpu.VMEM((2, 2 * LAT, LAT), BF16),
            pltpu.VMEM((2, LAT, LAT), BF16),
            pltpu.VMEM((2, LAT, LAT), BF16),
            pltpu.VMEM((LAT, LAT), BF16),
            pltpu.VMEM((LAT, VARS), BF16),
            pltpu.VMEM((6, ROWS, LAT), BF16),
            pltpu.VMEM((6, ROWS, LAT), BF16),
            pltpu.VMEM((ROWS, LAT), BF16),
            pltpu.VMEM((ROWS, LAT), BF16),
            pltpu.VMEM((4, ROWS, 128), F32),
            pltpu.VMEM((2, ROWS, LAT), BF16),
            pltpu.VMEM((2, ROWS, LAT), BF16),
            pltpu.VMEM((2, ROWS, LAT), BF16),
            pltpu.VMEM((2, ROWS, LAT), BF16),
            pltpu.VMEM((4, RUNS * PAD, 128), F32),
            pltpu.VMEM((ROWS, LAT), F32),
            pltpu.VMEM((ROWS, LAT), F32),
            pltpu.VMEM((2, TILE, LAT), BF16),
            pltpu.VMEM((2, TILE, LAT), BF16),
            pltpu.VMEM((ROWS, LAT), BF16),
            pltpu.VMEM((2, TILE, LAT), BF16),
            pltpu.VMEM((2, RUNS, LAT), BF16),
            pltpu.VMEM((2, 2, RUNS, LAT), BF16),
            dma((3, RING)), dma((3, RING)), dma((5,)), dma((2, 4)), dma((2,)), dma((2, 2)), dma((2, RING)), dma((2, RING)),
        ]
        next_state, after_state = pl.pallas_call(
            kernel,
            out_shape=(out, out),
            in_specs=[any_spec, any_spec, any_spec, vmem_spec] + [any_spec] * 9,
            out_specs=(any_spec, any_spec),
            scratch_shapes=scratch,
            compiler_params=pltpu.CompilerParams(collective_id=0, has_side_effects=True, vmem_limit_bytes=60 << 20),
            name="forecast",
        )(grid_lanes.reshape(2, RING, 2 * RUN, 256), mesh_lanes.reshape(2, RING, RUN, 128),
          x_cur.reshape(2, RING, 2 * RUN, VARS), norm_stats, wemb, w_embed_out, w_edge_in, w_edge_out, w_node_in,
          w_node_out, w_grid_self, w_out_hidden, w_out_final)
        return next_state.reshape(grid_dev, 128)[:, :VARS], after_state.reshape(grid_dev, 128)[:, :VARS]

    in_specs = (row_spec, row_spec, edge_spec, row_spec, row_spec, row_spec, row_spec, edge_spec, whole) + (whole,) * 11
    return jax.shard_map(local_run, mesh=mesh, in_specs=in_specs, out_specs=(row_spec, row_spec), check_vma=False)
```

```python
import functools

import jax
import jax.numpy as jnp
from jax import lax
from jax.experimental import pallas as pl
from jax.experimental.pallas import tpu as pltpu
from jax.sharding import PartitionSpec as P

F32 = jnp.float32
BF16 = jnp.bfloat16

RUNS = 16
RUN = 32
ROWS = RUNS * RUN
LAT = 512
VARS = 84
PAD0 = 32
PAD1 = 48
TILE = 256
TILES = 2
HALF = TILE // RUNS
CH = 32
RING = 8
LAYERS = 16
BLOCKS = LAYERS + 2
SLOTS = 4
FAR = ((2, 1), (3, -1), (4, 4), (5, -4))
NEAR = ((0, 1), (1, -1))
ORDER = (
    "before", "n1", "fx0", "bx0", "fx1", "bx1",
    "fn0", "fn1", "bn0", "bn1", "ax0", "fx2", "bx2",
    "ax1", "fx3", "bx3", "na", "ax2", "nb", "an0", "ax3", "project",
)


def dot(a, b):
    return jnp.dot(a, b, preferred_element_type=F32)


def silu(pre):
    return pre * jax.nn.sigmoid(pre)


def norm(y):
    centred = y - jnp.mean(y, axis=-1, keepdims=True)
    return centred * lax.rsqrt(jnp.mean(centred * centred, axis=-1, keepdims=True) + 1e-5)


def ring_place(dev):
    high = lax.div(dev, 4)
    return high * (4 + lax.rem(dev + 2, 4)) + (1 - high) * dev


def chunks():
    return range(0, TILE, CH)


def tile_rows(t):
    return pl.ds(t * TILE, TILE)


def part_rows(t, c):
    return pl.ds(t * TILE + c, CH)


def chunk_runs(c):
    return range(c // HALF, (c + CH) // HALF)


def pieces(t):
    return ((8, 16),) if t == 0 else ((0, 8), (24, 8))


def get_tiles(ref, rows):
    return jnp.concatenate([ref[j, rows, :] for j in range(ref.shape[0])], axis=1)


def set_tiles(ref, rows, value):
    for j in range(ref.shape[0]):
        ref[j, rows, :] = value[:, 128 * j:128 * j + 128]


def kernel(g_in, mf_in, xc_in, stats, wemb, w_embed_out, w_edge_in, w_edge_out, w_node_in, w_node_out, w_grid_self,
           w_out_hidden, w_out_final, out0, out1,
           g_buf, mf_buf, xc_buf, x_buf, gf, feat, we, weo, wself, woh, wof,
           enc_ei, enc_eo, enc_ni, enc_no, lay_ei, lay_eo, lay_ni, lay_no,
           edge_base, edge, h_mesh, h, hf, g2m, m2g, v, vc, proj0, proj1, recv, acc, hid, esum, dec, pre_buf,
           send_buf, halo_buf,
           in_send, in_recv, w_sem, enc_sem, lay_sem, halo_send, halo_recv, out_send, out_recv):
    me = lax.axis_index("gp")
    place = ring_place(me)

    def at(dev):
        return {"gp": dev}

    mesh_id = pl.DeviceIdType.MESH

    def block_copies(block, dst_refs, slot, sem):
        srcs = (w_edge_in, w_edge_out, w_node_in, w_node_out)
        return [pltpu.make_async_copy(src.at[block], dst.at[slot], sem.at[slot, i])
                for i, (src, dst) in enumerate(zip(srcs, dst_refs))]

    enc_refs = (enc_ei, enc_eo, enc_ni, enc_no)
    lay_refs = (lay_ei, lay_eo, lay_ni, lay_no)

    def enc_copies():
        return block_copies(0, enc_refs, 0, enc_sem)

    def slot_of(step, block):
        return lax.rem((BLOCKS - 1) * step + block - 1, SLOTS)

    def layer_copies(step, block):
        return block_copies(block, lay_refs, slot_of(step, block), lay_sem)

    class Weights:
        def __init__(self, refs, slot):
            self.edge = [refs[0].at[slot, pl.ds(i * LAT, LAT)] for i in range(3)]
            self.edge_out = refs[1].at[slot]
            self.node = [refs[2].at[slot, pl.ds(i * LAT, LAT)] for i in range(2)]
            self.node_out = refs[3].at[slot]

    def layer_weights(step, block):
        return Weights(lay_refs, slot_of(step, block))

    small = [
        pltpu.make_async_copy(wemb, we, w_sem.at[0]),
        pltpu.make_async_copy(w_embed_out, weo, w_sem.at[1]),
        pltpu.make_async_copy(w_grid_self, wself, w_sem.at[2]),
        pltpu.make_async_copy(w_out_hidden, woh, w_sem.at[3]),
        pltpu.make_async_copy(w_out_final, wof, w_sem.at[4]),
    ]
    for copy in small + enc_copies() + layer_copies(0, 1) + layer_copies(0, 2):
        copy.start()

    barrier = pltpu.get_barrier_semaphore()
    for hop in range(1, RING):
        pl.semaphore_signal(barrier, inc=1, device_id=at(lax.rem(me + hop, RING)), device_id_type=mesh_id)
    pl.semaphore_wait(barrier, RING - 1)

    parts = ((mf_in, mf_buf), (g_in, g_buf), (xc_in, xc_buf))

    def in_copy(part, hop):
        src, dst = parts[part]
        target = lax.rem(me + hop, RING)
        src = src.at[:, ring_place(target)]
        dst = dst.at[pl.ds(2 * me, 2)]
        if hop == 0:
            return pltpu.make_async_copy(src, dst, in_recv.at[part, 0])
        return pltpu.make_async_remote_copy(src_ref=src, dst_ref=dst, send_sem=in_send.at[part, hop],
                                            recv_sem=in_recv.at[part, hop], device_id=at(target),
                                            device_id_type=mesh_id)

    in_copies = [[in_copy(part, hop) for hop in range(RING)] for part in range(3)]
    for part in range(3):
        for copy in in_copies[part]:
            copy.start()

    def wait_in(part):
        in_copies[part][0].wait()
        for hop in range(1, RING):
            in_copies[part][hop].wait_recv()

    def pipeline(items):
        depth = max(len(item) for item in items)
        for beat in range(len(items) + depth - 1):
            for stage in range(depth):
                index = beat - stage
                if 0 <= index < len(items) and stage < len(items[index]):
                    items[index][stage](index)

    def hide(slot, pre, extra=None):
        for c in chunks():
            value = pre[c:c + CH]
            if extra is not None:
                value = value + extra(c)
            hid[slot, pl.ds(c, CH), :] = silu(value).astype(BF16)

    def embed_item(load, w_first, second, store):
        def first(i):
            hide(i % 2, dot(load(), we[w_first]))

        def last(i):
            y = dot(hid[i % 2], weo[second])
            for c in chunks():
                store(c, norm(y[c:c + CH]).astype(BF16))

        return [first, last]

    wait_in(0)
    for copy in small[:2]:
        copy.wait()
    mesh_feat = [jnp.concatenate([mf_buf[(q + 1) % RUNS].astype(F32)[r:r + n] for q in range(RUNS) for r, n in pieces(t)],
                                 axis=0).astype(BF16) for t in range(TILES)]
    items = []
    for t in range(TILES):
        def store_mesh(c, value, t=t):
            h_mesh[part_rows(t, c), :] = value
        items.append(embed_item(lambda t=t: mesh_feat[t], 0, 1, store_mesh))
        for p in range(2):
            def store_g2m(c, value, t=t, p=p):
                g2m[p, part_rows(t, c), :] = value
            items.append(embed_item(lambda t=t: mesh_feat[t], 1 + p, 2, store_g2m))
        for k in range(6):
            def store_edge(c, value, t=t, k=k):
                edge_base[k, part_rows(t, c), :] = value
            items.append(embed_item(lambda t=t: mesh_feat[t], 3 + k, 4, store_edge))
    pipeline(items)

    wait_in(1)
    for q in range(RUNS):
        set_tiles(gf, pl.ds(q * 2 * RUN, 2 * RUN), g_buf[q].astype(F32))
    for t in range(TILES):
        for p in range(2):
            for c in chunks():
                feat[p, part_rows(t, c), :] = jnp.concatenate(
                    [get_tiles(gf, pl.ds(q * 2 * RUN + 2 * r + p, n, stride=2)) for q in chunk_runs(c) for r, n in pieces(t)],
                    axis=0).astype(BF16)
    items = []
    for t in range(TILES):
        for p in range(2):
            def store_m2g(c, value, t=t, p=p):
                m2g[p, part_rows(t, c), :] = value
            items.append(embed_item(lambda t=t, p=p: feat[p, tile_rows(t), pl.ds(0, 128)], 9, 3, store_m2g))
    pipeline(items)
    for copy in small[2:] + enc_copies():
        copy.wait()

    left = ring_place(lax.rem(place + RING - 1, RING))
    right = ring_place(lax.rem(place + 1, RING))

    def halo_copies(slot):
        return [
            pltpu.make_async_remote_copy(src_ref=send_buf.at[side], dst_ref=halo_buf.at[slot, side],
                                         send_sem=halo_send.at[side], recv_sem=halo_recv.at[slot, side],
                                         device_id=at(target), device_id_type=mesh_id)
            for side, target in ((0, left), (1, right))
        ]

    def send_halo(slot):
        first = get_tiles(hf, pl.ds(0, RUNS, stride=HALF))
        final = get_tiles(hf, pl.ds(HALF - 1, RUNS, stride=HALF))
        first_on = jnp.concatenate([first[1:], first[:1]], axis=0)
        final_back = jnp.concatenate([final[-1:], final[:-1]], axis=0)
        send_buf[0] = jnp.where(place == 0, first_on, first).astype(BF16)
        send_buf[1] = jnp.where(place == RING - 1, final_back, final).astype(BF16)
        for copy in halo_copies(slot):
            copy.start()

    def wait_halo(slot):
        for copy in halo_copies(slot):
            copy.wait()

    def project_halo(slot, w):
        rows = jnp.concatenate([halo_buf[slot, 0], halo_buf[slot, 1]], axis=0)
        out = dot(rows, w.edge[1][...])
        set_tiles(proj1, pl.ds(8 + RUN, RUNS, stride=PAD1), out[:RUNS])
        set_tiles(proj1, pl.ds(7, RUNS, stride=PAD1), out[RUNS:])

    class Edge:
        def __init__(self, t, k, w, slot, run_shift=0, row_shift=0, source=None, first=False, final=False, keep=None):
            self.t, self.k, self.w, self.slot, self.keep = t, k, w, slot, keep
            self.run_shift, self.row_shift, self.first, self.final = run_shift, row_shift, first, final
            self.source = edge if source is None else source
            self.pre = None

        def a(self):
            self.pre = dot(self.source[self.k, tile_rows(self.t), :], self.w.edge[0][...])
            if self.keep is not None:
                for c in chunks():
                    pre_buf[self.keep, pl.ds(c, CH), :] = self.pre[c:c + CH]

        def resume(self):
            self.pre = pre_buf.at[self.keep]

        def extra(self, c):
            got = []
            for q in chunk_runs(c):
                base = (q + self.run_shift) % RUNS
                for r, n in pieces(self.t):
                    if self.t == 0:
                        got.append(get_tiles(proj0, pl.ds(base * PAD0 + r + self.row_shift, n)))
                    else:
                        got.append(get_tiles(proj1, pl.ds(base * PAD1 + 8 + r + self.row_shift, n)))
            return jnp.concatenate(got, axis=0) + recv[part_rows(self.t, c), :]

        def fin(self):
            hide(self.slot, self.pre, self.extra)

        def b(self):
            y = dot(hid[self.slot], self.w.edge_out[...])
            for c in chunks():
                part = part_rows(self.t, c)
                value = (self.source[self.k, part, :].astype(F32) + norm(y[c:c + CH])).astype(BF16)
                edge[self.k, part, :] = value
                total = value.astype(F32)
                if not self.first:
                    total = total + acc[part, :]
                if self.final:
                    esum[part, :] = total.astype(BF16)
                else:
                    acc[part, :] = total

    class Node:
        def __init__(self, t, base, w):
            self.t, self.base, self.w, self.slot = t, base, w, 6 + t

        def a(self):
            rows = tile_rows(self.t)
            hide(self.slot, dot(self.base[rows, :], self.w.node[0][...]) + dot(esum[rows, :], self.w.node[1][...]))

        def b(self):
            y = dot(hid[self.slot], self.w.node_out[...])
            for c in chunks():
                part = part_rows(self.t, c)
                value = (self.base[part, :].astype(F32) + norm(y[c:c + CH])).astype(BF16)
                h[part, :] = value
                if self.t == 1:
                    set_tiles(hf, pl.ds(c, CH), value.astype(F32))

    def project(t, w):
        out = dot(h[tile_rows(t), :], w.edge[1][...])
        for q in range(RUNS):
            row = q * HALF
            for r, n in pieces(t):
                if t == 0:
                    set_tiles(proj0, pl.ds(q * PAD0 + r, n), out[row:row + n])
                else:
                    set_tiles(proj1, pl.ds(q * PAD1 + 8 + r, n), out[row:row + n])
                row += n
        back = dot(h[tile_rows(t), :], w.edge[2][...])
        for c in chunks():
            recv[part_rows(t, c), :] = back[c:c + CH]
        if t == 1:
            for r in (7, 24):
                set_tiles(proj0, pl.ds(r, RUNS, stride=PAD0), get_tiles(proj1, pl.ds(8 + r, RUNS, stride=PAD1)))

    def share_rows():
        for r in (8, 23):
            set_tiles(proj1, pl.ds(8 + r, RUNS, stride=PAD1), get_tiles(proj0, pl.ds(r, RUNS, stride=PAD0)))

    def far_items(t, w, source=None, resume=False):
        items = [Edge(t, k, w, n, run_shift=s, source=source, first=n == 0, keep=4 * t + n) for n, (k, s) in enumerate(FAR)]
        if resume:
            for item in items:
                item.resume()
        return items

    def near_items(t, w, resume=False):
        items = [Edge(t, k, w, 4 + n, row_shift=s, final=n == 1, keep=8 + t if n == 0 else None)
                 for n, (k, s) in enumerate(NEAR)]
        if resume:
            items[0].resume()
        return items

    def nothing():
        pass


    def phase(x, n, node, next_x, next_n, before, after):
        table = {"before": before, "n1": n[1].a, "na": node.a, "nb": node.b, "project": after, "an0": next_n[0].a}
        for i in range(4):
            table[f"fx{i}"], table[f"bx{i}"] = x[i].fin, x[i].b
            table[f"ax{i}"] = next_x[i].a if next_x else nothing
        for i in range(2):
            table[f"fn{i}"], table[f"bn{i}"] = n[i].fin, n[i].b
        for name in ORDER:
            table[name]()

    def encoder(step):
        w = Weights(enc_refs, 0)
        w1 = layer_weights(step, 1)
        w2 = layer_weights(step, 2)
        for k in range(6):
            for t in range(TILES):
                if t == 1 or k < 2:
                    edge[k, tile_rows(t), :] = edge_base[k, tile_rows(t), :]
        for t in range(TILES):
            out = dot(h_mesh[tile_rows(t), :], w.edge[2][...])
            for c in chunks():
                recv[part_rows(t, c), :] = out[c:c + CH]
        items = []
        for t in range(TILES):
            for p in range(2):
                def in_first(i, t=t, p=p):
                    hide(i % 2, dot(feat[p, tile_rows(t), :], we[pl.ds(10 + 2 * step, 2)].reshape(256, LAT)))

                def in_last(i, t=t, p=p):
                    y = dot(hid[i % 2], weo[0])
                    for c in chunks():
                        v[p, part_rows(t, c), :] = norm(y[c:c + CH]).astype(BF16)

                def edge_first(i, t=t, p=p):
                    pre = dot(g2m[p, tile_rows(t), :], w.edge[0][...]) + dot(v[p, tile_rows(t), :], w.edge[1][...])
                    hide(2 + i % 2, pre, lambda c, t=t: recv[part_rows(t, c), :])

                def edge_last(i, t=t, p=p):
                    y = dot(hid[2 + i % 2], w.edge_out[...])
                    for c in chunks():
                        part = part_rows(t, c)
                        total = (g2m[p, part, :].astype(F32) + norm(y[c:c + CH])).astype(BF16).astype(F32)
                        if p == 0:
                            acc[part, :] = total
                        else:
                            esum[part, :] = (acc[part, :] + total).astype(BF16)

                items.append([in_first, in_last, edge_first, edge_last])
        pipeline(items)
        nodes = [Node(t, h_mesh, w) for t in range(TILES)]
        selfs = []
        for t in range(TILES):
            for p in range(2):
                def self_first(t=t, p=p):
                    hide(4 + p, dot(v[p, tile_rows(t), :], wself[0]))

                def self_last(t=t, p=p):
                    y = dot(hid[4 + p], wself[1])
                    for c in chunks():
                        part = part_rows(t, c)
                        vc[p, part, :] = (v[p, part, :].astype(F32) + norm(y[c:c + CH])).astype(BF16)

                selfs.append((self_first, self_last))
        y = far_items(0, w1, edge_base)
        x = far_items(1, w1)
        nodes[0].a()
        selfs[0][0]()
        nodes[1].a()
        selfs[1][0]()
        nodes[0].b()
        selfs[0][1]()
        nodes[1].b()
        selfs[1][1]()
        y[0].a()
        y[1].a()
        project(0, w1)
        y[2].a()
        y[3].a()
        project(1, w1)
        send_halo(0)
        share_rows()
        selfs[2][0]()
        selfs[3][0]()
        y[0].fin()
        y[0].b()
        y[1].fin()
        y[1].b()
        selfs[2][1]()
        y[2].fin()
        y[2].b()
        y[3].fin()
        y[3].b()
        selfs[3][1]()
        for item in x + far_items(0, w2) + near_items(0, w1)[:1]:
            item.a()

    def out_copies(step, out):
        copies = []
        for hop in range(RING):
            target = lax.rem(me + hop, RING)
            src, dst = x_buf.at[step + 1, pl.ds(2 * target, 2)], out.at[:, place]
            if hop == 0:
                copies.append(pltpu.make_async_copy(src, dst, out_recv.at[step, hop]))
            else:
                copies.append(pltpu.make_async_remote_copy(
                    src_ref=src, dst_ref=dst, send_sem=out_send.at[step, hop], recv_sem=out_recv.at[step, hop],
                    device_id=at(target), device_id_type=mesh_id))
        return copies

    def decoder_items(step):
        w = layer_weights(step, BLOCKS - 1)
        in_mean = stats[0:1, :]
        in_std = stats[1:2, :]
        diff_mean = stats[2:3, :]
        diff_std = stats[3:4, :]
        items = []
        for t in range(TILES):
            for p in range(2):
                def edge_first(i, t=t, p=p):
                    if p == 0 and t == 0:
                        for q in range(RUNS):
                            recv[pl.ds(q * HALF, HALF), :] = get_tiles(proj0, pl.ds(q * PAD0 + 8, HALF))
                    elif p == 0:
                        out = dot(h[tile_rows(t), :], w.edge[1][...])
                        for c in chunks():
                            recv[part_rows(t, c), :] = out[c:c + CH]
                    pre = dot(m2g[p, tile_rows(t), :], w.edge[0][...]) + dot(vc[p, tile_rows(t), :], w.edge[2][...])
                    hide(i % 2, pre, lambda c, t=t: recv[part_rows(t, c), :])

                def edge_last(i, t=t, p=p):
                    y = dot(hid[i % 2], w.edge_out[...])
                    for c in chunks():
                        part = part_rows(t, c)
                        dec[i % 2, pl.ds(c, CH), :] = (m2g[p, part, :].astype(F32) + norm(y[c:c + CH])).astype(BF16)

                def node_first(i, t=t, p=p):
                    hide(2 + i % 2, dot(vc[p, tile_rows(t), :], w.node[0][...]) + dot(dec[i % 2], w.node[1][...]))

                def node_last(i, t=t, p=p):
                    y = dot(hid[2 + i % 2], w.node_out[...])
                    for c in chunks():
                        part = part_rows(t, c)
                        v[p, part, :] = (vc[p, part, :].astype(F32) + norm(y[c:c + CH])).astype(BF16)

                def out_first(i, t=t, p=p):
                    hide(4 + i % 2, dot(v[p, tile_rows(t), :], woh[...]))

                def out_last(i, t=t, p=p):
                    pred = dot(hid[4 + i % 2], wof[...])
                    for c in chunks():
                        spots = [(q, pl.ds(2 * r + p, n, stride=2), n) for q in chunk_runs(c) for r, n in pieces(t)]
                        now = jnp.concatenate([x_buf[step, q, rows, :] for q, rows, n in spots], axis=0)[:, :VARS]
                        new = now + diff_std * pred[c:c + CH] + diff_mean
                        wide = jnp.concatenate([new, jnp.zeros((CH, 128 - VARS), F32)], axis=1)
                        row = 0
                        for q, rows, n in spots:
                            x_buf[step + 1, q, rows, :] = wide[row:row + n]
                            row += n
                        feat[p, part_rows(t, c), pl.ds(0, VARS)] = ((new - in_mean) / in_std).astype(BF16)

                items.append([edge_first, edge_last, node_first, node_last, out_first, out_last])
        return items

    def wait_all(copies):
        for copy in copies:
            copy.wait()

    def start_all(copies):
        for copy in copies:
            copy.start()

    def one_step(step, carry):
        wait_all(layer_copies(step, 1) + layer_copies(step, 2))
        start_all(layer_copies(step, 3))
        encoder(step)

        def one_layer(block, carry):
            halo_slot = lax.rem(block + 1, 2)
            wait_all(layer_copies(step, block + 2))

            @pl.when(block < LAYERS - 1)
            def _():
                start_all(layer_copies(step, block + 3))

            w, w1, w2 = (layer_weights(step, block + i) for i in range(3))
            phase(far_items(1, w, resume=True), near_items(0, w, resume=True), Node(0, h, w), far_items(1, w1),
                  near_items(1, w), share_rows, lambda: project(0, w1))
            wait_halo(halo_slot)
            phase(far_items(0, w1, resume=True), near_items(1, w, resume=True), Node(1, h, w), far_items(0, w2),
                  near_items(0, w1), lambda: project_halo(halo_slot, w), lambda: project(1, w1))
            send_halo(1 - halo_slot)
            return carry

        lax.fori_loop(1, LAYERS, one_layer, 0)
        @pl.when(step == 0)
        def _():
            start_all(layer_copies(1, 1) + layer_copies(1, 2))
            wait_in(2)
            for q in range(RUNS):
                x_buf[0, q, :, pl.ds(0, VARS)] = xc_buf[q]
                x_buf[0, q, :, pl.ds(VARS, 128 - VARS)] = jnp.zeros((2 * RUN, 128 - VARS), F32)

        w = layer_weights(step, LAYERS)
        w_last = layer_weights(step, BLOCKS - 1)
        n1 = near_items(1, w)
        phase(far_items(1, w, resume=True), near_items(0, w, resume=True), Node(0, h, w), None, n1, share_rows,
              lambda: project(0, w_last))
        n1[1].a()
        wait_halo(lax.rem(LAYERS + 1, 2))
        project_halo(lax.rem(LAYERS + 1, 2), w)
        last = Node(1, h, w)
        for item in n1:
            item.fin()
        for item in n1:
            item.b()
        last.a()
        last.b()
        pipeline(decoder_items(step))

        @pl.when(step == 0)
        def _():
            start_all(out_copies(0, out0))

        @pl.when(step == 1)
        def _():
            start_all(out_copies(1, out1))
        return carry

    lax.fori_loop(0, 2, one_step, 0)
    for part in range(3):
        for hop in range(1, RING):
            in_copies[part][hop].wait_send()
    for step, out in ((0, out0), (1, out1)):
        wait_all(out_copies(step, out))


def solution(mesh):
    row_spec = P(("dp", "gp"))
    edge_spec = P(("dp", "gp"), None, None)
    whole = P()

    def local_run(x_prev, x_cur, forcing, grid_static, g2m_feat, m2g_feat, mesh_feat, mesh_edge_feat, norm_stats,
                  w_grid_in, w_mesh_in, w_eemb_in, w_embed_out, w_edge_in, w_edge_out, w_node_in, w_node_out,
                  w_grid_self, w_out_hidden, w_out_final):
        grid_dev = x_prev.shape[0]
        mesh_dev = mesh_feat.shape[0]
        mean, std = norm_stats[0], norm_stats[1]

        def lanes(pieces, width):
            have = sum(piece.shape[1] for piece in pieces)
            rows = pieces[0].shape[0]
            return jnp.concatenate([piece.astype(BF16) for piece in pieces] + [jnp.zeros((rows, width - have), BF16)], axis=1)

        grid_lanes = jnp.concatenate([
            lanes([(x_prev - mean) / std, forcing[:, 0], grid_static, forcing[:, 1], m2g_feat], 128),
            lanes([(x_cur - mean) / std], 128)], axis=1)
        mesh_lanes = lanes([mesh_feat, mesh_edge_feat.reshape(mesh_dev, 24), g2m_feat.reshape(mesh_dev, 8)], 128)

        def placed(rows, start, height=128):
            return jnp.pad(rows, ((start, height - start - rows.shape[0]), (0, 0)))

        prev_rows, cur_rows = w_grid_in[:VARS], w_grid_in[VARS:2 * VARS]
        force_rows, static_rows = w_grid_in[2 * VARS:2 * VARS + 5], w_grid_in[2 * VARS + 5:]
        first_step = [placed(jnp.concatenate([prev_rows, force_rows, static_rows], axis=0), 0), placed(cur_rows, 0)]
        second_step = [placed(cur_rows, 0) + placed(static_rows, 89) + placed(force_rows, 94), placed(prev_rows, 0)]
        wemb = jnp.stack(
            [placed(w_mesh_in, 0)] + [placed(w_eemb_in[0], 27 + 4 * p) for p in range(2)]
            + [placed(w_eemb_in[2], 3 + 4 * k) for k in range(6)] + [placed(w_eemb_in[1], 99)]
            + first_step + second_step)

        any_spec = pl.BlockSpec(memory_space=pl.ANY)
        vmem_spec = pl.BlockSpec(memory_space=pltpu.VMEM)
        dma = pltpu.SemaphoreType.DMA
        out = jax.ShapeDtypeStruct((2, RING, 2 * RUN, 128), F32)
        scratch = [
            pltpu.VMEM((RUNS, 2 * RUN, 256), BF16),
            pltpu.VMEM((RUNS, RUN, 128), BF16),
            pltpu.VMEM((RUNS, 2 * RUN, VARS), F32),
            pltpu.VMEM((3, RUNS, 2 * RUN, 128), F32),
            pltpu.VMEM((2, RUNS * 2 * RUN, 128), F32),
            pltpu.VMEM((2, ROWS, 256), BF16),
            pltpu.VMEM((14, 128, LAT), BF16),
            pltpu.VMEM((5, LAT, LAT), BF16),
            pltpu.VMEM((2, LAT, LAT), BF16),
            pltpu.VMEM((LAT, LAT), BF16),
            pltpu.VMEM((LAT, VARS), BF16),
            pltpu.VMEM((1, 3 * LAT, LAT), BF16),
            pltpu.VMEM((1, LAT, LAT), BF16),
            pltpu.VMEM((1, 2 * LAT, LAT), BF16),
            pltpu.VMEM((1, LAT, LAT), BF16),
            pltpu.VMEM((SLOTS, 3 * LAT, LAT), BF16),
            pltpu.VMEM((SLOTS, LAT, LAT), BF16),
            pltpu.VMEM((SLOTS, 2 * LAT, LAT), BF16),
            pltpu.VMEM((SLOTS, LAT, LAT), BF16),
            pltpu.VMEM((6, ROWS, LAT), BF16),
            pltpu.VMEM((6, ROWS, LAT), BF16),
            pltpu.VMEM((ROWS, LAT), BF16),
            pltpu.VMEM((ROWS, LAT), BF16),
            pltpu.VMEM((LAT // 128, TILE, 128), F32),
            pltpu.VMEM((2, ROWS, LAT), BF16),
            pltpu.VMEM((2, ROWS, LAT), BF16),
            pltpu.VMEM((2, ROWS, LAT), BF16),
            pltpu.VMEM((2, ROWS, LAT), BF16),
            pltpu.VMEM((LAT // 128, RUNS * PAD0, 128), F32),
            pltpu.VMEM((LAT // 128, RUNS * PAD1, 128), F32),
            pltpu.VMEM((ROWS, LAT), F32),
            pltpu.VMEM((ROWS, LAT), F32),
            pltpu.VMEM((8, TILE, LAT), BF16),
            pltpu.VMEM((ROWS, LAT), BF16),
            pltpu.VMEM((2, TILE, LAT), BF16),
            pltpu.VMEM((10, TILE, LAT), F32),
            pltpu.VMEM((2, RUNS, LAT), BF16),
            pltpu.VMEM((2, 2, RUNS, LAT), BF16),
            dma((3, RING)), dma((3, RING)), dma((5,)), dma((1, 4)), dma((SLOTS, 4)), dma((2,)), dma((2, 2)),
            dma((2, RING)), dma((2, RING)),
        ]
        next_state, after_state = pl.pallas_call(
            kernel,
            out_shape=(out, out),
            in_specs=[any_spec, any_spec, any_spec, vmem_spec] + [any_spec] * 9,
            out_specs=(any_spec, any_spec),
            scratch_shapes=scratch,
            compiler_params=pltpu.CompilerParams(collective_id=0, has_side_effects=True, vmem_limit_bytes=60 << 20),
            name="forecast",
        )(grid_lanes.reshape(2, RING, 2 * RUN, 256), mesh_lanes.reshape(2, RING, RUN, 128),
          x_cur.reshape(2, RING, 2 * RUN, VARS), norm_stats, wemb, w_embed_out, w_edge_in, w_edge_out, w_node_in,
          w_node_out, w_grid_self, w_out_hidden, w_out_final)
        return next_state.reshape(grid_dev, 128)[:, :VARS], after_state.reshape(grid_dev, 128)[:, :VARS]

    in_specs = (row_spec, row_spec, edge_spec, row_spec, row_spec, row_spec, row_spec, edge_spec, whole) + (whole,) * 11
    return jax.shard_map(local_run, mesh=mesh, in_specs=in_specs, out_specs=(row_spec, row_spec), check_vma=False)
```

```python
import functools

import jax
import jax.numpy as jnp
from jax import lax
from jax.experimental import pallas as pl
from jax.experimental.pallas import tpu as pltpu
from jax.sharding import PartitionSpec as P

F32 = jnp.float32
BF16 = jnp.bfloat16

RUNS = 16
RUN = 32
GRID_RUN = 2 * RUN
ROWS = RUNS * RUN
ZERO, ONE, LAST = 0, 1, -1
LAT = 512
LANES = 128
PAIR = 2
VARS = 84
PAD0 = 32
PAD1 = 48
TILE = 256
TILES = 2
HALF = TILE // RUNS
CH = 32
RING = 8
LAYERS = 16
BLOCKS = LAYERS + 2
SLOTS = 4
FAR = ((2, 1), (3, -1), (4, 4), (5, -4))
NEAR = ((0, 1), (1, -1))
ORDER_A = (
    "nh", "before", "fx0", "bx0", "n1", "fx1", "bx1", "fn0", "fn1", "bn0", "bn1", "ax0", "fx2", "ax1", "fx3",
    "bx2", "na", "bx3", "ax2", "nb", "an0", "ax3", "pr", "ps",
)
ORDER_B = (
    "n1", "nh", "fx0", "bx0", "before", "fx1", "bx1", "fn0", "fn1", "bn0", "bn1", "ax0", "fx2", "bx2", "ax1",
    "fx3", "bx3", "na", "ax2", "nb", "an0", "ax3", "ps", "pr",
)


def dot(a, b):
    return jnp.dot(a, b, preferred_element_type=F32)


def silu(pre):
    return pre * jax.nn.sigmoid(pre)


def norm(y):
    centred = y - jnp.mean(y, axis=LAST, keepdims=True)
    return centred * lax.rsqrt(jnp.mean(centred * centred, axis=LAST, keepdims=True) + 1e-5)


def ring_place(dev):
    high = lax.div(dev, 4)
    return high * (4 + lax.rem(dev + 2, 4)) + (1 - high) * dev


def chunks():
    return range(0, TILE, CH)


def tile_rows(t):
    return pl.ds(t * TILE, TILE)


def part_rows(t, c):
    return pl.ds(t * TILE + c, CH)


def chunk_runs(c):
    return range(c // HALF, (c + CH) // HALF)


def pieces(t):
    return ((8, 16),) if t == 0 else ((0, 8), (24, 8))


def get_tiles(ref, rows):
    return jnp.concatenate([ref[j, rows, :] for j in range(ref.shape[0])], axis=ONE)


def set_tiles(ref, rows, value):
    for j in range(ref.shape[0]):
        ref[j, rows, :] = value[:, LANES * j:LANES * j + LANES]


def columns(n):
    return pl.ds(LANES * n, LANES)


def stack(ref, n, rows):
    base = LANES * n
    end = 0
    for at_row, value in rows:
        first = at_row // 8 * 8
        last = (at_row + value.shape[0]) // 8 * 8
        if first > end:
            ref[pl.ds(base + end, first - end), :] = jnp.zeros((first - end, LANES), F32)
        if last < at_row + value.shape[0]:
            ref[pl.ds(base + last, 8), :] = jnp.zeros((8, LANES), F32)
            end = last + 8
        else:
            end = last
        ref[pl.ds(base + at_row, value.shape[0]), :] = value
    if end < LANES:
        ref[pl.ds(base + end, LANES - end), :] = jnp.zeros((LANES - end, LANES), F32)


def pack_kernel(x_prev, x_cur, forcing, static, g2m_feat, m2g_feat, mesh_feat, mesh_edge_feat, stats, w_out_final,
                g_home, m_home, x_home, w_final, area):
    def turned(slot, n):
        return jnp.transpose(area[slot, pl.ds(LANES * n, LANES), :])

    for n in range(4):
        stack(area.at[2], n, [(0, mesh_feat[:, columns(n)])] + [(16 + 16 * k, mesh_edge_feat[k, :, columns(n)]) for k in range(6)])
    for n in range(LAT // LANES):
        stack(area.at[3], n, [(0, w_out_final[:, columns(n)].astype(F32))])
    for n in range(8):
        stack(area.at[0], n, [(0, x_prev[:, columns(n)]), (88, forcing[:, 0, columns(n)]), (96, static[:, columns(n)]),
                              (104, forcing[:, 1, columns(n)]), (112, m2g_feat[:, columns(n)]), (120, g2m_feat[:, columns(n)])])
        stack(area.at[1], n, [(0, x_cur[:, columns(n)])])
    for n in range(4):
        rows = turned(2, n).astype(BF16)
        for i in range(4):
            m_home[n // 2, 4 * (n % 2) + i] = rows[RUN * i:RUN * i + RUN]
    for n in range(LAT // LANES):
        w_final[columns(n), :] = turned(3, n).astype(BF16)
    rest = LANES - VARS
    wide_mean = jnp.concatenate([stats[0:1, :], jnp.zeros((1, rest), F32)], axis=ONE)
    wide_std = jnp.concatenate([stats[1:2, :], jnp.ones((1, rest), F32)], axis=ONE)
    for n in range(8):
        prev_rows = ((turned(0, n) - wide_mean) / wide_std).astype(BF16)
        cur = turned(1, n)
        cur_rows = ((cur - wide_mean) / wide_std).astype(BF16)
        for i in range(2):
            t, k, half = n // 4, 2 * (n % 4) + i, slice(GRID_RUN * i, GRID_RUN * i + GRID_RUN)
            g_home[t, k, :, pl.ds(ZERO, LANES)] = prev_rows[half]
            g_home[t, k, :, pl.ds(LANES, LANES)] = cur_rows[half]
            x_home[t, k] = cur[half]


def unpack_kernel(home0, home1, out0, out1):
    for home, out in ((home0, out0), (home1, out1)):
        for n in range(8):
            rows = jnp.concatenate([home[n // 4, 2 * (n % 4) + i] for i in range(2)], axis=ZERO)
            out[:, columns(n)] = jnp.transpose(rows)[:VARS]


def kernel(g_home, m_home, x_home, stats, w_grid_in, w_mesh_in,
           w_eemb_in, w_embed_out, w_edge_in, w_edge_out, w_node_in, w_node_out, w_grid_self, w_out_hidden, w_out_final,
           out0, out1,
           wgrid_raw, wmesh_raw, weemb_raw,
           g_buf, m_buf, x_buf, gf, feat, we, weo, wself, woh, wof,
           enc_ei, enc_eo, enc_ni, enc_no, lay_ei, lay_eo, lay_ni, lay_no,
           edge_base, edge, h_mesh, h, hf, g2m, m2g, v, vc, proj0, proj1, recv, acc, hid, esum, dec, pre_buf,
           send_buf, halo_buf,
           raw_sem, in_send, in_recv, w_sem, enc_sem, lay_sem, halo_send, halo_recv, out_send, out_recv):
    me = lax.axis_index("gp")
    place = ring_place(me)

    def at(dev):
        return {"gp": dev}

    mesh_id = pl.DeviceIdType.MESH

    def block_copies(block, dst_refs, slot, sem):
        srcs = (w_edge_in, w_edge_out, w_node_in, w_node_out)
        return [pltpu.make_async_copy(src.at[block], dst.at[slot], sem.at[slot, i])
                for i, (src, dst) in enumerate(zip(srcs, dst_refs))]

    enc_refs = (enc_ei, enc_eo, enc_ni, enc_no)
    lay_refs = (lay_ei, lay_eo, lay_ni, lay_no)

    def enc_copies():
        return block_copies(0, enc_refs, 0, enc_sem)

    def slot_of(step, block):
        return lax.rem((BLOCKS - 1) * step + block - 1, SLOTS)

    def layer_copies(step, block):
        return block_copies(block, lay_refs, slot_of(step, block), lay_sem)

    class Weights:
        def __init__(self, refs, slot):
            self.edge = [refs[0].at[slot, pl.ds(i * LAT, LAT)] for i in range(3)]
            self.edge_out = refs[1].at[slot]
            self.node = [refs[2].at[slot, pl.ds(i * LAT, LAT)] for i in range(2)]
            self.node_out = refs[3].at[slot]

    def layer_weights(step, block):
        return Weights(lay_refs, slot_of(step, block))

    raw = [pltpu.make_async_copy(src, dst, raw_sem.at[i]) for i, (src, dst) in enumerate(
        ((w_grid_in, wgrid_raw), (w_mesh_in, wmesh_raw), (w_eemb_in, weemb_raw)))]
    for copy in raw:
        copy.start()
    small = [
        pltpu.make_async_copy(w_embed_out, weo, w_sem.at[0]),
        pltpu.make_async_copy(w_grid_self, wself, w_sem.at[1]),
        pltpu.make_async_copy(w_out_hidden, woh, w_sem.at[2]),
        pltpu.make_async_copy(w_out_final, wof, w_sem.at[3]),
    ]
    for copy in small + enc_copies() + layer_copies(0, 1) + layer_copies(0, 2):
        copy.start()

    barrier = pltpu.get_barrier_semaphore()
    for hop in range(1, RING):
        pl.semaphore_signal(barrier, inc=1, device_id=at(lax.rem(me + hop, RING)), device_id_type=mesh_id)

    parts = ((m_home, m_buf), (g_home, g_buf), (x_home, x_buf.at[0]))

    def in_copy(part, hop):
        src, dst = parts[part]
        target = lax.rem(me + hop, RING)
        src = src.at[:, ring_place(target)]
        dst = dst.at[pl.ds(2 * me, 2)]
        if hop == 0:
            return pltpu.make_async_copy(src, dst, in_recv.at[part, 0])
        return pltpu.make_async_remote_copy(src_ref=src, dst_ref=dst, send_sem=in_send.at[part, hop],
                                            recv_sem=in_recv.at[part, hop], device_id=at(target),
                                            device_id_type=mesh_id)

    in_copies = [[in_copy(part, hop) for hop in range(RING)] for part in range(3)]

    def wait_in(part):
        in_copies[part][0].wait()
        for copy in in_copies[part][1:]:
            copy.wait_recv()

    pl.semaphore_wait(barrier, RING - 1)
    for part in range(3):
        for copy in in_copies[part]:
            copy.start()

    for copy in raw:
        copy.wait()
    wide = wgrid_raw[...].astype(F32)
    recv[pl.ds(ZERO, wide.shape[0]), :] = wide
    prev_w, cur_w = recv[pl.ds(ZERO, VARS), :], recv[pl.ds(VARS, VARS), :]
    force_w, static_w = recv[pl.ds(2 * VARS, 5), :], recv[pl.ds(2 * VARS + 5, 5), :]
    spread = [[(0, wmesh_raw[...].astype(F32))], [(120, weemb_raw[0].astype(F32))], [(112, weemb_raw[1].astype(F32))]]
    spread += [[(16 + 16 * k, weemb_raw[2].astype(F32))] for k in range(6)]
    spread += [[(0, prev_w), (88, force_w), (96, static_w)], [(0, cur_w)]]
    spread += [[(0, cur_w), (96, static_w), (104, force_w)], [(0, prev_w)]]
    for i, rows in enumerate(spread):
        base = LANES * (i % 4)
        acc[pl.ds(base, LANES), :] = jnp.zeros((LANES, LAT), F32)
        for at_row, value in rows:
            acc[pl.ds(base + at_row, value.shape[0]), :] = value
        we[i] = acc[pl.ds(base, LANES), :].astype(BF16)

    def pipeline(items):
        depth = max(len(item) for item in items)
        for beat in range(len(items) + depth - 1):
            for stage in range(depth):
                index = beat - stage
                if 0 <= index < len(items) and stage < len(items[index]):
                    items[index][stage](index)

    def hide(slot, pre, extra=None):
        for c in chunks():
            value = pre[c:c + CH]
            if extra is not None:
                value = value + extra(c)
            hid[slot, pl.ds(c, CH), :] = silu(value).astype(BF16)

    def embed_item(load, w_first, second, store):
        def first(i):
            hide(i % 2, dot(load(), we[w_first]))

        def last(i):
            y = dot(hid[i % 2], weo[second])
            for c in chunks():
                store(c, norm(y[c:c + CH]).astype(BF16))

        return [first, last]

    wait_in(0)
    small[0].wait()
    mesh_rows = [jnp.concatenate([m_buf[(q + 1) % RUNS].astype(F32)[r:r + n] for q in range(RUNS) for r, n in pieces(t)],
                                 axis=ZERO).astype(BF16) for t in range(TILES)]
    items = []
    for t in range(TILES):
        def store_mesh(c, value, t=t):
            h_mesh[part_rows(t, c), :] = value
        items.append(embed_item(lambda t=t: mesh_rows[t], 0, 1, store_mesh))
        for k in range(6):
            def store_edge(c, value, t=t, k=k):
                edge_base[k, part_rows(t, c), :] = value
            items.append(embed_item(lambda t=t: mesh_rows[t], 3 + k, 4, store_edge))
    pipeline(items)

    wait_in(1)
    for q in range(RUNS):
        set_tiles(gf, pl.ds(q * GRID_RUN, GRID_RUN), g_buf[q].astype(F32))
    for t in range(TILES):
        for p in range(PAIR):
            for c in chunks():
                feat[p, part_rows(t, c), :] = jnp.concatenate(
                    [get_tiles(gf, pl.ds(q * GRID_RUN + 2 * r + p, n, stride=2)) for q in chunk_runs(c) for r, n in pieces(t)],
                    axis=ZERO).astype(BF16)

    def next_run(t, p):
        lanes = pl.ds(ZERO, LANES)
        return jnp.concatenate([feat[p, pl.ds(t * TILE + HALF, TILE - HALF), lanes], feat[p, pl.ds(t * TILE, HALF), lanes]],
                               axis=ZERO)

    items = []
    for t in range(TILES):
        for p in range(PAIR):
            def store_m2g(c, value, t=t, p=p):
                m2g[p, part_rows(t, c), :] = value
            def store_g2m(c, value, t=t, p=p):
                g2m[p, part_rows(t, c), :] = value
            items.append(embed_item(lambda t=t, p=p: next_run(t, p), 1, 2, store_g2m))
            items.append(embed_item(lambda t=t, p=p: feat[p, tile_rows(t), pl.ds(ZERO, LANES)], 2, 3, store_m2g))
    pipeline(items)
    for copy in small[1:] + enc_copies():
        copy.wait()

    left = ring_place(lax.rem(place + RING - 1, RING))
    right = ring_place(lax.rem(place + 1, RING))

    def halo_copies(slot):
        return [
            pltpu.make_async_remote_copy(src_ref=send_buf.at[side], dst_ref=halo_buf.at[slot, side],
                                         send_sem=halo_send.at[side], recv_sem=halo_recv.at[slot, side],
                                         device_id=at(target), device_id_type=mesh_id)
            for side, target in ((0, left), (1, right))
        ]

    def send_halo(slot):
        first = get_tiles(hf, pl.ds(ZERO, RUNS, stride=HALF))
        final = get_tiles(hf, pl.ds(HALF - 1, RUNS, stride=HALF))
        first_on = jnp.concatenate([first[1:], first[:1]], axis=ZERO)
        final_back = jnp.concatenate([final[-1:], final[:-1]], axis=ZERO)
        send_buf[0] = jnp.where(place == 0, first_on, first).astype(BF16)
        send_buf[1] = jnp.where(place == RING - 1, final_back, final).astype(BF16)
        for copy in halo_copies(slot):
            copy.start()

    def wait_halo(slot):
        for copy in halo_copies(slot):
            copy.wait()

    def project_halo(slot, w):
        rows = jnp.concatenate([halo_buf[slot, 0], halo_buf[slot, 1]], axis=ZERO)
        out = dot(rows, w.edge[1][...])
        set_tiles(proj1, pl.ds(8 + RUN, RUNS, stride=PAD1), out[:RUNS])
        set_tiles(proj1, pl.ds(7, RUNS, stride=PAD1), out[RUNS:])

    class Edge:
        def __init__(self, t, k, w, slot, run_shift=0, row_shift=0, source=None, first=False, final=False, keep=None):
            self.t, self.k, self.w, self.slot, self.keep = t, k, w, slot, keep
            self.run_shift, self.row_shift, self.first, self.final = run_shift, row_shift, first, final
            self.source = edge if source is None else source
            self.pre = None

        def a(self):
            self.pre = dot(self.source[self.k, tile_rows(self.t), :], self.w.edge[0][...])
            if self.keep is not None:
                for c in chunks():
                    pre_buf[self.keep, pl.ds(c, CH), :] = self.pre[c:c + CH]

        def resume(self):
            self.pre = pre_buf.at[self.keep]

        def extra(self, c):
            got = []
            for q in chunk_runs(c):
                base = (q + self.run_shift) % RUNS
                for r, n in pieces(self.t):
                    if self.t == 0:
                        got.append(get_tiles(proj0, pl.ds(base * PAD0 + r + self.row_shift, n)))
                    else:
                        got.append(get_tiles(proj1, pl.ds(base * PAD1 + 8 + r + self.row_shift, n)))
            return jnp.concatenate(got, axis=ZERO) + recv[part_rows(self.t, c), :]

        def fin(self):
            hide(self.slot, self.pre, self.extra)

        def b(self):
            y = dot(hid[self.slot], self.w.edge_out[...])
            for c in chunks():
                part = part_rows(self.t, c)
                value = (self.source[self.k, part, :].astype(F32) + norm(y[c:c + CH])).astype(BF16)
                edge[self.k, part, :] = value
                total = value.astype(F32)
                if not self.first:
                    total = total + acc[part, :]
                if self.final:
                    esum[part, :] = total.astype(BF16)
                else:
                    acc[part, :] = total

    class Node:
        def __init__(self, t, base, w):
            self.t, self.base, self.w, self.slot = t, base, w, 6 + t

        def own(self):
            self.pre = dot(self.base[tile_rows(self.t), :], self.w.node[0][...])

        def a(self):
            hide(self.slot, self.pre + dot(esum[tile_rows(self.t), :], self.w.node[1][...]))

        def b(self):
            y = dot(hid[self.slot], self.w.node_out[...])
            for c in chunks():
                part = part_rows(self.t, c)
                value = (self.base[part, :].astype(F32) + norm(y[c:c + CH])).astype(BF16)
                h[part, :] = value
                if self.t == 1:
                    set_tiles(hf, pl.ds(c, CH), value.astype(F32))

    def project_send(t, w):
        out = dot(h[tile_rows(t), :], w.edge[1][...])
        for q in range(RUNS):
            row = q * HALF
            for r, n in pieces(t):
                if t == 0:
                    set_tiles(proj0, pl.ds(q * PAD0 + r, n), out[row:row + n])
                else:
                    set_tiles(proj1, pl.ds(q * PAD1 + 8 + r, n), out[row:row + n])
                row += n
        if t == 1:
            for r in (7, 24):
                set_tiles(proj0, pl.ds(r, RUNS, stride=PAD0), get_tiles(proj1, pl.ds(8 + r, RUNS, stride=PAD1)))

    def project_recv(t, w):
        out = dot(h[tile_rows(t), :], w.edge[2][...])
        for c in chunks():
            recv[part_rows(t, c), :] = out[c:c + CH]

    def project(t, w):
        project_send(t, w)
        project_recv(t, w)

    def share_rows():
        for r in (8, 23):
            set_tiles(proj1, pl.ds(8 + r, RUNS, stride=PAD1), get_tiles(proj0, pl.ds(r, RUNS, stride=PAD0)))

    def far_items(t, w, source=None, resume=False):
        items = [Edge(t, k, w, n, run_shift=s, source=source, first=n == 0, keep=4 * t + n) for n, (k, s) in enumerate(FAR)]
        if resume:
            for item in items:
                item.resume()
        return items

    def near_items(t, w, resume=False):
        items = [Edge(t, k, w, 4 + n, row_shift=s, final=n == 1, keep=8 + t if n == 0 else None)
                 for n, (k, s) in enumerate(NEAR)]
        if resume:
            items[0].resume()
        return items

    def nothing():
        pass


    def phase(order, x, n, node, next_x, next_n, before, w_next):
        table = {"before": before, "n1": n[1].a, "nh": node.own, "na": node.a, "nb": node.b, "an0": next_n[0].a,
                 "ps": lambda: project_send(node.t, w_next), "pr": lambda: project_recv(node.t, w_next)}
        for i in range(4):
            table[f"fx{i}"], table[f"bx{i}"] = x[i].fin, x[i].b
            table[f"ax{i}"] = next_x[i].a if next_x else nothing
        for i in range(2):
            table[f"fn{i}"], table[f"bn{i}"] = n[i].fin, n[i].b
        for name in order:
            table[name]()

    def encoder(step):
        w = Weights(enc_refs, 0)
        w1 = layer_weights(step, 1)
        w2 = layer_weights(step, 2)
        for k in range(6):
            for t in range(TILES):
                if t == 1 or k < 2:
                    edge[k, tile_rows(t), :] = edge_base[k, tile_rows(t), :]
        for t in range(TILES):
            out = dot(h_mesh[tile_rows(t), :], w.edge[2][...])
            for c in chunks():
                recv[part_rows(t, c), :] = out[c:c + CH]
        items = []
        for t in range(TILES):
            for p in range(PAIR):
                def in_first(i, t=t, p=p):
                    hide(i % 2, dot(feat[p, tile_rows(t), :], we[pl.ds(9 + 2 * step, 2)].reshape(256, LAT)))

                def in_last(i, t=t, p=p):
                    y = dot(hid[i % 2], weo[0])
                    for c in chunks():
                        v[p, part_rows(t, c), :] = norm(y[c:c + CH]).astype(BF16)

                def edge_first(i, t=t, p=p):
                    pre = dot(g2m[p, tile_rows(t), :], w.edge[0][...]) + dot(v[p, tile_rows(t), :], w.edge[1][...])
                    hide(2 + i % 2, pre, lambda c, t=t: recv[part_rows(t, c), :])

                def edge_last(i, t=t, p=p):
                    y = dot(hid[2 + i % 2], w.edge_out[...])
                    for c in chunks():
                        part = part_rows(t, c)
                        total = (g2m[p, part, :].astype(F32) + norm(y[c:c + CH])).astype(BF16).astype(F32)
                        if p == 0:
                            acc[part, :] = total
                        else:
                            esum[part, :] = (acc[part, :] + total).astype(BF16)

                items.append([in_first, in_last, edge_first, edge_last])
        pipeline(items)
        nodes = [Node(t, h_mesh, w) for t in range(TILES)]
        selfs = []
        for t in range(TILES):
            for p in range(PAIR):
                def self_first(t=t, p=p):
                    hide(4 + p, dot(v[p, tile_rows(t), :], wself[0]))

                def self_last(t=t, p=p):
                    y = dot(hid[4 + p], wself[1])
                    for c in chunks():
                        part = part_rows(t, c)
                        vc[p, part, :] = (v[p, part, :].astype(F32) + norm(y[c:c + CH])).astype(BF16)

                selfs.append((self_first, self_last))
        y = far_items(0, w1, edge_base)
        x = far_items(1, w1)
        nodes[0].own()
        nodes[0].a()
        selfs[0][0]()
        nodes[1].own()
        nodes[1].a()
        selfs[1][0]()
        nodes[0].b()
        selfs[0][1]()
        nodes[1].b()
        selfs[1][1]()
        y[0].a()
        y[1].a()
        project(0, w1)
        y[2].a()
        y[3].a()
        project(1, w1)
        send_halo(0)
        share_rows()
        selfs[2][0]()
        selfs[3][0]()
        y[0].fin()
        y[0].b()
        y[1].fin()
        y[1].b()
        selfs[2][1]()
        y[2].fin()
        y[2].b()
        y[3].fin()
        y[3].b()
        selfs[3][1]()
        for item in x + far_items(0, w2) + near_items(0, w1)[:1]:
            item.a()

    def out_copies(step, out):
        copies = []
        for hop in range(RING):
            target = lax.rem(me + hop, RING)
            src, dst = x_buf.at[step + 1, pl.ds(2 * target, 2)], out.at[:, place]
            if hop == 0:
                copies.append(pltpu.make_async_copy(src, dst, out_recv.at[step, hop]))
            else:
                copies.append(pltpu.make_async_remote_copy(
                    src_ref=src, dst_ref=dst, send_sem=out_send.at[step, hop], recv_sem=out_recv.at[step, hop],
                    device_id=at(target), device_id_type=mesh_id))
        return copies

    def decoder_items(step):
        w = layer_weights(step, BLOCKS - 1)
        in_mean = stats[0:1, :]
        in_std = stats[1:2, :]
        diff_mean, diff_std = (jnp.concatenate([stats[i:i + 1, :], jnp.zeros((1, LANES - VARS), F32)], axis=ONE) for i in (2, 3))
        items = []
        for t in range(TILES):
            for p in range(PAIR):
                def edge_first(i, t=t, p=p):
                    if p == 0 and t == 0:
                        for q in range(RUNS):
                            recv[pl.ds(q * HALF, HALF), :] = get_tiles(proj0, pl.ds(q * PAD0 + 8, HALF))
                    elif p == 0:
                        out = dot(h[tile_rows(t), :], w.edge[1][...])
                        for c in chunks():
                            recv[part_rows(t, c), :] = out[c:c + CH]
                    pre = dot(m2g[p, tile_rows(t), :], w.edge[0][...]) + dot(vc[p, tile_rows(t), :], w.edge[2][...])
                    hide(i % 2, pre, lambda c, t=t: recv[part_rows(t, c), :])

                def edge_last(i, t=t, p=p):
                    y = dot(hid[i % 2], w.edge_out[...])
                    for c in chunks():
                        part = part_rows(t, c)
                        dec[i % 2, pl.ds(c, CH), :] = (m2g[p, part, :].astype(F32) + norm(y[c:c + CH])).astype(BF16)

                def node_first(i, t=t, p=p):
                    hide(2 + i % 2, dot(vc[p, tile_rows(t), :], w.node[0][...]) + dot(dec[i % 2], w.node[1][...]))

                def node_last(i, t=t, p=p):
                    y = dot(hid[2 + i % 2], w.node_out[...])
                    for c in chunks():
                        part = part_rows(t, c)
                        v[p, part, :] = (vc[p, part, :].astype(F32) + norm(y[c:c + CH])).astype(BF16)

                def out_first(i, t=t, p=p):
                    hide(4 + i % 2, dot(v[p, tile_rows(t), :], woh[...]))

                def out_last(i, t=t, p=p):
                    pred = dot(hid[4 + i % 2], wof[...])
                    for c in chunks():
                        spots = [(q, pl.ds(2 * r + p, n, stride=2), n) for q in chunk_runs(c) for r, n in pieces(t)]
                        now = jnp.concatenate([x_buf[step, q, rows, :] for q, rows, n in spots], axis=ZERO)
                        new = now + diff_std * pred[c:c + CH] + diff_mean
                        row = 0
                        for q, rows, n in spots:
                            x_buf[step + 1, q, rows, :] = new[row:row + n]
                            row += n
                        scaled = (new[:, :VARS] - in_mean) / in_std
                        feat[p, part_rows(t, c), pl.ds(ZERO, VARS)] = scaled.astype(BF16)

                items.append([edge_first, edge_last, node_first, node_last, out_first, out_last])
        return items

    def wait_all(copies):
        for copy in copies:
            copy.wait()

    def start_all(copies):
        for copy in copies:
            copy.start()

    def one_step(step, carry):
        wait_all(layer_copies(step, 1) + layer_copies(step, 2))
        start_all(layer_copies(step, 3))
        encoder(step)

        def one_layer(block, carry):
            halo_slot = lax.rem(block + 1, 2)
            wait_all(layer_copies(step, block + 2))

            @pl.when(block < LAYERS - 1)
            def _():
                start_all(layer_copies(step, block + 3))

            w, w1, w2 = (layer_weights(step, block + i) for i in range(3))
            phase(ORDER_A, far_items(1, w, resume=True), near_items(0, w, resume=True), Node(0, h, w), far_items(1, w1),
                  near_items(1, w), share_rows, w1)
            wait_halo(halo_slot)
            phase(ORDER_B, far_items(0, w1, resume=True), near_items(1, w, resume=True), Node(1, h, w), far_items(0, w2),
                  near_items(0, w1), lambda: project_halo(halo_slot, w), w1)
            send_halo(1 - halo_slot)
            return carry

        lax.fori_loop(1, LAYERS, one_layer, 0)
        @pl.when(step == 0)
        def _():
            start_all(layer_copies(1, 1) + layer_copies(1, 2))
            wait_in(2)

        w = layer_weights(step, LAYERS)
        w_last = layer_weights(step, BLOCKS - 1)
        n1 = near_items(1, w)
        phase(ORDER_A, far_items(1, w, resume=True), near_items(0, w, resume=True), Node(0, h, w), None, n1, share_rows, w_last)
        n1[1].a()
        wait_halo(lax.rem(LAYERS + 1, 2))
        project_halo(lax.rem(LAYERS + 1, 2), w)
        last = Node(1, h, w)
        for item in n1:
            item.fin()
        for item in n1:
            item.b()
        last.own()
        last.a()
        last.b()
        pipeline(decoder_items(step))

        for which, out in ((0, out0), (1, out1)):
            @pl.when(step == which)
            def _():
                start_all(out_copies(which, out))
        return carry

    lax.fori_loop(0, 2, one_step, 0)
    for part in range(3):
        for copy in in_copies[part][1:]:
            copy.wait_send()
    wait_all(out_copies(0, out0) + out_copies(1, out1))


def solution(mesh):
    row_spec = P(("dp", "gp"))
    edge_spec = P(("dp", "gp"), None, None)
    whole = P()

    def local_run(x_prev, x_cur, forcing, grid_static, g2m_feat, m2g_feat, mesh_feat, mesh_edge_feat, norm_stats,
                  w_grid_in, w_mesh_in, w_eemb_in, w_embed_out, w_edge_in, w_edge_out, w_node_in, w_node_out,
                  w_grid_self, w_out_hidden, w_out_final):
        any_spec = pl.BlockSpec(memory_space=pl.ANY)
        vmem_spec = pl.BlockSpec(memory_space=pltpu.VMEM)
        dma = pltpu.SemaphoreType.DMA
        grid_dev = x_prev.shape[0]
        shape = jax.ShapeDtypeStruct
        home = shape((PAIR, RING, GRID_RUN, LANES), F32)
        g_home, m_home, x_home, w_final = pl.pallas_call(
            pack_kernel,
            out_shape=(shape((PAIR, RING, GRID_RUN, 256), BF16), shape((PAIR, RING, RUN, LANES), BF16), home, shape((LAT, LANES), BF16)),
            in_specs=[vmem_spec] * 10,
            out_specs=(vmem_spec,) * 4,
            scratch_shapes=[pltpu.VMEM((4, grid_dev, LANES), F32)],
            name="pack",
        )(x_prev.T, x_cur.T, forcing.T, grid_static.T, g2m_feat.T, m2g_feat.T, mesh_feat.T,
          jnp.transpose(mesh_edge_feat, (1, 2, 0)), norm_stats, w_out_final.T)
        scratch = [
            pltpu.VMEM((2 * VARS + 10, LAT), BF16),
            pltpu.VMEM((3, LAT), BF16),
            pltpu.VMEM((3, 4, LAT), BF16),
            pltpu.VMEM((RUNS, GRID_RUN, 256), BF16),
            pltpu.VMEM((RUNS, RUN, LANES), BF16),
            pltpu.VMEM((3, RUNS, GRID_RUN, LANES), F32),
            pltpu.VMEM((PAIR, RUNS * GRID_RUN, LANES), F32),
            pltpu.VMEM((PAIR, ROWS, 256), BF16),
            pltpu.VMEM((13, LANES, LAT), BF16),
            pltpu.VMEM((5, LAT, LAT), BF16),
            pltpu.VMEM((PAIR, LAT, LAT), BF16),
            pltpu.VMEM((LAT, LAT), BF16),
            pltpu.VMEM((LAT, LANES), BF16),
            pltpu.VMEM((1, 3 * LAT, LAT), BF16),
            pltpu.VMEM((1, LAT, LAT), BF16),
            pltpu.VMEM((1, 2 * LAT, LAT), BF16),
            pltpu.VMEM((1, LAT, LAT), BF16),
            pltpu.VMEM((SLOTS, 3 * LAT, LAT), BF16),
            pltpu.VMEM((SLOTS, LAT, LAT), BF16),
            pltpu.VMEM((SLOTS, 2 * LAT, LAT), BF16),
            pltpu.VMEM((SLOTS, LAT, LAT), BF16),
            pltpu.VMEM((6, ROWS, LAT), BF16),
            pltpu.VMEM((6, ROWS, LAT), BF16),
            pltpu.VMEM((ROWS, LAT), BF16),
            pltpu.VMEM((ROWS, LAT), BF16),
            pltpu.VMEM((LAT // LANES, TILE, LANES), F32),
            pltpu.VMEM((PAIR, ROWS, LAT), BF16),
            pltpu.VMEM((PAIR, ROWS, LAT), BF16),
            pltpu.VMEM((PAIR, ROWS, LAT), BF16),
            pltpu.VMEM((PAIR, ROWS, LAT), BF16),
            pltpu.VMEM((LAT // LANES, RUNS * PAD0, LANES), F32),
            pltpu.VMEM((LAT // LANES, RUNS * PAD1, LANES), F32),
            pltpu.VMEM((ROWS, LAT), F32),
            pltpu.VMEM((ROWS, LAT), F32),
            pltpu.VMEM((8, TILE, LAT), BF16),
            pltpu.VMEM((ROWS, LAT), BF16),
            pltpu.VMEM((PAIR, TILE, LAT), BF16),
            pltpu.VMEM((10, TILE, LAT), F32),
            pltpu.VMEM((PAIR, RUNS, LAT), BF16),
            pltpu.VMEM((PAIR, 2, RUNS, LAT), BF16),
            dma((3,)), dma((3, RING)), dma((3, RING)), dma((4,)), dma((1, 4)), dma((SLOTS, 4)), dma((2,)), dma((2, 2)),
            dma((2, RING)), dma((2, RING)),
        ]
        home0, home1 = pl.pallas_call(
            kernel,
            out_shape=(home, home),
            in_specs=[any_spec] * 3 + [vmem_spec] + [any_spec] * 11,
            out_specs=(any_spec, any_spec),
            scratch_shapes=scratch,
            compiler_params=pltpu.CompilerParams(collective_id=0, has_side_effects=True, vmem_limit_bytes=63 << 20),
            name="forecast",
        )(g_home, m_home, x_home, norm_stats, w_grid_in, w_mesh_in, w_eemb_in, w_embed_out, w_edge_in, w_edge_out, w_node_in,
          w_node_out, w_grid_self, w_out_hidden, w_final)
        out = shape((VARS, grid_dev), F32)
        next_state, after_state = pl.pallas_call(
            unpack_kernel, out_shape=(out, out), in_specs=[vmem_spec] * 2, out_specs=(vmem_spec,) * 2, name="unpack",
        )(home0, home1)
        return next_state.T, after_state.T

    in_specs = (row_spec, row_spec, edge_spec, row_spec, row_spec, row_spec, row_spec, edge_spec, whole) + (whole,) * 11
    return jax.shard_map(local_run, mesh=mesh, in_specs=in_specs, out_specs=(row_spec, row_spec), check_vma=False)
```

```python
import functools

import jax
import jax.numpy as jnp
from jax import lax
from jax.experimental import pallas as pl
from jax.experimental.pallas import tpu as pltpu
from jax.sharding import PartitionSpec as P

F32 = jnp.float32
BF16 = jnp.bfloat16

RUNS = 16
RUN = 32
GRID_RUN = 2 * RUN
ROWS = RUNS * RUN
ZERO, ONE, LAST = 0, 1, -1
LAT = 512
LANES = 128
PAIR = 2
VARS = 84
PAD0 = 32
PAD1 = 48
TILE = 256
TILES = 2
HALF = TILE // RUNS
CH = 32
RING = 8
LAYERS = 16
BLOCKS = LAYERS + 2
SLOTS = 4
FAR = ((2, 1), (3, -1), (4, 4), (5, -4))
NEAR = ((0, 1), (1, -1))
ORDER_A = (
    "nh", "before", "fx0", "bx0", "n1", "fx1", "bx1", "fn0", "fn1", "bn0", "bn1", "ax0", "fx2", "ax1", "fx3",
    "bx2", "na", "bx3", "ax2", "nb", "an0", "ax3", "ps", "pr",
)
ORDER_B = (
    "nh", "before", "fx0", "bx0", "n1", "fx1", "bx1", "fn0", "fn1", "bn0", "bn1", "ax0", "fx2", "ax1", "fx3",
    "bx2", "na", "bx3", "ax2", "nb", "an0", "ax3", "ps", "pr",
)
ORDER_E = (
    "copy", "r0", "va0", "va1", "r1", "vb0", "va2", "vb1", "va3", "vb2", "vb3", "ea0", "sa0", "ea1", "eb0",
    "sa1", "eb1", "ea2", "sb0", "ea3", "sb1", "nh0", "na0", "eb2", "sa2", "eb3", "nb0", "sa3", "sb2", "sb3",
    "ya0", "nh1", "na1", "ps0", "pr0", "ya1", "ya2", "nb1", "yf0", "yb0", "yf1", "yb1", "ya3", "ps1", "pr1",
    "yf2", "yb2", "yf3", "yb3", "xa0", "xa1", "xa2", "xa3", "za0", "za1", "za2", "za3", "n0", "share", "send",
)
ORDER_D = (
    "share", "nh0", "fx0", "bx0", "n01", "fx1", "bx1", "fn00", "fn01", "bn00", "bn01", "em0", "fx2", "bx2",
    "fx3", "bx3", "na0", "em1", "nb0", "n10", "n11", "dm0", "t0", "wait", "halo", "ea0", "fn10", "fn11",
    "bn10", "bn11", "ea1", "eb0", "eb1", "nh1", "na1", "dm1", "em2", "da0", "nb1", "da1", "dm2", "em3", "db0",
    "t1", "db1", "dm3", "oa0", "ea2", "oa1", "eb2", "ob0", "ea3", "ob1", "send0", "eb3", "da2", "da3", "db2",
    "db3", "oa2", "oa3", "ob2", "ob3", "send1",
)


def dot(a, b):
    return jnp.dot(a, b, preferred_element_type=F32)


def silu(pre):
    return pre * jax.nn.sigmoid(pre)


def norm(y):
    centred = y - jnp.mean(y, axis=LAST, keepdims=True)
    return centred * lax.rsqrt(jnp.mean(centred * centred, axis=LAST, keepdims=True) + 1e-5)


def ring_place(dev):
    high = lax.div(dev, 4)
    return high * (4 + lax.rem(dev + 2, 4)) + (1 - high) * dev


def chunks():
    return range(0, TILE, CH)


def tile_rows(t):
    return pl.ds(t * TILE, TILE)


def part_rows(t, c):
    return pl.ds(t * TILE + c, CH)


def chunk_runs(c):
    return range(c // HALF, (c + CH) // HALF)


def pieces(t):
    return ((8, 16),) if t == 0 else ((0, 8), (24, 8))


def get_tiles(ref, rows):
    return jnp.concatenate([ref[j, rows, :] for j in range(ref.shape[0])], axis=ONE)


def set_tiles(ref, rows, value):
    for j in range(ref.shape[0]):
        ref[j, rows, :] = value[:, LANES * j:LANES * j + LANES]


AT_FORCE, AT_STATIC, AT_NEXT, AT_M2G, AT_G2M = 88, 96, 104, 112, 120
PREV_AREA, CUR_AREA, NORM_AREA, MESH_AREA, OUT_AREA = range(5)


def columns(n):
    return pl.ds(LANES * n, LANES)


def stack(ref, n, rows):
    base = LANES * n
    end = 0
    for at_row, value in rows:
        first = at_row // 8 * 8
        last = (at_row + value.shape[0]) // 8 * 8
        if first > end:
            ref[pl.ds(base + end, first - end), :] = jnp.zeros((first - end, LANES), F32)
        if last < at_row + value.shape[0]:
            ref[pl.ds(base + last, 8), :] = jnp.zeros((8, LANES), F32)
            end = last + 8
        else:
            end = last
        ref[pl.ds(base + at_row, value.shape[0]), :] = value
    if end < LANES:
        ref[pl.ds(base + end, LANES - end), :] = jnp.zeros((LANES - end, LANES), F32)


def pack_kernel(x_prev, x_cur, forcing, static, g2m_feat, m2g_feat, mesh_feat, mesh_edge_feat, stats, w_out_final,
                g_home, m_home, x_home, w_final, area):
    def turned(slot, n):
        return jnp.transpose(area[slot, columns(n), :])

    blocks = range(x_cur.shape[1] // LANES)
    mesh_blocks = range(mesh_feat.shape[1] // LANES)
    weight_blocks = range(LAT // LANES)
    for n in mesh_blocks:
        stack(area.at[MESH_AREA], n, [(ZERO, mesh_feat[:, columns(n)])] + [
            (16 + 16 * k, mesh_edge_feat[k, :, columns(n)]) for k in range(6)])
    for n in weight_blocks:
        stack(area.at[OUT_AREA], n, [(ZERO, w_out_final[:, columns(n)].astype(F32))])
    for n in blocks:
        stack(area.at[PREV_AREA], n, [
            (ZERO, x_prev[:, columns(n)]), (AT_FORCE, forcing[:, ZERO, columns(n)]), (AT_STATIC, static[:, columns(n)]),
            (AT_NEXT, forcing[:, ONE, columns(n)]), (AT_M2G, m2g_feat[:, columns(n)]), (AT_G2M, g2m_feat[:, columns(n)])])
        stack(area.at[CUR_AREA], n, [(ZERO, x_cur[:, columns(n)])])
    for n in mesh_blocks:
        turned_rows = turned(MESH_AREA, n)
        for i in range(LANES // RUN):
            band, k = divmod(n * LANES + i * RUN, RING * RUN)
            for t in range(TILES):
                m_home[k // RUN, t, band] = jnp.concatenate(
                    [turned_rows[i * RUN + r:i * RUN + r + rows] for r, rows in pieces(t)], axis=ZERO).astype(BF16)
    for n in weight_blocks:
        w_final[columns(n), :] = turned(OUT_AREA, n).astype(BF16)
    rest = LANES - VARS
    wide_mean = jnp.concatenate([stats[ZERO:ONE, :], jnp.zeros((ONE, rest), F32)], axis=ONE)
    wide_std = jnp.concatenate([stats[ONE:PAIR, :], jnp.ones((ONE, rest), F32)], axis=ONE)
    for n in blocks:
        prev, cur = turned(PREV_AREA, n), turned(CUR_AREA, n)
        area[PREV_AREA, columns(n), :] = (prev - wide_mean) / wide_std
        area[CUR_AREA, columns(n), :] = cur
        area[NORM_AREA, columns(n), :] = (cur - wide_mean) / wide_std
    for band in range(PAIR):
        for k in range(RING):
            base = (band * RING + k) * GRID_RUN
            for p in range(PAIR):
                for t in range(TILES):
                    def rows_of(slot):
                        return jnp.concatenate([area[slot, pl.ds(base + PAIR * r + p, rows, stride=PAIR), :]
                                                for r, rows in pieces(t)], axis=ZERO)
                    g_home[k, p, t, band, :, pl.ds(ZERO, LANES)] = rows_of(PREV_AREA).astype(BF16)
                    g_home[k, p, t, band, :, pl.ds(LANES, LANES)] = rows_of(NORM_AREA).astype(BF16)
                    x_home[k, p, t, band] = rows_of(CUR_AREA)


def unpack_kernel(home0, home1, out0, out1, area):
    for home, out in ((home0, out0), (home1, out1)):
        for band in range(PAIR):
            for k in range(RING):
                for p in range(PAIR):
                    for t in range(TILES):
                        row = 0
                        for r, rows in pieces(t):
                            spot = pl.ds((band * RING + k) * GRID_RUN + PAIR * r + p, rows, stride=PAIR)
                            area[spot, :] = home[k, p, t, band, pl.ds(row, rows), :]
                            row += rows
        for n in range(out.shape[1] // LANES):
            out[:, columns(n)] = jnp.transpose(area[columns(n), :])[:VARS]


def kernel(g_home, m_home, x_home, stats, w_grid_in, w_mesh_in,
           w_eemb_in, w_embed_out, w_edge_in, w_edge_out, w_node_in, w_node_out, w_grid_self, w_out_hidden, w_out_final,
           out0, out1,
           wgrid_raw, wmesh_raw, weemb_raw,
           m_buf, x_buf, feat, we, weo, wself, woh, wof,
           enc_ei, enc_eo, enc_ni, enc_no, lay_ei, lay_eo, lay_ni, lay_no,
           edge_base, edge, h_mesh, h, hf, g2m, m2g, v, vc, proj0, proj1, recv, acc, hid, esum, dec, pre_buf,
           send_buf, halo_buf,
           raw_sem, in_send, in_recv, w_sem, enc_sem, lay_sem, halo_send, halo_recv, out_send, out_recv):
    me = lax.axis_index("gp")
    place = ring_place(me)

    def at(dev):
        return {"gp": dev}

    mesh_id = pl.DeviceIdType.MESH

    def block_copies(block, dst_refs, slot, sem):
        srcs = (w_edge_in, w_edge_out, w_node_in, w_node_out)
        return [pltpu.make_async_copy(src.at[block], dst.at[slot], sem.at[slot, i])
                for i, (src, dst) in enumerate(zip(srcs, dst_refs))]

    enc_refs = (enc_ei, enc_eo, enc_ni, enc_no)
    lay_refs = (lay_ei, lay_eo, lay_ni, lay_no)

    def enc_copies():
        return block_copies(0, enc_refs, 0, enc_sem)

    def slot_of(step, block):
        return lax.rem((BLOCKS - 1) * step + block - 1, SLOTS)

    def layer_copies(step, block):
        return block_copies(block, lay_refs, slot_of(step, block), lay_sem)

    class Weights:
        def __init__(self, refs, slot):
            self.edge = [refs[0].at[slot, pl.ds(i * LAT, LAT)] for i in range(3)]
            self.edge_out = refs[1].at[slot]
            self.node = [refs[2].at[slot, pl.ds(i * LAT, LAT)] for i in range(2)]
            self.node_out = refs[3].at[slot]

    def layer_weights(step, block):
        return Weights(lay_refs, slot_of(step, block))

    raw = [pltpu.make_async_copy(src, dst, raw_sem.at[i]) for i, (src, dst) in enumerate(
        ((w_grid_in, wgrid_raw), (w_mesh_in, wmesh_raw), (w_eemb_in, weemb_raw)))]
    for copy in raw:
        copy.start()
    small = [
        pltpu.make_async_copy(w_embed_out, weo, w_sem.at[0]),
        pltpu.make_async_copy(w_grid_self, wself, w_sem.at[1]),
        pltpu.make_async_copy(w_out_hidden, woh, w_sem.at[2]),
        pltpu.make_async_copy(w_out_final, wof, w_sem.at[3]),
    ]
    for copy in small + enc_copies() + layer_copies(0, 1) + layer_copies(0, 2):
        copy.start()

    barrier = pltpu.get_barrier_semaphore()
    for hop in range(1, RING):
        pl.semaphore_signal(barrier, inc=1, device_id=at(lax.rem(me + hop, RING)), device_id_type=mesh_id)

    mine = pl.ds(PAIR * me, PAIR)
    parts = ((m_home, m_buf.at[:, mine]), (g_home, feat.at[:, :, mine]), (x_home, x_buf.at[ZERO, :, :, mine]))

    def in_copy(part, hop):
        src, dst = parts[part]
        target = lax.rem(me + hop, RING)
        src = src.at[ring_place(target)]
        if hop == 0:
            return pltpu.make_async_copy(src, dst, in_recv.at[part, hop])
        return pltpu.make_async_remote_copy(src_ref=src, dst_ref=dst, send_sem=in_send.at[part, hop],
                                            recv_sem=in_recv.at[part, hop], device_id=at(target),
                                            device_id_type=mesh_id)

    in_copies = [[in_copy(part, hop) for hop in range(RING)] for part in range(3)]

    def wait_in(part):
        in_copies[part][0].wait()
        for copy in in_copies[part][1:]:
            copy.wait_recv()

    def start_in(part):
        for copy in in_copies[part]:
            copy.start()

    pl.semaphore_wait(barrier, RING - 1)
    start_in(0)
    start_in(1)

    for copy in raw:
        copy.wait()
    wide = wgrid_raw[...].astype(F32)
    recv[pl.ds(ZERO, wide.shape[0]), :] = wide
    prev_w, cur_w = recv[pl.ds(ZERO, VARS), :], recv[pl.ds(VARS, VARS), :]
    force_w, static_w = recv[pl.ds(2 * VARS, 5), :], recv[pl.ds(2 * VARS + 5, 5), :]
    spread = [[(0, wmesh_raw[...].astype(F32))], [(AT_G2M, weemb_raw[0].astype(F32))], [(AT_M2G, weemb_raw[1].astype(F32))]]
    spread += [[(16 + 16 * k, weemb_raw[2].astype(F32))] for k in range(6)]
    spread += [[(0, prev_w), (AT_FORCE, force_w), (AT_STATIC, static_w)], [(0, cur_w)]]
    spread += [[(0, cur_w), (AT_STATIC, static_w), (AT_NEXT, force_w)], [(0, prev_w)]]
    for i, rows in enumerate(spread):
        base = LANES * (i % 4)
        acc[pl.ds(base, LANES), :] = jnp.zeros((LANES, LAT), F32)
        for at_row, value in rows:
            acc[pl.ds(base + at_row, value.shape[0]), :] = value
        we[i] = acc[pl.ds(base, LANES), :].astype(BF16)

    def pipeline(items):
        depth = max(len(item) for item in items)
        for beat in range(len(items) + depth - 1):
            for stage in range(depth):
                index = beat - stage
                if 0 <= index < len(items) and stage < len(items[index]):
                    items[index][stage](index)

    def hide(slot, pre, extra=None):
        for c in chunks():
            value = pre[c:c + CH]
            if extra is not None:
                value = value + extra(c)
            hid[slot, pl.ds(c, CH), :] = silu(value).astype(BF16)

    def embed_item(load, w_first, second, store):
        def first(i):
            hide(i % PAIR, dot(load(), we[w_first]))

        def last(i):
            y = dot(hid[i % 2], weo[second])
            for c in chunks():
                store(c, norm(y[c:c + CH]).astype(BF16))

        return [first, last]

    wait_in(0)
    small[0].wait()
    def next_run(ref, *index):
        first = ref[(*index, pl.ds(ONE, RUNS - 1), slice(None), pl.ds(ZERO, LANES))]
        last = ref[(*index, pl.ds(ZERO, ONE), slice(None), pl.ds(ZERO, LANES))]
        return jnp.concatenate([first, last], axis=ZERO).reshape(TILE, LANES)

    mesh_rows = [next_run(m_buf, t) for t in range(TILES)]
    items = []
    for t in range(TILES):
        def store_mesh(c, value, t=t):
            h_mesh[part_rows(t, c), :] = value
        items.append(embed_item(lambda t=t: mesh_rows[t], 0, 1, store_mesh))
        for k in range(6):
            def store_edge(c, value, t=t, k=k):
                edge_base[k, part_rows(t, c), :] = value
            items.append(embed_item(lambda t=t: mesh_rows[t], 3 + k, 4, store_edge))
    pipeline(items)

    wait_in(1)
    start_in(PAIR)
    items = []
    for t in range(TILES):
        for p in range(PAIR):
            def store_m2g(c, value, t=t, p=p):
                m2g[p, part_rows(t, c), :] = value
            def store_g2m(c, value, t=t, p=p):
                g2m[p, part_rows(t, c), :] = value
            items.append(embed_item(lambda t=t, p=p: next_run(feat, p, t), 1, 2, store_g2m))
            items.append(embed_item(lambda t=t, p=p: feat[p, t, :, :, pl.ds(ZERO, LANES)].reshape(TILE, LANES), 2, 3, store_m2g))
    pipeline(items)
    for copy in small[1:] + enc_copies():
        copy.wait()

    left = ring_place(lax.rem(place + RING - 1, RING))
    right = ring_place(lax.rem(place + 1, RING))

    def halo_copies(slot):
        return [
            pltpu.make_async_remote_copy(src_ref=send_buf.at[side], dst_ref=halo_buf.at[slot, side],
                                         send_sem=halo_send.at[side], recv_sem=halo_recv.at[slot, side],
                                         device_id=at(target), device_id_type=mesh_id)
            for side, target in ((0, left), (1, right))
        ]

    def send_halo(slot):
        first = get_tiles(hf, pl.ds(ZERO, RUNS, stride=HALF))
        final = get_tiles(hf, pl.ds(HALF - 1, RUNS, stride=HALF))
        first_on = jnp.concatenate([first[1:], first[:1]], axis=ZERO)
        final_back = jnp.concatenate([final[-1:], final[:-1]], axis=ZERO)
        send_buf[0] = jnp.where(place == 0, first_on, first).astype(BF16)
        send_buf[1] = jnp.where(place == RING - 1, final_back, final).astype(BF16)
        for copy in halo_copies(slot):
            copy.start()

    def wait_halo(slot):
        for copy in halo_copies(slot):
            copy.wait()

    def project_halo(slot, w):
        rows = jnp.concatenate([halo_buf[slot, 0], halo_buf[slot, 1]], axis=ZERO)
        out = dot(rows, w.edge[1][...])
        set_tiles(proj1, pl.ds(8 + RUN, RUNS, stride=PAD1), out[:RUNS])
        set_tiles(proj1, pl.ds(7, RUNS, stride=PAD1), out[RUNS:])

    class Edge:
        def __init__(self, t, k, w, slot, run_shift=0, row_shift=0, source=None, first=False, final=False, keep=None):
            self.t, self.k, self.w, self.slot, self.keep = t, k, w, slot, keep
            self.run_shift, self.row_shift, self.first, self.final = run_shift, row_shift, first, final
            self.source = edge if source is None else source
            self.pre = None

        def a(self):
            self.pre = dot(self.source[self.k, tile_rows(self.t), :], self.w.edge[0][...])
            if self.keep is not None:
                for c in chunks():
                    pre_buf[self.keep, pl.ds(c, CH), :] = self.pre[c:c + CH]

        def resume(self):
            self.pre = pre_buf.at[self.keep]

        def extra(self, c):
            got = []
            for q in chunk_runs(c):
                base = (q + self.run_shift) % RUNS
                for r, n in pieces(self.t):
                    if self.t == 0:
                        got.append(get_tiles(proj0, pl.ds(base * PAD0 + r + self.row_shift, n)))
                    else:
                        got.append(get_tiles(proj1, pl.ds(base * PAD1 + 8 + r + self.row_shift, n)))
            return jnp.concatenate(got, axis=ZERO) + recv[part_rows(self.t, c), :]

        def fin(self):
            hide(self.slot, self.pre, self.extra)

        def b(self):
            y = dot(hid[self.slot], self.w.edge_out[...])
            for c in chunks():
                part = part_rows(self.t, c)
                value = (self.source[self.k, part, :].astype(F32) + norm(y[c:c + CH])).astype(BF16)
                edge[self.k, part, :] = value
                total = value.astype(F32)
                if not self.first:
                    total = total + acc[part, :]
                if self.final:
                    esum[part, :] = total.astype(BF16)
                else:
                    acc[part, :] = total

    class Node:
        def __init__(self, t, base, w):
            self.t, self.base, self.w, self.slot = t, base, w, 6 + t

        def own(self):
            self.pre = dot(self.base[tile_rows(self.t), :], self.w.node[0][...])

        def a(self):
            hide(self.slot, self.pre + dot(esum[tile_rows(self.t), :], self.w.node[1][...]))

        def b(self):
            y = dot(hid[self.slot], self.w.node_out[...])
            for c in chunks():
                part = part_rows(self.t, c)
                value = (self.base[part, :].astype(F32) + norm(y[c:c + CH])).astype(BF16)
                h[part, :] = value
                if self.t == 1:
                    set_tiles(hf, pl.ds(c, CH), value.astype(F32))

    def project_send(t, w):
        out = dot(h[tile_rows(t), :], w.edge[1][...])
        for q in range(RUNS):
            row = q * HALF
            for r, n in pieces(t):
                if t == 0:
                    set_tiles(proj0, pl.ds(q * PAD0 + r, n), out[row:row + n])
                else:
                    set_tiles(proj1, pl.ds(q * PAD1 + 8 + r, n), out[row:row + n])
                row += n
        if t == 1:
            for r in (7, 24):
                set_tiles(proj0, pl.ds(r, RUNS, stride=PAD0), get_tiles(proj1, pl.ds(8 + r, RUNS, stride=PAD1)))

    def project_recv(t, w):
        out = dot(h[tile_rows(t), :], w.edge[2][...])
        for c in chunks():
            recv[part_rows(t, c), :] = out[c:c + CH]

    def project(t, w):
        project_send(t, w)
        project_recv(t, w)

    def share_rows():
        for r in (8, 23):
            set_tiles(proj1, pl.ds(8 + r, RUNS, stride=PAD1), get_tiles(proj0, pl.ds(r, RUNS, stride=PAD0)))

    def far_items(t, w, source=None, resume=False):
        items = [Edge(t, k, w, n, run_shift=s, source=source, first=n == 0, keep=4 * t + n) for n, (k, s) in enumerate(FAR)]
        if resume:
            for item in items:
                item.resume()
        return items

    def near_items(t, w, resume=False):
        items = [Edge(t, k, w, 4 + n, row_shift=s, final=n == 1, keep=8 + t if n == 0 else None)
                 for n, (k, s) in enumerate(NEAR)]
        if resume:
            items[0].resume()
        return items

    def phase(order, x, n, node, next_x, next_n, before, w_next):
        table = {"before": before, "n1": n[1].a, "nh": node.own, "na": node.a, "nb": node.b, "an0": next_n[0].a,
                 "ps": lambda: project_send(node.t, w_next), "pr": lambda: project_recv(node.t, w_next)}
        for i in range(4):
            table[f"fx{i}"], table[f"bx{i}"], table[f"ax{i}"] = x[i].fin, x[i].b, next_x[i].a
        for i in range(PAIR):
            table[f"fn{i}"], table[f"bn{i}"] = n[i].fin, n[i].b
        run(order, table)

    def run(order, table):
        for name in order:
            table[name]()

    def encoder(step):
        w = Weights(enc_refs, ZERO)
        w1 = layer_weights(step, 1)
        w2 = layer_weights(step, 2)
        table = {"send": lambda: send_halo(ZERO), "share": share_rows}

        def spread():
            for k in range(6):
                for t in range(TILES):
                    if t == 1 or k < PAIR:
                        edge[k, tile_rows(t), :] = edge_base[k, tile_rows(t), :]

        table["copy"] = spread
        y, x, z, n = far_items(0, w1, edge_base), far_items(1, w1), far_items(0, w2), near_items(0, w1)
        for k in range(4):
            table[f"ya{k}"], table[f"yf{k}"], table[f"yb{k}"] = y[k].a, y[k].fin, y[k].b
            table[f"xa{k}"], table[f"za{k}"] = x[k].a, z[k].a
        table["n0"] = n[0].a
        for t in range(TILES):
            def back(t=t):
                out = dot(h_mesh[tile_rows(t), :], w.edge[2][...])
                for c in chunks():
                    recv[part_rows(t, c), :] = out[c:c + CH]

            node = Node(t, h_mesh, w)
            table[f"r{t}"], table[f"nh{t}"], table[f"na{t}"], table[f"nb{t}"] = back, node.own, node.a, node.b
            table[f"ps{t}"], table[f"pr{t}"] = functools.partial(project_send, t, w1), functools.partial(project_recv, t, w1)
            for p in range(PAIR):
                i = PAIR * t + p
                low, high = 8 + i, 12 + i

                def in_first(t=t, p=p, low=low):
                    hide(low, dot(feat[p, t].reshape(TILE, 2 * LANES), we[pl.ds(9 + PAIR * step, PAIR)].reshape(2 * LANES, LAT)))

                def in_last(t=t, p=p, low=low):
                    y = dot(hid[low], weo[ZERO])
                    for c in chunks():
                        v[p, part_rows(t, c), :] = norm(y[c:c + CH]).astype(BF16)

                def edge_first(t=t, p=p, high=high):
                    pre = dot(g2m[p, tile_rows(t), :], w.edge[0][...]) + dot(v[p, tile_rows(t), :], w.edge[1][...])
                    hide(high, pre, lambda c: recv[part_rows(t, c), :])

                def edge_last(t=t, p=p, high=high):
                    y = dot(hid[high], w.edge_out[...])
                    for c in chunks():
                        part = part_rows(t, c)
                        total = (g2m[p, part, :].astype(F32) + norm(y[c:c + CH])).astype(BF16).astype(F32)
                        if p == 0:
                            acc[part, :] = total
                        else:
                            esum[part, :] = (acc[part, :] + total).astype(BF16)

                def self_first(t=t, p=p, low=low):
                    hide(low, dot(v[p, tile_rows(t), :], wself[ZERO]))

                def self_last(t=t, p=p, low=low):
                    y = dot(hid[low], wself[ONE])
                    for c in chunks():
                        part = part_rows(t, c)
                        vc[p, part, :] = (v[p, part, :].astype(F32) + norm(y[c:c + CH])).astype(BF16)

                table[f"va{i}"], table[f"vb{i}"], table[f"ea{i}"], table[f"eb{i}"] = in_first, in_last, edge_first, edge_last
                table[f"sa{i}"], table[f"sb{i}"] = self_first, self_last
        run(ORDER_E, table)

    def out_copies(step, out, t):
        copies = []
        for hop in range(RING):
            target = lax.rem(me + hop, RING)
            src, dst = x_buf.at[step + 1, :, t, pl.ds(PAIR * target, PAIR)], out.at[place, :, t]
            if hop == 0:
                copies.append(pltpu.make_async_copy(src, dst, out_recv.at[step, t, hop]))
            else:
                copies.append(pltpu.make_async_remote_copy(
                    src_ref=src, dst_ref=dst, send_sem=out_send.at[step, t, hop], recv_sem=out_recv.at[step, t, hop],
                    device_id=at(target), device_id_type=mesh_id))
        return copies

    def decoder(step):
        w16 = layer_weights(step, LAYERS)
        w = layer_weights(step, BLOCKS - 1)
        in_mean = stats[ZERO:ONE, :]
        in_std = stats[ONE:PAIR, :]
        diff_mean, diff_std = (jnp.concatenate([stats[i:i + 1, :], jnp.zeros((ONE, LANES - VARS), F32)], axis=ONE) for i in (2, 3))
        halo_slot = lax.rem(LAYERS + 1, 2)
        table = {"share": share_rows, "wait": lambda: wait_halo(halo_slot), "halo": lambda: project_halo(halo_slot, w16)}
        x = far_items(1, w16, resume=True)
        for k in range(4):
            table[f"fx{k}"], table[f"bx{k}"] = x[k].fin, x[k].b
        for t in range(TILES):
            node = Node(t, h, w16)
            table[f"nh{t}"], table[f"na{t}"], table[f"nb{t}"] = node.own, node.a, node.b
            near = near_items(t, w16, resume=t == 0)
            for k in range(PAIR):
                table[f"n{t}{k}"], table[f"fn{t}{k}"], table[f"bn{t}{k}"] = near[k].a, near[k].fin, near[k].b

            def back(t=t):
                out = dot(h[tile_rows(t), :], w.edge[1][...])
                for c in chunks():
                    recv[part_rows(t, c), :] = out[c:c + CH]

            def send(t=t):
                for which, out in enumerate((out0, out1)):
                    @pl.when(step == which)
                    def _():
                        start_all(out_copies(which, out, t))

            table[f"t{t}"], table[f"send{t}"] = back, send
            for p in range(PAIR):
                i = PAIR * t + p
                low, high = 8 + i, 12 + i
                held = {}

                def edge_own(t=t, p=p, held=held):
                    held["edge"] = dot(m2g[p, tile_rows(t), :], w.edge[0][...]) + dot(vc[p, tile_rows(t), :], w.edge[2][...])

                def edge_first(t=t, low=low, held=held):
                    hide(low, held["edge"], lambda c: recv[part_rows(t, c), :])

                def edge_last(t=t, p=p, low=low, i=i):
                    y = dot(hid[low], w.edge_out[...])
                    for c in chunks():
                        part = part_rows(t, c)
                        dec[i, pl.ds(c, CH), :] = (m2g[p, part, :].astype(F32) + norm(y[c:c + CH])).astype(BF16)

                def node_own(t=t, p=p, held=held):
                    held["node"] = dot(vc[p, tile_rows(t), :], w.node[0][...])

                def node_first(high=high, i=i, held=held):
                    hide(high, held["node"] + dot(dec[i], w.node[1][...]))

                def node_last(t=t, p=p, high=high):
                    y = dot(hid[high], w.node_out[...])
                    for c in chunks():
                        part = part_rows(t, c)
                        v[p, part, :] = (vc[p, part, :].astype(F32) + norm(y[c:c + CH])).astype(BF16)

                def out_first(t=t, p=p, low=low):
                    hide(low, dot(v[p, tile_rows(t), :], woh[...]))

                def out_last(t=t, p=p, low=low):
                    pred = dot(hid[low], wof[...])
                    for c in chunks():
                        runs = pl.ds(c // HALF, CH // HALF)
                        now = x_buf[step, p, t, runs].reshape(CH, LANES)
                        new = now + diff_std * pred[c:c + CH] + diff_mean
                        x_buf[step + 1, p, t, runs] = new.reshape(CH // HALF, HALF, LANES)
                        scaled = ((new[:, :VARS] - in_mean) / in_std).astype(BF16)
                        feat[p, t, runs, :, pl.ds(ZERO, VARS)] = scaled.reshape(CH // HALF, HALF, VARS)

                table[f"em{i}"], table[f"ea{i}"], table[f"eb{i}"] = edge_own, edge_first, edge_last
                table[f"dm{i}"], table[f"da{i}"], table[f"db{i}"] = node_own, node_first, node_last
                table[f"oa{i}"], table[f"ob{i}"] = out_first, out_last
        run(ORDER_D, table)

    def wait_all(copies):
        for copy in copies:
            copy.wait()

    def start_all(copies):
        for copy in copies:
            copy.start()

    def one_step(step, carry):
        wait_all(layer_copies(step, 1) + layer_copies(step, 2))
        start_all(layer_copies(step, 3))
        encoder(step)

        def one_layer(block, carry):
            halo_slot = lax.rem(block + 1, 2)
            wait_all(layer_copies(step, block + 2))

            @pl.when(block < LAYERS - 1)
            def _():
                start_all(layer_copies(step, block + 3))

            w, w1, w2 = (layer_weights(step, block + i) for i in range(3))
            phase(ORDER_A, far_items(1, w, resume=True), near_items(0, w, resume=True), Node(0, h, w), far_items(1, w1),
                  near_items(1, w), share_rows, w1)
            wait_halo(halo_slot)
            phase(ORDER_B, far_items(0, w1, resume=True), near_items(1, w, resume=True), Node(1, h, w), far_items(0, w2),
                  near_items(0, w1), lambda: project_halo(halo_slot, w), w1)
            send_halo(1 - halo_slot)
            return carry

        lax.fori_loop(1, LAYERS, one_layer, 0)
        @pl.when(step == 0)
        def _():
            start_all(layer_copies(1, 1) + layer_copies(1, 2))
            wait_in(PAIR)

        decoder(step)
        return carry

    lax.fori_loop(0, 2, one_step, 0)
    for part in range(3):
        for copy in in_copies[part][1:]:
            copy.wait_send()
    for t in range(TILES):
        wait_all(out_copies(0, out0, t) + out_copies(1, out1, t))


def solution(mesh):
    row_spec = P(("dp", "gp"))
    edge_spec = P(("dp", "gp"), None, None)
    whole = P()

    def local_run(x_prev, x_cur, forcing, grid_static, g2m_feat, m2g_feat, mesh_feat, mesh_edge_feat, norm_stats,
                  w_grid_in, w_mesh_in, w_eemb_in, w_embed_out, w_edge_in, w_edge_out, w_node_in, w_node_out,
                  w_grid_self, w_out_hidden, w_out_final):
        any_spec = pl.BlockSpec(memory_space=pl.ANY)
        vmem_spec = pl.BlockSpec(memory_space=pltpu.VMEM)
        dma = pltpu.SemaphoreType.DMA
        grid_dev = x_prev.shape[0]
        shape = jax.ShapeDtypeStruct
        home = shape((RING, PAIR, TILES, PAIR, HALF, LANES), F32)
        g_home, m_home, x_home, w_final = pl.pallas_call(
            pack_kernel,
            out_shape=(shape((*home.shape[:-1], 2 * LANES), BF16), shape((RING, TILES, PAIR, HALF, LANES), BF16), home,
                       shape((LAT, LANES), BF16)),
            in_specs=[vmem_spec] * 10,
            out_specs=(vmem_spec,) * 4,
            scratch_shapes=[pltpu.VMEM((5, grid_dev, LANES), F32)],
            name="pack",
        )(x_prev.T, x_cur.T, forcing.T, grid_static.T, g2m_feat.T, m2g_feat.T, mesh_feat.T,
          jnp.transpose(mesh_edge_feat, (1, 2, 0)), norm_stats, w_out_final.T)
        scratch = [
            pltpu.VMEM((2 * VARS + 10, LAT), BF16),
            pltpu.VMEM((3, LAT), BF16),
            pltpu.VMEM((3, 4, LAT), BF16),
            pltpu.VMEM((TILES, RUNS, HALF, LANES), BF16),
            pltpu.VMEM((3, PAIR, TILES, RUNS, HALF, LANES), F32),
            pltpu.VMEM((PAIR, TILES, RUNS, HALF, 2 * LANES), BF16),
            pltpu.VMEM((13, LANES, LAT), BF16),
            pltpu.VMEM((5, LAT, LAT), BF16),
            pltpu.VMEM((PAIR, LAT, LAT), BF16),
            pltpu.VMEM((LAT, LAT), BF16),
            pltpu.VMEM((LAT, LANES), BF16),
            pltpu.VMEM((1, 3 * LAT, LAT), BF16),
            pltpu.VMEM((1, LAT, LAT), BF16),
            pltpu.VMEM((1, 2 * LAT, LAT), BF16),
            pltpu.VMEM((1, LAT, LAT), BF16),
            pltpu.VMEM((SLOTS, 3 * LAT, LAT), BF16),
            pltpu.VMEM((SLOTS, LAT, LAT), BF16),
            pltpu.VMEM((SLOTS, 2 * LAT, LAT), BF16),
            pltpu.VMEM((SLOTS, LAT, LAT), BF16),
            pltpu.VMEM((6, ROWS, LAT), BF16),
            pltpu.VMEM((6, ROWS, LAT), BF16),
            pltpu.VMEM((ROWS, LAT), BF16),
            pltpu.VMEM((ROWS, LAT), BF16),
            pltpu.VMEM((LAT // LANES, TILE, LANES), F32),
            pltpu.VMEM((PAIR, ROWS, LAT), BF16),
            pltpu.VMEM((PAIR, ROWS, LAT), BF16),
            pltpu.VMEM((PAIR, ROWS, LAT), BF16),
            pltpu.VMEM((PAIR, ROWS, LAT), BF16),
            pltpu.VMEM((LAT // LANES, RUNS * PAD0, LANES), F32),
            pltpu.VMEM((LAT // LANES, RUNS * PAD1, LANES), F32),
            pltpu.VMEM((ROWS, LAT), F32),
            pltpu.VMEM((ROWS, LAT), F32),
            pltpu.VMEM((16, TILE, LAT), BF16),
            pltpu.VMEM((ROWS, LAT), BF16),
            pltpu.VMEM((4, TILE, LAT), BF16),
            pltpu.VMEM((10, TILE, LAT), F32),
            pltpu.VMEM((PAIR, RUNS, LAT), BF16),
            pltpu.VMEM((PAIR, 2, RUNS, LAT), BF16),
            dma((3,)), dma((3, RING)), dma((3, RING)), dma((4,)), dma((1, 4)), dma((SLOTS, 4)), dma((PAIR,)), dma((PAIR, PAIR)),
            dma((PAIR, TILES, RING)), dma((PAIR, TILES, RING)),
        ]
        home0, home1 = pl.pallas_call(
            kernel,
            out_shape=(home, home),
            in_specs=[any_spec] * 3 + [vmem_spec] + [any_spec] * 11,
            out_specs=(any_spec, any_spec),
            scratch_shapes=scratch,
            compiler_params=pltpu.CompilerParams(collective_id=0, has_side_effects=True, vmem_limit_bytes=63 << 20),
            name="forecast",
        )(g_home, m_home, x_home, norm_stats, w_grid_in, w_mesh_in, w_eemb_in, w_embed_out, w_edge_in, w_edge_out, w_node_in,
          w_node_out, w_grid_self, w_out_hidden, w_final)
        out = shape((VARS, grid_dev), F32)
        next_state, after_state = pl.pallas_call(
            unpack_kernel, out_shape=(out, out), in_specs=[vmem_spec] * 2, out_specs=(vmem_spec,) * 2,
            scratch_shapes=[pltpu.VMEM((grid_dev, LANES), F32)], name="unpack",
        )(home0, home1)
        return next_state.T, after_state.T

    in_specs = (row_spec, row_spec, edge_spec, row_spec, row_spec, row_spec, row_spec, edge_spec, whole) + (whole,) * 11
    return jax.shard_map(local_run, mesh=mesh, in_specs=in_specs, out_specs=(row_spec, row_spec), check_vma=False)
```

```python
import functools

import jax
import jax.numpy as jnp
from jax import lax
from jax.experimental import pallas as pl
from jax.experimental.pallas import tpu as pltpu
from jax.sharding import PartitionSpec as P

F32 = jnp.float32
BF16 = jnp.bfloat16

RUNS = 16
RUN = 32
GRID_RUN = 2 * RUN
ROWS = RUNS * RUN
ZERO, ONE, LAST = 0, 1, -1
LAT = 512
LANES = 128
PAIR = 2
VARS = 84
PAD0 = 32
PAD1 = 48
TILE = 256
TILES = 2
HALF = TILE // RUNS
CH = 128
RING = 8
LAYERS = 16
BLOCKS = LAYERS + 2
SLOTS = 4
FAR = ((2, 1), (3, -1), (4, 4), (5, -4))
NEAR = ((0, 1), (1, -1))
ORDER_A = (
    "nh", "before", "fx0", "bx0", "n1", "fx1", "bx1", "fn0", "fn1", "bn0", "bn1", "ax0", "fx2", "ax1", "fx3",
    "bx2", "na", "bx3", "ax2", "nb", "an0", "ax3", "ps", "pr",
)
ORDER_B = (
    "nh", "before", "fx0", "bx0", "n1", "fx1", "bx1", "fn0", "fn1", "bn0", "bn1", "ax0", "fx2", "ax1", "fx3",
    "bx2", "na", "bx3", "ax2", "nb", "an0", "ax3", "ps", "pr",
)
ORDER_E = (
    "copy", "r0", "va0", "va1", "vb0", "va2", "vb1", "va3", "r1", "vb2", "vb3", "ea0", "sa0", "ea3", "ea1",
    "eb0", "sa1", "eb1", "sb0", "ea2", "sb1", "nh0", "na0", "eb2", "sa2", "eb3", "nb0", "sa3", "sb2", "sb3",
    "ya2", "ya0", "nh1", "ya1", "na1", "ps0", "pr0", "nb1", "yf0", "yb0", "yf1", "yb1", "ps1", "ya3", "pr1",
    "yf2", "yb2", "yf3", "yb3", "xa0", "xa1", "za1", "xa2", "xa3", "za0", "za2", "za3", "n0", "share", "send",
)
ORDER_D = (
    "fx0", "share", "nh0", "fx1", "bx0", "n01", "fn00", "fn01", "bn00", "bn01", "bx1", "em0", "fx2", "bx2",
    "fx3", "bx3", "na0", "em1", "nb0", "n11", "dm0", "wait", "n10", "t0", "halo", "ea0", "fn11", "fn10",
    "bn10", "bn11", "ea1", "eb0", "eb1", "nh1", "na1", "em2", "da0", "dm1", "nb1", "da1", "dm2", "em3", "db0",
    "t1", "db1", "oa0", "ea2", "eb2", "oa1", "ob0", "ea3", "ob1", "send0", "eb3", "da2", "dm3", "da3", "db2",
    "db3", "oa2", "oa3", "ob2", "ob3", "send1",
)


def dot(a, b):
    return jnp.dot(a, b, preferred_element_type=F32)


def silu(pre):
    return pre * jax.nn.sigmoid(pre)


def norm(y):
    centred = y - jnp.mean(y, axis=LAST, keepdims=True)
    return centred * lax.rsqrt(jnp.mean(centred * centred, axis=LAST, keepdims=True) + 1e-5)


def ring_place(dev):
    high = lax.div(dev, 4)
    return high * (4 + lax.rem(dev + 2, 4)) + (1 - high) * dev


def chunks():
    return range(0, TILE, CH)


def tile_rows(t):
    return pl.ds(t * TILE, TILE)


def part_rows(t, c):
    return pl.ds(t * TILE + c, CH)


def chunk_runs(c):
    return range(c // HALF, (c + CH) // HALF)


def pieces(t):
    return ((8, 16),) if t == 0 else ((0, 8), (24, 8))


def get_tiles(ref, rows):
    return jnp.concatenate([ref[j, rows, :] for j in range(ref.shape[0])], axis=ONE)


def set_tiles(ref, rows, value):
    for j in range(ref.shape[0]):
        ref[j, rows, :] = value[:, LANES * j:LANES * j + LANES]


AT_FORCE, AT_STATIC, AT_NEXT, AT_M2G, AT_G2M = 88, 96, 104, 112, 120


def columns(n):
    return pl.ds(LANES * n, LANES)


def stack(ref, rows):
    end = 0
    for at_row, value in rows:
        first = at_row // 8 * 8
        last = (at_row + value.shape[0]) // 8 * 8
        if first > end:
            ref[pl.ds(end, first - end), :] = jnp.zeros((first - end, LANES), F32)
        if last < at_row + value.shape[0]:
            ref[pl.ds(last, 8), :] = jnp.zeros((8, LANES), F32)
            end = last + 8
        else:
            end = last
        ref[pl.ds(at_row, value.shape[0]), :] = value
    if end < LANES:
        ref[pl.ds(end, LANES - end), :] = jnp.zeros((LANES - end, LANES), F32)


def unpack_kernel(home0, home1, out0, out1, area):
    for home, out in ((home0, out0), (home1, out1)):
        for band in range(PAIR):
            for k in range(RING):
                for p in range(PAIR):
                    for t in range(TILES):
                        row = 0
                        for r, rows in pieces(t):
                            spot = pl.ds((band * RING + k) * GRID_RUN + PAIR * r + p, rows, stride=PAIR)
                            area[spot, :] = home[k, p, t, band, pl.ds(row, rows), :]
                            row += rows
        for n in range(out.shape[1] // LANES):
            out[:, columns(n)] = jnp.transpose(area[columns(n), :])[:VARS]


def kernel(x_prev, x_cur, forcing, static, g2m_feat, m2g_feat, mesh_feat, mesh_edge_feat, stats, w_grid_in, w_mesh_in,
           w_eemb_in, w_embed_out, w_edge_in, w_edge_out, w_node_in, w_node_out, w_grid_self, w_out_hidden, w_out_final,
           out0, out1,
           mesh_raw, medge_raw, prev_raw, cur_raw, force_raw, static_raw, g2m_raw, m2g_raw,
           wgrid_raw, wmesh_raw, weemb_raw, wfin_raw, g_home, m_home, x_home,
           m_buf, x_buf, feat, we, weo, wself, woh, wof,
           enc_ei, enc_eo, enc_ni, enc_no, lay_ei, lay_eo, lay_ni, lay_no,
           edge_base, edge, h_mesh, h, hf, g2m, m2g, v, vc, proj0, proj1, recv, acc, hid, esum, dec, pre_buf,
           send_buf, halo_buf,
           raw_sem, in_send, in_recv, w_sem, enc_sem, lay_sem, halo_send, halo_recv, out_send, out_recv):
    me = lax.axis_index("gp")
    place = ring_place(me)

    def at(dev):
        return {"gp": dev}

    mesh_id = pl.DeviceIdType.MESH

    def block_copies(block, dst_refs, slot, sem):
        srcs = (w_edge_in, w_edge_out, w_node_in, w_node_out)
        return [pltpu.make_async_copy(src.at[block], dst.at[slot], sem.at[slot, i])
                for i, (src, dst) in enumerate(zip(srcs, dst_refs))]

    enc_refs = (enc_ei, enc_eo, enc_ni, enc_no)
    lay_refs = (lay_ei, lay_eo, lay_ni, lay_no)

    def enc_copies():
        return block_copies(0, enc_refs, 0, enc_sem)

    def slot_of(step, block):
        return lax.rem((BLOCKS - 1) * step + block - 1, SLOTS)

    def layer_copies(step, block):
        return block_copies(block, lay_refs, slot_of(step, block), lay_sem)

    class Weights:
        def __init__(self, refs, slot):
            self.edge = [refs[0].at[slot, pl.ds(i * LAT, LAT)] for i in range(3)]
            self.edge_out = refs[1].at[slot]
            self.node = [refs[2].at[slot, pl.ds(i * LAT, LAT)] for i in range(2)]
            self.node_out = refs[3].at[slot]

    def layer_weights(step, block):
        return Weights(lay_refs, slot_of(step, block))

    raw = [pltpu.make_async_copy(src, dst, raw_sem.at[i]) for i, (src, dst) in enumerate(
        ((mesh_feat, mesh_raw), (mesh_edge_feat, medge_raw), (x_prev, prev_raw), (x_cur, cur_raw), (forcing, force_raw),
         (static, static_raw), (g2m_feat, g2m_raw), (m2g_feat, m2g_raw),
         (w_grid_in, wgrid_raw), (w_mesh_in, wmesh_raw), (w_eemb_in, weemb_raw), (w_out_final, wfin_raw)))]
    for copy in raw:
        copy.start()
    small = [
        pltpu.make_async_copy(w_embed_out, weo, w_sem.at[0]),
        pltpu.make_async_copy(w_grid_self, wself, w_sem.at[1]),
        pltpu.make_async_copy(w_out_hidden, woh, w_sem.at[2]),
    ]
    small[0].start()

    barrier = pltpu.get_barrier_semaphore()
    for hop in range(1, RING):
        pl.semaphore_signal(barrier, inc=1, device_id=at(lax.rem(me + hop, RING)), device_id_type=mesh_id)

    mine = pl.ds(PAIR * me, PAIR)
    parts = ((m_home, m_buf.at[:, mine]), (g_home, feat.at[:, :, mine]), (x_home, x_buf.at[ZERO, :, :, mine]))

    def in_copy(part, hop):
        src, dst = parts[part]
        target = lax.rem(me + hop, RING)
        src = src.at[ring_place(target)]
        if hop == 0:
            return pltpu.make_async_copy(src, dst, in_recv.at[part, hop])
        return pltpu.make_async_remote_copy(src_ref=src, dst_ref=dst, send_sem=in_send.at[part, hop],
                                            recv_sem=in_recv.at[part, hop], device_id=at(target),
                                            device_id_type=mesh_id)

    in_copies = [[in_copy(part, hop) for hop in range(RING)] for part in range(3)]

    def wait_in(part):
        in_copies[part][0].wait()
        for copy in in_copies[part][1:]:
            copy.wait_recv()

    def start_in(part):
        for copy in in_copies[part]:
            copy.start()

    def place_of(area, n):
        ref, first = area
        return ref.at[first + n // 4, columns(n % 4)]

    prev_area, cur_area, norm_area, mesh_area, final_area = (proj0, 0), (proj0, PAIR), (proj1, 0), (proj1, 2), (proj1, 3)

    def turned(area, n):
        return jnp.transpose(place_of(area, n)[...])

    for copy in raw[:2]:
        copy.wait()
    for n in range(mesh_raw.shape[1] // LANES):
        stack(place_of(mesh_area, n), [(ZERO, mesh_raw[:, columns(n)])] + [
            (16 + 16 * k, medge_raw[k, :, columns(n)]) for k in range(6)])
    for n in range(mesh_raw.shape[1] // LANES):
        turned_rows = turned(mesh_area, n)
        for i in range(LANES // RUN):
            band, k = divmod(n * LANES + i * RUN, RING * RUN)
            for t in range(TILES):
                m_home[k // RUN, t, band] = jnp.concatenate(
                    [turned_rows[i * RUN + r:i * RUN + r + rows] for r, rows in pieces(t)], axis=ZERO).astype(BF16)
    pl.semaphore_wait(barrier, RING - 1)
    start_in(0)
    for copy in raw[2:8]:
        copy.wait()
    blocks = range(cur_raw.shape[1] // LANES)
    for n in blocks:
        stack(place_of(prev_area, n), [
            (ZERO, prev_raw[:, columns(n)]), (AT_FORCE, force_raw[:, ZERO, columns(n)]), (AT_STATIC, static_raw[:, columns(n)]),
            (AT_NEXT, force_raw[:, ONE, columns(n)]), (AT_M2G, m2g_raw[:, columns(n)]), (AT_G2M, g2m_raw[:, columns(n)])])
        stack(place_of(cur_area, n), [(ZERO, cur_raw[:, columns(n)])])
    rest = LANES - VARS
    wide_mean = jnp.concatenate([stats[ZERO:ONE, :], jnp.zeros((ONE, rest), F32)], axis=ONE)
    wide_std = jnp.concatenate([stats[ONE:PAIR, :], jnp.ones((ONE, rest), F32)], axis=ONE)
    for n in blocks:
        prev, cur = turned(prev_area, n), turned(cur_area, n)
        place_of(prev_area, n)[...] = (prev - wide_mean) / wide_std
        place_of(cur_area, n)[...] = cur
        place_of(norm_area, n)[...] = (cur - wide_mean) / wide_std
    for k in range(RING):
        for p in range(PAIR):
            for t in range(TILES):
                for band in range(PAIR):
                    def rows_of(area):
                        ref, first = area
                        return jnp.concatenate([ref[first + band, pl.ds(k * GRID_RUN + PAIR * r + p, rows, stride=PAIR), :]
                                                for r, rows in pieces(t)], axis=ZERO)
                    g_home[k, p, t, band, :, pl.ds(ZERO, LANES)] = rows_of(prev_area).astype(BF16)
                    g_home[k, p, t, band, :, pl.ds(LANES, LANES)] = rows_of(norm_area).astype(BF16)
                    x_home[k, p, t, band] = rows_of(cur_area)
    start_in(1)
    for copy in small[1:] + enc_copies() + layer_copies(0, 1) + layer_copies(0, 2):
        copy.start()

    for copy in raw[8:]:
        copy.wait()
    for n in range(LAT // LANES):
        stack(place_of(final_area, n), [(ZERO, wfin_raw[:, columns(n)].astype(F32))])
        wof[columns(n), :] = turned(final_area, n).astype(BF16)
    wide = wgrid_raw[...].astype(F32)
    recv[pl.ds(ZERO, wide.shape[0]), :] = wide
    prev_w, cur_w = recv[pl.ds(ZERO, VARS), :], recv[pl.ds(VARS, VARS), :]
    force_w, static_w = recv[pl.ds(2 * VARS, 5), :], recv[pl.ds(2 * VARS + 5, 5), :]
    spread = [[(0, wmesh_raw[...].astype(F32))], [(AT_G2M, weemb_raw[0].astype(F32))], [(AT_M2G, weemb_raw[1].astype(F32))]]
    spread += [[(16 + 16 * k, weemb_raw[2].astype(F32))] for k in range(6)]
    spread += [[(0, prev_w), (AT_FORCE, force_w), (AT_STATIC, static_w)], [(0, cur_w)]]
    spread += [[(0, cur_w), (AT_STATIC, static_w), (AT_NEXT, force_w)], [(0, prev_w)]]
    for i, rows in enumerate(spread):
        base = LANES * (i % 4)
        acc[pl.ds(base, LANES), :] = jnp.zeros((LANES, LAT), F32)
        for at_row, value in rows:
            acc[pl.ds(base + at_row, value.shape[0]), :] = value
        we[i] = acc[pl.ds(base, LANES), :].astype(BF16)

    def pipeline(items):
        depth = max(len(item) for item in items)
        for beat in range(len(items) + depth - 1):
            for stage in range(depth):
                index = beat - stage
                if 0 <= index < len(items) and stage < len(items[index]):
                    items[index][stage](index)

    def hide(slot, pre, extra=None):
        for c in chunks():
            value = pre[c:c + CH]
            if extra is not None:
                value = value + extra(c)
            hid[slot, pl.ds(c, CH), :] = silu(value).astype(BF16)

    def embed_item(load, w_first, second, store):
        def first(i):
            hide(i % PAIR, dot(load(), we[w_first]))

        def last(i):
            y = dot(hid[i % 2], weo[second])
            for c in chunks():
                store(c, norm(y[c:c + CH]).astype(BF16))

        return [first, last]

    wait_in(0)
    small[0].wait()
    def next_run(ref, *index):
        first = ref[(*index, pl.ds(ONE, RUNS - 1), slice(None), pl.ds(ZERO, LANES))]
        last = ref[(*index, pl.ds(ZERO, ONE), slice(None), pl.ds(ZERO, LANES))]
        return jnp.concatenate([first, last], axis=ZERO).reshape(TILE, LANES)

    mesh_rows = [next_run(m_buf, t) for t in range(TILES)]
    items = []
    for t in range(TILES):
        def store_mesh(c, value, t=t):
            h_mesh[part_rows(t, c), :] = value
        items.append(embed_item(lambda t=t: mesh_rows[t], 0, 1, store_mesh))
        for k in range(6):
            def store_edge(c, value, t=t, k=k):
                edge_base[k, part_rows(t, c), :] = value
            items.append(embed_item(lambda t=t: mesh_rows[t], 3 + k, 4, store_edge))
    pipeline(items)

    wait_in(1)
    start_in(PAIR)
    items = []
    for t in range(TILES):
        for p in range(PAIR):
            def store_m2g(c, value, t=t, p=p):
                m2g[p, part_rows(t, c), :] = value
            def store_g2m(c, value, t=t, p=p):
                g2m[p, part_rows(t, c), :] = value
            items.append(embed_item(lambda t=t, p=p: next_run(feat, p, t), 1, 2, store_g2m))
            items.append(embed_item(lambda t=t, p=p: feat[p, t, :, :, pl.ds(ZERO, LANES)].reshape(TILE, LANES), 2, 3, store_m2g))
    pipeline(items)
    for copy in small[1:] + enc_copies():
        copy.wait()

    left = ring_place(lax.rem(place + RING - 1, RING))
    right = ring_place(lax.rem(place + 1, RING))

    def halo_copies(slot):
        return [
            pltpu.make_async_remote_copy(src_ref=send_buf.at[side], dst_ref=halo_buf.at[slot, side],
                                         send_sem=halo_send.at[side], recv_sem=halo_recv.at[slot, side],
                                         device_id=at(target), device_id_type=mesh_id)
            for side, target in ((0, left), (1, right))
        ]

    def send_halo(slot):
        first = get_tiles(hf, pl.ds(ZERO, RUNS, stride=HALF))
        final = get_tiles(hf, pl.ds(HALF - 1, RUNS, stride=HALF))
        first_on = jnp.concatenate([first[1:], first[:1]], axis=ZERO)
        final_back = jnp.concatenate([final[-1:], final[:-1]], axis=ZERO)
        send_buf[0] = jnp.where(place == 0, first_on, first).astype(BF16)
        send_buf[1] = jnp.where(place == RING - 1, final_back, final).astype(BF16)
        for copy in halo_copies(slot):
            copy.start()

    def wait_halo(slot):
        for copy in halo_copies(slot):
            copy.wait()

    def project_halo(slot, w):
        rows = jnp.concatenate([halo_buf[slot, 0], halo_buf[slot, 1]], axis=ZERO)
        out = dot(rows, w.edge[1][...])
        set_tiles(proj1, pl.ds(8 + RUN, RUNS, stride=PAD1), out[:RUNS])
        set_tiles(proj1, pl.ds(7, RUNS, stride=PAD1), out[RUNS:])

    class Edge:
        def __init__(self, t, k, w, slot, run_shift=0, row_shift=0, source=None, first=False, final=False, keep=None):
            self.t, self.k, self.w, self.slot, self.keep = t, k, w, slot, keep
            self.run_shift, self.row_shift, self.first, self.final = run_shift, row_shift, first, final
            self.source = edge if source is None else source
            self.pre = None

        def a(self):
            self.pre = dot(self.source[self.k, tile_rows(self.t), :], self.w.edge[0][...])
            if self.keep is not None:
                for c in chunks():
                    pre_buf[self.keep, pl.ds(c, CH), :] = self.pre[c:c + CH]

        def resume(self):
            self.pre = pre_buf.at[self.keep]

        def extra(self, c):
            got = []
            for q in chunk_runs(c):
                base = (q + self.run_shift) % RUNS
                for r, n in pieces(self.t):
                    if self.t == 0:
                        got.append(get_tiles(proj0, pl.ds(base * PAD0 + r + self.row_shift, n)))
                    else:
                        got.append(get_tiles(proj1, pl.ds(base * PAD1 + 8 + r + self.row_shift, n)))
            return jnp.concatenate(got, axis=ZERO) + recv[part_rows(self.t, c), :]

        def fin(self):
            hide(self.slot, self.pre, self.extra)

        def b(self):
            y = dot(hid[self.slot], self.w.edge_out[...])
            for c in chunks():
                part = part_rows(self.t, c)
                value = (self.source[self.k, part, :].astype(F32) + norm(y[c:c + CH])).astype(BF16)
                edge[self.k, part, :] = value
                total = value.astype(F32)
                if not self.first:
                    total = total + acc[part, :]
                if self.final:
                    esum[part, :] = total.astype(BF16)
                else:
                    acc[part, :] = total

    class Node:
        def __init__(self, t, base, w):
            self.t, self.base, self.w, self.slot = t, base, w, 6 + t

        def own(self):
            self.pre = dot(self.base[tile_rows(self.t), :], self.w.node[0][...])

        def a(self):
            hide(self.slot, self.pre + dot(esum[tile_rows(self.t), :], self.w.node[1][...]))

        def b(self):
            y = dot(hid[self.slot], self.w.node_out[...])
            for c in chunks():
                part = part_rows(self.t, c)
                value = (self.base[part, :].astype(F32) + norm(y[c:c + CH])).astype(BF16)
                h[part, :] = value
                if self.t == 1:
                    set_tiles(hf, pl.ds(c, CH), value.astype(F32))

    def project_send(t, w):
        out = dot(h[tile_rows(t), :], w.edge[1][...])
        for q in range(RUNS):
            row = q * HALF
            for r, n in pieces(t):
                if t == 0:
                    set_tiles(proj0, pl.ds(q * PAD0 + r, n), out[row:row + n])
                else:
                    set_tiles(proj1, pl.ds(q * PAD1 + 8 + r, n), out[row:row + n])
                row += n
        if t == 1:
            for r in (7, 24):
                set_tiles(proj0, pl.ds(r, RUNS, stride=PAD0), get_tiles(proj1, pl.ds(8 + r, RUNS, stride=PAD1)))

    def project_recv(t, w):
        out = dot(h[tile_rows(t), :], w.edge[2][...])
        for c in chunks():
            recv[part_rows(t, c), :] = out[c:c + CH]

    def project(t, w):
        project_send(t, w)
        project_recv(t, w)

    def share_rows():
        for r in (8, 23):
            set_tiles(proj1, pl.ds(8 + r, RUNS, stride=PAD1), get_tiles(proj0, pl.ds(r, RUNS, stride=PAD0)))

    def far_items(t, w, source=None, resume=False):
        items = [Edge(t, k, w, n, run_shift=s, source=source, first=n == 0, keep=4 * t + n) for n, (k, s) in enumerate(FAR)]
        if resume:
            for item in items:
                item.resume()
        return items

    def near_items(t, w, resume=False):
        items = [Edge(t, k, w, 4 + n, row_shift=s, final=n == 1, keep=8 + t if n == 0 else None)
                 for n, (k, s) in enumerate(NEAR)]
        if resume:
            items[0].resume()
        return items

    def phase(order, x, n, node, next_x, next_n, before, w_next):
        table = {"before": before, "n1": n[1].a, "nh": node.own, "na": node.a, "nb": node.b, "an0": next_n[0].a,
                 "ps": lambda: project_send(node.t, w_next), "pr": lambda: project_recv(node.t, w_next)}
        for i in range(4):
            table[f"fx{i}"], table[f"bx{i}"], table[f"ax{i}"] = x[i].fin, x[i].b, next_x[i].a
        for i in range(PAIR):
            table[f"fn{i}"], table[f"bn{i}"] = n[i].fin, n[i].b
        run(order, table)

    def run(order, table):
        for name in order:
            table[name]()

    def encoder(step):
        w = Weights(enc_refs, ZERO)
        w1 = layer_weights(step, 1)
        w2 = layer_weights(step, 2)
        table = {"send": lambda: send_halo(ZERO), "share": share_rows}

        def spread():
            for k in range(6):
                for t in range(TILES):
                    if t == 1 or k < PAIR:
                        edge[k, tile_rows(t), :] = edge_base[k, tile_rows(t), :]

        table["copy"] = spread
        y, x, z, n = far_items(0, w1, edge_base), far_items(1, w1), far_items(0, w2), near_items(0, w1)
        for k in range(4):
            table[f"ya{k}"], table[f"yf{k}"], table[f"yb{k}"] = y[k].a, y[k].fin, y[k].b
            table[f"xa{k}"], table[f"za{k}"] = x[k].a, z[k].a
        table["n0"] = n[0].a
        for t in range(TILES):
            def back(t=t):
                out = dot(h_mesh[tile_rows(t), :], w.edge[2][...])
                for c in chunks():
                    recv[part_rows(t, c), :] = out[c:c + CH]

            node = Node(t, h_mesh, w)
            table[f"r{t}"], table[f"nh{t}"], table[f"na{t}"], table[f"nb{t}"] = back, node.own, node.a, node.b
            table[f"ps{t}"], table[f"pr{t}"] = functools.partial(project_send, t, w1), functools.partial(project_recv, t, w1)
            for p in range(PAIR):
                i = PAIR * t + p
                low, high = 8 + i, 12 + i

                def in_first(t=t, p=p, low=low):
                    hide(low, dot(feat[p, t].reshape(TILE, 2 * LANES), we[pl.ds(9 + PAIR * step, PAIR)].reshape(2 * LANES, LAT)))

                def in_last(t=t, p=p, low=low):
                    y = dot(hid[low], weo[ZERO])
                    for c in chunks():
                        v[p, part_rows(t, c), :] = norm(y[c:c + CH]).astype(BF16)

                def edge_first(t=t, p=p, high=high):
                    pre = dot(g2m[p, tile_rows(t), :], w.edge[0][...]) + dot(v[p, tile_rows(t), :], w.edge[1][...])
                    hide(high, pre, lambda c: recv[part_rows(t, c), :])

                def edge_last(t=t, p=p, high=high):
                    y = dot(hid[high], w.edge_out[...])
                    for c in chunks():
                        part = part_rows(t, c)
                        total = (g2m[p, part, :].astype(F32) + norm(y[c:c + CH])).astype(BF16).astype(F32)
                        if p == 0:
                            acc[part, :] = total
                        else:
                            esum[part, :] = (acc[part, :] + total).astype(BF16)

                def self_first(t=t, p=p, low=low):
                    hide(low, dot(v[p, tile_rows(t), :], wself[ZERO]))

                def self_last(t=t, p=p, low=low):
                    y = dot(hid[low], wself[ONE])
                    for c in chunks():
                        part = part_rows(t, c)
                        vc[p, part, :] = (v[p, part, :].astype(F32) + norm(y[c:c + CH])).astype(BF16)

                table[f"va{i}"], table[f"vb{i}"], table[f"ea{i}"], table[f"eb{i}"] = in_first, in_last, edge_first, edge_last
                table[f"sa{i}"], table[f"sb{i}"] = self_first, self_last
        run(ORDER_E, table)

    def out_copies(step, out, t):
        copies = []
        for hop in range(RING):
            target = lax.rem(me + hop, RING)
            src, dst = x_buf.at[step + 1, :, t, pl.ds(PAIR * target, PAIR)], out.at[place, :, t]
            if hop == 0:
                copies.append(pltpu.make_async_copy(src, dst, out_recv.at[step, t, hop]))
            else:
                copies.append(pltpu.make_async_remote_copy(
                    src_ref=src, dst_ref=dst, send_sem=out_send.at[step, t, hop], recv_sem=out_recv.at[step, t, hop],
                    device_id=at(target), device_id_type=mesh_id))
        return copies

    def decoder(step):
        w16 = layer_weights(step, LAYERS)
        w = layer_weights(step, BLOCKS - 1)
        in_mean = stats[ZERO:ONE, :]
        in_std = stats[ONE:PAIR, :]
        diff_mean, diff_std = (jnp.concatenate([stats[i:i + 1, :], jnp.zeros((ONE, LANES - VARS), F32)], axis=ONE) for i in (2, 3))
        halo_slot = lax.rem(LAYERS + 1, 2)
        table = {"share": share_rows, "wait": lambda: wait_halo(halo_slot), "halo": lambda: project_halo(halo_slot, w16)}
        x = far_items(1, w16, resume=True)
        for k in range(4):
            table[f"fx{k}"], table[f"bx{k}"] = x[k].fin, x[k].b
        for t in range(TILES):
            node = Node(t, h, w16)
            table[f"nh{t}"], table[f"na{t}"], table[f"nb{t}"] = node.own, node.a, node.b
            near = near_items(t, w16, resume=t == 0)
            for k in range(PAIR):
                table[f"n{t}{k}"], table[f"fn{t}{k}"], table[f"bn{t}{k}"] = near[k].a, near[k].fin, near[k].b

            def back(t=t):
                out = dot(h[tile_rows(t), :], w.edge[1][...])
                for c in chunks():
                    recv[part_rows(t, c), :] = out[c:c + CH]

            def send(t=t):
                for which, out in enumerate((out0, out1)):
                    @pl.when(step == which)
                    def _():
                        start_all(out_copies(which, out, t))

            table[f"t{t}"], table[f"send{t}"] = back, send
            for p in range(PAIR):
                i = PAIR * t + p
                low, high = 8 + i, 12 + i
                held = {}

                def edge_own(t=t, p=p, held=held):
                    held["edge"] = dot(m2g[p, tile_rows(t), :], w.edge[0][...]) + dot(vc[p, tile_rows(t), :], w.edge[2][...])

                def edge_first(t=t, low=low, held=held):
                    hide(low, held["edge"], lambda c: recv[part_rows(t, c), :])

                def edge_last(t=t, p=p, low=low, i=i):
                    y = dot(hid[low], w.edge_out[...])
                    for c in chunks():
                        part = part_rows(t, c)
                        dec[i, pl.ds(c, CH), :] = (m2g[p, part, :].astype(F32) + norm(y[c:c + CH])).astype(BF16)

                def node_own(t=t, p=p, held=held):
                    held["node"] = dot(vc[p, tile_rows(t), :], w.node[0][...])

                def node_first(high=high, i=i, held=held):
                    hide(high, held["node"] + dot(dec[i], w.node[1][...]))

                def node_last(t=t, p=p, high=high):
                    y = dot(hid[high], w.node_out[...])
                    for c in chunks():
                        part = part_rows(t, c)
                        v[p, part, :] = (vc[p, part, :].astype(F32) + norm(y[c:c + CH])).astype(BF16)

                def out_first(t=t, p=p, low=low):
                    hide(low, dot(v[p, tile_rows(t), :], woh[...]))

                def out_last(t=t, p=p, low=low):
                    pred = dot(hid[low], wof[...])
                    for c in chunks():
                        runs = pl.ds(c // HALF, CH // HALF)
                        now = x_buf[step, p, t, runs].reshape(CH, LANES)
                        new = now + diff_std * pred[c:c + CH] + diff_mean
                        x_buf[step + 1, p, t, runs] = new.reshape(CH // HALF, HALF, LANES)
                        scaled = ((new[:, :VARS] - in_mean) / in_std).astype(BF16)
                        feat[p, t, runs, :, pl.ds(ZERO, VARS)] = scaled.reshape(CH // HALF, HALF, VARS)

                table[f"em{i}"], table[f"ea{i}"], table[f"eb{i}"] = edge_own, edge_first, edge_last
                table[f"dm{i}"], table[f"da{i}"], table[f"db{i}"] = node_own, node_first, node_last
                table[f"oa{i}"], table[f"ob{i}"] = out_first, out_last
        run(ORDER_D, table)

    def wait_all(copies):
        for copy in copies:
            copy.wait()

    def start_all(copies):
        for copy in copies:
            copy.start()

    def one_step(step, carry):
        wait_all(layer_copies(step, 1) + layer_copies(step, 2))
        start_all(layer_copies(step, 3))
        encoder(step)

        def one_layer(block, carry):
            halo_slot = lax.rem(block + 1, 2)
            w, w1, w2 = (layer_weights(step, block + i) for i in range(3))
            phase(ORDER_A, far_items(1, w, resume=True), near_items(0, w, resume=True), Node(0, h, w), far_items(1, w1),
                  near_items(1, w), share_rows, w1)
            wait_halo(halo_slot)
            wait_all(layer_copies(step, block + 2))

            @pl.when(block < LAYERS - 1)
            def _():
                start_all(layer_copies(step, block + 3))

            phase(ORDER_B, far_items(0, w1, resume=True), near_items(1, w, resume=True), Node(1, h, w), far_items(0, w2),
                  near_items(0, w1), lambda: project_halo(halo_slot, w), w1)
            send_halo(1 - halo_slot)
            return carry

        lax.fori_loop(1, LAYERS, one_layer, 0)
        @pl.when(step == 0)
        def _():
            start_all(layer_copies(1, 1) + layer_copies(1, 2))
            wait_in(PAIR)

        decoder(step)
        return carry

    lax.fori_loop(0, 2, one_step, 0)
    for part in range(3):
        for copy in in_copies[part][1:]:
            copy.wait_send()
    for t in range(TILES):
        wait_all(out_copies(0, out0, t) + out_copies(1, out1, t))


def solution(mesh):
    row_spec = P(("dp", "gp"))
    edge_spec = P(("dp", "gp"), None, None)
    whole = P()

    def local_run(x_prev, x_cur, forcing, grid_static, g2m_feat, m2g_feat, mesh_feat, mesh_edge_feat, norm_stats,
                  w_grid_in, w_mesh_in, w_eemb_in, w_embed_out, w_edge_in, w_edge_out, w_node_in, w_node_out,
                  w_grid_self, w_out_hidden, w_out_final):
        any_spec = pl.BlockSpec(memory_space=pl.ANY)
        vmem_spec = pl.BlockSpec(memory_space=pltpu.VMEM)
        dma = pltpu.SemaphoreType.DMA
        grid_dev = x_prev.shape[0]
        shape = jax.ShapeDtypeStruct
        home = shape((RING, PAIR, TILES, PAIR, HALF, LANES), F32)
        bulk = [
            pltpu.VMEM(shape_, F32) for shape_ in (
                (3, mesh_feat.shape[0]), (6, 4, mesh_feat.shape[0]), (VARS, grid_dev), (VARS, grid_dev), (5, PAIR, grid_dev),
                (5, grid_dev), (4, grid_dev), (4, grid_dev))
        ]
        scratch = bulk + [
            pltpu.VMEM((2 * VARS + 10, LAT), BF16),
            pltpu.VMEM((3, LAT), BF16),
            pltpu.VMEM((3, 4, LAT), BF16),
            pltpu.VMEM((VARS, LAT), BF16),
            pltpu.VMEM((*home.shape[:-1], 2 * LANES), BF16),
            pltpu.VMEM((RING, TILES, PAIR, HALF, LANES), BF16),
            pltpu.VMEM(home.shape, F32),
            pltpu.VMEM((TILES, RUNS, HALF, LANES), BF16),
            pltpu.VMEM((3, PAIR, TILES, RUNS, HALF, LANES), F32),
            pltpu.VMEM((PAIR, TILES, RUNS, HALF, 2 * LANES), BF16),
            pltpu.VMEM((13, LANES, LAT), BF16),
            pltpu.VMEM((5, LAT, LAT), BF16),
            pltpu.VMEM((PAIR, LAT, LAT), BF16),
            pltpu.VMEM((LAT, LAT), BF16),
            pltpu.VMEM((LAT, LANES), BF16),
            pltpu.VMEM((1, 3 * LAT, LAT), BF16),
            pltpu.VMEM((1, LAT, LAT), BF16),
            pltpu.VMEM((1, 2 * LAT, LAT), BF16),
            pltpu.VMEM((1, LAT, LAT), BF16),
            pltpu.VMEM((SLOTS, 3 * LAT, LAT), BF16),
            pltpu.VMEM((SLOTS, LAT, LAT), BF16),
            pltpu.VMEM((SLOTS, 2 * LAT, LAT), BF16),
            pltpu.VMEM((SLOTS, LAT, LAT), BF16),
            pltpu.VMEM((6, ROWS, LAT), BF16),
            pltpu.VMEM((6, ROWS, LAT), BF16),
            pltpu.VMEM((ROWS, LAT), BF16),
            pltpu.VMEM((ROWS, LAT), BF16),
            pltpu.VMEM((LAT // LANES, TILE, LANES), F32),
            pltpu.VMEM((PAIR, ROWS, LAT), BF16),
            pltpu.VMEM((PAIR, ROWS, LAT), BF16),
            pltpu.VMEM((PAIR, ROWS, LAT), BF16),
            pltpu.VMEM((PAIR, ROWS, LAT), BF16),
            pltpu.VMEM((LAT // LANES, RUNS * PAD0, LANES), F32),
            pltpu.VMEM((LAT // LANES, RUNS * PAD1, LANES), F32),
            pltpu.VMEM((ROWS, LAT), F32),
            pltpu.VMEM((ROWS, LAT), F32),
            pltpu.VMEM((16, TILE, LAT), BF16),
            pltpu.VMEM((ROWS, LAT), BF16),
            pltpu.VMEM((4, TILE, LAT), BF16),
            pltpu.VMEM((10, TILE, LAT), F32),
            pltpu.VMEM((PAIR, RUNS, LAT), BF16),
            pltpu.VMEM((PAIR, 2, RUNS, LAT), BF16),
            dma((12,)), dma((3, RING)), dma((3, RING)), dma((4,)), dma((1, 4)), dma((SLOTS, 4)), dma((PAIR,)), dma((PAIR, PAIR)),
            dma((PAIR, TILES, RING)), dma((PAIR, TILES, RING)),
        ]
        home0, home1 = pl.pallas_call(
            kernel,
            out_shape=(home, home),
            in_specs=[any_spec] * 8 + [vmem_spec] + [any_spec] * 11,
            out_specs=(any_spec, any_spec),
            scratch_shapes=scratch,
            compiler_params=pltpu.CompilerParams(collective_id=0, has_side_effects=True, vmem_limit_bytes=63 << 20),
            name="forecast",
        )(x_prev.T, x_cur.T, forcing.T, grid_static.T, g2m_feat.T, m2g_feat.T, mesh_feat.T,
          jnp.transpose(mesh_edge_feat, (1, 2, 0)), norm_stats, w_grid_in, w_mesh_in, w_eemb_in, w_embed_out, w_edge_in,
          w_edge_out, w_node_in, w_node_out, w_grid_self, w_out_hidden, w_out_final.T)
        out = shape((VARS, grid_dev), F32)
        next_state, after_state = pl.pallas_call(
            unpack_kernel, out_shape=(out, out), in_specs=[vmem_spec] * 2, out_specs=(vmem_spec,) * 2,
            scratch_shapes=[pltpu.VMEM((grid_dev, LANES), F32)], name="unpack",
        )(home0, home1)
        return next_state.T, after_state.T

    in_specs = (row_spec, row_spec, edge_spec, row_spec, row_spec, row_spec, row_spec, edge_spec, whole) + (whole,) * 11
    return jax.shard_map(local_run, mesh=mesh, in_specs=in_specs, out_specs=(row_spec, row_spec), check_vma=False)
```

```python
import functools

import jax
import jax.numpy as jnp
from jax import lax
from jax.experimental import pallas as pl
from jax.experimental.pallas import tpu as pltpu
from jax.sharding import PartitionSpec as P

F32 = jnp.float32
BF16 = jnp.bfloat16

RUNS = 16
RUN = 32
GRID_RUN = 2 * RUN
ROWS = RUNS * RUN
ZERO, ONE, LAST = 0, 1, -1
LAT = 512
LANES = 128
PAIR = 2
VARS = 84
PAD0 = 32
PAD1 = 48
TILE = 256
TILES = 2
HALF = TILE // RUNS
CH = 128
RING = 8
LAYERS = 16
BLOCKS = LAYERS + 2
SLOTS = 4
FAR = ((2, 1), (3, -1), (4, 4), (5, -4))
NEAR = ((0, 1), (1, -1))
ORDER_A = (
    "nh", "before", "fx0", "n1", "fx1", "bx0", "bx1", "fn0", "bn0", "fn1", "bn1", "ax0", "fx2", "fx3", "bx2",
    "na", "ax1", "bx3", "ax2", "nb", "an0", "ax3", "pr", "ps",
)
ORDER_B = (
    "nh", "before", "fx0", "fx1", "bx0", "n1", "fn1", "bx1", "fn0", "bn0", "bn1", "ax0", "fx2", "ax1", "fx3",
    "bx2", "na", "bx3", "ax2", "nb", "ax3", "an0", "ps", "pr",
)
ORDER_E = (
    "copy", "r0", "va0", "va1", "vb0", "va2", "vb1", "va3", "r1", "vb2", "vb3", "ea0", "sa0", "ea3", "ea1",
    "eb0", "sa1", "eb1", "sb0", "ea2", "sb1", "nh0", "na0", "eb2", "sa2", "eb3", "nb0", "sa3", "sb2", "sb3",
    "ya2", "ya0", "nh1", "ya1", "na1", "ps0", "pr0", "nb1", "yf0", "yb0", "yf1", "yb1", "ps1", "ya3", "pr1",
    "yf2", "yb2", "yf3", "yb3", "xa0", "xa1", "za1", "xa2", "xa3", "za0", "za2", "za3", "n0", "share", "send",
)
ORDER_D = (
    "n01", "fx1", "nh0", "fx0", "share", "bx0", "fn00", "fn01", "bn00", "bn01", "bx1", "em0", "fx2", "bx2",
    "fx3", "na0", "em1", "nb0", "n11", "wait", "dm0", "n10", "t0", "halo", "bx3", "ea0", "fn11", "fn10",
    "bn10", "eb0", "bn11", "ea1", "eb1", "nh1", "em2", "em3", "na1", "da0", "dm1", "nb1", "da1", "dm2", "db0",
    "t1", "db1", "oa0", "ea2", "eb2", "oa1", "ob0", "ea3", "dm3", "ob1", "send0", "send1", "eb3", "da2", "da3",
    "db2", "db3", "oa2", "oa3", "ob2", "send2", "ob3", "send3",
)


def dot(a, b):
    return jnp.dot(a, b, preferred_element_type=F32)


def silu(pre):
    return pre * jax.nn.sigmoid(pre)


def norm(y):
    centred = y - jnp.mean(y, axis=LAST, keepdims=True)
    return centred * lax.rsqrt(jnp.mean(centred * centred, axis=LAST, keepdims=True) + 1e-5)


def ring_place(dev):
    high = lax.div(dev, 4)
    return high * (4 + lax.rem(dev + 2, 4)) + (1 - high) * dev


def chunks():
    return range(0, TILE, CH)


def tile_rows(t):
    return pl.ds(t * TILE, TILE)


def part_rows(t, c):
    return pl.ds(t * TILE + c, CH)


def chunk_runs(c):
    return range(c // HALF, (c + CH) // HALF)


def pieces(t):
    return ((8, 16),) if t == 0 else ((0, 8), (24, 8))


def get_tiles(ref, rows):
    return jnp.concatenate([ref[j, rows, :] for j in range(ref.shape[0])], axis=ONE)


def set_tiles(ref, rows, value):
    for j in range(ref.shape[0]):
        ref[j, rows, :] = value[:, LANES * j:LANES * j + LANES]


AT_FORCE, AT_STATIC, AT_NEXT, AT_M2G, AT_G2M = 88, 96, 104, 112, 120


def columns(n):
    return pl.ds(LANES * n, LANES)


def stack(ref, rows):
    end = 0
    for at_row, value in rows:
        first = at_row // 8 * 8
        last = (at_row + value.shape[0]) // 8 * 8
        if first > end:
            ref[pl.ds(end, first - end), :] = jnp.zeros((first - end, LANES), F32)
        if last < at_row + value.shape[0]:
            ref[pl.ds(last, 8), :] = jnp.zeros((8, LANES), F32)
            end = last + 8
        else:
            end = last
        ref[pl.ds(at_row, value.shape[0]), :] = value
    if end < LANES:
        ref[pl.ds(end, LANES - end), :] = jnp.zeros((LANES - end, LANES), F32)


def unpack_kernel(homes, out0, out1, area):
    for home, out in ((homes.at[ZERO], out0), (homes.at[ONE], out1)):
        for band in range(PAIR):
            for k in range(RING):
                for p in range(PAIR):
                    for t in range(TILES):
                        row = 0
                        for r, rows in pieces(t):
                            spot = pl.ds((band * RING + k) * GRID_RUN + PAIR * r + p, rows, stride=PAIR)
                            area[spot, :] = home[k, p, t, band, pl.ds(row, rows), :]
                            row += rows
        for n in range(out.shape[1] // LANES):
            out[:, columns(n)] = jnp.transpose(area[columns(n), :])[:VARS]


def kernel(x_prev, x_cur, forcing, static, g2m_feat, m2g_feat, mesh_feat, mesh_edge_feat, stats, w_grid_in, w_mesh_in,
           w_eemb_in, w_embed_out, w_edge_in, w_edge_out, w_node_in, w_node_out, w_grid_self, w_out_hidden, w_out_final,
           out,
           mesh_raw, medge_raw, prev_raw, cur_raw, force_raw, static_raw, g2m_raw, m2g_raw,
           wgrid_raw, wmesh_raw, weemb_raw, wfin_raw, g_home, m_home, x_home,
           m_buf, x_buf, feat, we, weo, wself, woh, wof,
           enc_ei, enc_eo, enc_ni, enc_no, lay_ei, lay_eo, lay_ni, lay_no,
           edge_base, edge, h_mesh, h, hf, g2m, m2g, v, vc, proj0, proj1, recv, acc, hid, esum, dec, pre_buf,
           send_buf, halo_buf,
           raw_sem, in_send, in_recv, w_sem, enc_sem, lay_sem, halo_send, halo_recv, out_send, out_recv):
    me = lax.axis_index("gp")
    place = ring_place(me)

    def at(dev):
        return {"gp": dev}

    mesh_id = pl.DeviceIdType.MESH

    def block_copies(block, dst_refs, slot, sem):
        srcs = (w_edge_in, w_edge_out, w_node_in, w_node_out)
        return [pltpu.make_async_copy(src.at[block], dst.at[slot], sem.at[slot, i])
                for i, (src, dst) in enumerate(zip(srcs, dst_refs))]

    enc_refs = (enc_ei, enc_eo, enc_ni, enc_no)
    lay_refs = (lay_ei, lay_eo, lay_ni, lay_no)

    def enc_copies():
        return block_copies(0, enc_refs, 0, enc_sem)

    def slot_of(step, block):
        return lax.rem((BLOCKS - 1) * step + block - 1, SLOTS)

    def layer_copies(step, block):
        return block_copies(block, lay_refs, slot_of(step, block), lay_sem)

    class Weights:
        def __init__(self, refs, slot):
            self.edge = [refs[0].at[slot, pl.ds(i * LAT, LAT)] for i in range(3)]
            self.edge_out = refs[1].at[slot]
            self.node = [refs[2].at[slot, pl.ds(i * LAT, LAT)] for i in range(2)]
            self.node_out = refs[3].at[slot]

    def layer_weights(step, block):
        return Weights(lay_refs, slot_of(step, block))

    raw = [pltpu.make_async_copy(src, dst, raw_sem.at[i]) for i, (src, dst) in enumerate(
        ((mesh_feat, mesh_raw), (mesh_edge_feat, medge_raw), (x_prev, prev_raw), (x_cur, cur_raw), (forcing, force_raw),
         (static, static_raw), (g2m_feat, g2m_raw), (m2g_feat, m2g_raw),
         (w_grid_in, wgrid_raw), (w_mesh_in, wmesh_raw), (w_eemb_in, weemb_raw), (w_out_final, wfin_raw)))]
    for copy in raw:
        copy.start()
    small = [
        pltpu.make_async_copy(w_embed_out, weo, w_sem.at[0]),
        pltpu.make_async_copy(w_grid_self, wself, w_sem.at[1]),
        pltpu.make_async_copy(w_out_hidden, woh, w_sem.at[2]),
    ]
    small[0].start()

    barrier = pltpu.get_barrier_semaphore()
    for hop in range(1, RING):
        pl.semaphore_signal(barrier, inc=1, device_id=at(lax.rem(me + hop, RING)), device_id_type=mesh_id)

    mine = pl.ds(PAIR * me, PAIR)
    prev_lanes, cur_lanes = pl.ds(ZERO, LANES), pl.ds(LANES, LANES)
    parts = ((m_home, m_buf.at[:, mine]), (g_home.at[..., prev_lanes], feat.at[:, :, mine, :, prev_lanes]),
             (g_home.at[..., cur_lanes], feat.at[:, :, mine, :, cur_lanes]), (x_home, x_buf.at[ZERO, :, :, mine]))

    def in_copy(part, hop):
        src, dst = parts[part]
        target = lax.rem(me + hop, RING)
        src = src.at[ring_place(target)]
        if hop == 0:
            return pltpu.make_async_copy(src, dst, in_recv.at[part, hop])
        return pltpu.make_async_remote_copy(src_ref=src, dst_ref=dst, send_sem=in_send.at[part, hop],
                                            recv_sem=in_recv.at[part, hop], device_id=at(target),
                                            device_id_type=mesh_id)

    in_copies = [[in_copy(part, hop) for hop in range(RING)] for part in range(len(parts))]

    def wait_in(part):
        in_copies[part][0].wait()
        for copy in in_copies[part][1:]:
            copy.wait_recv()

    def start_in(part):
        for copy in in_copies[part]:
            copy.start()

    def place_of(area, n):
        ref, first = area
        return ref.at[first + n // 4, columns(n % 4)]

    prev_area, cur_area, norm_area, mesh_area, final_area = (proj0, 0), (proj0, PAIR), (proj1, 0), (proj1, 2), (proj1, 3)

    def turned(area, n):
        return jnp.transpose(place_of(area, n)[...])

    for copy in raw[:2]:
        copy.wait()
    for n in range(mesh_raw.shape[1] // LANES):
        stack(place_of(mesh_area, n), [(ZERO, mesh_raw[:, columns(n)])] + [
            (16 + 16 * k, medge_raw[k, :, columns(n)]) for k in range(6)])
    for n in range(mesh_raw.shape[1] // LANES):
        turned_rows = turned(mesh_area, n)
        for i in range(LANES // RUN):
            band, k = divmod(n * LANES + i * RUN, RING * RUN)
            for t in range(TILES):
                m_home[k // RUN, t, band] = jnp.concatenate(
                    [turned_rows[i * RUN + r:i * RUN + r + rows] for r, rows in pieces(t)], axis=ZERO).astype(BF16)
    pl.semaphore_wait(barrier, RING - 1)
    start_in(0)
    for copy in raw[2:8]:
        copy.wait()
    blocks = range(cur_raw.shape[1] // LANES)
    rest = LANES - VARS
    wide_mean = jnp.concatenate([stats[ZERO:ONE, :], jnp.zeros((ONE, rest), F32)], axis=ONE)
    wide_std = jnp.concatenate([stats[ONE:PAIR, :], jnp.ones((ONE, rest), F32)], axis=ONE)

    def spread(area, store):
        ref, first = area
        for k in range(RING):
            for p in range(PAIR):
                for t in range(TILES):
                    for band in range(PAIR):
                        store((k, p, t, band), jnp.concatenate(
                            [ref[first + band, pl.ds(k * GRID_RUN + PAIR * r + p, rows, stride=PAIR), :] for r, rows in pieces(t)],
                            axis=ZERO))

    def store_prev(spot, rows):
        g_home[(*spot, slice(None), prev_lanes)] = rows.astype(BF16)

    def store_norm(spot, rows):
        g_home[(*spot, slice(None), cur_lanes)] = rows.astype(BF16)

    def store_cur(spot, rows):
        x_home[spot] = rows

    for n in blocks:
        stack(place_of(prev_area, n), [
            (ZERO, prev_raw[:, columns(n)]), (AT_FORCE, force_raw[:, ZERO, columns(n)]), (AT_STATIC, static_raw[:, columns(n)]),
            (AT_NEXT, force_raw[:, ONE, columns(n)]), (AT_M2G, m2g_raw[:, columns(n)]), (AT_G2M, g2m_raw[:, columns(n)])])
    for n in blocks:
        place_of(prev_area, n)[...] = (turned(prev_area, n) - wide_mean) / wide_std
    spread(prev_area, store_prev)
    start_in(1)
    for n in blocks:
        stack(place_of(cur_area, n), [(ZERO, cur_raw[:, columns(n)])])
    for n in blocks:
        cur = turned(cur_area, n)
        place_of(cur_area, n)[...] = cur
        place_of(norm_area, n)[...] = (cur - wide_mean) / wide_std
    spread(norm_area, store_norm)
    start_in(2)
    spread(cur_area, store_cur)
    for copy in small[1:] + enc_copies() + layer_copies(0, 1) + layer_copies(0, 2):
        copy.start()

    for copy in raw[8:]:
        copy.wait()
    for n in range(LAT // LANES):
        stack(place_of(final_area, n), [(ZERO, wfin_raw[:, columns(n)].astype(F32))])
        wof[columns(n), :] = turned(final_area, n).astype(BF16)
    wide = wgrid_raw[...].astype(F32)
    recv[pl.ds(ZERO, wide.shape[0]), :] = wide
    prev_w, cur_w = recv[pl.ds(ZERO, VARS), :], recv[pl.ds(VARS, VARS), :]
    force_w, static_w = recv[pl.ds(2 * VARS, 5), :], recv[pl.ds(2 * VARS + 5, 5), :]
    spread = [[(0, wmesh_raw[...].astype(F32))], [(AT_G2M, weemb_raw[0].astype(F32))], [(AT_M2G, weemb_raw[1].astype(F32))]]
    spread += [[(16 + 16 * k, weemb_raw[2].astype(F32))] for k in range(6)]
    spread += [[(0, prev_w), (AT_FORCE, force_w), (AT_STATIC, static_w)], [(0, cur_w)]]
    spread += [[(0, cur_w), (AT_STATIC, static_w), (AT_NEXT, force_w)], [(0, prev_w)]]
    for i, rows in enumerate(spread):
        base = LANES * (i % 4)
        acc[pl.ds(base, LANES), :] = jnp.zeros((LANES, LAT), F32)
        for at_row, value in rows:
            acc[pl.ds(base + at_row, value.shape[0]), :] = value
        we[i] = acc[pl.ds(base, LANES), :].astype(BF16)

    def pipeline(items):
        depth = max(len(item) for item in items)
        for beat in range(len(items) + depth - 1):
            for stage in range(depth):
                index = beat - stage
                if 0 <= index < len(items) and stage < len(items[index]):
                    items[index][stage](index)

    def hide(slot, pre, extra=None):
        for c in chunks():
            value = pre[c:c + CH]
            if extra is not None:
                value = value + extra(c)
            hid[slot, pl.ds(c, CH), :] = silu(value).astype(BF16)

    def embed_item(load, w_first, second, store):
        def first(i):
            hide(i % PAIR, dot(load(), we[w_first]))

        def last(i):
            y = dot(hid[i % 2], weo[second])
            for c in chunks():
                store(c, norm(y[c:c + CH]).astype(BF16))

        return [first, last]

    wait_in(0)
    small[0].wait()
    def next_run(ref, *index):
        first = ref[(*index, pl.ds(ONE, RUNS - 1), slice(None), pl.ds(ZERO, LANES))]
        last = ref[(*index, pl.ds(ZERO, ONE), slice(None), pl.ds(ZERO, LANES))]
        return jnp.concatenate([first, last], axis=ZERO).reshape(TILE, LANES)

    mesh_rows = [next_run(m_buf, t) for t in range(TILES)]
    items = []
    for t in range(TILES):
        def store_mesh(c, value, t=t):
            h_mesh[part_rows(t, c), :] = value
        items.append(embed_item(lambda t=t: mesh_rows[t], 0, 1, store_mesh))
        for k in range(6):
            def store_edge(c, value, t=t, k=k):
                edge_base[k, part_rows(t, c), :] = value
            items.append(embed_item(lambda t=t: mesh_rows[t], 3 + k, 4, store_edge))
    pipeline(items)

    wait_in(1)
    items = []
    for t in range(TILES):
        for p in range(PAIR):
            def store_m2g(c, value, t=t, p=p):
                m2g[p, part_rows(t, c), :] = value
            def store_g2m(c, value, t=t, p=p):
                g2m[p, part_rows(t, c), :] = value
            items.append(embed_item(lambda t=t, p=p: next_run(feat, p, t), 1, 2, store_g2m))
            items.append(embed_item(lambda t=t, p=p: feat[p, t, :, :, pl.ds(ZERO, LANES)].reshape(TILE, LANES), 2, 3, store_m2g))
    pipeline(items)
    wait_in(2)
    start_in(3)
    for copy in small[1:] + enc_copies():
        copy.wait()

    left = ring_place(lax.rem(place + RING - 1, RING))
    right = ring_place(lax.rem(place + 1, RING))

    def halo_copies(slot):
        return [
            pltpu.make_async_remote_copy(src_ref=send_buf.at[side], dst_ref=halo_buf.at[slot, side],
                                         send_sem=halo_send.at[side], recv_sem=halo_recv.at[slot, side],
                                         device_id=at(target), device_id_type=mesh_id)
            for side, target in ((0, left), (1, right))
        ]

    def send_halo(slot):
        first = get_tiles(hf, pl.ds(ZERO, RUNS, stride=HALF))
        final = get_tiles(hf, pl.ds(HALF - 1, RUNS, stride=HALF))
        first_on = jnp.concatenate([first[1:], first[:1]], axis=ZERO)
        final_back = jnp.concatenate([final[-1:], final[:-1]], axis=ZERO)
        send_buf[0] = jnp.where(place == 0, first_on, first).astype(BF16)
        send_buf[1] = jnp.where(place == RING - 1, final_back, final).astype(BF16)
        for copy in halo_copies(slot):
            copy.start()

    def wait_halo(slot):
        for copy in halo_copies(slot):
            copy.wait()

    def project_halo(slot, w):
        rows = jnp.concatenate([halo_buf[slot, 0], halo_buf[slot, 1]], axis=ZERO)
        out = dot(rows, w.edge[1][...])
        set_tiles(proj1, pl.ds(8 + RUN, RUNS, stride=PAD1), out[:RUNS])
        set_tiles(proj1, pl.ds(7, RUNS, stride=PAD1), out[RUNS:])

    class Edge:
        def __init__(self, t, k, w, slot, run_shift=0, row_shift=0, source=None, first=False, final=False, keep=None):
            self.t, self.k, self.w, self.slot, self.keep = t, k, w, slot, keep
            self.run_shift, self.row_shift, self.first, self.final = run_shift, row_shift, first, final
            self.source = edge if source is None else source
            self.pre = None

        def a(self):
            self.pre = dot(self.source[self.k, tile_rows(self.t), :], self.w.edge[0][...])
            if self.keep is not None:
                for c in chunks():
                    pre_buf[self.keep, pl.ds(c, CH), :] = self.pre[c:c + CH]

        def resume(self):
            self.pre = pre_buf.at[self.keep]

        def extra(self, c):
            got = []
            for q in chunk_runs(c):
                base = (q + self.run_shift) % RUNS
                for r, n in pieces(self.t):
                    if self.t == 0:
                        got.append(get_tiles(proj0, pl.ds(base * PAD0 + r + self.row_shift, n)))
                    else:
                        got.append(get_tiles(proj1, pl.ds(base * PAD1 + 8 + r + self.row_shift, n)))
            return jnp.concatenate(got, axis=ZERO) + recv[part_rows(self.t, c), :]

        def fin(self):
            hide(self.slot, self.pre, self.extra)

        def b(self):
            y = dot(hid[self.slot], self.w.edge_out[...])
            for c in chunks():
                part = part_rows(self.t, c)
                value = (self.source[self.k, part, :].astype(F32) + norm(y[c:c + CH])).astype(BF16)
                edge[self.k, part, :] = value
                total = value.astype(F32)
                if not self.first:
                    total = total + acc[part, :]
                if self.final:
                    esum[part, :] = total.astype(BF16)
                else:
                    acc[part, :] = total

    class Node:
        def __init__(self, t, base, w):
            self.t, self.base, self.w, self.slot = t, base, w, 6 + t

        def own(self):
            self.pre = dot(self.base[tile_rows(self.t), :], self.w.node[0][...])

        def a(self):
            hide(self.slot, self.pre + dot(esum[tile_rows(self.t), :], self.w.node[1][...]))

        def b(self):
            y = dot(hid[self.slot], self.w.node_out[...])
            for c in chunks():
                part = part_rows(self.t, c)
                value = (self.base[part, :].astype(F32) + norm(y[c:c + CH])).astype(BF16)
                h[part, :] = value
                if self.t == 1:
                    set_tiles(hf, pl.ds(c, CH), value.astype(F32))

    def project_send(t, w):
        out = dot(h[tile_rows(t), :], w.edge[1][...])
        for q in range(RUNS):
            row = q * HALF
            for r, n in pieces(t):
                if t == 0:
                    set_tiles(proj0, pl.ds(q * PAD0 + r, n), out[row:row + n])
                else:
                    set_tiles(proj1, pl.ds(q * PAD1 + 8 + r, n), out[row:row + n])
                row += n
        if t == 1:
            for r in (7, 24):
                set_tiles(proj0, pl.ds(r, RUNS, stride=PAD0), get_tiles(proj1, pl.ds(8 + r, RUNS, stride=PAD1)))

    def project_recv(t, w):
        out = dot(h[tile_rows(t), :], w.edge[2][...])
        for c in chunks():
            recv[part_rows(t, c), :] = out[c:c + CH]

    def project(t, w):
        project_send(t, w)
        project_recv(t, w)

    def share_rows():
        for r in (8, 23):
            set_tiles(proj1, pl.ds(8 + r, RUNS, stride=PAD1), get_tiles(proj0, pl.ds(r, RUNS, stride=PAD0)))

    def far_items(t, w, source=None, resume=False):
        items = [Edge(t, k, w, n, run_shift=s, source=source, first=n == 0, keep=4 * t + n) for n, (k, s) in enumerate(FAR)]
        if resume:
            for item in items:
                item.resume()
        return items

    def near_items(t, w, resume=False):
        items = [Edge(t, k, w, 4 + n, row_shift=s, final=n == 1, keep=8 + t if n == 0 else None)
                 for n, (k, s) in enumerate(NEAR)]
        if resume:
            items[0].resume()
        return items

    def phase(order, x, n, node, next_x, next_n, before, w_next):
        table = {"before": before, "n1": n[1].a, "nh": node.own, "na": node.a, "nb": node.b, "an0": next_n[0].a,
                 "ps": lambda: project_send(node.t, w_next), "pr": lambda: project_recv(node.t, w_next)}
        for i in range(4):
            table[f"fx{i}"], table[f"bx{i}"], table[f"ax{i}"] = x[i].fin, x[i].b, next_x[i].a
        for i in range(PAIR):
            table[f"fn{i}"], table[f"bn{i}"] = n[i].fin, n[i].b
        run(order, table)

    def run(order, table):
        for name in order:
            table[name]()

    def encoder(step):
        w = Weights(enc_refs, ZERO)
        w1 = layer_weights(step, 1)
        w2 = layer_weights(step, 2)
        table = {"send": lambda: send_halo(ZERO), "share": share_rows}

        def spread():
            for k in range(6):
                for t in range(TILES):
                    if t == 1 or k < PAIR:
                        edge[k, tile_rows(t), :] = edge_base[k, tile_rows(t), :]

        table["copy"] = spread
        y, x, z, n = far_items(0, w1, edge_base), far_items(1, w1), far_items(0, w2), near_items(0, w1)
        for k in range(4):
            table[f"ya{k}"], table[f"yf{k}"], table[f"yb{k}"] = y[k].a, y[k].fin, y[k].b
            table[f"xa{k}"], table[f"za{k}"] = x[k].a, z[k].a
        table["n0"] = n[0].a
        for t in range(TILES):
            def back(t=t):
                out = dot(h_mesh[tile_rows(t), :], w.edge[2][...])
                for c in chunks():
                    recv[part_rows(t, c), :] = out[c:c + CH]

            node = Node(t, h_mesh, w)
            table[f"r{t}"], table[f"nh{t}"], table[f"na{t}"], table[f"nb{t}"] = back, node.own, node.a, node.b
            table[f"ps{t}"], table[f"pr{t}"] = functools.partial(project_send, t, w1), functools.partial(project_recv, t, w1)
            for p in range(PAIR):
                i = PAIR * t + p
                low, high = 8 + i, 12 + i

                def in_first(t=t, p=p, low=low):
                    hide(low, dot(feat[p, t].reshape(TILE, 2 * LANES), we[pl.ds(9 + PAIR * step, PAIR)].reshape(2 * LANES, LAT)))

                def in_last(t=t, p=p, low=low):
                    y = dot(hid[low], weo[ZERO])
                    for c in chunks():
                        v[p, part_rows(t, c), :] = norm(y[c:c + CH]).astype(BF16)

                def edge_first(t=t, p=p, high=high):
                    pre = dot(g2m[p, tile_rows(t), :], w.edge[0][...]) + dot(v[p, tile_rows(t), :], w.edge[1][...])
                    hide(high, pre, lambda c: recv[part_rows(t, c), :])

                def edge_last(t=t, p=p, high=high):
                    y = dot(hid[high], w.edge_out[...])
                    for c in chunks():
                        part = part_rows(t, c)
                        total = (g2m[p, part, :].astype(F32) + norm(y[c:c + CH])).astype(BF16).astype(F32)
                        if p == 0:
                            acc[part, :] = total
                        else:
                            esum[part, :] = (acc[part, :] + total).astype(BF16)

                def self_first(t=t, p=p, low=low):
                    hide(low, dot(v[p, tile_rows(t), :], wself[ZERO]))

                def self_last(t=t, p=p, low=low):
                    y = dot(hid[low], wself[ONE])
                    for c in chunks():
                        part = part_rows(t, c)
                        vc[p, part, :] = (v[p, part, :].astype(F32) + norm(y[c:c + CH])).astype(BF16)

                table[f"va{i}"], table[f"vb{i}"], table[f"ea{i}"], table[f"eb{i}"] = in_first, in_last, edge_first, edge_last
                table[f"sa{i}"], table[f"sb{i}"] = self_first, self_last
        run(ORDER_E, table)

    def out_copies(step, i):
        t, p = divmod(i, PAIR)
        copies = []
        for hop in range(RING):
            target = lax.rem(me + hop, RING)
            src, dst = x_buf.at[step + 1, p, t, pl.ds(PAIR * target, PAIR)], out.at[step, place, p, t]
            if hop == 0:
                copies.append(pltpu.make_async_copy(src, dst, out_recv.at[step, i, hop]))
            else:
                copies.append(pltpu.make_async_remote_copy(
                    src_ref=src, dst_ref=dst, send_sem=out_send.at[step, i, hop], recv_sem=out_recv.at[step, i, hop],
                    device_id=at(target), device_id_type=mesh_id))
        return copies

    def decoder(step):
        w16 = layer_weights(step, LAYERS)
        w = layer_weights(step, BLOCKS - 1)
        in_mean = stats[ZERO:ONE, :]
        in_std = stats[ONE:PAIR, :]
        diff_mean, diff_std = (jnp.concatenate([stats[i:i + 1, :], jnp.zeros((ONE, LANES - VARS), F32)], axis=ONE) for i in (2, 3))
        halo_slot = lax.rem(LAYERS + 1, 2)
        table = {"share": share_rows, "wait": lambda: wait_halo(halo_slot), "halo": lambda: project_halo(halo_slot, w16)}
        x = far_items(1, w16, resume=True)
        for k in range(4):
            table[f"fx{k}"], table[f"bx{k}"] = x[k].fin, x[k].b
        for t in range(TILES):
            node = Node(t, h, w16)
            table[f"nh{t}"], table[f"na{t}"], table[f"nb{t}"] = node.own, node.a, node.b
            near = near_items(t, w16, resume=t == 0)
            for k in range(PAIR):
                table[f"n{t}{k}"], table[f"fn{t}{k}"], table[f"bn{t}{k}"] = near[k].a, near[k].fin, near[k].b

            def back(t=t):
                out = dot(h[tile_rows(t), :], w.edge[1][...])
                for c in chunks():
                    recv[part_rows(t, c), :] = out[c:c + CH]

            table[f"t{t}"] = back
            for p in range(PAIR):
                i = PAIR * t + p
                low, high = 8 + i, 12 + i
                held = {}

                def edge_own(t=t, p=p, held=held):
                    held["edge"] = dot(m2g[p, tile_rows(t), :], w.edge[0][...]) + dot(vc[p, tile_rows(t), :], w.edge[2][...])

                def edge_first(t=t, low=low, held=held):
                    hide(low, held["edge"], lambda c: recv[part_rows(t, c), :])

                def edge_last(t=t, p=p, low=low, i=i):
                    y = dot(hid[low], w.edge_out[...])
                    for c in chunks():
                        part = part_rows(t, c)
                        dec[i, pl.ds(c, CH), :] = (m2g[p, part, :].astype(F32) + norm(y[c:c + CH])).astype(BF16)

                def node_own(t=t, p=p, held=held):
                    held["node"] = dot(vc[p, tile_rows(t), :], w.node[0][...])

                def node_first(high=high, i=i, held=held):
                    hide(high, held["node"] + dot(dec[i], w.node[1][...]))

                def node_last(t=t, p=p, high=high):
                    y = dot(hid[high], w.node_out[...])
                    for c in chunks():
                        part = part_rows(t, c)
                        v[p, part, :] = (vc[p, part, :].astype(F32) + norm(y[c:c + CH])).astype(BF16)

                def out_first(t=t, p=p, low=low):
                    hide(low, dot(v[p, tile_rows(t), :], woh[...]))

                def out_last(t=t, p=p, low=low):
                    pred = dot(hid[low], wof[...])
                    for c in chunks():
                        runs = pl.ds(c // HALF, CH // HALF)
                        now = x_buf[step, p, t, runs].reshape(CH, LANES)
                        new = now + diff_std * pred[c:c + CH] + diff_mean
                        x_buf[step + 1, p, t, runs] = new.reshape(CH // HALF, HALF, LANES)
                        scaled = ((new[:, :VARS] - in_mean) / in_std).astype(BF16)
                        feat[p, t, runs, :, pl.ds(ZERO, VARS)] = scaled.reshape(CH // HALF, HALF, VARS)

                table[f"em{i}"], table[f"ea{i}"], table[f"eb{i}"] = edge_own, edge_first, edge_last
                table[f"dm{i}"], table[f"da{i}"], table[f"db{i}"] = node_own, node_first, node_last
                def send(i=i):
                    start_all(out_copies(step, i))

                table[f"oa{i}"], table[f"ob{i}"], table[f"send{i}"] = out_first, out_last, send
        run(ORDER_D, table)

    def wait_all(copies):
        for copy in copies:
            copy.wait()

    def start_all(copies):
        for copy in copies:
            copy.start()

    def one_step(step, carry):
        wait_all(layer_copies(step, 1) + layer_copies(step, 2))
        start_all(layer_copies(step, 3))
        encoder(step)

        def one_layer(block, carry):
            halo_slot = lax.rem(block + 1, 2)
            w, w1, w2 = (layer_weights(step, block + i) for i in range(3))
            phase(ORDER_A, far_items(1, w, resume=True), near_items(0, w, resume=True), Node(0, h, w), far_items(1, w1),
                  near_items(1, w), share_rows, w1)
            wait_halo(halo_slot)
            wait_all(layer_copies(step, block + 2))

            @pl.when(block < LAYERS - 1)
            def _():
                start_all(layer_copies(step, block + 3))

            phase(ORDER_B, far_items(0, w1, resume=True), near_items(1, w, resume=True), Node(1, h, w), far_items(0, w2),
                  near_items(0, w1), lambda: project_halo(halo_slot, w), w1)
            send_halo(1 - halo_slot)
            return carry

        lax.fori_loop(1, LAYERS, one_layer, 0)
        @pl.when(step == 0)
        def _():
            start_all(layer_copies(1, 1) + layer_copies(1, 2))
            wait_in(3)

        decoder(step)
        return carry

    lax.fori_loop(0, 2, one_step, 0)
    for copies in in_copies:
        for copy in copies[1:]:
            copy.wait_send()
    for i in range(PAIR * TILES):
        wait_all(out_copies(0, i) + out_copies(1, i))


def solution(mesh):
    row_spec = P(("dp", "gp"))
    edge_spec = P(("dp", "gp"), None, None)
    whole = P()

    def local_run(x_prev, x_cur, forcing, grid_static, g2m_feat, m2g_feat, mesh_feat, mesh_edge_feat, norm_stats,
                  w_grid_in, w_mesh_in, w_eemb_in, w_embed_out, w_edge_in, w_edge_out, w_node_in, w_node_out,
                  w_grid_self, w_out_hidden, w_out_final):
        any_spec = pl.BlockSpec(memory_space=pl.ANY)
        vmem_spec = pl.BlockSpec(memory_space=pltpu.VMEM)
        dma = pltpu.SemaphoreType.DMA
        grid_dev = x_prev.shape[0]
        shape = jax.ShapeDtypeStruct
        home = shape((RING, PAIR, TILES, PAIR, HALF, LANES), F32)
        bulk = [
            pltpu.VMEM(shape_, F32) for shape_ in (
                (3, mesh_feat.shape[0]), (6, 4, mesh_feat.shape[0]), (VARS, grid_dev), (VARS, grid_dev), (5, PAIR, grid_dev),
                (5, grid_dev), (4, grid_dev), (4, grid_dev))
        ]
        scratch = bulk + [
            pltpu.VMEM((2 * VARS + 10, LAT), BF16),
            pltpu.VMEM((3, LAT), BF16),
            pltpu.VMEM((3, 4, LAT), BF16),
            pltpu.VMEM((VARS, LAT), BF16),
            pltpu.VMEM((*home.shape[:-1], 2 * LANES), BF16),
            pltpu.VMEM((RING, TILES, PAIR, HALF, LANES), BF16),
            pltpu.VMEM(home.shape, F32),
            pltpu.VMEM((TILES, RUNS, HALF, LANES), BF16),
            pltpu.VMEM((3, PAIR, TILES, RUNS, HALF, LANES), F32),
            pltpu.VMEM((PAIR, TILES, RUNS, HALF, 2 * LANES), BF16),
            pltpu.VMEM((13, LANES, LAT), BF16),
            pltpu.VMEM((5, LAT, LAT), BF16),
            pltpu.VMEM((PAIR, LAT, LAT), BF16),
            pltpu.VMEM((LAT, LAT), BF16),
            pltpu.VMEM((LAT, LANES), BF16),
            pltpu.VMEM((1, 3 * LAT, LAT), BF16),
            pltpu.VMEM((1, LAT, LAT), BF16),
            pltpu.VMEM((1, 2 * LAT, LAT), BF16),
            pltpu.VMEM((1, LAT, LAT), BF16),
            pltpu.VMEM((SLOTS, 3 * LAT, LAT), BF16),
            pltpu.VMEM((SLOTS, LAT, LAT), BF16),
            pltpu.VMEM((SLOTS, 2 * LAT, LAT), BF16),
            pltpu.VMEM((SLOTS, LAT, LAT), BF16),
            pltpu.VMEM((6, ROWS, LAT), BF16),
            pltpu.VMEM((6, ROWS, LAT), BF16),
            pltpu.VMEM((ROWS, LAT), BF16),
            pltpu.VMEM((ROWS, LAT), BF16),
            pltpu.VMEM((LAT // LANES, TILE, LANES), F32),
            pltpu.VMEM((PAIR, ROWS, LAT), BF16),
            pltpu.VMEM((PAIR, ROWS, LAT), BF16),
            pltpu.VMEM((PAIR, ROWS, LAT), BF16),
            pltpu.VMEM((PAIR, ROWS, LAT), BF16),
            pltpu.VMEM((LAT // LANES, RUNS * PAD0, LANES), F32),
            pltpu.VMEM((LAT // LANES, RUNS * PAD1, LANES), F32),
            pltpu.VMEM((ROWS, LAT), F32),
            pltpu.VMEM((ROWS, LAT), F32),
            pltpu.VMEM((16, TILE, LAT), BF16),
            pltpu.VMEM((ROWS, LAT), BF16),
            pltpu.VMEM((4, TILE, LAT), BF16),
            pltpu.VMEM((10, TILE, LAT), F32),
            pltpu.VMEM((PAIR, RUNS, LAT), BF16),
            pltpu.VMEM((PAIR, 2, RUNS, LAT), BF16),
            dma((12,)), dma((4, RING)), dma((4, RING)), dma((4,)), dma((1, 4)), dma((SLOTS, 4)), dma((PAIR,)), dma((PAIR, PAIR)),
            dma((PAIR, PAIR * TILES, RING)), dma((PAIR, PAIR * TILES, RING)),
        ]
        homes = pl.pallas_call(
            kernel,
            out_shape=shape((PAIR, *home.shape), F32),
            in_specs=[any_spec] * 8 + [vmem_spec] + [any_spec] * 11,
            out_specs=any_spec,
            scratch_shapes=scratch,
            compiler_params=pltpu.CompilerParams(collective_id=0, has_side_effects=True, vmem_limit_bytes=63 << 20),
            name="forecast",
        )(x_prev.T, x_cur.T, forcing.T, grid_static.T, g2m_feat.T, m2g_feat.T, mesh_feat.T,
          jnp.transpose(mesh_edge_feat, (1, 2, 0)), norm_stats, w_grid_in, w_mesh_in, w_eemb_in, w_embed_out, w_edge_in,
          w_edge_out, w_node_in, w_node_out, w_grid_self, w_out_hidden, w_out_final.T)
        out = shape((VARS, grid_dev), F32)
        next_state, after_state = pl.pallas_call(
            unpack_kernel, out_shape=(out, out), in_specs=[vmem_spec], out_specs=(vmem_spec,) * 2,
            scratch_shapes=[pltpu.VMEM((grid_dev, LANES), F32)], name="unpack",
        )(homes)
        return next_state.T, after_state.T

    in_specs = (row_spec, row_spec, edge_spec, row_spec, row_spec, row_spec, row_spec, edge_spec, whole) + (whole,) * 11
    return jax.shard_map(local_run, mesh=mesh, in_specs=in_specs, out_specs=(row_spec, row_spec), check_vma=False)
```

```python
import functools

import jax
import jax.numpy as jnp
from jax import lax
from jax.experimental import pallas as pl
from jax.experimental.pallas import tpu as pltpu
from jax.sharding import PartitionSpec as P

F32 = jnp.float32
BF16 = jnp.bfloat16

RUNS = 16
RUN = 32
GRID_RUN = 2 * RUN
ROWS = RUNS * RUN
ZERO, ONE, LAST = 0, 1, -1
LAT = 512
LANES = 128
PAIR = 2
VARS = 84
PAD0 = 32
PAD1 = 48
TILE = 256
TILES = 2
HALF = TILE // RUNS
CH = 128
RING = 8
LAYERS = 16
BLOCKS = LAYERS + 2
SLOTS = 4
FAR = ((2, 1), (3, -1), (4, 4), (5, -4))
NEAR = ((0, 1), (1, -1))
ORDER_A = (
    "nh", "before", "fx0", "n1", "fx1", "bx0", "bx1", "fn0", "bn0", "fn1", "bn1", "ax0", "fx2", "fx3", "bx2",
    "na", "ax1", "bx3", "ax2", "nb", "an0", "ax3", "pr", "ps",
)
ORDER_B = (
    "nh", "before", "fx0", "fx1", "bx0", "n1", "fn1", "bx1", "fn0", "bn0", "bn1", "ax0", "fx2", "ax1", "fx3",
    "bx2", "na", "bx3", "ax2", "nb", "ax3", "an0", "ps", "pr",
)
ORDER_E = (
    "copy", "r0", "va1", "va0", "va2", "vb1", "vb0", "va3", "r1", "vb2", "vb3", "ea0", "sa0", "ea1", "sa1",
    "eb0", "ea3", "sa2", "eb1", "sb0", "ea2", "sb1", "ya2", "nh0", "eb2", "na0", "sa3", "eb3", "nb0", "sb2",
    "sb3", "ya0", "nh1", "ya1", "na1", "ps0", "pr0", "nb1", "yf0", "yb0", "yf1", "yb1", "ps1", "ya3", "pr1",
    "yf2", "za1", "yb2", "yf3", "yb3", "xa0", "share", "xa1", "za3", "xa3", "za0", "za2", "xa2", "n0", "send",
)
ORDER_D = (
    "n01", "fx1", "nh0", "fx0", "share", "bx0", "fn00", "fn01", "bn00", "bn01", "bx1", "em0", "fx2", "bx2",
    "fx3", "na0", "em1", "nb0", "n11", "wait", "dm0", "n10", "t0", "halo", "bx3", "ea0", "fn11", "fn10",
    "bn10", "eb0", "bn11", "ea1", "eb1", "nh1", "em2", "em3", "na1", "da0", "dm1", "nb1", "da1", "dm2", "db0",
    "t1", "db1", "oa0", "ea2", "eb2", "oa1", "ob0", "ea3", "dm3", "ob1", "send0", "eb3", "da2", "da3", "db2",
    "db3", "oa2", "oa3", "ob2", "ob3", "send1",
)


def dot(a, b):
    return jnp.dot(a, b, preferred_element_type=F32)


def silu(pre):
    return pre * jax.nn.sigmoid(pre)


def norm(y):
    centred = y - jnp.mean(y, axis=LAST, keepdims=True)
    return centred * lax.rsqrt(jnp.mean(centred * centred, axis=LAST, keepdims=True) + 1e-5)


def ring_place(dev):
    high = lax.div(dev, 4)
    return high * (4 + lax.rem(dev + 2, 4)) + (1 - high) * dev


def chunks():
    return range(0, TILE, CH)


def tile_rows(t):
    return pl.ds(t * TILE, TILE)


def part_rows(t, c):
    return pl.ds(t * TILE + c, CH)


def chunk_runs(c):
    return range(c // HALF, (c + CH) // HALF)


def pieces(t):
    return ((8, 16),) if t == 0 else ((0, 8), (24, 8))


def get_tiles(ref, rows):
    return jnp.concatenate([ref[j, rows, :] for j in range(ref.shape[0])], axis=ONE)


def set_tiles(ref, rows, value):
    for j in range(ref.shape[0]):
        ref[j, rows, :] = value[:, LANES * j:LANES * j + LANES]


AT_FORCE, AT_STATIC, AT_NEXT, AT_M2G, AT_G2M = 88, 96, 104, 112, 120


def columns(n):
    return pl.ds(LANES * n, LANES)


def stack(ref, rows):
    end = 0
    for at_row, value in rows:
        first = at_row // 8 * 8
        last = (at_row + value.shape[0]) // 8 * 8
        if first > end:
            ref[pl.ds(end, first - end), :] = jnp.zeros((first - end, LANES), F32)
        if last < at_row + value.shape[0]:
            ref[pl.ds(last, 8), :] = jnp.zeros((8, LANES), F32)
            end = last + 8
        else:
            end = last
        ref[pl.ds(at_row, value.shape[0]), :] = value
    if end < LANES:
        ref[pl.ds(end, LANES - end), :] = jnp.zeros((LANES - end, LANES), F32)


def unpack_kernel(homes, out0, out1, area):
    for home, out in ((homes.at[ZERO], out0), (homes.at[ONE], out1)):
        for band in range(PAIR):
            for k in range(RING):
                for p in range(PAIR):
                    for t in range(TILES):
                        row = 0
                        for r, rows in pieces(t):
                            spot = pl.ds((band * RING + k) * GRID_RUN + PAIR * r + p, rows, stride=PAIR)
                            area[spot, :] = home[k, p, t, band, pl.ds(row, rows), :]
                            row += rows
        for n in range(out.shape[1] // LANES):
            out[:, columns(n)] = jnp.transpose(area[columns(n), :])[:VARS]


def kernel(x_prev, x_cur, forcing, static, g2m_feat, m2g_feat, mesh_feat, mesh_edge_feat, stats, w_grid_in, w_mesh_in,
           w_eemb_in, w_embed_out, w_edge_in, w_edge_out, w_node_in, w_node_out, w_grid_self, w_out_hidden, w_out_final,
           out,
           mesh_raw, medge_raw, prev_raw, cur_raw, force_raw, static_raw, g2m_raw, m2g_raw,
           wgrid_raw, wmesh_raw, weemb_raw, wfin_raw, g_home, m_home, x_home,
           m_buf, x_buf, feat, we, weo, wself, woh, wof,
           enc_ei, enc_eo, enc_ni, enc_no, lay_ei, lay_eo, lay_ni, lay_no,
           edge_base, edge, h_mesh, h, hf, g2m, m2g, v, vc, proj0, proj1, recv, acc, hid, esum, dec, pre_buf,
           send_buf, halo_buf,
           raw_sem, in_send, in_recv, w_sem, enc_sem, lay_sem, halo_send, halo_recv, out_send, out_recv):
    me = lax.axis_index("gp")
    place = ring_place(me)

    def at(dev):
        return {"gp": dev}

    mesh_id = pl.DeviceIdType.MESH

    def block_copies(block, dst_refs, slot, sem):
        srcs = (w_edge_in, w_edge_out, w_node_in, w_node_out)
        return [pltpu.make_async_copy(src.at[block], dst.at[slot], sem.at[slot, i])
                for i, (src, dst) in enumerate(zip(srcs, dst_refs))]

    enc_refs = (enc_ei, enc_eo, enc_ni, enc_no)
    lay_refs = (lay_ei, lay_eo, lay_ni, lay_no)

    def enc_copies():
        return block_copies(0, enc_refs, 0, enc_sem)

    def slot_of(step, block):
        return lax.rem((BLOCKS - 1) * step + block - 1, SLOTS)

    def layer_copies(step, block):
        return block_copies(block, lay_refs, slot_of(step, block), lay_sem)

    class Weights:
        def __init__(self, refs, slot):
            self.edge = [refs[0].at[slot, pl.ds(i * LAT, LAT)] for i in range(3)]
            self.edge_out = refs[1].at[slot]
            self.node = [refs[2].at[slot, pl.ds(i * LAT, LAT)] for i in range(2)]
            self.node_out = refs[3].at[slot]

    def layer_weights(step, block):
        return Weights(lay_refs, slot_of(step, block))

    raw = [pltpu.make_async_copy(src, dst, raw_sem.at[i]) for i, (src, dst) in enumerate(
        ((mesh_feat, mesh_raw), (mesh_edge_feat, medge_raw), (x_prev, prev_raw), (x_cur, cur_raw), (forcing, force_raw),
         (static, static_raw), (g2m_feat, g2m_raw), (m2g_feat, m2g_raw),
         (w_grid_in, wgrid_raw), (w_mesh_in, wmesh_raw), (w_eemb_in, weemb_raw), (w_out_final, wfin_raw)))]
    for copy in raw:
        copy.start()
    small = [
        pltpu.make_async_copy(w_embed_out, weo, w_sem.at[0]),
        pltpu.make_async_copy(w_grid_self, wself, w_sem.at[1]),
        pltpu.make_async_copy(w_out_hidden, woh, w_sem.at[2]),
    ]
    small[0].start()

    barrier = pltpu.get_barrier_semaphore()
    for hop in range(1, RING):
        pl.semaphore_signal(barrier, inc=1, device_id=at(lax.rem(me + hop, RING)), device_id_type=mesh_id)

    mine = pl.ds(PAIR * me, PAIR)
    parts = ((m_home, m_buf.at[:, mine]), (g_home, feat.at[:, :, mine]), (x_home, x_buf.at[ZERO, :, :, mine]))

    def in_copy(part, hop):
        src, dst = parts[part]
        target = lax.rem(me + hop, RING)
        src = src.at[ring_place(target)]
        if hop == 0:
            return pltpu.make_async_copy(src, dst, in_recv.at[part, hop])
        return pltpu.make_async_remote_copy(src_ref=src, dst_ref=dst, send_sem=in_send.at[part, hop],
                                            recv_sem=in_recv.at[part, hop], device_id=at(target),
                                            device_id_type=mesh_id)

    in_copies = [[in_copy(part, hop) for hop in range(RING)] for part in range(3)]

    def wait_in(part):
        in_copies[part][0].wait()
        for copy in in_copies[part][1:]:
            copy.wait_recv()

    def start_in(part):
        for copy in in_copies[part]:
            copy.start()

    def place_of(area, n):
        ref, first = area
        return ref.at[first + n // 4, columns(n % 4)]

    prev_area, cur_area, norm_area, mesh_area, final_area = (proj0, 0), (proj0, PAIR), (proj1, 0), (proj1, 2), (proj1, 3)

    def turned(area, n):
        return jnp.transpose(place_of(area, n)[...])

    for copy in raw[:2]:
        copy.wait()
    for n in range(mesh_raw.shape[1] // LANES):
        stack(place_of(mesh_area, n), [(ZERO, mesh_raw[:, columns(n)])] + [
            (16 + 16 * k, medge_raw[k, :, columns(n)]) for k in range(6)])
    for n in range(mesh_raw.shape[1] // LANES):
        turned_rows = turned(mesh_area, n)
        for i in range(LANES // RUN):
            band, k = divmod(n * LANES + i * RUN, RING * RUN)
            for t in range(TILES):
                m_home[k // RUN, t, band] = jnp.concatenate(
                    [turned_rows[i * RUN + r:i * RUN + r + rows] for r, rows in pieces(t)], axis=ZERO).astype(BF16)
    pl.semaphore_wait(barrier, RING - 1)
    start_in(0)
    for copy in raw[2:8]:
        copy.wait()
    blocks = range(cur_raw.shape[1] // LANES)
    for n in blocks:
        stack(place_of(prev_area, n), [
            (ZERO, prev_raw[:, columns(n)]), (AT_FORCE, force_raw[:, ZERO, columns(n)]), (AT_STATIC, static_raw[:, columns(n)]),
            (AT_NEXT, force_raw[:, ONE, columns(n)]), (AT_M2G, m2g_raw[:, columns(n)]), (AT_G2M, g2m_raw[:, columns(n)])])
        stack(place_of(cur_area, n), [(ZERO, cur_raw[:, columns(n)])])
    rest = LANES - VARS
    wide_mean = jnp.concatenate([stats[ZERO:ONE, :], jnp.zeros((ONE, rest), F32)], axis=ONE)
    wide_std = jnp.concatenate([stats[ONE:PAIR, :], jnp.ones((ONE, rest), F32)], axis=ONE)
    for n in blocks:
        prev, cur = turned(prev_area, n), turned(cur_area, n)
        place_of(prev_area, n)[...] = (prev - wide_mean) / wide_std
        place_of(cur_area, n)[...] = cur
        place_of(norm_area, n)[...] = (cur - wide_mean) / wide_std
    for k in range(RING):
        for p in range(PAIR):
            for t in range(TILES):
                for band in range(PAIR):
                    def rows_of(area):
                        ref, first = area
                        return jnp.concatenate([ref[first + band, pl.ds(k * GRID_RUN + PAIR * r + p, rows, stride=PAIR), :]
                                                for r, rows in pieces(t)], axis=ZERO)
                    g_home[k, p, t, band, :, pl.ds(ZERO, LANES)] = rows_of(prev_area).astype(BF16)
                    g_home[k, p, t, band, :, pl.ds(LANES, LANES)] = rows_of(norm_area).astype(BF16)
                    x_home[k, p, t, band] = rows_of(cur_area)
    start_in(1)
    for copy in small[1:] + enc_copies() + layer_copies(0, 1) + layer_copies(0, 2):
        copy.start()

    for copy in raw[8:]:
        copy.wait()
    for n in range(LAT // LANES):
        stack(place_of(final_area, n), [(ZERO, wfin_raw[:, columns(n)].astype(F32))])
        wof[columns(n), :] = turned(final_area, n).astype(BF16)
    wide = wgrid_raw[...].astype(F32)
    recv[pl.ds(ZERO, wide.shape[0]), :] = wide
    prev_w, cur_w = recv[pl.ds(ZERO, VARS), :], recv[pl.ds(VARS, VARS), :]
    force_w, static_w = recv[pl.ds(2 * VARS, 5), :], recv[pl.ds(2 * VARS + 5, 5), :]
    spread = [[(0, wmesh_raw[...].astype(F32))], [(AT_G2M, weemb_raw[0].astype(F32))], [(AT_M2G, weemb_raw[1].astype(F32))]]
    spread += [[(16 + 16 * k, weemb_raw[2].astype(F32))] for k in range(6)]
    spread += [[(0, prev_w), (AT_FORCE, force_w), (AT_STATIC, static_w)], [(0, cur_w)]]
    spread += [[(0, cur_w), (AT_STATIC, static_w), (AT_NEXT, force_w)], [(0, prev_w)]]
    for i, rows in enumerate(spread):
        base = LANES * (i % 4)
        acc[pl.ds(base, LANES), :] = jnp.zeros((LANES, LAT), F32)
        for at_row, value in rows:
            acc[pl.ds(base + at_row, value.shape[0]), :] = value
        we[i] = acc[pl.ds(base, LANES), :].astype(BF16)

    def pipeline(items):
        depth = max(len(item) for item in items)
        for beat in range(len(items) + depth - 1):
            for stage in range(depth):
                index = beat - stage
                if 0 <= index < len(items) and stage < len(items[index]):
                    items[index][stage](index)

    def hide(slot, pre, extra=None):
        for c in chunks():
            value = pre[c:c + CH]
            if extra is not None:
                value = value + extra(c)
            hid[slot, pl.ds(c, CH), :] = silu(value).astype(BF16)

    def embed_item(load, w_first, second, store):
        def first(i):
            hide(i % PAIR, dot(load(), we[w_first]))

        def last(i):
            y = dot(hid[i % 2], weo[second])
            for c in chunks():
                store(c, norm(y[c:c + CH]).astype(BF16))

        return [first, last]

    wait_in(0)
    small[0].wait()
    def next_run(ref, *index):
        first = ref[(*index, pl.ds(ONE, RUNS - 1), slice(None), pl.ds(ZERO, LANES))]
        last = ref[(*index, pl.ds(ZERO, ONE), slice(None), pl.ds(ZERO, LANES))]
        return jnp.concatenate([first, last], axis=ZERO).reshape(TILE, LANES)

    mesh_rows = [next_run(m_buf, t) for t in range(TILES)]
    items = []
    for t in range(TILES):
        def store_mesh(c, value, t=t):
            h_mesh[part_rows(t, c), :] = value
        items.append(embed_item(lambda t=t: mesh_rows[t], 0, 1, store_mesh))
        for k in range(6):
            def store_edge(c, value, t=t, k=k):
                edge_base[k, part_rows(t, c), :] = value
            items.append(embed_item(lambda t=t: mesh_rows[t], 3 + k, 4, store_edge))
    pipeline(items)

    wait_in(1)
    start_in(PAIR)
    items = []
    for t in range(TILES):
        for p in range(PAIR):
            def store_m2g(c, value, t=t, p=p):
                m2g[p, part_rows(t, c), :] = value
            def store_g2m(c, value, t=t, p=p):
                g2m[p, part_rows(t, c), :] = value
            items.append(embed_item(lambda t=t, p=p: next_run(feat, p, t), 1, 2, store_g2m))
            items.append(embed_item(lambda t=t, p=p: feat[p, t, :, :, pl.ds(ZERO, LANES)].reshape(TILE, LANES), 2, 3, store_m2g))
    pipeline(items)
    for copy in small[1:] + enc_copies():
        copy.wait()

    left = ring_place(lax.rem(place + RING - 1, RING))
    right = ring_place(lax.rem(place + 1, RING))

    def halo_copies(slot):
        return [
            pltpu.make_async_remote_copy(src_ref=send_buf.at[side], dst_ref=halo_buf.at[slot, side],
                                         send_sem=halo_send.at[side], recv_sem=halo_recv.at[slot, side],
                                         device_id=at(target), device_id_type=mesh_id)
            for side, target in ((0, left), (1, right))
        ]

    def send_halo(slot):
        first = get_tiles(hf, pl.ds(ZERO, RUNS, stride=HALF))
        final = get_tiles(hf, pl.ds(HALF - 1, RUNS, stride=HALF))
        first_on = jnp.concatenate([first[1:], first[:1]], axis=ZERO)
        final_back = jnp.concatenate([final[-1:], final[:-1]], axis=ZERO)
        send_buf[0] = jnp.where(place == 0, first_on, first).astype(BF16)
        send_buf[1] = jnp.where(place == RING - 1, final_back, final).astype(BF16)
        for copy in halo_copies(slot):
            copy.start()

    def wait_halo(slot):
        for copy in halo_copies(slot):
            copy.wait()

    def project_halo(slot, w):
        rows = jnp.concatenate([halo_buf[slot, 0], halo_buf[slot, 1]], axis=ZERO)
        out = dot(rows, w.edge[1][...])
        set_tiles(proj1, pl.ds(8 + RUN, RUNS, stride=PAD1), out[:RUNS])
        set_tiles(proj1, pl.ds(7, RUNS, stride=PAD1), out[RUNS:])

    class Edge:
        def __init__(self, t, k, w, slot, run_shift=0, row_shift=0, source=None, first=False, final=False, keep=None):
            self.t, self.k, self.w, self.slot, self.keep = t, k, w, slot, keep
            self.run_shift, self.row_shift, self.first, self.final = run_shift, row_shift, first, final
            self.source = edge if source is None else source
            self.pre = None

        def a(self):
            self.pre = dot(self.source[self.k, tile_rows(self.t), :], self.w.edge[0][...])
            if self.keep is not None:
                for c in chunks():
                    pre_buf[self.keep, pl.ds(c, CH), :] = self.pre[c:c + CH]

        def resume(self):
            self.pre = pre_buf.at[self.keep]

        def extra(self, c):
            got = []
            for q in chunk_runs(c):
                base = (q + self.run_shift) % RUNS
                for r, n in pieces(self.t):
                    if self.t == 0:
                        got.append(get_tiles(proj0, pl.ds(base * PAD0 + r + self.row_shift, n)))
                    else:
                        got.append(get_tiles(proj1, pl.ds(base * PAD1 + 8 + r + self.row_shift, n)))
            return jnp.concatenate(got, axis=ZERO) + recv[part_rows(self.t, c), :]

        def fin(self):
            hide(self.slot, self.pre, self.extra)

        def b(self):
            y = dot(hid[self.slot], self.w.edge_out[...])
            for c in chunks():
                part = part_rows(self.t, c)
                value = (self.source[self.k, part, :].astype(F32) + norm(y[c:c + CH])).astype(BF16)
                edge[self.k, part, :] = value
                total = value.astype(F32)
                if not self.first:
                    total = total + acc[part, :]
                if self.final:
                    esum[part, :] = total.astype(BF16)
                else:
                    acc[part, :] = total

    class Node:
        def __init__(self, t, base, w):
            self.t, self.base, self.w, self.slot = t, base, w, 6 + t

        def own(self):
            self.pre = dot(self.base[tile_rows(self.t), :], self.w.node[0][...])

        def a(self):
            hide(self.slot, self.pre + dot(esum[tile_rows(self.t), :], self.w.node[1][...]))

        def b(self):
            y = dot(hid[self.slot], self.w.node_out[...])
            for c in chunks():
                part = part_rows(self.t, c)
                value = (self.base[part, :].astype(F32) + norm(y[c:c + CH])).astype(BF16)
                h[part, :] = value
                if self.t == 1:
                    set_tiles(hf, pl.ds(c, CH), value.astype(F32))

    def project_send(t, w):
        out = dot(h[tile_rows(t), :], w.edge[1][...])
        for q in range(RUNS):
            row = q * HALF
            for r, n in pieces(t):
                if t == 0:
                    set_tiles(proj0, pl.ds(q * PAD0 + r, n), out[row:row + n])
                else:
                    set_tiles(proj1, pl.ds(q * PAD1 + 8 + r, n), out[row:row + n])
                row += n
        if t == 1:
            for r in (7, 24):
                set_tiles(proj0, pl.ds(r, RUNS, stride=PAD0), get_tiles(proj1, pl.ds(8 + r, RUNS, stride=PAD1)))

    def project_recv(t, w):
        out = dot(h[tile_rows(t), :], w.edge[2][...])
        for c in chunks():
            recv[part_rows(t, c), :] = out[c:c + CH]

    def project(t, w):
        project_send(t, w)
        project_recv(t, w)

    def share_rows():
        for r in (8, 23):
            set_tiles(proj1, pl.ds(8 + r, RUNS, stride=PAD1), get_tiles(proj0, pl.ds(r, RUNS, stride=PAD0)))

    def far_items(t, w, source=None, resume=False):
        items = [Edge(t, k, w, n, run_shift=s, source=source, first=n == 0, keep=4 * t + n) for n, (k, s) in enumerate(FAR)]
        if resume:
            for item in items:
                item.resume()
        return items

    def near_items(t, w, resume=False):
        items = [Edge(t, k, w, 4 + n, row_shift=s, final=n == 1, keep=8 + t if n == 0 else None)
                 for n, (k, s) in enumerate(NEAR)]
        if resume:
            items[0].resume()
        return items

    def phase(order, x, n, node, next_x, next_n, before, w_next):
        table = {"before": before, "n1": n[1].a, "nh": node.own, "na": node.a, "nb": node.b, "an0": next_n[0].a,
                 "ps": lambda: project_send(node.t, w_next), "pr": lambda: project_recv(node.t, w_next)}
        for i in range(4):
            table[f"fx{i}"], table[f"bx{i}"], table[f"ax{i}"] = x[i].fin, x[i].b, next_x[i].a
        for i in range(PAIR):
            table[f"fn{i}"], table[f"bn{i}"] = n[i].fin, n[i].b
        run(order, table)

    def run(order, table):
        for name in order:
            table[name]()

    def encoder(step):
        w = Weights(enc_refs, ZERO)
        w1 = layer_weights(step, 1)
        w2 = layer_weights(step, 2)
        table = {"send": lambda: send_halo(ZERO), "share": share_rows}

        def spread():
            for k in range(6):
                for t in range(TILES):
                    if t == 1 or k < PAIR:
                        edge[k, tile_rows(t), :] = edge_base[k, tile_rows(t), :]

        table["copy"] = spread
        y, x, z, n = far_items(0, w1, edge_base), far_items(1, w1), far_items(0, w2), near_items(0, w1)
        for k in range(4):
            table[f"ya{k}"], table[f"yf{k}"], table[f"yb{k}"] = y[k].a, y[k].fin, y[k].b
            table[f"xa{k}"], table[f"za{k}"] = x[k].a, z[k].a
        table["n0"] = n[0].a
        for t in range(TILES):
            def back(t=t):
                out = dot(h_mesh[tile_rows(t), :], w.edge[2][...])
                for c in chunks():
                    recv[part_rows(t, c), :] = out[c:c + CH]

            node = Node(t, h_mesh, w)
            table[f"r{t}"], table[f"nh{t}"], table[f"na{t}"], table[f"nb{t}"] = back, node.own, node.a, node.b
            table[f"ps{t}"], table[f"pr{t}"] = functools.partial(project_send, t, w1), functools.partial(project_recv, t, w1)
            for p in range(PAIR):
                i = PAIR * t + p
                low, high = 8 + i, 12 + i

                def in_first(t=t, p=p, low=low):
                    hide(low, dot(feat[p, t].reshape(TILE, 2 * LANES), we[pl.ds(9 + PAIR * step, PAIR)].reshape(2 * LANES, LAT)))

                def in_last(t=t, p=p, low=low):
                    y = dot(hid[low], weo[ZERO])
                    for c in chunks():
                        v[p, part_rows(t, c), :] = norm(y[c:c + CH]).astype(BF16)

                def edge_first(t=t, p=p, high=high):
                    pre = dot(g2m[p, tile_rows(t), :], w.edge[0][...]) + dot(v[p, tile_rows(t), :], w.edge[1][...])
                    hide(high, pre, lambda c: recv[part_rows(t, c), :])

                def edge_last(t=t, p=p, high=high):
                    y = dot(hid[high], w.edge_out[...])
                    for c in chunks():
                        part = part_rows(t, c)
                        total = (g2m[p, part, :].astype(F32) + norm(y[c:c + CH])).astype(BF16).astype(F32)
                        if p == 0:
                            acc[part, :] = total
                        else:
                            esum[part, :] = (acc[part, :] + total).astype(BF16)

                def self_first(t=t, p=p, low=low):
                    hide(low, dot(v[p, tile_rows(t), :], wself[ZERO]))

                def self_last(t=t, p=p, low=low):
                    y = dot(hid[low], wself[ONE])
                    for c in chunks():
                        part = part_rows(t, c)
                        vc[p, part, :] = (v[p, part, :].astype(F32) + norm(y[c:c + CH])).astype(BF16)

                table[f"va{i}"], table[f"vb{i}"], table[f"ea{i}"], table[f"eb{i}"] = in_first, in_last, edge_first, edge_last
                table[f"sa{i}"], table[f"sb{i}"] = self_first, self_last
        run(ORDER_E, table)

    def out_copies(step, t):
        copies = []
        for hop in range(RING):
            target = lax.rem(me + hop, RING)
            src, dst = x_buf.at[step + 1, :, t, pl.ds(PAIR * target, PAIR)], out.at[step, place, :, t]
            if hop == 0:
                copies.append(pltpu.make_async_copy(src, dst, out_recv.at[step, t, hop]))
            else:
                copies.append(pltpu.make_async_remote_copy(
                    src_ref=src, dst_ref=dst, send_sem=out_send.at[step, t, hop], recv_sem=out_recv.at[step, t, hop],
                    device_id=at(target), device_id_type=mesh_id))
        return copies

    def decoder(step):
        w16 = layer_weights(step, LAYERS)
        w = layer_weights(step, BLOCKS - 1)
        in_mean = stats[ZERO:ONE, :]
        in_std = stats[ONE:PAIR, :]
        diff_mean, diff_std = (jnp.concatenate([stats[i:i + 1, :], jnp.zeros((ONE, LANES - VARS), F32)], axis=ONE) for i in (2, 3))
        halo_slot = lax.rem(LAYERS + 1, 2)
        table = {"share": share_rows, "wait": lambda: wait_halo(halo_slot), "halo": lambda: project_halo(halo_slot, w16)}
        x = far_items(1, w16, resume=True)
        for k in range(4):
            table[f"fx{k}"], table[f"bx{k}"] = x[k].fin, x[k].b
        for t in range(TILES):
            node = Node(t, h, w16)
            table[f"nh{t}"], table[f"na{t}"], table[f"nb{t}"] = node.own, node.a, node.b
            near = near_items(t, w16, resume=t == 0)
            for k in range(PAIR):
                table[f"n{t}{k}"], table[f"fn{t}{k}"], table[f"bn{t}{k}"] = near[k].a, near[k].fin, near[k].b

            def back(t=t):
                out = dot(h[tile_rows(t), :], w.edge[1][...])
                for c in chunks():
                    recv[part_rows(t, c), :] = out[c:c + CH]

            def send(t=t):
                start_all(out_copies(step, t))

            table[f"t{t}"], table[f"send{t}"] = back, send
            for p in range(PAIR):
                i = PAIR * t + p
                low, high = 8 + i, 12 + i
                held = {}

                def edge_own(t=t, p=p, held=held):
                    held["edge"] = dot(m2g[p, tile_rows(t), :], w.edge[0][...]) + dot(vc[p, tile_rows(t), :], w.edge[2][...])

                def edge_first(t=t, low=low, held=held):
                    hide(low, held["edge"], lambda c: recv[part_rows(t, c), :])

                def edge_last(t=t, p=p, low=low, i=i):
                    y = dot(hid[low], w.edge_out[...])
                    for c in chunks():
                        part = part_rows(t, c)
                        dec[i, pl.ds(c, CH), :] = (m2g[p, part, :].astype(F32) + norm(y[c:c + CH])).astype(BF16)

                def node_own(t=t, p=p, held=held):
                    held["node"] = dot(vc[p, tile_rows(t), :], w.node[0][...])

                def node_first(high=high, i=i, held=held):
                    hide(high, held["node"] + dot(dec[i], w.node[1][...]))

                def node_last(t=t, p=p, high=high):
                    y = dot(hid[high], w.node_out[...])
                    for c in chunks():
                        part = part_rows(t, c)
                        v[p, part, :] = (vc[p, part, :].astype(F32) + norm(y[c:c + CH])).astype(BF16)

                def out_first(t=t, p=p, low=low):
                    hide(low, dot(v[p, tile_rows(t), :], woh[...]))

                def out_last(t=t, p=p, low=low):
                    pred = dot(hid[low], wof[...])
                    for c in chunks():
                        runs = pl.ds(c // HALF, CH // HALF)
                        now = x_buf[step, p, t, runs].reshape(CH, LANES)
                        new = now + diff_std * pred[c:c + CH] + diff_mean
                        x_buf[step + 1, p, t, runs] = new.reshape(CH // HALF, HALF, LANES)
                        scaled = ((new[:, :VARS] - in_mean) / in_std).astype(BF16)
                        feat[p, t, runs, :, pl.ds(ZERO, VARS)] = scaled.reshape(CH // HALF, HALF, VARS)

                table[f"em{i}"], table[f"ea{i}"], table[f"eb{i}"] = edge_own, edge_first, edge_last
                table[f"dm{i}"], table[f"da{i}"], table[f"db{i}"] = node_own, node_first, node_last
                table[f"oa{i}"], table[f"ob{i}"] = out_first, out_last
        run(ORDER_D, table)

    def wait_all(copies):
        for copy in copies:
            copy.wait()

    def start_all(copies):
        for copy in copies:
            copy.start()

    def one_step(step, carry):
        wait_all(layer_copies(step, 1) + layer_copies(step, 2))
        start_all(layer_copies(step, 3))
        encoder(step)

        def one_layer(block, carry):
            halo_slot = lax.rem(block + 1, 2)
            w, w1, w2 = (layer_weights(step, block + i) for i in range(3))
            phase(ORDER_A, far_items(1, w, resume=True), near_items(0, w, resume=True), Node(0, h, w), far_items(1, w1),
                  near_items(1, w), share_rows, w1)
            wait_halo(halo_slot)
            wait_all(layer_copies(step, block + 2))

            @pl.when(block < LAYERS - 1)
            def _():
                start_all(layer_copies(step, block + 3))

            phase(ORDER_B, far_items(0, w1, resume=True), near_items(1, w, resume=True), Node(1, h, w), far_items(0, w2),
                  near_items(0, w1), lambda: project_halo(halo_slot, w), w1)
            send_halo(1 - halo_slot)
            return carry

        lax.fori_loop(1, LAYERS, one_layer, 0)
        @pl.when(step == 0)
        def _():
            start_all(layer_copies(1, 1) + layer_copies(1, 2))
            wait_in(PAIR)

        decoder(step)
        return carry

    lax.fori_loop(0, 2, one_step, 0)
    for part in range(3):
        for copy in in_copies[part][1:]:
            copy.wait_send()
    for t in range(TILES):
        wait_all(out_copies(0, t) + out_copies(1, t))


def solution(mesh):
    row_spec = P(("dp", "gp"))
    edge_spec = P(("dp", "gp"), None, None)
    whole = P()

    def local_run(x_prev, x_cur, forcing, grid_static, g2m_feat, m2g_feat, mesh_feat, mesh_edge_feat, norm_stats,
                  w_grid_in, w_mesh_in, w_eemb_in, w_embed_out, w_edge_in, w_edge_out, w_node_in, w_node_out,
                  w_grid_self, w_out_hidden, w_out_final):
        any_spec = pl.BlockSpec(memory_space=pl.ANY)
        vmem_spec = pl.BlockSpec(memory_space=pltpu.VMEM)
        dma = pltpu.SemaphoreType.DMA
        grid_dev = x_prev.shape[0]
        shape = jax.ShapeDtypeStruct
        home = shape((RING, PAIR, TILES, PAIR, HALF, LANES), F32)
        bulk = [
            pltpu.VMEM(shape_, F32) for shape_ in (
                (3, mesh_feat.shape[0]), (6, 4, mesh_feat.shape[0]), (VARS, grid_dev), (VARS, grid_dev), (5, PAIR, grid_dev),
                (5, grid_dev), (4, grid_dev), (4, grid_dev))
        ]
        scratch = bulk + [
            pltpu.VMEM((2 * VARS + 10, LAT), BF16),
            pltpu.VMEM((3, LAT), BF16),
            pltpu.VMEM((3, 4, LAT), BF16),
            pltpu.VMEM((VARS, LAT), BF16),
            pltpu.VMEM((*home.shape[:-1], 2 * LANES), BF16),
            pltpu.VMEM((RING, TILES, PAIR, HALF, LANES), BF16),
            pltpu.VMEM(home.shape, F32),
            pltpu.VMEM((TILES, RUNS, HALF, LANES), BF16),
            pltpu.VMEM((3, PAIR, TILES, RUNS, HALF, LANES), F32),
            pltpu.VMEM((PAIR, TILES, RUNS, HALF, 2 * LANES), BF16),
            pltpu.VMEM((13, LANES, LAT), BF16),
            pltpu.VMEM((5, LAT, LAT), BF16),
            pltpu.VMEM((PAIR, LAT, LAT), BF16),
            pltpu.VMEM((LAT, LAT), BF16),
            pltpu.VMEM((LAT, LANES), BF16),
            pltpu.VMEM((1, 3 * LAT, LAT), BF16),
            pltpu.VMEM((1, LAT, LAT), BF16),
            pltpu.VMEM((1, 2 * LAT, LAT), BF16),
            pltpu.VMEM((1, LAT, LAT), BF16),
            pltpu.VMEM((SLOTS, 3 * LAT, LAT), BF16),
            pltpu.VMEM((SLOTS, LAT, LAT), BF16),
            pltpu.VMEM((SLOTS, 2 * LAT, LAT), BF16),
            pltpu.VMEM((SLOTS, LAT, LAT), BF16),
            pltpu.VMEM((6, ROWS, LAT), BF16),
            pltpu.VMEM((6, ROWS, LAT), BF16),
            pltpu.VMEM((ROWS, LAT), BF16),
            pltpu.VMEM((ROWS, LAT), BF16),
            pltpu.VMEM((LAT // LANES, TILE, LANES), F32),
            pltpu.VMEM((PAIR, ROWS, LAT), BF16),
            pltpu.VMEM((PAIR, ROWS, LAT), BF16),
            pltpu.VMEM((PAIR, ROWS, LAT), BF16),
            pltpu.VMEM((PAIR, ROWS, LAT), BF16),
            pltpu.VMEM((LAT // LANES, RUNS * PAD0, LANES), F32),
            pltpu.VMEM((LAT // LANES, RUNS * PAD1, LANES), F32),
            pltpu.VMEM((ROWS, LAT), F32),
            pltpu.VMEM((ROWS, LAT), F32),
            pltpu.VMEM((16, TILE, LAT), BF16),
            pltpu.VMEM((ROWS, LAT), BF16),
            pltpu.VMEM((4, TILE, LAT), BF16),
            pltpu.VMEM((10, TILE, LAT), F32),
            pltpu.VMEM((PAIR, RUNS, LAT), BF16),
            pltpu.VMEM((PAIR, 2, RUNS, LAT), BF16),
            dma((12,)), dma((3, RING)), dma((3, RING)), dma((4,)), dma((1, 4)), dma((SLOTS, 4)), dma((PAIR,)), dma((PAIR, PAIR)),
            dma((PAIR, TILES, RING)), dma((PAIR, TILES, RING)),
        ]
        homes = pl.pallas_call(
            kernel,
            out_shape=shape((PAIR, *home.shape), F32),
            in_specs=[any_spec] * 8 + [vmem_spec] + [any_spec] * 11,
            out_specs=any_spec,
            scratch_shapes=scratch,
            compiler_params=pltpu.CompilerParams(collective_id=0, has_side_effects=True, vmem_limit_bytes=63 << 20),
            name="forecast",
        )(x_prev.T, x_cur.T, forcing.T, grid_static.T, g2m_feat.T, m2g_feat.T, mesh_feat.T,
          jnp.transpose(mesh_edge_feat, (1, 2, 0)), norm_stats, w_grid_in, w_mesh_in, w_eemb_in, w_embed_out, w_edge_in,
          w_edge_out, w_node_in, w_node_out, w_grid_self, w_out_hidden, w_out_final.T)
        out = shape((VARS, grid_dev), F32)
        next_state, after_state = pl.pallas_call(
            unpack_kernel, out_shape=(out, out), in_specs=[vmem_spec], out_specs=(vmem_spec,) * 2,
            scratch_shapes=[pltpu.VMEM((grid_dev, LANES), F32)], name="unpack",
        )(homes)
        return next_state.T, after_state.T

    in_specs = (row_spec, row_spec, edge_spec, row_spec, row_spec, row_spec, row_spec, edge_spec, whole) + (whole,) * 11
    return jax.shard_map(local_run, mesh=mesh, in_specs=in_specs, out_specs=(row_spec, row_spec), check_vma=False)
```

```python
import functools

import jax
import jax.numpy as jnp
from jax import lax
from jax.experimental import pallas as pl
from jax.experimental.pallas import tpu as pltpu
from jax.sharding import PartitionSpec as P

F32 = jnp.float32
BF16 = jnp.bfloat16

RUNS = 16
RUN = 32
GRID_RUN = 2 * RUN
ROWS = RUNS * RUN
ZERO, ONE, LAST = 0, 1, -1
LAT = 512
LANES = 128
PAIR = 2
VARS = 84
PAD0 = 32
PAD1 = 48
TILE = 256
TILES = 2
HALF = TILE // RUNS
CH = 128
RING = 8
LAYERS = 16
BLOCKS = LAYERS + 2
SLOTS = 4
FAR = ((2, 1), (3, -1), (4, 4), (5, -4))
NEAR = ((0, 1), (1, -1))
ORDER_A = (
    "nh", "before", "fx0", "n1", "fx1", "bx0", "bx1", "fn0", "bn0", "fn1", "bn1", "ax0", "fx2", "fx3", "bx2",
    "na", "ax1", "bx3", "ax2", "nb", "an0", "ax3", "pr", "ps",
)
ORDER_B = (
    "nh", "before", "fx0", "fx1", "bx0", "n1", "fn1", "bx1", "fn0", "bn0", "bn1", "ax0", "fx2", "ax1", "fx3",
    "bx2", "na", "bx3", "ax2", "nb", "ax3", "an0", "ps", "pr",
)
ORDER_E = (
    "copy", "r0", "va1", "va0", "va2", "vb1", "vb0", "va3", "r1", "vb2", "vb3", "ea0", "sa0", "ea1", "sa1",
    "eb0", "ea3", "sa2", "eb1", "sb0", "ea2", "sb1", "ya2", "nh0", "eb2", "na0", "sa3", "eb3", "nb0", "sb2",
    "sb3", "ya0", "nh1", "ya1", "na1", "ps0", "pr0", "nb1", "yf0", "yb0", "yf1", "yb1", "ps1", "ya3", "pr1",
    "yf2", "za1", "yb2", "yf3", "yb3", "xa0", "share", "xa1", "za3", "xa3", "za0", "za2", "xa2", "n0", "send",
)
ORDER_D = (
    "n01", "fx1", "nh0", "fx0", "share", "bx0", "fn00", "fn01", "bn00", "bn01", "bx1", "em0", "fx2", "bx2",
    "fx3", "na0", "em1", "nb0", "n11", "wait", "dm0", "n10", "t0", "halo", "bx3", "ea0", "fn11", "fn10",
    "bn10", "eb0", "bn11", "ea1", "eb1", "nh1", "em2", "em3", "na1", "da0", "dm1", "nb1", "da1", "dm2", "db0",
    "t1", "db1", "oa0", "ea2", "eb2", "oa1", "ob0", "ea3", "dm3", "ob1", "eb3", "da2", "da3", "db2", "db3",
    "oa2", "oa3", "ob2", "ob3", "send1", "send0",
)


def dot(a, b):
    return jnp.dot(a, b, preferred_element_type=F32)


def silu(pre):
    return pre * jax.nn.sigmoid(pre)


def norm(y):
    centred = y - jnp.mean(y, axis=LAST, keepdims=True)
    return centred * lax.rsqrt(jnp.mean(centred * centred, axis=LAST, keepdims=True) + 1e-5)


def ring_place(dev):
    high = lax.div(dev, 4)
    return high * (4 + lax.rem(dev + 2, 4)) + (1 - high) * dev


def chunks():
    return range(0, TILE, CH)


def tile_rows(t):
    return pl.ds(t * TILE, TILE)


def part_rows(t, c):
    return pl.ds(t * TILE + c, CH)


def chunk_runs(c):
    return range(c // HALF, (c + CH) // HALF)


def pieces(t):
    return ((8, 16),) if t == 0 else ((0, 8), (24, 8))


def get_tiles(ref, rows):
    return jnp.concatenate([ref[j, rows, :] for j in range(ref.shape[0])], axis=ONE)


def set_tiles(ref, rows, value):
    for j in range(ref.shape[0]):
        ref[j, rows, :] = value[:, LANES * j:LANES * j + LANES]


AT_FORCE, AT_STATIC, AT_NEXT, AT_M2G, AT_G2M = 88, 96, 104, 112, 120


def columns(n):
    return pl.ds(LANES * n, LANES)


def stack(ref, rows):
    end = 0
    for at_row, value in rows:
        first = at_row // 8 * 8
        last = (at_row + value.shape[0]) // 8 * 8
        if first > end:
            ref[pl.ds(end, first - end), :] = jnp.zeros((first - end, LANES), F32)
        if last < at_row + value.shape[0]:
            ref[pl.ds(last, 8), :] = jnp.zeros((8, LANES), F32)
            end = last + 8
        else:
            end = last
        ref[pl.ds(at_row, value.shape[0]), :] = value
    if end < LANES:
        ref[pl.ds(end, LANES - end), :] = jnp.zeros((LANES - end, LANES), F32)


def unpack_kernel(homes, out0, out1, area):
    for home, out in ((homes.at[ZERO], out0), (homes.at[ONE], out1)):
        for band in range(PAIR):
            for k in range(RING):
                for p in range(PAIR):
                    for t in range(TILES):
                        row = 0
                        for r, rows in pieces(t):
                            spot = pl.ds((band * RING + k) * GRID_RUN + PAIR * r + p, rows, stride=PAIR)
                            area[spot, :] = home[k, p, t, band, pl.ds(row, rows), :]
                            row += rows
        for n in range(out.shape[1] // LANES):
            out[:, columns(n)] = jnp.transpose(area[columns(n), :])[:VARS]


def kernel(x_prev, x_cur, forcing, static, g2m_feat, m2g_feat, mesh_feat, mesh_edge_feat, stats, w_grid_in, w_mesh_in,
           w_eemb_in, w_embed_out, w_edge_in, w_edge_out, w_node_in, w_node_out, w_grid_self, w_out_hidden, w_out_final,
           out,
           mesh_raw, medge_raw, prev_raw, cur_raw, force_raw, static_raw, g2m_raw, m2g_raw,
           wgrid_raw, wmesh_raw, weemb_raw, wfin_raw, g_home, m_home, x_home,
           m_buf, x_buf, feat, we, weo, wself, woh, wof,
           enc_ei, enc_eo, enc_ni, enc_no, lay_ei, lay_eo, lay_ni, lay_no,
           edge_base, edge, h_mesh, h, hf, g2m, m2g, v, vc, proj0, proj1, recv, acc, hid, esum, dec, pre_buf,
           send_buf, halo_buf,
           raw_sem, in_send, in_recv, w_sem, enc_sem, lay_sem, halo_send, halo_recv, out_send, out_recv):
    me = lax.axis_index("gp")
    place = ring_place(me)

    def at(dev):
        return {"gp": dev}

    mesh_id = pl.DeviceIdType.MESH

    def block_copies(block, dst_refs, slot, sem):
        srcs = (w_edge_in, w_edge_out, w_node_in, w_node_out)
        return [pltpu.make_async_copy(src.at[block], dst.at[slot], sem.at[slot, i])
                for i, (src, dst) in enumerate(zip(srcs, dst_refs))]

    enc_refs = (enc_ei, enc_eo, enc_ni, enc_no)
    lay_refs = (lay_ei, lay_eo, lay_ni, lay_no)

    def enc_copies():
        return block_copies(0, enc_refs, 0, enc_sem)

    def slot_of(step, block):
        return lax.rem((BLOCKS - 1) * step + block - 1, SLOTS)

    def layer_copies(step, block):
        return block_copies(block, lay_refs, slot_of(step, block), lay_sem)

    class Weights:
        def __init__(self, refs, slot):
            self.edge = [refs[0].at[slot, pl.ds(i * LAT, LAT)] for i in range(3)]
            self.edge_out = refs[1].at[slot]
            self.node = [refs[2].at[slot, pl.ds(i * LAT, LAT)] for i in range(2)]
            self.node_out = refs[3].at[slot]

    def layer_weights(step, block):
        return Weights(lay_refs, slot_of(step, block))

    raw = [pltpu.make_async_copy(src, dst, raw_sem.at[i]) for i, (src, dst) in enumerate(
        ((mesh_feat, mesh_raw), (mesh_edge_feat, medge_raw), (x_prev, prev_raw), (x_cur, cur_raw), (forcing, force_raw),
         (static, static_raw), (g2m_feat, g2m_raw), (m2g_feat, m2g_raw),
         (w_grid_in, wgrid_raw), (w_mesh_in, wmesh_raw), (w_eemb_in, weemb_raw), (w_out_final, wfin_raw)))]
    for copy in raw:
        copy.start()
    small = [
        pltpu.make_async_copy(w_embed_out, weo, w_sem.at[0]),
        pltpu.make_async_copy(w_grid_self, wself, w_sem.at[1]),
        pltpu.make_async_copy(w_out_hidden, woh, w_sem.at[2]),
    ]
    small[0].start()

    barrier = pltpu.get_barrier_semaphore()
    for hop in range(1, RING):
        pl.semaphore_signal(barrier, inc=1, device_id=at(lax.rem(me + hop, RING)), device_id_type=mesh_id)

    mine = pl.ds(PAIR * me, PAIR)
    parts = ((m_home, m_buf.at[:, mine]), (g_home, feat.at[:, :, mine]), (x_home, x_buf.at[ZERO, :, :, mine]))

    def in_copy(part, hop):
        src, dst = parts[part]
        target = lax.rem(me + hop, RING)
        src = src.at[ring_place(target)]
        if hop == 0:
            return pltpu.make_async_copy(src, dst, in_recv.at[part, hop])
        return pltpu.make_async_remote_copy(src_ref=src, dst_ref=dst, send_sem=in_send.at[part, hop],
                                            recv_sem=in_recv.at[part, hop], device_id=at(target),
                                            device_id_type=mesh_id)

    in_copies = [[in_copy(part, hop) for hop in range(RING)] for part in range(3)]

    def wait_in(part):
        in_copies[part][0].wait()
        for copy in in_copies[part][1:]:
            copy.wait_recv()

    def start_in(part):
        for copy in in_copies[part]:
            copy.start()

    def place_of(area, n):
        ref, first = area
        return ref.at[first + n // 4, columns(n % 4)]

    prev_area, cur_area, norm_area, mesh_area, final_area = (proj0, 0), (proj0, PAIR), (proj1, 0), (proj1, 2), (proj1, 3)

    def turned(area, n):
        return jnp.transpose(place_of(area, n)[...])

    for copy in raw[:2]:
        copy.wait()
    for n in range(mesh_raw.shape[1] // LANES):
        stack(place_of(mesh_area, n), [(ZERO, mesh_raw[:, columns(n)])] + [
            (16 + 16 * k, medge_raw[k, :, columns(n)]) for k in range(6)])
    for n in range(mesh_raw.shape[1] // LANES):
        turned_rows = turned(mesh_area, n)
        for i in range(LANES // RUN):
            band, k = divmod(n * LANES + i * RUN, RING * RUN)
            for t in range(TILES):
                m_home[k // RUN, t, band] = jnp.concatenate(
                    [turned_rows[i * RUN + r:i * RUN + r + rows] for r, rows in pieces(t)], axis=ZERO).astype(BF16)
    pl.semaphore_wait(barrier, RING - 1)
    start_in(0)
    for copy in raw[2:8]:
        copy.wait()
    blocks = range(cur_raw.shape[1] // LANES)
    for n in blocks:
        stack(place_of(prev_area, n), [
            (ZERO, prev_raw[:, columns(n)]), (AT_FORCE, force_raw[:, ZERO, columns(n)]), (AT_STATIC, static_raw[:, columns(n)]),
            (AT_NEXT, force_raw[:, ONE, columns(n)]), (AT_M2G, m2g_raw[:, columns(n)]), (AT_G2M, g2m_raw[:, columns(n)])])
        stack(place_of(cur_area, n), [(ZERO, cur_raw[:, columns(n)])])
    rest = LANES - VARS
    wide_mean = jnp.concatenate([stats[ZERO:ONE, :], jnp.zeros((ONE, rest), F32)], axis=ONE)
    wide_std = jnp.concatenate([stats[ONE:PAIR, :], jnp.ones((ONE, rest), F32)], axis=ONE)
    for n in blocks:
        prev, cur = turned(prev_area, n), turned(cur_area, n)
        place_of(prev_area, n)[...] = (prev - wide_mean) / wide_std
        place_of(cur_area, n)[...] = cur
        place_of(norm_area, n)[...] = (cur - wide_mean) / wide_std
    for k in range(RING):
        for p in range(PAIR):
            for t in range(TILES):
                for band in range(PAIR):
                    def rows_of(area):
                        ref, first = area
                        return jnp.concatenate([ref[first + band, pl.ds(k * GRID_RUN + PAIR * r + p, rows, stride=PAIR), :]
                                                for r, rows in pieces(t)], axis=ZERO)
                    g_home[k, p, t, band, :, pl.ds(ZERO, LANES)] = rows_of(prev_area).astype(BF16)
                    g_home[k, p, t, band, :, pl.ds(LANES, LANES)] = rows_of(norm_area).astype(BF16)
                    x_home[k, p, t, band] = rows_of(cur_area)
    start_in(1)
    for copy in small[1:] + enc_copies() + layer_copies(0, 1) + layer_copies(0, 2):
        copy.start()

    for copy in raw[8:]:
        copy.wait()
    for n in range(LAT // LANES):
        stack(place_of(final_area, n), [(ZERO, wfin_raw[:, columns(n)].astype(F32))])
        wof[columns(n), :] = turned(final_area, n).astype(BF16)
    wide = wgrid_raw[...].astype(F32)
    recv[pl.ds(ZERO, wide.shape[0]), :] = wide
    prev_w, cur_w = recv[pl.ds(ZERO, VARS), :], recv[pl.ds(VARS, VARS), :]
    force_w, static_w = recv[pl.ds(2 * VARS, 5), :], recv[pl.ds(2 * VARS + 5, 5), :]
    spread = [[(0, wmesh_raw[...].astype(F32))], [(AT_G2M, weemb_raw[0].astype(F32))], [(AT_M2G, weemb_raw[1].astype(F32))]]
    spread += [[(16 + 16 * k, weemb_raw[2].astype(F32))] for k in range(6)]
    spread += [[(0, prev_w), (AT_FORCE, force_w), (AT_STATIC, static_w)], [(0, cur_w)]]
    spread += [[(0, cur_w), (AT_STATIC, static_w), (AT_NEXT, force_w)], [(0, prev_w)]]
    for i, rows in enumerate(spread):
        base = LANES * (i % 4)
        acc[pl.ds(base, LANES), :] = jnp.zeros((LANES, LAT), F32)
        for at_row, value in rows:
            acc[pl.ds(base + at_row, value.shape[0]), :] = value
        we[i] = acc[pl.ds(base, LANES), :].astype(BF16)

    def pipeline(items):
        depth = max(len(item) for item in items)
        for beat in range(len(items) + depth - 1):
            for stage in range(depth):
                index = beat - stage
                if 0 <= index < len(items) and stage < len(items[index]):
                    items[index][stage](index)

    def hide(slot, pre, extra=None):
        for c in chunks():
            value = pre[c:c + CH]
            if extra is not None:
                value = value + extra(c)
            hid[slot, pl.ds(c, CH), :] = silu(value).astype(BF16)

    def embed_item(load, w_first, second, store):
        def first(i):
            hide(i % PAIR, dot(load(), we[w_first]))

        def last(i):
            y = dot(hid[i % 2], weo[second])
            for c in chunks():
                store(c, norm(y[c:c + CH]).astype(BF16))

        return [first, last]

    wait_in(0)
    small[0].wait()
    def next_run(ref, *index):
        first = ref[(*index, pl.ds(ONE, RUNS - 1), slice(None), pl.ds(ZERO, LANES))]
        last = ref[(*index, pl.ds(ZERO, ONE), slice(None), pl.ds(ZERO, LANES))]
        return jnp.concatenate([first, last], axis=ZERO).reshape(TILE, LANES)

    mesh_rows = [next_run(m_buf, t) for t in range(TILES)]
    items = []
    for t in range(TILES):
        def store_mesh(c, value, t=t):
            h_mesh[part_rows(t, c), :] = value
        items.append(embed_item(lambda t=t: mesh_rows[t], 0, 1, store_mesh))
        for k in range(6):
            def store_edge(c, value, t=t, k=k):
                edge_base[k, part_rows(t, c), :] = value
            items.append(embed_item(lambda t=t: mesh_rows[t], 3 + k, 4, store_edge))
    pipeline(items)

    wait_in(1)
    start_in(PAIR)
    items = []
    for t in range(TILES):
        for p in range(PAIR):
            def store_m2g(c, value, t=t, p=p):
                m2g[p, part_rows(t, c), :] = value
            def store_g2m(c, value, t=t, p=p):
                g2m[p, part_rows(t, c), :] = value
            items.append(embed_item(lambda t=t, p=p: next_run(feat, p, t), 1, 2, store_g2m))
            items.append(embed_item(lambda t=t, p=p: feat[p, t, :, :, pl.ds(ZERO, LANES)].reshape(TILE, LANES), 2, 3, store_m2g))
    pipeline(items)
    for copy in small[1:] + enc_copies():
        copy.wait()

    left = ring_place(lax.rem(place + RING - 1, RING))
    right = ring_place(lax.rem(place + 1, RING))

    def halo_copies(slot):
        return [
            pltpu.make_async_remote_copy(src_ref=send_buf.at[side], dst_ref=halo_buf.at[slot, side],
                                         send_sem=halo_send.at[side], recv_sem=halo_recv.at[slot, side],
                                         device_id=at(target), device_id_type=mesh_id)
            for side, target in ((0, left), (1, right))
        ]

    def send_halo(slot):
        first = get_tiles(hf, pl.ds(ZERO, RUNS, stride=HALF))
        final = get_tiles(hf, pl.ds(HALF - 1, RUNS, stride=HALF))
        first_on = jnp.concatenate([first[1:], first[:1]], axis=ZERO)
        final_back = jnp.concatenate([final[-1:], final[:-1]], axis=ZERO)
        send_buf[0] = jnp.where(place == 0, first_on, first).astype(BF16)
        send_buf[1] = jnp.where(place == RING - 1, final_back, final).astype(BF16)
        for copy in halo_copies(slot):
            copy.start()

    def wait_halo(slot):
        for copy in halo_copies(slot):
            copy.wait()

    def project_halo(slot, w):
        rows = jnp.concatenate([halo_buf[slot, 0], halo_buf[slot, 1]], axis=ZERO)
        out = dot(rows, w.edge[1][...])
        set_tiles(proj1, pl.ds(8 + RUN, RUNS, stride=PAD1), out[:RUNS])
        set_tiles(proj1, pl.ds(7, RUNS, stride=PAD1), out[RUNS:])

    class Edge:
        def __init__(self, t, k, w, slot, run_shift=0, row_shift=0, source=None, first=False, final=False, keep=None):
            self.t, self.k, self.w, self.slot, self.keep = t, k, w, slot, keep
            self.run_shift, self.row_shift, self.first, self.final = run_shift, row_shift, first, final
            self.source = edge if source is None else source
            self.pre = None

        def a(self):
            self.pre = dot(self.source[self.k, tile_rows(self.t), :], self.w.edge[0][...])
            if self.keep is not None:
                for c in chunks():
                    pre_buf[self.keep, pl.ds(c, CH), :] = self.pre[c:c + CH]

        def resume(self):
            self.pre = pre_buf.at[self.keep]

        def extra(self, c):
            got = []
            for q in chunk_runs(c):
                base = (q + self.run_shift) % RUNS
                for r, n in pieces(self.t):
                    if self.t == 0:
                        got.append(get_tiles(proj0, pl.ds(base * PAD0 + r + self.row_shift, n)))
                    else:
                        got.append(get_tiles(proj1, pl.ds(base * PAD1 + 8 + r + self.row_shift, n)))
            return jnp.concatenate(got, axis=ZERO) + recv[part_rows(self.t, c), :]

        def fin(self):
            hide(self.slot, self.pre, self.extra)

        def b(self):
            y = dot(hid[self.slot], self.w.edge_out[...])
            for c in chunks():
                part = part_rows(self.t, c)
                value = (self.source[self.k, part, :].astype(F32) + norm(y[c:c + CH])).astype(BF16)
                edge[self.k, part, :] = value
                total = value.astype(F32)
                if not self.first:
                    total = total + acc[part, :]
                if self.final:
                    esum[part, :] = total.astype(BF16)
                else:
                    acc[part, :] = total

    class Node:
        def __init__(self, t, base, w):
            self.t, self.base, self.w, self.slot = t, base, w, 6 + t

        def own(self):
            self.pre = dot(self.base[tile_rows(self.t), :], self.w.node[0][...])

        def a(self):
            hide(self.slot, self.pre + dot(esum[tile_rows(self.t), :], self.w.node[1][...]))

        def b(self):
            y = dot(hid[self.slot], self.w.node_out[...])
            for c in chunks():
                part = part_rows(self.t, c)
                value = (self.base[part, :].astype(F32) + norm(y[c:c + CH])).astype(BF16)
                h[part, :] = value
                if self.t == 1:
                    set_tiles(hf, pl.ds(c, CH), value.astype(F32))

    def project_send(t, w):
        out = dot(h[tile_rows(t), :], w.edge[1][...])
        for q in range(RUNS):
            row = q * HALF
            for r, n in pieces(t):
                if t == 0:
                    set_tiles(proj0, pl.ds(q * PAD0 + r, n), out[row:row + n])
                else:
                    set_tiles(proj1, pl.ds(q * PAD1 + 8 + r, n), out[row:row + n])
                row += n
        if t == 1:
            for r in (7, 24):
                set_tiles(proj0, pl.ds(r, RUNS, stride=PAD0), get_tiles(proj1, pl.ds(8 + r, RUNS, stride=PAD1)))

    def project_recv(t, w):
        out = dot(h[tile_rows(t), :], w.edge[2][...])
        for c in chunks():
            recv[part_rows(t, c), :] = out[c:c + CH]

    def project(t, w):
        project_send(t, w)
        project_recv(t, w)

    def share_rows():
        for r in (8, 23):
            set_tiles(proj1, pl.ds(8 + r, RUNS, stride=PAD1), get_tiles(proj0, pl.ds(r, RUNS, stride=PAD0)))

    def far_items(t, w, source=None, resume=False):
        items = [Edge(t, k, w, n, run_shift=s, source=source, first=n == 0, keep=4 * t + n) for n, (k, s) in enumerate(FAR)]
        if resume:
            for item in items:
                item.resume()
        return items

    def near_items(t, w, resume=False):
        items = [Edge(t, k, w, 4 + n, row_shift=s, final=n == 1, keep=8 + t if n == 0 else None)
                 for n, (k, s) in enumerate(NEAR)]
        if resume:
            items[0].resume()
        return items

    def phase(order, x, n, node, next_x, next_n, before, w_next):
        table = {"before": before, "n1": n[1].a, "nh": node.own, "na": node.a, "nb": node.b, "an0": next_n[0].a,
                 "ps": lambda: project_send(node.t, w_next), "pr": lambda: project_recv(node.t, w_next)}
        for i in range(4):
            table[f"fx{i}"], table[f"bx{i}"], table[f"ax{i}"] = x[i].fin, x[i].b, next_x[i].a
        for i in range(PAIR):
            table[f"fn{i}"], table[f"bn{i}"] = n[i].fin, n[i].b
        run(order, table)

    def run(order, table):
        for name in order:
            table[name]()

    def encoder(step):
        w = Weights(enc_refs, ZERO)
        w1 = layer_weights(step, 1)
        w2 = layer_weights(step, 2)
        table = {"send": lambda: send_halo(ZERO), "share": share_rows}

        def spread():
            for k in range(6):
                for t in range(TILES):
                    if t == 1 or k < PAIR:
                        edge[k, tile_rows(t), :] = edge_base[k, tile_rows(t), :]

        table["copy"] = spread
        y, x, z, n = far_items(0, w1, edge_base), far_items(1, w1), far_items(0, w2), near_items(0, w1)
        for k in range(4):
            table[f"ya{k}"], table[f"yf{k}"], table[f"yb{k}"] = y[k].a, y[k].fin, y[k].b
            table[f"xa{k}"], table[f"za{k}"] = x[k].a, z[k].a
        table["n0"] = n[0].a
        for t in range(TILES):
            def back(t=t):
                out = dot(h_mesh[tile_rows(t), :], w.edge[2][...])
                for c in chunks():
                    recv[part_rows(t, c), :] = out[c:c + CH]

            node = Node(t, h_mesh, w)
            table[f"r{t}"], table[f"nh{t}"], table[f"na{t}"], table[f"nb{t}"] = back, node.own, node.a, node.b
            table[f"ps{t}"], table[f"pr{t}"] = functools.partial(project_send, t, w1), functools.partial(project_recv, t, w1)
            for p in range(PAIR):
                i = PAIR * t + p
                low, high = 8 + i, 12 + i

                def in_first(t=t, p=p, low=low):
                    hide(low, dot(feat[p, t].reshape(TILE, 2 * LANES), we[pl.ds(9 + PAIR * step, PAIR)].reshape(2 * LANES, LAT)))

                def in_last(t=t, p=p, low=low):
                    y = dot(hid[low], weo[ZERO])
                    for c in chunks():
                        v[p, part_rows(t, c), :] = norm(y[c:c + CH]).astype(BF16)

                def edge_first(t=t, p=p, high=high):
                    pre = dot(g2m[p, tile_rows(t), :], w.edge[0][...]) + dot(v[p, tile_rows(t), :], w.edge[1][...])
                    hide(high, pre, lambda c: recv[part_rows(t, c), :])

                def edge_last(t=t, p=p, high=high):
                    y = dot(hid[high], w.edge_out[...])
                    for c in chunks():
                        part = part_rows(t, c)
                        total = (g2m[p, part, :].astype(F32) + norm(y[c:c + CH])).astype(BF16).astype(F32)
                        if p == 0:
                            acc[part, :] = total
                        else:
                            esum[part, :] = (acc[part, :] + total).astype(BF16)

                def self_first(t=t, p=p, low=low):
                    hide(low, dot(v[p, tile_rows(t), :], wself[ZERO]))

                def self_last(t=t, p=p, low=low):
                    y = dot(hid[low], wself[ONE])
                    for c in chunks():
                        part = part_rows(t, c)
                        vc[p, part, :] = (v[p, part, :].astype(F32) + norm(y[c:c + CH])).astype(BF16)

                table[f"va{i}"], table[f"vb{i}"], table[f"ea{i}"], table[f"eb{i}"] = in_first, in_last, edge_first, edge_last
                table[f"sa{i}"], table[f"sb{i}"] = self_first, self_last
        run(ORDER_E, table)

    def out_copies(step, t):
        copies = []
        for hop in range(RING):
            target = lax.rem(me + hop, RING)
            src, dst = x_buf.at[step + 1, :, t, pl.ds(PAIR * target, PAIR)], out.at[step, place, :, t]
            if hop == 0:
                copies.append(pltpu.make_async_copy(src, dst, out_recv.at[step, t, hop]))
            else:
                copies.append(pltpu.make_async_remote_copy(
                    src_ref=src, dst_ref=dst, send_sem=out_send.at[step, t, hop], recv_sem=out_recv.at[step, t, hop],
                    device_id=at(target), device_id_type=mesh_id))
        return copies

    def decoder(step):
        w16 = layer_weights(step, LAYERS)
        w = layer_weights(step, BLOCKS - 1)
        in_mean = stats[ZERO:ONE, :]
        in_std = stats[ONE:PAIR, :]
        diff_mean, diff_std = (jnp.concatenate([stats[i:i + 1, :], jnp.zeros((ONE, LANES - VARS), F32)], axis=ONE) for i in (2, 3))
        halo_slot = lax.rem(LAYERS + 1, 2)
        table = {"share": share_rows, "wait": lambda: wait_halo(halo_slot), "halo": lambda: project_halo(halo_slot, w16)}
        x = far_items(1, w16, resume=True)
        for k in range(4):
            table[f"fx{k}"], table[f"bx{k}"] = x[k].fin, x[k].b
        for t in range(TILES):
            node = Node(t, h, w16)
            table[f"nh{t}"], table[f"na{t}"], table[f"nb{t}"] = node.own, node.a, node.b
            near = near_items(t, w16, resume=t == 0)
            for k in range(PAIR):
                table[f"n{t}{k}"], table[f"fn{t}{k}"], table[f"bn{t}{k}"] = near[k].a, near[k].fin, near[k].b

            def back(t=t):
                out = dot(h[tile_rows(t), :], w.edge[1][...])
                for c in chunks():
                    recv[part_rows(t, c), :] = out[c:c + CH]

            def send(t=t):
                start_all(out_copies(step, t))

            table[f"t{t}"], table[f"send{t}"] = back, send
            for p in range(PAIR):
                i = PAIR * t + p
                low, high = 8 + i, 12 + i
                held = {}

                def edge_own(t=t, p=p, held=held):
                    held["edge"] = dot(m2g[p, tile_rows(t), :], w.edge[0][...]) + dot(vc[p, tile_rows(t), :], w.edge[2][...])

                def edge_first(t=t, low=low, held=held):
                    hide(low, held["edge"], lambda c: recv[part_rows(t, c), :])

                def edge_last(t=t, p=p, low=low, i=i):
                    y = dot(hid[low], w.edge_out[...])
                    for c in chunks():
                        part = part_rows(t, c)
                        dec[i, pl.ds(c, CH), :] = (m2g[p, part, :].astype(F32) + norm(y[c:c + CH])).astype(BF16)

                def node_own(t=t, p=p, held=held):
                    held["node"] = dot(vc[p, tile_rows(t), :], w.node[0][...])

                def node_first(high=high, i=i, held=held):
                    hide(high, held["node"] + dot(dec[i], w.node[1][...]))

                def node_last(t=t, p=p, high=high):
                    y = dot(hid[high], w.node_out[...])
                    for c in chunks():
                        part = part_rows(t, c)
                        v[p, part, :] = (vc[p, part, :].astype(F32) + norm(y[c:c + CH])).astype(BF16)

                def out_first(t=t, p=p, low=low):
                    hide(low, dot(v[p, tile_rows(t), :], woh[...]))

                def out_last(t=t, p=p, low=low):
                    pred = dot(hid[low], wof[...])
                    for c in chunks():
                        runs = pl.ds(c // HALF, CH // HALF)
                        now = x_buf[step, p, t, runs].reshape(CH, LANES)
                        new = now + diff_std * pred[c:c + CH] + diff_mean
                        x_buf[step + 1, p, t, runs] = new.reshape(CH // HALF, HALF, LANES)
                        scaled = ((new[:, :VARS] - in_mean) / in_std).astype(BF16)
                        feat[p, t, runs, :, pl.ds(ZERO, VARS)] = scaled.reshape(CH // HALF, HALF, VARS)

                table[f"em{i}"], table[f"ea{i}"], table[f"eb{i}"] = edge_own, edge_first, edge_last
                table[f"dm{i}"], table[f"da{i}"], table[f"db{i}"] = node_own, node_first, node_last
                table[f"oa{i}"], table[f"ob{i}"] = out_first, out_last
        run(ORDER_D, table)

    def wait_all(copies):
        for copy in copies:
            copy.wait()

    def start_all(copies):
        for copy in copies:
            copy.start()

    def one_step(step, carry):
        wait_all(layer_copies(step, 1) + layer_copies(step, 2))
        start_all(layer_copies(step, 3))
        encoder(step)

        def one_layer(block, carry):
            halo_slot = lax.rem(block + 1, 2)
            w, w1, w2 = (layer_weights(step, block + i) for i in range(3))
            phase(ORDER_A, far_items(1, w, resume=True), near_items(0, w, resume=True), Node(0, h, w), far_items(1, w1),
                  near_items(1, w), share_rows, w1)
            wait_halo(halo_slot)
            wait_all(layer_copies(step, block + 2))

            @pl.when(block < LAYERS - 1)
            def _():
                start_all(layer_copies(step, block + 3))

            phase(ORDER_B, far_items(0, w1, resume=True), near_items(1, w, resume=True), Node(1, h, w), far_items(0, w2),
                  near_items(0, w1), lambda: project_halo(halo_slot, w), w1)
            send_halo(1 - halo_slot)
            return carry

        lax.fori_loop(1, LAYERS, one_layer, 0)
        @pl.when(step == 0)
        def _():
            start_all(layer_copies(1, 1) + layer_copies(1, 2))
            wait_in(PAIR)

        decoder(step)
        return carry

    lax.fori_loop(0, 2, one_step, 0)
    for part in range(3):
        for copy in in_copies[part][1:]:
            copy.wait_send()
    for t in range(TILES):
        wait_all(out_copies(0, t) + out_copies(1, t))


def solution(mesh):
    row_spec = P(("dp", "gp"))
    edge_spec = P(("dp", "gp"), None, None)
    whole = P()

    def local_run(x_prev, x_cur, forcing, grid_static, g2m_feat, m2g_feat, mesh_feat, mesh_edge_feat, norm_stats,
                  w_grid_in, w_mesh_in, w_eemb_in, w_embed_out, w_edge_in, w_edge_out, w_node_in, w_node_out,
                  w_grid_self, w_out_hidden, w_out_final):
        any_spec = pl.BlockSpec(memory_space=pl.ANY)
        vmem_spec = pl.BlockSpec(memory_space=pltpu.VMEM)
        dma = pltpu.SemaphoreType.DMA
        grid_dev = x_prev.shape[0]
        shape = jax.ShapeDtypeStruct
        home = shape((RING, PAIR, TILES, PAIR, HALF, LANES), F32)
        bulk = [
            pltpu.VMEM(shape_, F32) for shape_ in (
                (3, mesh_feat.shape[0]), (6, 4, mesh_feat.shape[0]), (VARS, grid_dev), (VARS, grid_dev), (5, PAIR, grid_dev),
                (5, grid_dev), (4, grid_dev), (4, grid_dev))
        ]
        scratch = bulk + [
            pltpu.VMEM((2 * VARS + 10, LAT), BF16),
            pltpu.VMEM((3, LAT), BF16),
            pltpu.VMEM((3, 4, LAT), BF16),
            pltpu.VMEM((VARS, LAT), BF16),
            pltpu.VMEM((*home.shape[:-1], 2 * LANES), BF16),
            pltpu.VMEM((RING, TILES, PAIR, HALF, LANES), BF16),
            pltpu.VMEM(home.shape, F32),
            pltpu.VMEM((TILES, RUNS, HALF, LANES), BF16),
            pltpu.VMEM((3, PAIR, TILES, RUNS, HALF, LANES), F32),
            pltpu.VMEM((PAIR, TILES, RUNS, HALF, 2 * LANES), BF16),
            pltpu.VMEM((13, LANES, LAT), BF16),
            pltpu.VMEM((5, LAT, LAT), BF16),
            pltpu.VMEM((PAIR, LAT, LAT), BF16),
            pltpu.VMEM((LAT, LAT), BF16),
            pltpu.VMEM((LAT, LANES), BF16),
            pltpu.VMEM((1, 3 * LAT, LAT), BF16),
            pltpu.VMEM((1, LAT, LAT), BF16),
            pltpu.VMEM((1, 2 * LAT, LAT), BF16),
            pltpu.VMEM((1, LAT, LAT), BF16),
            pltpu.VMEM((SLOTS, 3 * LAT, LAT), BF16),
            pltpu.VMEM((SLOTS, LAT, LAT), BF16),
            pltpu.VMEM((SLOTS, 2 * LAT, LAT), BF16),
            pltpu.VMEM((SLOTS, LAT, LAT), BF16),
            pltpu.VMEM((6, ROWS, LAT), BF16),
            pltpu.VMEM((6, ROWS, LAT), BF16),
            pltpu.VMEM((ROWS, LAT), BF16),
            pltpu.VMEM((ROWS, LAT), BF16),
            pltpu.VMEM((LAT // LANES, TILE, LANES), F32),
            pltpu.VMEM((PAIR, ROWS, LAT), BF16),
            pltpu.VMEM((PAIR, ROWS, LAT), BF16),
            pltpu.VMEM((PAIR, ROWS, LAT), BF16),
            pltpu.VMEM((PAIR, ROWS, LAT), BF16),
            pltpu.VMEM((LAT // LANES, RUNS * PAD0, LANES), F32),
            pltpu.VMEM((LAT // LANES, RUNS * PAD1, LANES), F32),
            pltpu.VMEM((ROWS, LAT), F32),
            pltpu.VMEM((ROWS, LAT), F32),
            pltpu.VMEM((16, TILE, LAT), BF16),
            pltpu.VMEM((ROWS, LAT), BF16),
            pltpu.VMEM((4, TILE, LAT), BF16),
            pltpu.VMEM((10, TILE, LAT), F32),
            pltpu.VMEM((PAIR, RUNS, LAT), BF16),
            pltpu.VMEM((PAIR, 2, RUNS, LAT), BF16),
            dma((12,)), dma((3, RING)), dma((3, RING)), dma((4,)), dma((1, 4)), dma((SLOTS, 4)), dma((PAIR,)), dma((PAIR, PAIR)),
            dma((PAIR, TILES, RING)), dma((PAIR, TILES, RING)),
        ]
        homes = pl.pallas_call(
            kernel,
            out_shape=shape((PAIR, *home.shape), F32),
            in_specs=[any_spec] * 8 + [vmem_spec] + [any_spec] * 11,
            out_specs=any_spec,
            scratch_shapes=scratch,
            compiler_params=pltpu.CompilerParams(collective_id=0, has_side_effects=True, vmem_limit_bytes=63 << 20),
            name="forecast",
        )(x_prev.T, x_cur.T, forcing.T, grid_static.T, g2m_feat.T, m2g_feat.T, mesh_feat.T,
          jnp.transpose(mesh_edge_feat, (1, 2, 0)), norm_stats, w_grid_in, w_mesh_in, w_eemb_in, w_embed_out, w_edge_in,
          w_edge_out, w_node_in, w_node_out, w_grid_self, w_out_hidden, w_out_final.T)
        out = shape((VARS, grid_dev), F32)
        next_state, after_state = pl.pallas_call(
            unpack_kernel, out_shape=(out, out), in_specs=[vmem_spec], out_specs=(vmem_spec,) * 2,
            scratch_shapes=[pltpu.VMEM((grid_dev, LANES), F32)], name="unpack",
        )(homes)
        return next_state.T, after_state.T

    in_specs = (row_spec, row_spec, edge_spec, row_spec, row_spec, row_spec, row_spec, edge_spec, whole) + (whole,) * 11
    return jax.shard_map(local_run, mesh=mesh, in_specs=in_specs, out_specs=(row_spec, row_spec), check_vma=False)
```

```python
import functools

import jax
import jax.numpy as jnp
from jax import lax
from jax.experimental import pallas as pl
from jax.experimental.pallas import tpu as pltpu
from jax.sharding import PartitionSpec as P

F32 = jnp.float32
BF16 = jnp.bfloat16

RUNS = 16
RUN = 32
GRID_RUN = 2 * RUN
ROWS = RUNS * RUN
ZERO, ONE, LAST = 0, 1, -1
LAT = 512
LANES = 128
PAIR = 2
VARS = 84
PAD0 = 32
PAD1 = 48
TILE = 256
TILES = 2
HALF = TILE // RUNS
CH = 128
RING = 8
LAYERS = 16
BLOCKS = LAYERS + 2
SLOTS = 4
FAR = ((2, 1), (3, -1), (4, 4), (5, -4))
NEAR = ((0, 1), (1, -1))
ORDER_A = (
    "fx1", "before", "fx0", "nh", "n1", "bx0", "bx1", "fn0", "bn0", "fn1", "bn1", "ax0", "fx2", "fx3", "bx2",
    "na", "bx3", "ax2", "nb", "ax1", "an0", "ax3", "pr", "ps",
)
ORDER_B = (
    "before", "fx0", "fx1", "bx0", "n1", "fn1", "bx1", "fx2", "nh", "fn0", "bn0", "bn1", "ax0", "ax1", "fx3",
    "bx2", "na", "bx3", "ax2", "nb", "an0", "ax3", "ps", "pr",
)
ORDER_E = (
    "copy", "r0", "va1", "va0", "va2", "vb1", "vb0", "va3", "r1", "vb2", "vb3", "ea0", "sa0", "ea1", "sa1",
    "eb0", "ea3", "sa2", "eb1", "sb0", "ea2", "sb1", "ya2", "nh0", "eb2", "na0", "sa3", "eb3", "nb0", "sb2",
    "sb3", "ya0", "nh1", "ya1", "na1", "ps0", "pr0", "nb1", "yf0", "yb0", "yf1", "yb1", "ps1", "ya3", "pr1",
    "yf2", "za1", "yb2", "yf3", "yb3", "xa0", "share", "xa1", "za3", "xa3", "za0", "za2", "xa2", "n0", "send",
)
ORDER_D = (
    "n01", "fx1", "nh0", "fx0", "share", "bx0", "fn00", "fn01", "bn00", "bn01", "bx1", "em0", "fx2", "bx2",
    "fx3", "na0", "em1", "nb0", "n11", "wait", "dm0", "n10", "t0", "halo", "bx3", "ea0", "fn11", "fn10",
    "bn10", "eb0", "bn11", "ea1", "eb1", "nh1", "em2", "em3", "na1", "da0", "dm1", "nb1", "da1", "dm2", "db0",
    "t1", "db1", "oa0", "ea2", "eb2", "oa1", "ob0", "ea3", "dm3", "ob1", "send0", "eb3", "da2", "da3", "db2",
    "db3", "oa2", "oa3", "ob2", "ob3", "send1",
)


def dot(a, b):
    return jnp.dot(a, b, preferred_element_type=F32)


def silu(pre):
    return pre * jax.nn.sigmoid(pre)


def norm(y):
    centred = y - jnp.mean(y, axis=LAST, keepdims=True)
    return centred * lax.rsqrt(jnp.mean(centred * centred, axis=LAST, keepdims=True) + 1e-5)


def ring_place(dev):
    high = lax.div(dev, 4)
    return high * (4 + lax.rem(dev + 2, 4)) + (1 - high) * dev


def chunks():
    return range(0, TILE, CH)


def tile_rows(t):
    return pl.ds(t * TILE, TILE)


def part_rows(t, c):
    return pl.ds(t * TILE + c, CH)


def chunk_runs(c):
    return range(c // HALF, (c + CH) // HALF)


def pieces(t):
    return ((8, 16),) if t == 0 else ((0, 8), (24, 8))


def get_tiles(ref, rows):
    return jnp.concatenate([ref[j, rows, :] for j in range(ref.shape[0])], axis=ONE)


def set_tiles(ref, rows, value):
    for j in range(ref.shape[0]):
        ref[j, rows, :] = value[:, LANES * j:LANES * j + LANES]


AT_FORCE, AT_STATIC, AT_NEXT, AT_M2G, AT_G2M = 88, 96, 104, 112, 120


def columns(n):
    return pl.ds(LANES * n, LANES)


def stack(ref, rows):
    end = 0
    for at_row, value in rows:
        first = at_row // 8 * 8
        last = (at_row + value.shape[0]) // 8 * 8
        if first > end:
            ref[pl.ds(end, first - end), :] = jnp.zeros((first - end, LANES), F32)
        if last < at_row + value.shape[0]:
            ref[pl.ds(last, 8), :] = jnp.zeros((8, LANES), F32)
            end = last + 8
        else:
            end = last
        ref[pl.ds(at_row, value.shape[0]), :] = value
    if end < LANES:
        ref[pl.ds(end, LANES - end), :] = jnp.zeros((LANES - end, LANES), F32)


def unpack_kernel(homes, out0, out1, area):
    for home, out in ((homes.at[ZERO], out0), (homes.at[ONE], out1)):
        for band in range(PAIR):
            for k in range(RING):
                for p in range(PAIR):
                    for t in range(TILES):
                        row = 0
                        for r, rows in pieces(t):
                            spot = pl.ds((band * RING + k) * GRID_RUN + PAIR * r + p, rows, stride=PAIR)
                            area[spot, :] = home[k, p, t, band, pl.ds(row, rows), :]
                            row += rows
        for n in range(out.shape[1] // LANES):
            out[:, columns(n)] = jnp.transpose(area[columns(n), :])[:VARS]


def kernel(x_prev, x_cur, forcing, static, g2m_feat, m2g_feat, mesh_feat, mesh_edge_feat, stats, w_grid_in, w_mesh_in,
           w_eemb_in, w_embed_out, w_edge_in, w_edge_out, w_node_in, w_node_out, w_grid_self, w_out_hidden, w_out_final,
           out,
           mesh_raw, medge_raw, prev_raw, cur_raw, force_raw, static_raw, g2m_raw, m2g_raw,
           wgrid_raw, wmesh_raw, weemb_raw, wfin_raw, g_home, m_home, x_home,
           m_buf, x_buf, feat, we, weo, wself, woh, wof,
           enc_ei, enc_eo, enc_ni, enc_no, lay_ei, lay_eo, lay_ni, lay_no,
           edge_base, edge, h_mesh, h, hf, g2m, m2g, v, vc, proj0, proj1, recv, acc, hid, esum, dec, pre_buf,
           send_buf, halo_buf,
           raw_sem, in_send, in_recv, w_sem, enc_sem, lay_sem, halo_send, halo_recv, out_send, out_recv):
    me = lax.axis_index("gp")
    place = ring_place(me)

    def at(dev):
        return {"gp": dev}

    mesh_id = pl.DeviceIdType.MESH

    def block_copies(block, dst_refs, slot, sem):
        srcs = (w_edge_in, w_edge_out, w_node_in, w_node_out)
        return [pltpu.make_async_copy(src.at[block], dst.at[slot], sem.at[slot, i])
                for i, (src, dst) in enumerate(zip(srcs, dst_refs))]

    enc_refs = (enc_ei, enc_eo, enc_ni, enc_no)
    lay_refs = (lay_ei, lay_eo, lay_ni, lay_no)

    def enc_copies():
        return block_copies(0, enc_refs, 0, enc_sem)

    def slot_of(step, block):
        return lax.rem((BLOCKS - 1) * step + block - 1, SLOTS)

    def layer_copies(step, block):
        return block_copies(block, lay_refs, slot_of(step, block), lay_sem)

    class Weights:
        def __init__(self, refs, slot):
            self.edge = [refs[0].at[slot, pl.ds(i * LAT, LAT)] for i in range(3)]
            self.edge_out = refs[1].at[slot]
            self.node = [refs[2].at[slot, pl.ds(i * LAT, LAT)] for i in range(2)]
            self.node_out = refs[3].at[slot]

    def layer_weights(step, block):
        return Weights(lay_refs, slot_of(step, block))

    raw = [pltpu.make_async_copy(src, dst, raw_sem.at[i]) for i, (src, dst) in enumerate(
        ((mesh_feat, mesh_raw), (mesh_edge_feat, medge_raw), (x_prev, prev_raw), (x_cur, cur_raw), (forcing, force_raw),
         (static, static_raw), (g2m_feat, g2m_raw), (m2g_feat, m2g_raw),
         (w_grid_in, wgrid_raw), (w_mesh_in, wmesh_raw), (w_eemb_in, weemb_raw), (w_out_final, wfin_raw)))]
    for copy in raw:
        copy.start()
    small = [
        pltpu.make_async_copy(w_embed_out, weo, w_sem.at[0]),
        pltpu.make_async_copy(w_grid_self, wself, w_sem.at[1]),
        pltpu.make_async_copy(w_out_hidden, woh, w_sem.at[2]),
    ]
    small[0].start()

    barrier = pltpu.get_barrier_semaphore()
    for hop in range(1, RING):
        pl.semaphore_signal(barrier, inc=1, device_id=at(lax.rem(me + hop, RING)), device_id_type=mesh_id)

    mine = pl.ds(PAIR * me, PAIR)
    parts = ((m_home, m_buf.at[:, mine]), (g_home, feat.at[:, :, mine]), (x_home, x_buf.at[ZERO, :, :, mine]))

    def in_copy(part, hop):
        src, dst = parts[part]
        target = lax.rem(me + hop, RING)
        src = src.at[ring_place(target)]
        if hop == 0:
            return pltpu.make_async_copy(src, dst, in_recv.at[part, hop])
        return pltpu.make_async_remote_copy(src_ref=src, dst_ref=dst, send_sem=in_send.at[part, hop],
                                            recv_sem=in_recv.at[part, hop], device_id=at(target),
                                            device_id_type=mesh_id)

    in_copies = [[in_copy(part, hop) for hop in range(RING)] for part in range(3)]

    def wait_in(part):
        in_copies[part][0].wait()
        for copy in in_copies[part][1:]:
            copy.wait_recv()

    def start_in(part):
        for copy in in_copies[part]:
            copy.start()

    def place_of(area, n):
        ref, first = area
        return ref.at[first + n // 4, columns(n % 4)]

    prev_area, cur_area, norm_area, mesh_area, final_area = (proj0, 0), (proj0, PAIR), (proj1, 0), (proj1, 2), (proj1, 3)

    def turned(area, n):
        return jnp.transpose(place_of(area, n)[...])

    for copy in raw[:2]:
        copy.wait()
    for n in range(mesh_raw.shape[1] // LANES):
        stack(place_of(mesh_area, n), [(ZERO, mesh_raw[:, columns(n)])] + [
            (16 + 16 * k, medge_raw[k, :, columns(n)]) for k in range(6)])
    for n in range(mesh_raw.shape[1] // LANES):
        turned_rows = turned(mesh_area, n)
        for i in range(LANES // RUN):
            band, k = divmod(n * LANES + i * RUN, RING * RUN)
            for t in range(TILES):
                m_home[k // RUN, t, band] = jnp.concatenate(
                    [turned_rows[i * RUN + r:i * RUN + r + rows] for r, rows in pieces(t)], axis=ZERO).astype(BF16)
    pl.semaphore_wait(barrier, RING - 1)
    start_in(0)
    for copy in raw[2:8]:
        copy.wait()
    blocks = range(cur_raw.shape[1] // LANES)
    for n in blocks:
        stack(place_of(prev_area, n), [
            (ZERO, prev_raw[:, columns(n)]), (AT_FORCE, force_raw[:, ZERO, columns(n)]), (AT_STATIC, static_raw[:, columns(n)]),
            (AT_NEXT, force_raw[:, ONE, columns(n)]), (AT_M2G, m2g_raw[:, columns(n)]), (AT_G2M, g2m_raw[:, columns(n)])])
        stack(place_of(cur_area, n), [(ZERO, cur_raw[:, columns(n)])])
    rest = LANES - VARS
    wide_mean = jnp.concatenate([stats[ZERO:ONE, :], jnp.zeros((ONE, rest), F32)], axis=ONE)
    wide_std = jnp.concatenate([stats[ONE:PAIR, :], jnp.ones((ONE, rest), F32)], axis=ONE)
    for n in blocks:
        prev, cur = turned(prev_area, n), turned(cur_area, n)
        place_of(prev_area, n)[...] = (prev - wide_mean) / wide_std
        place_of(cur_area, n)[...] = cur
        place_of(norm_area, n)[...] = (cur - wide_mean) / wide_std
    for k in range(RING):
        for p in range(PAIR):
            for t in range(TILES):
                for band in range(PAIR):
                    def rows_of(area):
                        ref, first = area
                        return jnp.concatenate([ref[first + band, pl.ds(k * GRID_RUN + PAIR * r + p, rows, stride=PAIR), :]
                                                for r, rows in pieces(t)], axis=ZERO)
                    g_home[k, p, t, band, :, pl.ds(ZERO, LANES)] = rows_of(prev_area).astype(BF16)
                    g_home[k, p, t, band, :, pl.ds(LANES, LANES)] = rows_of(norm_area).astype(BF16)
                    x_home[k, p, t, band] = rows_of(cur_area)
    start_in(1)
    for copy in small[1:] + enc_copies() + layer_copies(0, 1) + layer_copies(0, 2):
        copy.start()

    for copy in raw[8:]:
        copy.wait()
    for n in range(LAT // LANES):
        stack(place_of(final_area, n), [(ZERO, wfin_raw[:, columns(n)].astype(F32))])
        wof[columns(n), :] = turned(final_area, n).astype(BF16)
    wide = wgrid_raw[...].astype(F32)
    recv[pl.ds(ZERO, wide.shape[0]), :] = wide
    prev_w, cur_w = recv[pl.ds(ZERO, VARS), :], recv[pl.ds(VARS, VARS), :]
    force_w, static_w = recv[pl.ds(2 * VARS, 5), :], recv[pl.ds(2 * VARS + 5, 5), :]
    spread = [[(0, wmesh_raw[...].astype(F32))], [(AT_G2M, weemb_raw[0].astype(F32))], [(AT_M2G, weemb_raw[1].astype(F32))]]
    spread += [[(16 + 16 * k, weemb_raw[2].astype(F32))] for k in range(6)]
    spread += [[(0, prev_w), (AT_FORCE, force_w), (AT_STATIC, static_w)], [(0, cur_w)]]
    spread += [[(0, cur_w), (AT_STATIC, static_w), (AT_NEXT, force_w)], [(0, prev_w)]]
    for i, rows in enumerate(spread):
        base = LANES * (i % 4)
        acc[pl.ds(base, LANES), :] = jnp.zeros((LANES, LAT), F32)
        for at_row, value in rows:
            acc[pl.ds(base + at_row, value.shape[0]), :] = value
        we[i] = acc[pl.ds(base, LANES), :].astype(BF16)

    def pipeline(items):
        depth = max(len(item) for item in items)
        for beat in range(len(items) + depth - 1):
            for stage in range(depth):
                index = beat - stage
                if 0 <= index < len(items) and stage < len(items[index]):
                    items[index][stage](index)

    def hide(slot, pre, extra=None):
        for c in chunks():
            value = pre[c:c + CH]
            if extra is not None:
                value = value + extra(c)
            hid[slot, pl.ds(c, CH), :] = silu(value).astype(BF16)

    def embed_item(load, w_first, second, store):
        def first(i):
            hide(i % PAIR, dot(load(), we[w_first]))

        def last(i):
            y = dot(hid[i % 2], weo[second])
            for c in chunks():
                store(c, norm(y[c:c + CH]).astype(BF16))

        return [first, last]

    wait_in(0)
    small[0].wait()
    def next_run(ref, *index):
        first = ref[(*index, pl.ds(ONE, RUNS - 1), slice(None), pl.ds(ZERO, LANES))]
        last = ref[(*index, pl.ds(ZERO, ONE), slice(None), pl.ds(ZERO, LANES))]
        return jnp.concatenate([first, last], axis=ZERO).reshape(TILE, LANES)

    mesh_rows = [next_run(m_buf, t) for t in range(TILES)]
    items = []
    for t in range(TILES):
        def store_mesh(c, value, t=t):
            h_mesh[part_rows(t, c), :] = value
        items.append(embed_item(lambda t=t: mesh_rows[t], 0, 1, store_mesh))
        for k in range(6):
            def store_edge(c, value, t=t, k=k):
                edge_base[k, part_rows(t, c), :] = value
            items.append(embed_item(lambda t=t: mesh_rows[t], 3 + k, 4, store_edge))
    pipeline(items)

    wait_in(1)
    start_in(PAIR)
    items = []
    for t in range(TILES):
        for p in range(PAIR):
            def store_m2g(c, value, t=t, p=p):
                m2g[p, part_rows(t, c), :] = value
            def store_g2m(c, value, t=t, p=p):
                g2m[p, part_rows(t, c), :] = value
            items.append(embed_item(lambda t=t, p=p: next_run(feat, p, t), 1, 2, store_g2m))
            items.append(embed_item(lambda t=t, p=p: feat[p, t, :, :, pl.ds(ZERO, LANES)].reshape(TILE, LANES), 2, 3, store_m2g))
    pipeline(items)
    for copy in small[1:] + enc_copies():
        copy.wait()

    left = ring_place(lax.rem(place + RING - 1, RING))
    right = ring_place(lax.rem(place + 1, RING))

    def halo_copies(slot):
        return [
            pltpu.make_async_remote_copy(src_ref=send_buf.at[side], dst_ref=halo_buf.at[slot, side],
                                         send_sem=halo_send.at[side], recv_sem=halo_recv.at[slot, side],
                                         device_id=at(target), device_id_type=mesh_id)
            for side, target in ((0, left), (1, right))
        ]

    def send_halo(slot):
        first = get_tiles(hf, pl.ds(ZERO, RUNS, stride=HALF))
        final = get_tiles(hf, pl.ds(HALF - 1, RUNS, stride=HALF))
        first_on = jnp.concatenate([first[1:], first[:1]], axis=ZERO)
        final_back = jnp.concatenate([final[-1:], final[:-1]], axis=ZERO)
        send_buf[0] = jnp.where(place == 0, first_on, first).astype(BF16)
        send_buf[1] = jnp.where(place == RING - 1, final_back, final).astype(BF16)
        for copy in halo_copies(slot):
            copy.start()

    def wait_halo(slot):
        for copy in halo_copies(slot):
            copy.wait()

    def project_halo(slot, w):
        rows = jnp.concatenate([halo_buf[slot, 0], halo_buf[slot, 1]], axis=ZERO)
        out = dot(rows, w.edge[1][...])
        set_tiles(proj1, pl.ds(8 + RUN, RUNS, stride=PAD1), out[:RUNS])
        set_tiles(proj1, pl.ds(7, RUNS, stride=PAD1), out[RUNS:])

    class Edge:
        def __init__(self, t, k, w, slot, run_shift=0, row_shift=0, source=None, first=False, final=False, keep=None):
            self.t, self.k, self.w, self.slot, self.keep = t, k, w, slot, keep
            self.run_shift, self.row_shift, self.first, self.final = run_shift, row_shift, first, final
            self.source = edge if source is None else source
            self.pre = None

        def a(self):
            self.pre = dot(self.source[self.k, tile_rows(self.t), :], self.w.edge[0][...])
            if self.keep is not None:
                for c in chunks():
                    pre_buf[self.keep, pl.ds(c, CH), :] = self.pre[c:c + CH]

        def resume(self):
            self.pre = pre_buf.at[self.keep]

        def extra(self, c):
            got = []
            for q in chunk_runs(c):
                base = (q + self.run_shift) % RUNS
                for r, n in pieces(self.t):
                    if self.t == 0:
                        got.append(get_tiles(proj0, pl.ds(base * PAD0 + r + self.row_shift, n)))
                    else:
                        got.append(get_tiles(proj1, pl.ds(base * PAD1 + 8 + r + self.row_shift, n)))
            return jnp.concatenate(got, axis=ZERO) + recv[part_rows(self.t, c), :]

        def fin(self):
            hide(self.slot, self.pre, self.extra)

        def b(self):
            y = dot(hid[self.slot], self.w.edge_out[...])
            for c in chunks():
                part = part_rows(self.t, c)
                value = (self.source[self.k, part, :].astype(F32) + norm(y[c:c + CH])).astype(BF16)
                edge[self.k, part, :] = value
                total = value.astype(F32)
                if not self.first:
                    total = total + acc[part, :]
                if self.final:
                    esum[part, :] = total.astype(BF16)
                else:
                    acc[part, :] = total

    class Node:
        def __init__(self, t, base, w):
            self.t, self.base, self.w, self.slot = t, base, w, 6 + t

        def own(self):
            self.pre = dot(self.base[tile_rows(self.t), :], self.w.node[0][...])

        def a(self):
            hide(self.slot, self.pre + dot(esum[tile_rows(self.t), :], self.w.node[1][...]))

        def b(self):
            y = dot(hid[self.slot], self.w.node_out[...])
            for c in chunks():
                part = part_rows(self.t, c)
                value = (self.base[part, :].astype(F32) + norm(y[c:c + CH])).astype(BF16)
                h[part, :] = value
                if self.t == 1:
                    set_tiles(hf, pl.ds(c, CH), value.astype(F32))

    def project_send(t, w):
        out = dot(h[tile_rows(t), :], w.edge[1][...])
        for q in range(RUNS):
            row = q * HALF
            for r, n in pieces(t):
                if t == 0:
                    set_tiles(proj0, pl.ds(q * PAD0 + r, n), out[row:row + n])
                else:
                    set_tiles(proj1, pl.ds(q * PAD1 + 8 + r, n), out[row:row + n])
                row += n
        if t == 1:
            for r in (7, 24):
                set_tiles(proj0, pl.ds(r, RUNS, stride=PAD0), get_tiles(proj1, pl.ds(8 + r, RUNS, stride=PAD1)))

    def project_recv(t, w):
        out = dot(h[tile_rows(t), :], w.edge[2][...])
        for c in chunks():
            recv[part_rows(t, c), :] = out[c:c + CH]

    def project(t, w):
        project_send(t, w)
        project_recv(t, w)

    def share_rows():
        for r in (8, 23):
            set_tiles(proj1, pl.ds(8 + r, RUNS, stride=PAD1), get_tiles(proj0, pl.ds(r, RUNS, stride=PAD0)))

    def far_items(t, w, source=None, resume=False):
        items = [Edge(t, k, w, n, run_shift=s, source=source, first=n == 0, keep=4 * t + n) for n, (k, s) in enumerate(FAR)]
        if resume:
            for item in items:
                item.resume()
        return items

    def near_items(t, w, resume=False):
        items = [Edge(t, k, w, 4 + n, row_shift=s, final=n == 1, keep=8 + t if n == 0 else None)
                 for n, (k, s) in enumerate(NEAR)]
        if resume:
            items[0].resume()
        return items

    def phase(order, x, n, node, next_x, next_n, before, w_next):
        table = {"before": before, "n1": n[1].a, "nh": node.own, "na": node.a, "nb": node.b, "an0": next_n[0].a,
                 "ps": lambda: project_send(node.t, w_next), "pr": lambda: project_recv(node.t, w_next)}
        for i in range(4):
            table[f"fx{i}"], table[f"bx{i}"], table[f"ax{i}"] = x[i].fin, x[i].b, next_x[i].a
        for i in range(PAIR):
            table[f"fn{i}"], table[f"bn{i}"] = n[i].fin, n[i].b
        run(order, table)

    def run(order, table):
        for name in order:
            table[name]()

    def encoder(step):
        w = Weights(enc_refs, ZERO)
        w1 = layer_weights(step, 1)
        w2 = layer_weights(step, 2)
        table = {"send": lambda: send_halo(ZERO), "share": share_rows}

        def spread():
            for k in range(6):
                for t in range(TILES):
                    if t == 1 or k < PAIR:
                        edge[k, tile_rows(t), :] = edge_base[k, tile_rows(t), :]

        table["copy"] = spread
        y, x, z, n = far_items(0, w1, edge_base), far_items(1, w1), far_items(0, w2), near_items(0, w1)
        for k in range(4):
            table[f"ya{k}"], table[f"yf{k}"], table[f"yb{k}"] = y[k].a, y[k].fin, y[k].b
            table[f"xa{k}"], table[f"za{k}"] = x[k].a, z[k].a
        table["n0"] = n[0].a
        for t in range(TILES):
            def back(t=t):
                out = dot(h_mesh[tile_rows(t), :], w.edge[2][...])
                for c in chunks():
                    recv[part_rows(t, c), :] = out[c:c + CH]

            node = Node(t, h_mesh, w)
            table[f"r{t}"], table[f"nh{t}"], table[f"na{t}"], table[f"nb{t}"] = back, node.own, node.a, node.b
            table[f"ps{t}"], table[f"pr{t}"] = functools.partial(project_send, t, w1), functools.partial(project_recv, t, w1)
            for p in range(PAIR):
                i = PAIR * t + p
                low, high = 8 + i, 12 + i

                def in_first(t=t, p=p, low=low):
                    hide(low, dot(feat[p, t].reshape(TILE, 2 * LANES), we[pl.ds(9 + PAIR * step, PAIR)].reshape(2 * LANES, LAT)))

                def in_last(t=t, p=p, low=low):
                    y = dot(hid[low], weo[ZERO])
                    for c in chunks():
                        v[p, part_rows(t, c), :] = norm(y[c:c + CH]).astype(BF16)

                def edge_first(t=t, p=p, high=high):
                    pre = dot(g2m[p, tile_rows(t), :], w.edge[0][...]) + dot(v[p, tile_rows(t), :], w.edge[1][...])
                    hide(high, pre, lambda c: recv[part_rows(t, c), :])

                def edge_last(t=t, p=p, high=high):
                    y = dot(hid[high], w.edge_out[...])
                    for c in chunks():
                        part = part_rows(t, c)
                        total = (g2m[p, part, :].astype(F32) + norm(y[c:c + CH])).astype(BF16).astype(F32)
                        if p == 0:
                            acc[part, :] = total
                        else:
                            esum[part, :] = (acc[part, :] + total).astype(BF16)

                def self_first(t=t, p=p, low=low):
                    hide(low, dot(v[p, tile_rows(t), :], wself[ZERO]))

                def self_last(t=t, p=p, low=low):
                    y = dot(hid[low], wself[ONE])
                    for c in chunks():
                        part = part_rows(t, c)
                        vc[p, part, :] = (v[p, part, :].astype(F32) + norm(y[c:c + CH])).astype(BF16)

                table[f"va{i}"], table[f"vb{i}"], table[f"ea{i}"], table[f"eb{i}"] = in_first, in_last, edge_first, edge_last
                table[f"sa{i}"], table[f"sb{i}"] = self_first, self_last
        run(ORDER_E, table)

    def out_copies(step, t):
        copies = []
        for hop in range(RING):
            target = lax.rem(me + hop, RING)
            src, dst = x_buf.at[step + 1, :, t, pl.ds(PAIR * target, PAIR)], out.at[step, place, :, t]
            if hop == 0:
                copies.append(pltpu.make_async_copy(src, dst, out_recv.at[step, t, hop]))
            else:
                copies.append(pltpu.make_async_remote_copy(
                    src_ref=src, dst_ref=dst, send_sem=out_send.at[step, t, hop], recv_sem=out_recv.at[step, t, hop],
                    device_id=at(target), device_id_type=mesh_id))
        return copies

    def decoder(step):
        w16 = layer_weights(step, LAYERS)
        w = layer_weights(step, BLOCKS - 1)
        in_mean = stats[ZERO:ONE, :]
        in_std = stats[ONE:PAIR, :]
        diff_mean, diff_std = (jnp.concatenate([stats[i:i + 1, :], jnp.zeros((ONE, LANES - VARS), F32)], axis=ONE) for i in (2, 3))
        halo_slot = lax.rem(LAYERS + 1, 2)
        table = {"share": share_rows, "wait": lambda: wait_halo(halo_slot), "halo": lambda: project_halo(halo_slot, w16)}
        x = far_items(1, w16, resume=True)
        for k in range(4):
            table[f"fx{k}"], table[f"bx{k}"] = x[k].fin, x[k].b
        for t in range(TILES):
            node = Node(t, h, w16)
            table[f"nh{t}"], table[f"na{t}"], table[f"nb{t}"] = node.own, node.a, node.b
            near = near_items(t, w16, resume=t == 0)
            for k in range(PAIR):
                table[f"n{t}{k}"], table[f"fn{t}{k}"], table[f"bn{t}{k}"] = near[k].a, near[k].fin, near[k].b

            def back(t=t):
                out = dot(h[tile_rows(t), :], w.edge[1][...])
                for c in chunks():
                    recv[part_rows(t, c), :] = out[c:c + CH]

            def send(t=t):
                start_all(out_copies(step, t))

            table[f"t{t}"], table[f"send{t}"] = back, send
            for p in range(PAIR):
                i = PAIR * t + p
                low, high = 8 + i, 12 + i
                held = {}

                def edge_own(t=t, p=p, held=held):
                    held["edge"] = dot(m2g[p, tile_rows(t), :], w.edge[0][...]) + dot(vc[p, tile_rows(t), :], w.edge[2][...])

                def edge_first(t=t, low=low, held=held):
                    hide(low, held["edge"], lambda c: recv[part_rows(t, c), :])

                def edge_last(t=t, p=p, low=low, i=i):
                    y = dot(hid[low], w.edge_out[...])
                    for c in chunks():
                        part = part_rows(t, c)
                        dec[i, pl.ds(c, CH), :] = (m2g[p, part, :].astype(F32) + norm(y[c:c + CH])).astype(BF16)

                def node_own(t=t, p=p, held=held):
                    held["node"] = dot(vc[p, tile_rows(t), :], w.node[0][...])

                def node_first(high=high, i=i, held=held):
                    hide(high, held["node"] + dot(dec[i], w.node[1][...]))

                def node_last(t=t, p=p, high=high):
                    y = dot(hid[high], w.node_out[...])
                    for c in chunks():
                        part = part_rows(t, c)
                        v[p, part, :] = (vc[p, part, :].astype(F32) + norm(y[c:c + CH])).astype(BF16)

                def out_first(t=t, p=p, low=low):
                    hide(low, dot(v[p, tile_rows(t), :], woh[...]))

                def out_last(t=t, p=p, low=low):
                    pred = dot(hid[low], wof[...])
                    for c in chunks():
                        runs = pl.ds(c // HALF, CH // HALF)
                        now = x_buf[step, p, t, runs].reshape(CH, LANES)
                        new = now + diff_std * pred[c:c + CH] + diff_mean
                        x_buf[step + 1, p, t, runs] = new.reshape(CH // HALF, HALF, LANES)
                        scaled = ((new[:, :VARS] - in_mean) / in_std).astype(BF16)
                        feat[p, t, runs, :, pl.ds(ZERO, VARS)] = scaled.reshape(CH // HALF, HALF, VARS)

                table[f"em{i}"], table[f"ea{i}"], table[f"eb{i}"] = edge_own, edge_first, edge_last
                table[f"dm{i}"], table[f"da{i}"], table[f"db{i}"] = node_own, node_first, node_last
                table[f"oa{i}"], table[f"ob{i}"] = out_first, out_last
        run(ORDER_D, table)

    def wait_all(copies):
        for copy in copies:
            copy.wait()

    def start_all(copies):
        for copy in copies:
            copy.start()

    def one_step(step, carry):
        wait_all(layer_copies(step, 1) + layer_copies(step, 2))
        start_all(layer_copies(step, 3))
        encoder(step)

        def one_layer(block, carry):
            halo_slot = lax.rem(block + 1, 2)
            w, w1, w2 = (layer_weights(step, block + i) for i in range(3))
            phase(ORDER_A, far_items(1, w, resume=True), near_items(0, w, resume=True), Node(0, h, w), far_items(1, w1),
                  near_items(1, w), share_rows, w1)
            wait_halo(halo_slot)
            wait_all(layer_copies(step, block + 2))

            @pl.when(block < LAYERS - 1)
            def _():
                start_all(layer_copies(step, block + 3))

            phase(ORDER_B, far_items(0, w1, resume=True), near_items(1, w, resume=True), Node(1, h, w), far_items(0, w2),
                  near_items(0, w1), lambda: project_halo(halo_slot, w), w1)
            send_halo(1 - halo_slot)
            return carry

        lax.fori_loop(1, LAYERS, one_layer, 0)
        @pl.when(step == 0)
        def _():
            start_all(layer_copies(1, 1) + layer_copies(1, 2))
            wait_in(PAIR)

        decoder(step)
        return carry

    lax.fori_loop(0, 2, one_step, 0)
    for part in range(3):
        for copy in in_copies[part][1:]:
            copy.wait_send()
    for t in range(TILES):
        wait_all(out_copies(0, t) + out_copies(1, t))


def solution(mesh):
    row_spec = P(("dp", "gp"))
    edge_spec = P(("dp", "gp"), None, None)
    whole = P()

    def local_run(x_prev, x_cur, forcing, grid_static, g2m_feat, m2g_feat, mesh_feat, mesh_edge_feat, norm_stats,
                  w_grid_in, w_mesh_in, w_eemb_in, w_embed_out, w_edge_in, w_edge_out, w_node_in, w_node_out,
                  w_grid_self, w_out_hidden, w_out_final):
        any_spec = pl.BlockSpec(memory_space=pl.ANY)
        vmem_spec = pl.BlockSpec(memory_space=pltpu.VMEM)
        dma = pltpu.SemaphoreType.DMA
        grid_dev = x_prev.shape[0]
        shape = jax.ShapeDtypeStruct
        home = shape((RING, PAIR, TILES, PAIR, HALF, LANES), F32)
        bulk = [
            pltpu.VMEM(shape_, F32) for shape_ in (
                (3, mesh_feat.shape[0]), (6, 4, mesh_feat.shape[0]), (VARS, grid_dev), (VARS, grid_dev), (5, PAIR, grid_dev),
                (5, grid_dev), (4, grid_dev), (4, grid_dev))
        ]
        scratch = bulk + [
            pltpu.VMEM((2 * VARS + 10, LAT), BF16),
            pltpu.VMEM((3, LAT), BF16),
            pltpu.VMEM((3, 4, LAT), BF16),
            pltpu.VMEM((VARS, LAT), BF16),
            pltpu.VMEM((*home.shape[:-1], 2 * LANES), BF16),
            pltpu.VMEM((RING, TILES, PAIR, HALF, LANES), BF16),
            pltpu.VMEM(home.shape, F32),
            pltpu.VMEM((TILES, RUNS, HALF, LANES), BF16),
            pltpu.VMEM((3, PAIR, TILES, RUNS, HALF, LANES), F32),
            pltpu.VMEM((PAIR, TILES, RUNS, HALF, 2 * LANES), BF16),
            pltpu.VMEM((13, LANES, LAT), BF16),
            pltpu.VMEM((5, LAT, LAT), BF16),
            pltpu.VMEM((PAIR, LAT, LAT), BF16),
            pltpu.VMEM((LAT, LAT), BF16),
            pltpu.VMEM((LAT, LANES), BF16),
            pltpu.VMEM((1, 3 * LAT, LAT), BF16),
            pltpu.VMEM((1, LAT, LAT), BF16),
            pltpu.VMEM((1, 2 * LAT, LAT), BF16),
            pltpu.VMEM((1, LAT, LAT), BF16),
            pltpu.VMEM((SLOTS, 3 * LAT, LAT), BF16),
            pltpu.VMEM((SLOTS, LAT, LAT), BF16),
            pltpu.VMEM((SLOTS, 2 * LAT, LAT), BF16),
            pltpu.VMEM((SLOTS, LAT, LAT), BF16),
            pltpu.VMEM((6, ROWS, LAT), BF16),
            pltpu.VMEM((6, ROWS, LAT), BF16),
            pltpu.VMEM((ROWS, LAT), BF16),
            pltpu.VMEM((ROWS, LAT), BF16),
            pltpu.VMEM((LAT // LANES, TILE, LANES), F32),
            pltpu.VMEM((PAIR, ROWS, LAT), BF16),
            pltpu.VMEM((PAIR, ROWS, LAT), BF16),
            pltpu.VMEM((PAIR, ROWS, LAT), BF16),
            pltpu.VMEM((PAIR, ROWS, LAT), BF16),
            pltpu.VMEM((LAT // LANES, RUNS * PAD0, LANES), F32),
            pltpu.VMEM((LAT // LANES, RUNS * PAD1, LANES), F32),
            pltpu.VMEM((ROWS, LAT), F32),
            pltpu.VMEM((ROWS, LAT), F32),
            pltpu.VMEM((16, TILE, LAT), BF16),
            pltpu.VMEM((ROWS, LAT), BF16),
            pltpu.VMEM((4, TILE, LAT), BF16),
            pltpu.VMEM((10, TILE, LAT), F32),
            pltpu.VMEM((PAIR, RUNS, LAT), BF16),
            pltpu.VMEM((PAIR, 2, RUNS, LAT), BF16),
            dma((12,)), dma((3, RING)), dma((3, RING)), dma((4,)), dma((1, 4)), dma((SLOTS, 4)), dma((PAIR,)), dma((PAIR, PAIR)),
            dma((PAIR, TILES, RING)), dma((PAIR, TILES, RING)),
        ]
        homes = pl.pallas_call(
            kernel,
            out_shape=shape((PAIR, *home.shape), F32),
            in_specs=[any_spec] * 8 + [vmem_spec] + [any_spec] * 11,
            out_specs=any_spec,
            scratch_shapes=scratch,
            compiler_params=pltpu.CompilerParams(collective_id=0, has_side_effects=True, vmem_limit_bytes=63 << 20),
            name="forecast",
        )(x_prev.T, x_cur.T, forcing.T, grid_static.T, g2m_feat.T, m2g_feat.T, mesh_feat.T,
          jnp.transpose(mesh_edge_feat, (1, 2, 0)), norm_stats, w_grid_in, w_mesh_in, w_eemb_in, w_embed_out, w_edge_in,
          w_edge_out, w_node_in, w_node_out, w_grid_self, w_out_hidden, w_out_final.T)
        out = shape((VARS, grid_dev), F32)
        next_state, after_state = pl.pallas_call(
            unpack_kernel, out_shape=(out, out), in_specs=[vmem_spec], out_specs=(vmem_spec,) * 2,
            scratch_shapes=[pltpu.VMEM((grid_dev, LANES), F32)], name="unpack",
        )(homes)
        return next_state.T, after_state.T

    in_specs = (row_spec, row_spec, edge_spec, row_spec, row_spec, row_spec, row_spec, edge_spec, whole) + (whole,) * 11
    return jax.shard_map(local_run, mesh=mesh, in_specs=in_specs, out_specs=(row_spec, row_spec), check_vma=False)
```

```python
import functools

import jax
import jax.numpy as jnp
from jax import lax
from jax.experimental import pallas as pl
from jax.experimental.pallas import tpu as pltpu
from jax.sharding import PartitionSpec as P

F32 = jnp.float32
BF16 = jnp.bfloat16

RUNS = 16
RUN = 32
GRID_RUN = 2 * RUN
ROWS = RUNS * RUN
ZERO, ONE, LAST = 0, 1, -1
LAT = 512
LANES = 128
PAIR = 2
VARS = 84
PAD0 = 32
PAD1 = 48
TILE = 256
TILES = 2
HALF = TILE // RUNS
CH = 128
RING = 8
LAYERS = 16
BLOCKS = LAYERS + 2
SLOTS = 4
FAR = ((2, 1), (3, -1), (4, 4), (5, -4))
NEAR = ((0, 1), (1, -1))
ORDER_A = (
    "fx1", "before", "fx0", "nh", "n1", "bx0", "bx1", "fn0", "bn0", "fn1", "bn1", "ax0", "fx2", "fx3", "bx2",
    "na", "bx3", "ax2", "nb", "ax1", "an0", "ax3", "pr", "ps",
)
ORDER_B = (
    "before", "fx0", "fx1", "bx0", "n1", "fn1", "bx1", "fx2", "nh", "fn0", "bn0", "bn1", "ax0", "ax1", "fx3",
    "bx2", "na", "bx3", "ax2", "nb", "an0", "ax3", "ps", "pr",
)
ORDER_E = (
    "copy", "r0", "va1", "va0", "va2", "vb1", "vb0", "va3", "r1", "vb2", "vb3", "ea0", "sa0", "ea1", "sa1",
    "eb0", "ea3", "sa2", "eb1", "sb0", "ea2", "sb1", "ya2", "nh0", "eb2", "na0", "sa3", "eb3", "nb0", "sb2",
    "sb3", "ya0", "nh1", "ya1", "na1", "ps0", "pr0", "nb1", "yf0", "yb0", "yf1", "yb1", "ps1", "ya3", "pr1",
    "yf2", "za1", "yb2", "yf3", "yb3", "xa0", "share", "xa1", "za3", "xa3", "za0", "za2", "xa2", "n0", "send",
)
ORDER_D = (
    "n01", "fx1", "nh0", "fx0", "share", "bx0", "fn00", "fn01", "bx1", "fx2", "bn00", "bn01", "fx3", "em0",
    "bx2", "na0", "em1", "nb0", "n11", "wait", "dm0", "n10", "t0", "halo", "bx3", "ea0", "fn11", "fn10",
    "bn10", "eb0", "bn11", "ea1", "eb1", "nh1", "em2", "em3", "na1", "da0", "dm1", "nb1", "da1", "dm2", "db0",
    "t1", "db1", "oa0", "ea2", "eb2", "oa1", "ob0", "ea3", "dm3", "ob1", "eb3", "send0", "da2", "da3", "db2",
    "db3", "oa2", "oa3", "ob2", "ob3", "send1",
)


def dot(a, b):
    return jnp.dot(a, b, preferred_element_type=F32)


def silu(pre):
    return pre * jax.nn.sigmoid(pre)


def norm(y):
    centred = y - jnp.mean(y, axis=LAST, keepdims=True)
    return centred * lax.rsqrt(jnp.mean(centred * centred, axis=LAST, keepdims=True) + 1e-5)


def ring_place(dev):
    high = lax.div(dev, 4)
    return high * (4 + lax.rem(dev + 2, 4)) + (1 - high) * dev


def chunks():
    return range(0, TILE, CH)


def tile_rows(t):
    return pl.ds(t * TILE, TILE)


def part_rows(t, c):
    return pl.ds(t * TILE + c, CH)


def chunk_runs(c):
    return range(c // HALF, (c + CH) // HALF)


def pieces(t):
    return ((8, 16),) if t == 0 else ((0, 8), (24, 8))


def get_tiles(ref, rows):
    return jnp.concatenate([ref[j, rows, :] for j in range(ref.shape[0])], axis=ONE)


def set_tiles(ref, rows, value):
    for j in range(ref.shape[0]):
        ref[j, rows, :] = value[:, LANES * j:LANES * j + LANES]


AT_FORCE, AT_STATIC, AT_NEXT, AT_M2G, AT_G2M = 88, 96, 104, 112, 120


def columns(n):
    return pl.ds(LANES * n, LANES)


def stack(ref, rows):
    end = 0
    for at_row, value in rows:
        first = at_row // 8 * 8
        last = (at_row + value.shape[0]) // 8 * 8
        if first > end:
            ref[pl.ds(end, first - end), :] = jnp.zeros((first - end, LANES), F32)
        if last < at_row + value.shape[0]:
            ref[pl.ds(last, 8), :] = jnp.zeros((8, LANES), F32)
            end = last + 8
        else:
            end = last
        ref[pl.ds(at_row, value.shape[0]), :] = value
    if end < LANES:
        ref[pl.ds(end, LANES - end), :] = jnp.zeros((LANES - end, LANES), F32)


def unpack_kernel(homes, out0, out1, area):
    for home, out in ((homes.at[ZERO], out0), (homes.at[ONE], out1)):
        for band in range(PAIR):
            for k in range(RING):
                for p in range(PAIR):
                    for t in range(TILES):
                        row = 0
                        for r, rows in pieces(t):
                            spot = pl.ds((band * RING + k) * GRID_RUN + PAIR * r + p, rows, stride=PAIR)
                            area[spot, :] = home[k, p, t, band, pl.ds(row, rows), :]
                            row += rows
        for n in range(out.shape[1] // LANES):
            out[:, columns(n)] = jnp.transpose(area[columns(n), :])[:VARS]


def kernel(x_prev, x_cur, forcing, static, g2m_feat, m2g_feat, mesh_feat, mesh_edge_feat, stats, w_grid_in, w_mesh_in,
           w_eemb_in, w_embed_out, w_edge_in, w_edge_out, w_node_in, w_node_out, w_grid_self, w_out_hidden, w_out_final,
           out,
           mesh_raw, medge_raw, prev_raw, cur_raw, force_raw, static_raw, g2m_raw, m2g_raw,
           wgrid_raw, wmesh_raw, weemb_raw, wfin_raw, g_home, m_home, x_home,
           m_buf, x_buf, feat, we, weo, wself, woh, wof,
           enc_ei, enc_eo, enc_ni, enc_no, lay_ei, lay_eo, lay_ni, lay_no,
           edge_base, edge, h_mesh, h, hf, g2m, m2g, v, vc, proj0, proj1, recv, acc, hid, esum, dec, pre_buf,
           send_buf, halo_buf,
           raw_sem, in_send, in_recv, w_sem, enc_sem, lay_sem, halo_send, halo_recv, out_send, out_recv):
    me = lax.axis_index("gp")
    place = ring_place(me)

    def at(dev):
        return {"gp": dev}

    mesh_id = pl.DeviceIdType.MESH

    def block_copies(block, dst_refs, slot, sem):
        srcs = (w_edge_in, w_edge_out, w_node_in, w_node_out)
        return [pltpu.make_async_copy(src.at[block], dst.at[slot], sem.at[slot, i])
                for i, (src, dst) in enumerate(zip(srcs, dst_refs))]

    enc_refs = (enc_ei, enc_eo, enc_ni, enc_no)
    lay_refs = (lay_ei, lay_eo, lay_ni, lay_no)

    def enc_copies():
        return block_copies(0, enc_refs, 0, enc_sem)

    def slot_of(step, block):
        return lax.rem((BLOCKS - 1) * step + block - 1, SLOTS)

    def layer_copies(step, block):
        return block_copies(block, lay_refs, slot_of(step, block), lay_sem)

    class Weights:
        def __init__(self, refs, slot):
            self.edge = [refs[0].at[slot, pl.ds(i * LAT, LAT)] for i in range(3)]
            self.edge_out = refs[1].at[slot]
            self.node = [refs[2].at[slot, pl.ds(i * LAT, LAT)] for i in range(2)]
            self.node_out = refs[3].at[slot]

    def layer_weights(step, block):
        return Weights(lay_refs, slot_of(step, block))

    raw = [pltpu.make_async_copy(src, dst, raw_sem.at[i]) for i, (src, dst) in enumerate(
        ((mesh_feat, mesh_raw), (mesh_edge_feat, medge_raw), (x_prev, prev_raw), (x_cur, cur_raw), (forcing, force_raw),
         (static, static_raw), (g2m_feat, g2m_raw), (m2g_feat, m2g_raw),
         (w_grid_in, wgrid_raw), (w_mesh_in, wmesh_raw), (w_eemb_in, weemb_raw), (w_out_final, wfin_raw)))]
    for copy in raw:
        copy.start()
    small = [
        pltpu.make_async_copy(w_embed_out, weo, w_sem.at[0]),
        pltpu.make_async_copy(w_grid_self, wself, w_sem.at[1]),
        pltpu.make_async_copy(w_out_hidden, woh, w_sem.at[2]),
    ]
    small[0].start()

    barrier = pltpu.get_barrier_semaphore()
    for hop in range(1, RING):
        pl.semaphore_signal(barrier, inc=1, device_id=at(lax.rem(me + hop, RING)), device_id_type=mesh_id)

    mine = pl.ds(PAIR * me, PAIR)
    parts = ((m_home, m_buf.at[:, mine]), (g_home, feat.at[:, :, mine]), (x_home, x_buf.at[ZERO, :, :, mine]))

    def in_copy(part, hop):
        src, dst = parts[part]
        target = lax.rem(me + hop, RING)
        src = src.at[ring_place(target)]
        if hop == 0:
            return pltpu.make_async_copy(src, dst, in_recv.at[part, hop])
        return pltpu.make_async_remote_copy(src_ref=src, dst_ref=dst, send_sem=in_send.at[part, hop],
                                            recv_sem=in_recv.at[part, hop], device_id=at(target),
                                            device_id_type=mesh_id)

    in_copies = [[in_copy(part, hop) for hop in range(RING)] for part in range(3)]

    def wait_in(part):
        in_copies[part][0].wait()
        for copy in in_copies[part][1:]:
            copy.wait_recv()

    def start_in(part):
        for copy in in_copies[part]:
            copy.start()

    def place_of(area, n):
        ref, first = area
        return ref.at[first + n // 4, columns(n % 4)]

    prev_area, cur_area, norm_area, mesh_area, final_area = (proj0, 0), (proj0, PAIR), (proj1, 0), (proj1, 2), (proj1, 3)

    def turned(area, n):
        return jnp.transpose(place_of(area, n)[...])

    for copy in raw[:2]:
        copy.wait()
    for n in range(mesh_raw.shape[1] // LANES):
        stack(place_of(mesh_area, n), [(ZERO, mesh_raw[:, columns(n)])] + [
            (16 + 16 * k, medge_raw[k, :, columns(n)]) for k in range(6)])
    for n in range(mesh_raw.shape[1] // LANES):
        turned_rows = turned(mesh_area, n)
        for i in range(LANES // RUN):
            band, k = divmod(n * LANES + i * RUN, RING * RUN)
            for t in range(TILES):
                m_home[k // RUN, t, band] = jnp.concatenate(
                    [turned_rows[i * RUN + r:i * RUN + r + rows] for r, rows in pieces(t)], axis=ZERO).astype(BF16)
    pl.semaphore_wait(barrier, RING - 1)
    start_in(0)
    for copy in raw[2:8]:
        copy.wait()
    blocks = range(cur_raw.shape[1] // LANES)
    for n in blocks:
        stack(place_of(prev_area, n), [
            (ZERO, prev_raw[:, columns(n)]), (AT_FORCE, force_raw[:, ZERO, columns(n)]), (AT_STATIC, static_raw[:, columns(n)]),
            (AT_NEXT, force_raw[:, ONE, columns(n)]), (AT_M2G, m2g_raw[:, columns(n)]), (AT_G2M, g2m_raw[:, columns(n)])])
        stack(place_of(cur_area, n), [(ZERO, cur_raw[:, columns(n)])])
    rest = LANES - VARS
    wide_mean = jnp.concatenate([stats[ZERO:ONE, :], jnp.zeros((ONE, rest), F32)], axis=ONE)
    wide_std = jnp.concatenate([stats[ONE:PAIR, :], jnp.ones((ONE, rest), F32)], axis=ONE)
    for n in blocks:
        prev, cur = turned(prev_area, n), turned(cur_area, n)
        place_of(prev_area, n)[...] = (prev - wide_mean) / wide_std
        place_of(cur_area, n)[...] = cur
        place_of(norm_area, n)[...] = (cur - wide_mean) / wide_std
    for k in range(RING):
        for p in range(PAIR):
            for t in range(TILES):
                for band in range(PAIR):
                    def rows_of(area):
                        ref, first = area
                        return jnp.concatenate([ref[first + band, pl.ds(k * GRID_RUN + PAIR * r + p, rows, stride=PAIR), :]
                                                for r, rows in pieces(t)], axis=ZERO)
                    g_home[k, p, t, band, :, pl.ds(ZERO, LANES)] = rows_of(prev_area).astype(BF16)
                    g_home[k, p, t, band, :, pl.ds(LANES, LANES)] = rows_of(norm_area).astype(BF16)
                    x_home[k, p, t, band] = rows_of(cur_area)
    start_in(1)
    for copy in small[1:] + enc_copies() + layer_copies(0, 1) + layer_copies(0, 2):
        copy.start()

    for copy in raw[8:]:
        copy.wait()
    for n in range(LAT // LANES):
        stack(place_of(final_area, n), [(ZERO, wfin_raw[:, columns(n)].astype(F32))])
        wof[columns(n), :] = turned(final_area, n).astype(BF16)
    wide = wgrid_raw[...].astype(F32)
    recv[pl.ds(ZERO, wide.shape[0]), :] = wide
    prev_w, cur_w = recv[pl.ds(ZERO, VARS), :], recv[pl.ds(VARS, VARS), :]
    force_w, static_w = recv[pl.ds(2 * VARS, 5), :], recv[pl.ds(2 * VARS + 5, 5), :]
    spread = [[(0, wmesh_raw[...].astype(F32))], [(AT_G2M, weemb_raw[0].astype(F32))], [(AT_M2G, weemb_raw[1].astype(F32))]]
    spread += [[(16 + 16 * k, weemb_raw[2].astype(F32))] for k in range(6)]
    spread += [[(0, prev_w), (AT_FORCE, force_w), (AT_STATIC, static_w)], [(0, cur_w)]]
    spread += [[(0, cur_w), (AT_STATIC, static_w), (AT_NEXT, force_w)], [(0, prev_w)]]
    for i, rows in enumerate(spread):
        base = LANES * (i % 4)
        acc[pl.ds(base, LANES), :] = jnp.zeros((LANES, LAT), F32)
        for at_row, value in rows:
            acc[pl.ds(base + at_row, value.shape[0]), :] = value
        we[i] = acc[pl.ds(base, LANES), :].astype(BF16)

    def pipeline(items):
        depth = max(len(item) for item in items)
        for beat in range(len(items) + depth - 1):
            for stage in range(depth):
                index = beat - stage
                if 0 <= index < len(items) and stage < len(items[index]):
                    items[index][stage](index)

    def hide(slot, pre, extra=None):
        for c in chunks():
            value = pre[c:c + CH]
            if extra is not None:
                value = value + extra(c)
            hid[slot, pl.ds(c, CH), :] = silu(value).astype(BF16)

    def embed_item(load, w_first, second, store):
        def first(i):
            hide(i % PAIR, dot(load(), we[w_first]))

        def last(i):
            y = dot(hid[i % 2], weo[second])
            for c in chunks():
                store(c, norm(y[c:c + CH]).astype(BF16))

        return [first, last]

    wait_in(0)
    small[0].wait()
    def next_run(ref, *index):
        first = ref[(*index, pl.ds(ONE, RUNS - 1), slice(None), pl.ds(ZERO, LANES))]
        last = ref[(*index, pl.ds(ZERO, ONE), slice(None), pl.ds(ZERO, LANES))]
        return jnp.concatenate([first, last], axis=ZERO).reshape(TILE, LANES)

    mesh_rows = [next_run(m_buf, t) for t in range(TILES)]
    items = []
    for t in range(TILES):
        def store_mesh(c, value, t=t):
            h_mesh[part_rows(t, c), :] = value
        items.append(embed_item(lambda t=t: mesh_rows[t], 0, 1, store_mesh))
        for k in range(6):
            def store_edge(c, value, t=t, k=k):
                edge_base[k, part_rows(t, c), :] = value
            items.append(embed_item(lambda t=t: mesh_rows[t], 3 + k, 4, store_edge))
    pipeline(items)

    wait_in(1)
    start_in(PAIR)
    items = []
    for t in range(TILES):
        for p in range(PAIR):
            def store_m2g(c, value, t=t, p=p):
                m2g[p, part_rows(t, c), :] = value
            def store_g2m(c, value, t=t, p=p):
                g2m[p, part_rows(t, c), :] = value
            items.append(embed_item(lambda t=t, p=p: next_run(feat, p, t), 1, 2, store_g2m))
            items.append(embed_item(lambda t=t, p=p: feat[p, t, :, :, pl.ds(ZERO, LANES)].reshape(TILE, LANES), 2, 3, store_m2g))
    pipeline(items)
    for copy in small[1:] + enc_copies():
        copy.wait()

    left = ring_place(lax.rem(place + RING - 1, RING))
    right = ring_place(lax.rem(place + 1, RING))

    def halo_copies(slot):
        return [
            pltpu.make_async_remote_copy(src_ref=send_buf.at[side], dst_ref=halo_buf.at[slot, side],
                                         send_sem=halo_send.at[side], recv_sem=halo_recv.at[slot, side],
                                         device_id=at(target), device_id_type=mesh_id)
            for side, target in ((0, left), (1, right))
        ]

    def send_halo(slot):
        first = get_tiles(hf, pl.ds(ZERO, RUNS, stride=HALF))
        final = get_tiles(hf, pl.ds(HALF - 1, RUNS, stride=HALF))
        first_on = jnp.concatenate([first[1:], first[:1]], axis=ZERO)
        final_back = jnp.concatenate([final[-1:], final[:-1]], axis=ZERO)
        send_buf[0] = jnp.where(place == 0, first_on, first).astype(BF16)
        send_buf[1] = jnp.where(place == RING - 1, final_back, final).astype(BF16)
        for copy in halo_copies(slot):
            copy.start()

    def wait_halo(slot):
        for copy in halo_copies(slot):
            copy.wait()

    def project_halo(slot, w):
        rows = jnp.concatenate([halo_buf[slot, 0], halo_buf[slot, 1]], axis=ZERO)
        out = dot(rows, w.edge[1][...])
        set_tiles(proj1, pl.ds(8 + RUN, RUNS, stride=PAD1), out[:RUNS])
        set_tiles(proj1, pl.ds(7, RUNS, stride=PAD1), out[RUNS:])

    class Edge:
        def __init__(self, t, k, w, slot, run_shift=0, row_shift=0, source=None, first=False, final=False, keep=None):
            self.t, self.k, self.w, self.slot, self.keep = t, k, w, slot, keep
            self.run_shift, self.row_shift, self.first, self.final = run_shift, row_shift, first, final
            self.source = edge if source is None else source
            self.pre = None

        def a(self):
            self.pre = dot(self.source[self.k, tile_rows(self.t), :], self.w.edge[0][...])
            if self.keep is not None:
                for c in chunks():
                    pre_buf[self.keep, pl.ds(c, CH), :] = self.pre[c:c + CH]

        def resume(self):
            self.pre = pre_buf.at[self.keep]

        def extra(self, c):
            got = []
            for q in chunk_runs(c):
                base = (q + self.run_shift) % RUNS
                for r, n in pieces(self.t):
                    if self.t == 0:
                        got.append(get_tiles(proj0, pl.ds(base * PAD0 + r + self.row_shift, n)))
                    else:
                        got.append(get_tiles(proj1, pl.ds(base * PAD1 + 8 + r + self.row_shift, n)))
            return jnp.concatenate(got, axis=ZERO) + recv[part_rows(self.t, c), :]

        def fin(self):
            hide(self.slot, self.pre, self.extra)

        def b(self):
            y = dot(hid[self.slot], self.w.edge_out[...])
            for c in chunks():
                part = part_rows(self.t, c)
                value = (self.source[self.k, part, :].astype(F32) + norm(y[c:c + CH])).astype(BF16)
                edge[self.k, part, :] = value
                total = value.astype(F32)
                if not self.first:
                    total = total + acc[part, :]
                if self.final:
                    esum[part, :] = total.astype(BF16)
                else:
                    acc[part, :] = total

    class Node:
        def __init__(self, t, base, w):
            self.t, self.base, self.w, self.slot = t, base, w, 6 + t

        def own(self):
            self.pre = dot(self.base[tile_rows(self.t), :], self.w.node[0][...])

        def a(self):
            hide(self.slot, self.pre + dot(esum[tile_rows(self.t), :], self.w.node[1][...]))

        def b(self):
            y = dot(hid[self.slot], self.w.node_out[...])
            for c in chunks():
                part = part_rows(self.t, c)
                value = (self.base[part, :].astype(F32) + norm(y[c:c + CH])).astype(BF16)
                h[part, :] = value
                if self.t == 1:
                    set_tiles(hf, pl.ds(c, CH), value.astype(F32))

    def project_send(t, w):
        out = dot(h[tile_rows(t), :], w.edge[1][...])
        for q in range(RUNS):
            row = q * HALF
            for r, n in pieces(t):
                if t == 0:
                    set_tiles(proj0, pl.ds(q * PAD0 + r, n), out[row:row + n])
                else:
                    set_tiles(proj1, pl.ds(q * PAD1 + 8 + r, n), out[row:row + n])
                row += n
        if t == 1:
            for r in (7, 24):
                set_tiles(proj0, pl.ds(r, RUNS, stride=PAD0), get_tiles(proj1, pl.ds(8 + r, RUNS, stride=PAD1)))

    def project_recv(t, w):
        out = dot(h[tile_rows(t), :], w.edge[2][...])
        for c in chunks():
            recv[part_rows(t, c), :] = out[c:c + CH]

    def project(t, w):
        project_send(t, w)
        project_recv(t, w)

    def share_rows():
        for r in (8, 23):
            set_tiles(proj1, pl.ds(8 + r, RUNS, stride=PAD1), get_tiles(proj0, pl.ds(r, RUNS, stride=PAD0)))

    def far_items(t, w, source=None, resume=False):
        items = [Edge(t, k, w, n, run_shift=s, source=source, first=n == 0, keep=4 * t + n) for n, (k, s) in enumerate(FAR)]
        if resume:
            for item in items:
                item.resume()
        return items

    def near_items(t, w, resume=False):
        items = [Edge(t, k, w, 4 + n, row_shift=s, final=n == 1, keep=8 + t if n == 0 else None)
                 for n, (k, s) in enumerate(NEAR)]
        if resume:
            items[0].resume()
        return items

    def phase(order, x, n, node, next_x, next_n, before, w_next):
        table = {"before": before, "n1": n[1].a, "nh": node.own, "na": node.a, "nb": node.b, "an0": next_n[0].a,
                 "ps": lambda: project_send(node.t, w_next), "pr": lambda: project_recv(node.t, w_next)}
        for i in range(4):
            table[f"fx{i}"], table[f"bx{i}"], table[f"ax{i}"] = x[i].fin, x[i].b, next_x[i].a
        for i in range(PAIR):
            table[f"fn{i}"], table[f"bn{i}"] = n[i].fin, n[i].b
        run(order, table)

    def run(order, table):
        for name in order:
            table[name]()

    def encoder(step):
        w = Weights(enc_refs, ZERO)
        w1 = layer_weights(step, 1)
        w2 = layer_weights(step, 2)
        table = {"send": lambda: send_halo(ZERO), "share": share_rows}

        def spread():
            for k in range(6):
                for t in range(TILES):
                    if t == 1 or k < PAIR:
                        edge[k, tile_rows(t), :] = edge_base[k, tile_rows(t), :]

        table["copy"] = spread
        y, x, z, n = far_items(0, w1, edge_base), far_items(1, w1), far_items(0, w2), near_items(0, w1)
        for k in range(4):
            table[f"ya{k}"], table[f"yf{k}"], table[f"yb{k}"] = y[k].a, y[k].fin, y[k].b
            table[f"xa{k}"], table[f"za{k}"] = x[k].a, z[k].a
        table["n0"] = n[0].a
        for t in range(TILES):
            def back(t=t):
                out = dot(h_mesh[tile_rows(t), :], w.edge[2][...])
                for c in chunks():
                    recv[part_rows(t, c), :] = out[c:c + CH]

            node = Node(t, h_mesh, w)
            table[f"r{t}"], table[f"nh{t}"], table[f"na{t}"], table[f"nb{t}"] = back, node.own, node.a, node.b
            table[f"ps{t}"], table[f"pr{t}"] = functools.partial(project_send, t, w1), functools.partial(project_recv, t, w1)
            for p in range(PAIR):
                i = PAIR * t + p
                low, high = 8 + i, 12 + i

                def in_first(t=t, p=p, low=low):
                    hide(low, dot(feat[p, t].reshape(TILE, 2 * LANES), we[pl.ds(9 + PAIR * step, PAIR)].reshape(2 * LANES, LAT)))

                def in_last(t=t, p=p, low=low):
                    y = dot(hid[low], weo[ZERO])
                    for c in chunks():
                        v[p, part_rows(t, c), :] = norm(y[c:c + CH]).astype(BF16)

                def edge_first(t=t, p=p, high=high):
                    pre = dot(g2m[p, tile_rows(t), :], w.edge[0][...]) + dot(v[p, tile_rows(t), :], w.edge[1][...])
                    hide(high, pre, lambda c: recv[part_rows(t, c), :])

                def edge_last(t=t, p=p, high=high):
                    y = dot(hid[high], w.edge_out[...])
                    for c in chunks():
                        part = part_rows(t, c)
                        total = (g2m[p, part, :].astype(F32) + norm(y[c:c + CH])).astype(BF16).astype(F32)
                        if p == 0:
                            acc[part, :] = total
                        else:
                            esum[part, :] = (acc[part, :] + total).astype(BF16)

                def self_first(t=t, p=p, low=low):
                    hide(low, dot(v[p, tile_rows(t), :], wself[ZERO]))

                def self_last(t=t, p=p, low=low):
                    y = dot(hid[low], wself[ONE])
                    for c in chunks():
                        part = part_rows(t, c)
                        vc[p, part, :] = (v[p, part, :].astype(F32) + norm(y[c:c + CH])).astype(BF16)

                table[f"va{i}"], table[f"vb{i}"], table[f"ea{i}"], table[f"eb{i}"] = in_first, in_last, edge_first, edge_last
                table[f"sa{i}"], table[f"sb{i}"] = self_first, self_last
        run(ORDER_E, table)

    def out_copies(step, t):
        copies = []
        for hop in range(RING):
            target = lax.rem(me + hop, RING)
            src, dst = x_buf.at[step + 1, :, t, pl.ds(PAIR * target, PAIR)], out.at[step, place, :, t]
            if hop == 0:
                copies.append(pltpu.make_async_copy(src, dst, out_recv.at[step, t, hop]))
            else:
                copies.append(pltpu.make_async_remote_copy(
                    src_ref=src, dst_ref=dst, send_sem=out_send.at[step, t, hop], recv_sem=out_recv.at[step, t, hop],
                    device_id=at(target), device_id_type=mesh_id))
        return copies

    def decoder(step):
        w16 = layer_weights(step, LAYERS)
        w = layer_weights(step, BLOCKS - 1)
        in_mean = stats[ZERO:ONE, :]
        in_std = stats[ONE:PAIR, :]
        diff_mean, diff_std = (jnp.concatenate([stats[i:i + 1, :], jnp.zeros((ONE, LANES - VARS), F32)], axis=ONE) for i in (2, 3))
        halo_slot = lax.rem(LAYERS + 1, 2)
        table = {"share": share_rows, "wait": lambda: wait_halo(halo_slot), "halo": lambda: project_halo(halo_slot, w16)}
        x = far_items(1, w16, resume=True)
        for k in range(4):
            table[f"fx{k}"], table[f"bx{k}"] = x[k].fin, x[k].b
        for t in range(TILES):
            node = Node(t, h, w16)
            table[f"nh{t}"], table[f"na{t}"], table[f"nb{t}"] = node.own, node.a, node.b
            near = near_items(t, w16, resume=t == 0)
            for k in range(PAIR):
                table[f"n{t}{k}"], table[f"fn{t}{k}"], table[f"bn{t}{k}"] = near[k].a, near[k].fin, near[k].b

            def back(t=t):
                out = dot(h[tile_rows(t), :], w.edge[1][...])
                for c in chunks():
                    recv[part_rows(t, c), :] = out[c:c + CH]

            def send(t=t):
                start_all(out_copies(step, t))

            table[f"t{t}"], table[f"send{t}"] = back, send
            for p in range(PAIR):
                i = PAIR * t + p
                low, high = 8 + i, 12 + i
                held = {}

                def edge_own(t=t, p=p, held=held):
                    held["edge"] = dot(m2g[p, tile_rows(t), :], w.edge[0][...]) + dot(vc[p, tile_rows(t), :], w.edge[2][...])

                def edge_first(t=t, low=low, held=held):
                    hide(low, held["edge"], lambda c: recv[part_rows(t, c), :])

                def edge_last(t=t, p=p, low=low, i=i):
                    y = dot(hid[low], w.edge_out[...])
                    for c in chunks():
                        part = part_rows(t, c)
                        dec[i, pl.ds(c, CH), :] = (m2g[p, part, :].astype(F32) + norm(y[c:c + CH])).astype(BF16)

                def node_own(t=t, p=p, held=held):
                    held["node"] = dot(vc[p, tile_rows(t), :], w.node[0][...])

                def node_first(high=high, i=i, held=held):
                    hide(high, held["node"] + dot(dec[i], w.node[1][...]))

                def node_last(t=t, p=p, high=high):
                    y = dot(hid[high], w.node_out[...])
                    for c in chunks():
                        part = part_rows(t, c)
                        v[p, part, :] = (vc[p, part, :].astype(F32) + norm(y[c:c + CH])).astype(BF16)

                def out_first(t=t, p=p, low=low):
                    hide(low, dot(v[p, tile_rows(t), :], woh[...]))

                def out_last(t=t, p=p, low=low):
                    pred = dot(hid[low], wof[...])
                    for c in chunks():
                        runs = pl.ds(c // HALF, CH // HALF)
                        now = x_buf[step, p, t, runs].reshape(CH, LANES)
                        new = now + diff_std * pred[c:c + CH] + diff_mean
                        x_buf[step + 1, p, t, runs] = new.reshape(CH // HALF, HALF, LANES)
                        scaled = ((new[:, :VARS] - in_mean) / in_std).astype(BF16)
                        feat[p, t, runs, :, pl.ds(ZERO, VARS)] = scaled.reshape(CH // HALF, HALF, VARS)

                table[f"em{i}"], table[f"ea{i}"], table[f"eb{i}"] = edge_own, edge_first, edge_last
                table[f"dm{i}"], table[f"da{i}"], table[f"db{i}"] = node_own, node_first, node_last
                table[f"oa{i}"], table[f"ob{i}"] = out_first, out_last
        run(ORDER_D, table)

    def wait_all(copies):
        for copy in copies:
            copy.wait()

    def start_all(copies):
        for copy in copies:
            copy.start()

    def one_step(step, carry):
        wait_all(layer_copies(step, 1) + layer_copies(step, 2))
        start_all(layer_copies(step, 3))
        encoder(step)

        def one_layer(block, carry):
            halo_slot = lax.rem(block + 1, 2)
            w, w1, w2 = (layer_weights(step, block + i) for i in range(3))
            phase(ORDER_A, far_items(1, w, resume=True), near_items(0, w, resume=True), Node(0, h, w), far_items(1, w1),
                  near_items(1, w), share_rows, w1)
            wait_halo(halo_slot)
            wait_all(layer_copies(step, block + 2))

            @pl.when(block < LAYERS - 1)
            def _():
                start_all(layer_copies(step, block + 3))

            phase(ORDER_B, far_items(0, w1, resume=True), near_items(1, w, resume=True), Node(1, h, w), far_items(0, w2),
                  near_items(0, w1), lambda: project_halo(halo_slot, w), w1)
            send_halo(1 - halo_slot)
            return carry

        lax.fori_loop(1, LAYERS, one_layer, 0)
        @pl.when(step == 0)
        def _():
            start_all(layer_copies(1, 1) + layer_copies(1, 2))
            wait_in(PAIR)

        decoder(step)
        return carry

    lax.fori_loop(0, 2, one_step, 0)
    for part in range(3):
        for copy in in_copies[part][1:]:
            copy.wait_send()
    for t in range(TILES):
        wait_all(out_copies(0, t) + out_copies(1, t))


def solution(mesh):
    row_spec = P(("dp", "gp"))
    edge_spec = P(("dp", "gp"), None, None)
    whole = P()

    def local_run(x_prev, x_cur, forcing, grid_static, g2m_feat, m2g_feat, mesh_feat, mesh_edge_feat, norm_stats,
                  w_grid_in, w_mesh_in, w_eemb_in, w_embed_out, w_edge_in, w_edge_out, w_node_in, w_node_out,
                  w_grid_self, w_out_hidden, w_out_final):
        any_spec = pl.BlockSpec(memory_space=pl.ANY)
        vmem_spec = pl.BlockSpec(memory_space=pltpu.VMEM)
        dma = pltpu.SemaphoreType.DMA
        grid_dev = x_prev.shape[0]
        shape = jax.ShapeDtypeStruct
        home = shape((RING, PAIR, TILES, PAIR, HALF, LANES), F32)
        bulk = [
            pltpu.VMEM(shape_, F32) for shape_ in (
                (3, mesh_feat.shape[0]), (6, 4, mesh_feat.shape[0]), (VARS, grid_dev), (VARS, grid_dev), (5, PAIR, grid_dev),
                (5, grid_dev), (4, grid_dev), (4, grid_dev))
        ]
        scratch = bulk + [
            pltpu.VMEM((2 * VARS + 10, LAT), BF16),
            pltpu.VMEM((3, LAT), BF16),
            pltpu.VMEM((3, 4, LAT), BF16),
            pltpu.VMEM((VARS, LAT), BF16),
            pltpu.VMEM((*home.shape[:-1], 2 * LANES), BF16),
            pltpu.VMEM((RING, TILES, PAIR, HALF, LANES), BF16),
            pltpu.VMEM(home.shape, F32),
            pltpu.VMEM((TILES, RUNS, HALF, LANES), BF16),
            pltpu.VMEM((3, PAIR, TILES, RUNS, HALF, LANES), F32),
            pltpu.VMEM((PAIR, TILES, RUNS, HALF, 2 * LANES), BF16),
            pltpu.VMEM((13, LANES, LAT), BF16),
            pltpu.VMEM((5, LAT, LAT), BF16),
            pltpu.VMEM((PAIR, LAT, LAT), BF16),
            pltpu.VMEM((LAT, LAT), BF16),
            pltpu.VMEM((LAT, LANES), BF16),
            pltpu.VMEM((1, 3 * LAT, LAT), BF16),
            pltpu.VMEM((1, LAT, LAT), BF16),
            pltpu.VMEM((1, 2 * LAT, LAT), BF16),
            pltpu.VMEM((1, LAT, LAT), BF16),
            pltpu.VMEM((SLOTS, 3 * LAT, LAT), BF16),
            pltpu.VMEM((SLOTS, LAT, LAT), BF16),
            pltpu.VMEM((SLOTS, 2 * LAT, LAT), BF16),
            pltpu.VMEM((SLOTS, LAT, LAT), BF16),
            pltpu.VMEM((6, ROWS, LAT), BF16),
            pltpu.VMEM((6, ROWS, LAT), BF16),
            pltpu.VMEM((ROWS, LAT), BF16),
            pltpu.VMEM((ROWS, LAT), BF16),
            pltpu.VMEM((LAT // LANES, TILE, LANES), F32),
            pltpu.VMEM((PAIR, ROWS, LAT), BF16),
            pltpu.VMEM((PAIR, ROWS, LAT), BF16),
            pltpu.VMEM((PAIR, ROWS, LAT), BF16),
            pltpu.VMEM((PAIR, ROWS, LAT), BF16),
            pltpu.VMEM((LAT // LANES, RUNS * PAD0, LANES), F32),
            pltpu.VMEM((LAT // LANES, RUNS * PAD1, LANES), F32),
            pltpu.VMEM((ROWS, LAT), F32),
            pltpu.VMEM((ROWS, LAT), F32),
            pltpu.VMEM((16, TILE, LAT), BF16),
            pltpu.VMEM((ROWS, LAT), BF16),
            pltpu.VMEM((4, TILE, LAT), BF16),
            pltpu.VMEM((10, TILE, LAT), F32),
            pltpu.VMEM((PAIR, RUNS, LAT), BF16),
            pltpu.VMEM((PAIR, 2, RUNS, LAT), BF16),
            dma((12,)), dma((3, RING)), dma((3, RING)), dma((4,)), dma((1, 4)), dma((SLOTS, 4)), dma((PAIR,)), dma((PAIR, PAIR)),
            dma((PAIR, TILES, RING)), dma((PAIR, TILES, RING)),
        ]
        homes = pl.pallas_call(
            kernel,
            out_shape=shape((PAIR, *home.shape), F32),
            in_specs=[any_spec] * 8 + [vmem_spec] + [any_spec] * 11,
            out_specs=any_spec,
            scratch_shapes=scratch,
            compiler_params=pltpu.CompilerParams(collective_id=0, has_side_effects=True, vmem_limit_bytes=63 << 20),
            name="forecast",
        )(x_prev.T, x_cur.T, forcing.T, grid_static.T, g2m_feat.T, m2g_feat.T, mesh_feat.T,
          jnp.transpose(mesh_edge_feat, (1, 2, 0)), norm_stats, w_grid_in, w_mesh_in, w_eemb_in, w_embed_out, w_edge_in,
          w_edge_out, w_node_in, w_node_out, w_grid_self, w_out_hidden, w_out_final.T)
        out = shape((VARS, grid_dev), F32)
        next_state, after_state = pl.pallas_call(
            unpack_kernel, out_shape=(out, out), in_specs=[vmem_spec], out_specs=(vmem_spec,) * 2,
            scratch_shapes=[pltpu.VMEM((grid_dev, LANES), F32)], name="unpack",
        )(homes)
        return next_state.T, after_state.T

    in_specs = (row_spec, row_spec, edge_spec, row_spec, row_spec, row_spec, row_spec, edge_spec, whole) + (whole,) * 11
    return jax.shard_map(local_run, mesh=mesh, in_specs=in_specs, out_specs=(row_spec, row_spec), check_vma=False)
```

```python
import functools

import jax
import jax.numpy as jnp
from jax import lax
from jax.experimental import pallas as pl
from jax.experimental.pallas import tpu as pltpu
from jax.sharding import PartitionSpec as P

F32 = jnp.float32
BF16 = jnp.bfloat16

RUNS = 16
RUN = 32
GRID_RUN = 2 * RUN
ROWS = RUNS * RUN
ZERO, ONE, LAST = 0, 1, -1
LAT = 512
LANES = 128
PAIR = 2
VARS = 84
PAD0 = 32
PAD1 = 48
TILE = 256
TILES = 2
HALF = TILE // RUNS
CH = 128
RING = 8
LAYERS = 16
BLOCKS = LAYERS + 2
SLOTS = 4
FAR = ((2, 1), (3, -1), (4, 4), (5, -4))
NEAR = ((0, 1), (1, -1))
ORDER_A = (
    "fx1", "before", "fx0", "nh", "n1", "bx0", "bx1", "fn0", "bn0", "fn1", "bn1", "ax0", "fx2", "fx3", "bx2",
    "na", "bx3", "ax2", "nb", "ax1", "an0", "ax3", "pr", "ps",
)
ORDER_B = (
    "before", "fx0", "fx1", "bx0", "n1", "fn1", "bx1", "fx2", "nh", "fn0", "bn0", "bn1", "ax0", "ax1", "fx3",
    "bx2", "na", "bx3", "ax2", "nb", "an0", "ax3", "ps", "pr",
)
ORDER_E = (
    "copy", "r0", "va1", "va0", "va2", "vb1", "vb0", "va3", "r1", "vb2", "sa0", "vb3", "ea0", "ea1", "sa1",
    "eb0", "ea2", "ea3", "sa2", "eb1", "sb0", "sb1", "ya2", "nh0", "eb2", "na0", "sa3", "eb3", "nb0", "sb2",
    "ya0", "nh1", "ya1", "na1", "ps0", "pr0", "sb3", "nb1", "yf0", "yb0", "yf1", "yb1", "ps1", "share", "ya3",
    "pr1", "yf2", "za1", "yb2", "yf3", "yb3", "xa0", "xa1", "za3", "xa3", "za0", "za2", "xa2", "n0", "send",
)
ORDER_D = (
    "n01", "fx1", "nh0", "fx0", "share", "bx0", "fn00", "fn01", "bx1", "fx2", "bn00", "bn01", "fx3", "em0",
    "bx2", "na0", "em1", "nb0", "n11", "wait", "dm0", "n10", "t0", "halo", "bx3", "ea0", "fn11", "fn10",
    "bn10", "eb0", "bn11", "ea1", "eb1", "nh1", "em2", "em3", "na1", "da0", "dm1", "nb1", "da1", "dm2", "db0",
    "t1", "db1", "oa0", "ea2", "eb2", "oa1", "ob0", "ea3", "dm3", "ob1", "eb3", "send0", "da2", "da3", "db2",
    "db3", "oa2", "oa3", "ob2", "ob3", "send1",
)


def dot(a, b):
    return jnp.dot(a, b, preferred_element_type=F32)


def silu(pre):
    return pre * jax.nn.sigmoid(pre)


def norm(y):
    centred = y - jnp.mean(y, axis=LAST, keepdims=True)
    return centred * lax.rsqrt(jnp.mean(centred * centred, axis=LAST, keepdims=True) + 1e-5)


def ring_place(dev):
    high = lax.div(dev, 4)
    return high * (4 + lax.rem(dev + 2, 4)) + (1 - high) * dev


def chunks():
    return range(0, TILE, CH)


def tile_rows(t):
    return pl.ds(t * TILE, TILE)


def part_rows(t, c):
    return pl.ds(t * TILE + c, CH)


def chunk_runs(c):
    return range(c // HALF, (c + CH) // HALF)


def pieces(t):
    return ((8, 16),) if t == 0 else ((0, 8), (24, 8))


def get_tiles(ref, rows):
    return jnp.concatenate([ref[j, rows, :] for j in range(ref.shape[0])], axis=ONE)


def set_tiles(ref, rows, value):
    for j in range(ref.shape[0]):
        ref[j, rows, :] = value[:, LANES * j:LANES * j + LANES]


AT_FORCE, AT_STATIC, AT_NEXT, AT_M2G, AT_G2M = 88, 96, 104, 112, 120


def columns(n):
    return pl.ds(LANES * n, LANES)


def stack(ref, rows):
    end = 0
    for at_row, value in rows:
        first = at_row // 8 * 8
        last = (at_row + value.shape[0]) // 8 * 8
        if first > end:
            ref[pl.ds(end, first - end), :] = jnp.zeros((first - end, LANES), F32)
        if last < at_row + value.shape[0]:
            ref[pl.ds(last, 8), :] = jnp.zeros((8, LANES), F32)
            end = last + 8
        else:
            end = last
        ref[pl.ds(at_row, value.shape[0]), :] = value
    if end < LANES:
        ref[pl.ds(end, LANES - end), :] = jnp.zeros((LANES - end, LANES), F32)


def unpack_kernel(homes, out0, out1, area):
    for home, out in ((homes.at[ZERO], out0), (homes.at[ONE], out1)):
        for band in range(PAIR):
            for k in range(RING):
                for p in range(PAIR):
                    for t in range(TILES):
                        row = 0
                        for r, rows in pieces(t):
                            spot = pl.ds((band * RING + k) * GRID_RUN + PAIR * r + p, rows, stride=PAIR)
                            area[spot, :] = home[k, p, t, band, pl.ds(row, rows), :]
                            row += rows
        for n in range(out.shape[1] // LANES):
            out[:, columns(n)] = jnp.transpose(area[columns(n), :])[:VARS]


def kernel(x_prev, x_cur, forcing, static, g2m_feat, m2g_feat, mesh_feat, mesh_edge_feat, stats, w_grid_in, w_mesh_in,
           w_eemb_in, w_embed_out, w_edge_in, w_edge_out, w_node_in, w_node_out, w_grid_self, w_out_hidden, w_out_final,
           out,
           mesh_raw, medge_raw, prev_raw, cur_raw, force_raw, static_raw, g2m_raw, m2g_raw,
           wgrid_raw, wmesh_raw, weemb_raw, wfin_raw, g_home, m_home, x_home,
           m_buf, x_buf, feat, we, weo, wself, woh, wof,
           enc_ei, enc_eo, enc_ni, enc_no, lay_ei, lay_eo, lay_ni, lay_no,
           edge_base, edge, h_mesh, h, hf, g2m, m2g, v, vc, proj0, proj1, recv, acc, hid, esum, dec, pre_buf,
           send_buf, halo_buf,
           raw_sem, in_send, in_recv, w_sem, enc_sem, lay_sem, halo_send, halo_recv, out_send, out_recv):
    me = lax.axis_index("gp")
    place = ring_place(me)

    def at(dev):
        return {"gp": dev}

    mesh_id = pl.DeviceIdType.MESH

    def block_copies(block, dst_refs, slot, sem):
        srcs = (w_edge_in, w_edge_out, w_node_in, w_node_out)
        return [pltpu.make_async_copy(src.at[block], dst.at[slot], sem.at[slot, i])
                for i, (src, dst) in enumerate(zip(srcs, dst_refs))]

    enc_refs = (enc_ei, enc_eo, enc_ni, enc_no)
    lay_refs = (lay_ei, lay_eo, lay_ni, lay_no)

    def enc_copies():
        return block_copies(0, enc_refs, 0, enc_sem)

    def slot_of(step, block):
        return lax.rem((BLOCKS - 1) * step + block - 1, SLOTS)

    def layer_copies(step, block):
        return block_copies(block, lay_refs, slot_of(step, block), lay_sem)

    class Weights:
        def __init__(self, refs, slot):
            self.edge = [refs[0].at[slot, pl.ds(i * LAT, LAT)] for i in range(3)]
            self.edge_out = refs[1].at[slot]
            self.node = [refs[2].at[slot, pl.ds(i * LAT, LAT)] for i in range(2)]
            self.node_out = refs[3].at[slot]

    def layer_weights(step, block):
        return Weights(lay_refs, slot_of(step, block))

    raw = [pltpu.make_async_copy(src, dst, raw_sem.at[i]) for i, (src, dst) in enumerate(
        ((mesh_feat, mesh_raw), (mesh_edge_feat, medge_raw), (x_prev, prev_raw), (x_cur, cur_raw), (forcing, force_raw),
         (static, static_raw), (g2m_feat, g2m_raw), (m2g_feat, m2g_raw),
         (w_grid_in, wgrid_raw), (w_mesh_in, wmesh_raw), (w_eemb_in, weemb_raw), (w_out_final, wfin_raw)))]
    for copy in raw:
        copy.start()
    small = [
        pltpu.make_async_copy(w_embed_out, weo, w_sem.at[0]),
        pltpu.make_async_copy(w_grid_self, wself, w_sem.at[1]),
        pltpu.make_async_copy(w_out_hidden, woh, w_sem.at[2]),
    ]
    small[0].start()

    barrier = pltpu.get_barrier_semaphore()
    for hop in range(1, RING):
        pl.semaphore_signal(barrier, inc=1, device_id=at(lax.rem(me + hop, RING)), device_id_type=mesh_id)

    mine = pl.ds(PAIR * me, PAIR)
    parts = ((m_home, m_buf.at[:, mine]), (g_home, feat.at[:, :, mine]), (x_home, x_buf.at[ZERO, :, :, mine]))

    def in_copy(part, hop):
        src, dst = parts[part]
        target = lax.rem(me + hop, RING)
        src = src.at[ring_place(target)]
        if hop == 0:
            return pltpu.make_async_copy(src, dst, in_recv.at[part, hop])
        return pltpu.make_async_remote_copy(src_ref=src, dst_ref=dst, send_sem=in_send.at[part, hop],
                                            recv_sem=in_recv.at[part, hop], device_id=at(target),
                                            device_id_type=mesh_id)

    in_copies = [[in_copy(part, hop) for hop in range(RING)] for part in range(3)]

    def wait_in(part):
        in_copies[part][0].wait()
        for copy in in_copies[part][1:]:
            copy.wait_recv()

    def start_in(part):
        for copy in in_copies[part]:
            copy.start()

    def place_of(area, n):
        ref, first = area
        return ref.at[first + n // 4, columns(n % 4)]

    prev_area, cur_area, norm_area, mesh_area, final_area = (proj0, 0), (proj0, PAIR), (proj1, 0), (proj1, 2), (proj1, 3)

    def turned(area, n):
        return jnp.transpose(place_of(area, n)[...])

    for copy in raw[:2]:
        copy.wait()
    for n in range(mesh_raw.shape[1] // LANES):
        stack(place_of(mesh_area, n), [(ZERO, mesh_raw[:, columns(n)])] + [
            (16 + 16 * k, medge_raw[k, :, columns(n)]) for k in range(6)])
    for n in range(mesh_raw.shape[1] // LANES):
        turned_rows = turned(mesh_area, n)
        for i in range(LANES // RUN):
            band, k = divmod(n * LANES + i * RUN, RING * RUN)
            for t in range(TILES):
                m_home[k // RUN, t, band] = jnp.concatenate(
                    [turned_rows[i * RUN + r:i * RUN + r + rows] for r, rows in pieces(t)], axis=ZERO).astype(BF16)
    pl.semaphore_wait(barrier, RING - 1)
    start_in(0)
    for copy in raw[2:8]:
        copy.wait()
    blocks = range(cur_raw.shape[1] // LANES)
    for n in blocks:
        stack(place_of(prev_area, n), [
            (ZERO, prev_raw[:, columns(n)]), (AT_FORCE, force_raw[:, ZERO, columns(n)]), (AT_STATIC, static_raw[:, columns(n)]),
            (AT_NEXT, force_raw[:, ONE, columns(n)]), (AT_M2G, m2g_raw[:, columns(n)]), (AT_G2M, g2m_raw[:, columns(n)])])
        stack(place_of(cur_area, n), [(ZERO, cur_raw[:, columns(n)])])
    rest = LANES - VARS
    wide_mean = jnp.concatenate([stats[ZERO:ONE, :], jnp.zeros((ONE, rest), F32)], axis=ONE)
    wide_std = jnp.concatenate([stats[ONE:PAIR, :], jnp.ones((ONE, rest), F32)], axis=ONE)
    for n in blocks:
        prev, cur = turned(prev_area, n), turned(cur_area, n)
        place_of(prev_area, n)[...] = (prev - wide_mean) / wide_std
        place_of(cur_area, n)[...] = cur
        place_of(norm_area, n)[...] = (cur - wide_mean) / wide_std
    for k in range(RING):
        for p in range(PAIR):
            for t in range(TILES):
                for band in range(PAIR):
                    def rows_of(area):
                        ref, first = area
                        return jnp.concatenate([ref[first + band, pl.ds(k * GRID_RUN + PAIR * r + p, rows, stride=PAIR), :]
                                                for r, rows in pieces(t)], axis=ZERO)
                    g_home[k, p, t, band, :, pl.ds(ZERO, LANES)] = rows_of(prev_area).astype(BF16)
                    g_home[k, p, t, band, :, pl.ds(LANES, LANES)] = rows_of(norm_area).astype(BF16)
                    x_home[k, p, t, band] = rows_of(cur_area)
    start_in(1)
    for copy in small[1:] + enc_copies() + layer_copies(0, 1) + layer_copies(0, 2):
        copy.start()

    for copy in raw[8:]:
        copy.wait()
    for n in range(LAT // LANES):
        stack(place_of(final_area, n), [(ZERO, wfin_raw[:, columns(n)].astype(F32))])
        wof[columns(n), :] = turned(final_area, n).astype(BF16)
    wide = wgrid_raw[...].astype(F32)
    recv[pl.ds(ZERO, wide.shape[0]), :] = wide
    prev_w, cur_w = recv[pl.ds(ZERO, VARS), :], recv[pl.ds(VARS, VARS), :]
    force_w, static_w = recv[pl.ds(2 * VARS, 5), :], recv[pl.ds(2 * VARS + 5, 5), :]
    spread = [[(0, wmesh_raw[...].astype(F32))], [(AT_G2M, weemb_raw[0].astype(F32))], [(AT_M2G, weemb_raw[1].astype(F32))]]
    spread += [[(16 + 16 * k, weemb_raw[2].astype(F32))] for k in range(6)]
    spread += [[(0, prev_w), (AT_FORCE, force_w), (AT_STATIC, static_w)], [(0, cur_w)]]
    spread += [[(0, cur_w), (AT_STATIC, static_w), (AT_NEXT, force_w)], [(0, prev_w)]]
    for i, rows in enumerate(spread):
        base = LANES * (i % 4)
        acc[pl.ds(base, LANES), :] = jnp.zeros((LANES, LAT), F32)
        for at_row, value in rows:
            acc[pl.ds(base + at_row, value.shape[0]), :] = value
        we[i] = acc[pl.ds(base, LANES), :].astype(BF16)

    def pipeline(items):
        depth = max(len(item) for item in items)
        for beat in range(len(items) + depth - 1):
            for stage in range(depth):
                index = beat - stage
                if 0 <= index < len(items) and stage < len(items[index]):
                    items[index][stage](index)

    def hide(slot, pre, extra=None):
        for c in chunks():
            value = pre[c:c + CH]
            if extra is not None:
                value = value + extra(c)
            hid[slot, pl.ds(c, CH), :] = silu(value).astype(BF16)

    def embed_item(load, w_first, second, store):
        def first(i):
            hide(i % PAIR, dot(load(), we[w_first]))

        def last(i):
            y = dot(hid[i % 2], weo[second])
            for c in chunks():
                store(c, norm(y[c:c + CH]).astype(BF16))

        return [first, last]

    wait_in(0)
    small[0].wait()
    def next_run(ref, *index):
        first = ref[(*index, pl.ds(ONE, RUNS - 1), slice(None), pl.ds(ZERO, LANES))]
        last = ref[(*index, pl.ds(ZERO, ONE), slice(None), pl.ds(ZERO, LANES))]
        return jnp.concatenate([first, last], axis=ZERO).reshape(TILE, LANES)

    mesh_rows = [next_run(m_buf, t) for t in range(TILES)]
    items = []
    for t in range(TILES):
        def store_mesh(c, value, t=t):
            h_mesh[part_rows(t, c), :] = value
        items.append(embed_item(lambda t=t: mesh_rows[t], 0, 1, store_mesh))
        for k in range(6):
            def store_edge(c, value, t=t, k=k):
                edge_base[k, part_rows(t, c), :] = value
            items.append(embed_item(lambda t=t: mesh_rows[t], 3 + k, 4, store_edge))
    pipeline(items)

    wait_in(1)
    start_in(PAIR)
    items = []
    for t in range(TILES):
        for p in range(PAIR):
            def store_m2g(c, value, t=t, p=p):
                m2g[p, part_rows(t, c), :] = value
            def store_g2m(c, value, t=t, p=p):
                g2m[p, part_rows(t, c), :] = value
            items.append(embed_item(lambda t=t, p=p: next_run(feat, p, t), 1, 2, store_g2m))
            items.append(embed_item(lambda t=t, p=p: feat[p, t, :, :, pl.ds(ZERO, LANES)].reshape(TILE, LANES), 2, 3, store_m2g))
    pipeline(items)
    for copy in small[1:] + enc_copies():
        copy.wait()

    left = ring_place(lax.rem(place + RING - 1, RING))
    right = ring_place(lax.rem(place + 1, RING))

    def halo_copies(slot):
        return [
            pltpu.make_async_remote_copy(src_ref=send_buf.at[side], dst_ref=halo_buf.at[slot, side],
                                         send_sem=halo_send.at[side], recv_sem=halo_recv.at[slot, side],
                                         device_id=at(target), device_id_type=mesh_id)
            for side, target in ((0, left), (1, right))
        ]

    def send_halo(slot):
        first = get_tiles(hf, pl.ds(ZERO, RUNS, stride=HALF))
        final = get_tiles(hf, pl.ds(HALF - 1, RUNS, stride=HALF))
        first_on = jnp.concatenate([first[1:], first[:1]], axis=ZERO)
        final_back = jnp.concatenate([final[-1:], final[:-1]], axis=ZERO)
        send_buf[0] = jnp.where(place == 0, first_on, first).astype(BF16)
        send_buf[1] = jnp.where(place == RING - 1, final_back, final).astype(BF16)
        for copy in halo_copies(slot):
            copy.start()

    def wait_halo(slot):
        for copy in halo_copies(slot):
            copy.wait()

    def project_halo(slot, w):
        rows = jnp.concatenate([halo_buf[slot, 0], halo_buf[slot, 1]], axis=ZERO)
        out = dot(rows, w.edge[1][...])
        set_tiles(proj1, pl.ds(8 + RUN, RUNS, stride=PAD1), out[:RUNS])
        set_tiles(proj1, pl.ds(7, RUNS, stride=PAD1), out[RUNS:])

    class Edge:
        def __init__(self, t, k, w, slot, run_shift=0, row_shift=0, source=None, first=False, final=False, keep=None):
            self.t, self.k, self.w, self.slot, self.keep = t, k, w, slot, keep
            self.run_shift, self.row_shift, self.first, self.final = run_shift, row_shift, first, final
            self.source = edge if source is None else source
            self.pre = None

        def a(self):
            self.pre = dot(self.source[self.k, tile_rows(self.t), :], self.w.edge[0][...])
            if self.keep is not None:
                for c in chunks():
                    pre_buf[self.keep, pl.ds(c, CH), :] = self.pre[c:c + CH]

        def resume(self):
            self.pre = pre_buf.at[self.keep]

        def extra(self, c):
            got = []
            for q in chunk_runs(c):
                base = (q + self.run_shift) % RUNS
                for r, n in pieces(self.t):
                    if self.t == 0:
                        got.append(get_tiles(proj0, pl.ds(base * PAD0 + r + self.row_shift, n)))
                    else:
                        got.append(get_tiles(proj1, pl.ds(base * PAD1 + 8 + r + self.row_shift, n)))
            return jnp.concatenate(got, axis=ZERO) + recv[part_rows(self.t, c), :]

        def fin(self):
            hide(self.slot, self.pre, self.extra)

        def b(self):
            y = dot(hid[self.slot], self.w.edge_out[...])
            for c in chunks():
                part = part_rows(self.t, c)
                value = (self.source[self.k, part, :].astype(F32) + norm(y[c:c + CH])).astype(BF16)
                edge[self.k, part, :] = value
                total = value.astype(F32)
                if not self.first:
                    total = total + acc[part, :]
                if self.final:
                    esum[part, :] = total.astype(BF16)
                else:
                    acc[part, :] = total

    class Node:
        def __init__(self, t, base, w):
            self.t, self.base, self.w, self.slot = t, base, w, 6 + t

        def own(self):
            self.pre = dot(self.base[tile_rows(self.t), :], self.w.node[0][...])

        def a(self):
            hide(self.slot, self.pre + dot(esum[tile_rows(self.t), :], self.w.node[1][...]))

        def b(self):
            y = dot(hid[self.slot], self.w.node_out[...])
            for c in chunks():
                part = part_rows(self.t, c)
                value = (self.base[part, :].astype(F32) + norm(y[c:c + CH])).astype(BF16)
                h[part, :] = value
                if self.t == 1:
                    set_tiles(hf, pl.ds(c, CH), value.astype(F32))

    def project_send(t, w):
        out = dot(h[tile_rows(t), :], w.edge[1][...])
        for q in range(RUNS):
            row = q * HALF
            for r, n in pieces(t):
                if t == 0:
                    set_tiles(proj0, pl.ds(q * PAD0 + r, n), out[row:row + n])
                else:
                    set_tiles(proj1, pl.ds(q * PAD1 + 8 + r, n), out[row:row + n])
                row += n
        if t == 1:
            for r in (7, 24):
                set_tiles(proj0, pl.ds(r, RUNS, stride=PAD0), get_tiles(proj1, pl.ds(8 + r, RUNS, stride=PAD1)))

    def project_recv(t, w):
        out = dot(h[tile_rows(t), :], w.edge[2][...])
        for c in chunks():
            recv[part_rows(t, c), :] = out[c:c + CH]

    def project(t, w):
        project_send(t, w)
        project_recv(t, w)

    def share_rows():
        for r in (8, 23):
            set_tiles(proj1, pl.ds(8 + r, RUNS, stride=PAD1), get_tiles(proj0, pl.ds(r, RUNS, stride=PAD0)))

    def far_items(t, w, source=None, resume=False):
        items = [Edge(t, k, w, n, run_shift=s, source=source, first=n == 0, keep=4 * t + n) for n, (k, s) in enumerate(FAR)]
        if resume:
            for item in items:
                item.resume()
        return items

    def near_items(t, w, resume=False):
        items = [Edge(t, k, w, 4 + n, row_shift=s, final=n == 1, keep=8 + t if n == 0 else None)
                 for n, (k, s) in enumerate(NEAR)]
        if resume:
            items[0].resume()
        return items

    def phase(order, x, n, node, next_x, next_n, before, w_next):
        table = {"before": before, "n1": n[1].a, "nh": node.own, "na": node.a, "nb": node.b, "an0": next_n[0].a,
                 "ps": lambda: project_send(node.t, w_next), "pr": lambda: project_recv(node.t, w_next)}
        for i in range(4):
            table[f"fx{i}"], table[f"bx{i}"], table[f"ax{i}"] = x[i].fin, x[i].b, next_x[i].a
        for i in range(PAIR):
            table[f"fn{i}"], table[f"bn{i}"] = n[i].fin, n[i].b
        run(order, table)

    def run(order, table):
        for name in order:
            table[name]()

    def encoder(step):
        w = Weights(enc_refs, ZERO)
        w1 = layer_weights(step, 1)
        w2 = layer_weights(step, 2)
        table = {"send": lambda: send_halo(ZERO), "share": share_rows}

        def spread():
            for k in range(6):
                for t in range(TILES):
                    if t == 1 or k < PAIR:
                        edge[k, tile_rows(t), :] = edge_base[k, tile_rows(t), :]

        table["copy"] = spread
        y, x, z, n = far_items(0, w1, edge_base), far_items(1, w1), far_items(0, w2), near_items(0, w1)
        for k in range(4):
            table[f"ya{k}"], table[f"yf{k}"], table[f"yb{k}"] = y[k].a, y[k].fin, y[k].b
            table[f"xa{k}"], table[f"za{k}"] = x[k].a, z[k].a
        table["n0"] = n[0].a
        for t in range(TILES):
            def back(t=t):
                out = dot(h_mesh[tile_rows(t), :], w.edge[2][...])
                for c in chunks():
                    recv[part_rows(t, c), :] = out[c:c + CH]

            node = Node(t, h_mesh, w)
            table[f"r{t}"], table[f"nh{t}"], table[f"na{t}"], table[f"nb{t}"] = back, node.own, node.a, node.b
            table[f"ps{t}"], table[f"pr{t}"] = functools.partial(project_send, t, w1), functools.partial(project_recv, t, w1)
            for p in range(PAIR):
                i = PAIR * t + p
                low, high = 8 + i, 12 + i

                def in_first(t=t, p=p, low=low):
                    hide(low, dot(feat[p, t].reshape(TILE, 2 * LANES), we[pl.ds(9 + PAIR * step, PAIR)].reshape(2 * LANES, LAT)))

                def in_last(t=t, p=p, low=low):
                    y = dot(hid[low], weo[ZERO])
                    for c in chunks():
                        v[p, part_rows(t, c), :] = norm(y[c:c + CH]).astype(BF16)

                def edge_first(t=t, p=p, high=high):
                    pre = dot(g2m[p, tile_rows(t), :], w.edge[0][...]) + dot(v[p, tile_rows(t), :], w.edge[1][...])
                    hide(high, pre, lambda c: recv[part_rows(t, c), :])

                def edge_last(t=t, p=p, high=high):
                    y = dot(hid[high], w.edge_out[...])
                    for c in chunks():
                        part = part_rows(t, c)
                        total = (g2m[p, part, :].astype(F32) + norm(y[c:c + CH])).astype(BF16).astype(F32)
                        if p == 0:
                            acc[part, :] = total
                        else:
                            esum[part, :] = (acc[part, :] + total).astype(BF16)

                def self_first(t=t, p=p, low=low):
                    hide(low, dot(v[p, tile_rows(t), :], wself[ZERO]))

                def self_last(t=t, p=p, low=low):
                    y = dot(hid[low], wself[ONE])
                    for c in chunks():
                        part = part_rows(t, c)
                        vc[p, part, :] = (v[p, part, :].astype(F32) + norm(y[c:c + CH])).astype(BF16)

                table[f"va{i}"], table[f"vb{i}"], table[f"ea{i}"], table[f"eb{i}"] = in_first, in_last, edge_first, edge_last
                table[f"sa{i}"], table[f"sb{i}"] = self_first, self_last
        run(ORDER_E, table)

    def out_copies(step, t):
        copies = []
        for hop in range(RING):
            target = lax.rem(me + hop, RING)
            src, dst = x_buf.at[step + 1, :, t, pl.ds(PAIR * target, PAIR)], out.at[step, place, :, t]
            if hop == 0:
                copies.append(pltpu.make_async_copy(src, dst, out_recv.at[step, t, hop]))
            else:
                copies.append(pltpu.make_async_remote_copy(
                    src_ref=src, dst_ref=dst, send_sem=out_send.at[step, t, hop], recv_sem=out_recv.at[step, t, hop],
                    device_id=at(target), device_id_type=mesh_id))
        return copies

    def decoder(step):
        w16 = layer_weights(step, LAYERS)
        w = layer_weights(step, BLOCKS - 1)
        in_mean = stats[ZERO:ONE, :]
        in_std = stats[ONE:PAIR, :]
        diff_mean, diff_std = (jnp.concatenate([stats[i:i + 1, :], jnp.zeros((ONE, LANES - VARS), F32)], axis=ONE) for i in (2, 3))
        halo_slot = lax.rem(LAYERS + 1, 2)
        table = {"share": share_rows, "wait": lambda: wait_halo(halo_slot), "halo": lambda: project_halo(halo_slot, w16)}
        x = far_items(1, w16, resume=True)
        for k in range(4):
            table[f"fx{k}"], table[f"bx{k}"] = x[k].fin, x[k].b
        for t in range(TILES):
            node = Node(t, h, w16)
            table[f"nh{t}"], table[f"na{t}"], table[f"nb{t}"] = node.own, node.a, node.b
            near = near_items(t, w16, resume=t == 0)
            for k in range(PAIR):
                table[f"n{t}{k}"], table[f"fn{t}{k}"], table[f"bn{t}{k}"] = near[k].a, near[k].fin, near[k].b

            def back(t=t):
                out = dot(h[tile_rows(t), :], w.edge[1][...])
                for c in chunks():
                    recv[part_rows(t, c), :] = out[c:c + CH]

            def send(t=t):
                start_all(out_copies(step, t))

            table[f"t{t}"], table[f"send{t}"] = back, send
            for p in range(PAIR):
                i = PAIR * t + p
                low, high = 8 + i, 12 + i
                held = {}

                def edge_own(t=t, p=p, held=held):
                    held["edge"] = dot(m2g[p, tile_rows(t), :], w.edge[0][...]) + dot(vc[p, tile_rows(t), :], w.edge[2][...])

                def edge_first(t=t, low=low, held=held):
                    hide(low, held["edge"], lambda c: recv[part_rows(t, c), :])

                def edge_last(t=t, p=p, low=low, i=i):
                    y = dot(hid[low], w.edge_out[...])
                    for c in chunks():
                        part = part_rows(t, c)
                        dec[i, pl.ds(c, CH), :] = (m2g[p, part, :].astype(F32) + norm(y[c:c + CH])).astype(BF16)

                def node_own(t=t, p=p, held=held):
                    held["node"] = dot(vc[p, tile_rows(t), :], w.node[0][...])

                def node_first(high=high, i=i, held=held):
                    hide(high, held["node"] + dot(dec[i], w.node[1][...]))

                def node_last(t=t, p=p, high=high):
                    y = dot(hid[high], w.node_out[...])
                    for c in chunks():
                        part = part_rows(t, c)
                        v[p, part, :] = (vc[p, part, :].astype(F32) + norm(y[c:c + CH])).astype(BF16)

                def out_first(t=t, p=p, low=low):
                    hide(low, dot(v[p, tile_rows(t), :], woh[...]))

                def out_last(t=t, p=p, low=low):
                    pred = dot(hid[low], wof[...])
                    for c in chunks():
                        runs = pl.ds(c // HALF, CH // HALF)
                        now = x_buf[step, p, t, runs].reshape(CH, LANES)
                        new = now + diff_std * pred[c:c + CH] + diff_mean
                        x_buf[step + 1, p, t, runs] = new.reshape(CH // HALF, HALF, LANES)
                        scaled = ((new[:, :VARS] - in_mean) / in_std).astype(BF16)
                        feat[p, t, runs, :, pl.ds(ZERO, VARS)] = scaled.reshape(CH // HALF, HALF, VARS)

                table[f"em{i}"], table[f"ea{i}"], table[f"eb{i}"] = edge_own, edge_first, edge_last
                table[f"dm{i}"], table[f"da{i}"], table[f"db{i}"] = node_own, node_first, node_last
                table[f"oa{i}"], table[f"ob{i}"] = out_first, out_last
        run(ORDER_D, table)

    def wait_all(copies):
        for copy in copies:
            copy.wait()

    def start_all(copies):
        for copy in copies:
            copy.start()

    def one_step(step, carry):
        wait_all(layer_copies(step, 1) + layer_copies(step, 2))
        start_all(layer_copies(step, 3))
        encoder(step)

        def one_layer(block, carry):
            halo_slot = lax.rem(block + 1, 2)
            w, w1, w2 = (layer_weights(step, block + i) for i in range(3))
            phase(ORDER_A, far_items(1, w, resume=True), near_items(0, w, resume=True), Node(0, h, w), far_items(1, w1),
                  near_items(1, w), share_rows, w1)
            wait_halo(halo_slot)
            wait_all(layer_copies(step, block + 2))

            @pl.when(block < LAYERS - 1)
            def _():
                start_all(layer_copies(step, block + 3))

            phase(ORDER_B, far_items(0, w1, resume=True), near_items(1, w, resume=True), Node(1, h, w), far_items(0, w2),
                  near_items(0, w1), lambda: project_halo(halo_slot, w), w1)
            send_halo(1 - halo_slot)
            return carry

        lax.fori_loop(1, LAYERS, one_layer, 0)
        @pl.when(step == 0)
        def _():
            start_all(layer_copies(1, 1) + layer_copies(1, 2))
            wait_in(PAIR)

        decoder(step)
        return carry

    lax.fori_loop(0, 2, one_step, 0)
    for part in range(3):
        for copy in in_copies[part][1:]:
            copy.wait_send()
    for t in range(TILES):
        wait_all(out_copies(0, t) + out_copies(1, t))


def solution(mesh):
    row_spec = P(("dp", "gp"))
    edge_spec = P(("dp", "gp"), None, None)
    whole = P()

    def local_run(x_prev, x_cur, forcing, grid_static, g2m_feat, m2g_feat, mesh_feat, mesh_edge_feat, norm_stats,
                  w_grid_in, w_mesh_in, w_eemb_in, w_embed_out, w_edge_in, w_edge_out, w_node_in, w_node_out,
                  w_grid_self, w_out_hidden, w_out_final):
        any_spec = pl.BlockSpec(memory_space=pl.ANY)
        vmem_spec = pl.BlockSpec(memory_space=pltpu.VMEM)
        dma = pltpu.SemaphoreType.DMA
        grid_dev = x_prev.shape[0]
        shape = jax.ShapeDtypeStruct
        home = shape((RING, PAIR, TILES, PAIR, HALF, LANES), F32)
        bulk = [
            pltpu.VMEM(shape_, F32) for shape_ in (
                (3, mesh_feat.shape[0]), (6, 4, mesh_feat.shape[0]), (VARS, grid_dev), (VARS, grid_dev), (5, PAIR, grid_dev),
                (5, grid_dev), (4, grid_dev), (4, grid_dev))
        ]
        scratch = bulk + [
            pltpu.VMEM((2 * VARS + 10, LAT), BF16),
            pltpu.VMEM((3, LAT), BF16),
            pltpu.VMEM((3, 4, LAT), BF16),
            pltpu.VMEM((VARS, LAT), BF16),
            pltpu.VMEM((*home.shape[:-1], 2 * LANES), BF16),
            pltpu.VMEM((RING, TILES, PAIR, HALF, LANES), BF16),
            pltpu.VMEM(home.shape, F32),
            pltpu.VMEM((TILES, RUNS, HALF, LANES), BF16),
            pltpu.VMEM((3, PAIR, TILES, RUNS, HALF, LANES), F32),
            pltpu.VMEM((PAIR, TILES, RUNS, HALF, 2 * LANES), BF16),
            pltpu.VMEM((13, LANES, LAT), BF16),
            pltpu.VMEM((5, LAT, LAT), BF16),
            pltpu.VMEM((PAIR, LAT, LAT), BF16),
            pltpu.VMEM((LAT, LAT), BF16),
            pltpu.VMEM((LAT, LANES), BF16),
            pltpu.VMEM((1, 3 * LAT, LAT), BF16),
            pltpu.VMEM((1, LAT, LAT), BF16),
            pltpu.VMEM((1, 2 * LAT, LAT), BF16),
            pltpu.VMEM((1, LAT, LAT), BF16),
            pltpu.VMEM((SLOTS, 3 * LAT, LAT), BF16),
            pltpu.VMEM((SLOTS, LAT, LAT), BF16),
            pltpu.VMEM((SLOTS, 2 * LAT, LAT), BF16),
            pltpu.VMEM((SLOTS, LAT, LAT), BF16),
            pltpu.VMEM((6, ROWS, LAT), BF16),
            pltpu.VMEM((6, ROWS, LAT), BF16),
            pltpu.VMEM((ROWS, LAT), BF16),
            pltpu.VMEM((ROWS, LAT), BF16),
            pltpu.VMEM((LAT // LANES, TILE, LANES), F32),
            pltpu.VMEM((PAIR, ROWS, LAT), BF16),
            pltpu.VMEM((PAIR, ROWS, LAT), BF16),
            pltpu.VMEM((PAIR, ROWS, LAT), BF16),
            pltpu.VMEM((PAIR, ROWS, LAT), BF16),
            pltpu.VMEM((LAT // LANES, RUNS * PAD0, LANES), F32),
            pltpu.VMEM((LAT // LANES, RUNS * PAD1, LANES), F32),
            pltpu.VMEM((ROWS, LAT), F32),
            pltpu.VMEM((ROWS, LAT), F32),
            pltpu.VMEM((16, TILE, LAT), BF16),
            pltpu.VMEM((ROWS, LAT), BF16),
            pltpu.VMEM((4, TILE, LAT), BF16),
            pltpu.VMEM((10, TILE, LAT), F32),
            pltpu.VMEM((PAIR, RUNS, LAT), BF16),
            pltpu.VMEM((PAIR, 2, RUNS, LAT), BF16),
            dma((12,)), dma((3, RING)), dma((3, RING)), dma((4,)), dma((1, 4)), dma((SLOTS, 4)), dma((PAIR,)), dma((PAIR, PAIR)),
            dma((PAIR, TILES, RING)), dma((PAIR, TILES, RING)),
        ]
        homes = pl.pallas_call(
            kernel,
            out_shape=shape((PAIR, *home.shape), F32),
            in_specs=[any_spec] * 8 + [vmem_spec] + [any_spec] * 11,
            out_specs=any_spec,
            scratch_shapes=scratch,
            compiler_params=pltpu.CompilerParams(collective_id=0, has_side_effects=True, vmem_limit_bytes=63 << 20),
            name="forecast",
        )(x_prev.T, x_cur.T, forcing.T, grid_static.T, g2m_feat.T, m2g_feat.T, mesh_feat.T,
          jnp.transpose(mesh_edge_feat, (1, 2, 0)), norm_stats, w_grid_in, w_mesh_in, w_eemb_in, w_embed_out, w_edge_in,
          w_edge_out, w_node_in, w_node_out, w_grid_self, w_out_hidden, w_out_final.T)
        out = shape((VARS, grid_dev), F32)
        next_state, after_state = pl.pallas_call(
            unpack_kernel, out_shape=(out, out), in_specs=[vmem_spec], out_specs=(vmem_spec,) * 2,
            scratch_shapes=[pltpu.VMEM((grid_dev, LANES), F32)], name="unpack",
        )(homes)
        return next_state.T, after_state.T

    in_specs = (row_spec, row_spec, edge_spec, row_spec, row_spec, row_spec, row_spec, edge_spec, whole) + (whole,) * 11
    return jax.shard_map(local_run, mesh=mesh, in_specs=in_specs, out_specs=(row_spec, row_spec), check_vma=False)
```
